32 devices in a mesh: tp: 4 (over z), dp: 8 (over y, x, core).
Axes of the slice: x: 2, y: 2, z: 4, core: 2. Of those that a mesh axis runs over, the one named last changes fastest.
Arguments:
- x_in: bfloat16 [4096, 2304], P('dp')
- w_gate: bfloat16 [2304, 9216], P('dp', 'tp')
- w_up: bfloat16 [2304, 9216], P('dp', 'tp')
- w_down: bfloat16 [9216, 2304], P('tp', 'dp')
- dy_in: bfloat16 [4096, 2304], P('dp')
Outputs:
- output 1: bfloat16 [4096, 2304], P('dp')
- output 2: bfloat16 [4096, 2304], P('dp')
- output 3: float32 [2304, 9216], P('dp', 'tp')
- output 4: float32 [2304, 9216], P('dp', 'tp')
- output 5: float32 [9216, 2304], P('tp', 'dp')
All inputs are finite; a program needn't handle non-finite values.
Results may differ from the reference program's by a relative error of at most 0.001.
Values are sent between devices in bfloat16 or wider.
A program may use at most 1 GiB of HBM per device.

```python
import jax
import jax.numpy as jnp
from jax import lax

MODEL_DIM = 2304
HIDDEN_DIM = 9216
SHARD_TOKENS = 512
DATA_SHARDS = 8


def setup_inputs(seed: int = 0) -> dict:
    key_list = jax.random.split(jax.random.key(seed), 5)
    row_count = DATA_SHARDS * SHARD_TOKENS
    x_vals = jax.random.normal(key_list[0], (row_count, MODEL_DIM), jnp.float32)
    gate_vals = jax.random.normal(key_list[1], (MODEL_DIM, HIDDEN_DIM), jnp.float32) * MODEL_DIM ** -0.5
    up_vals = jax.random.normal(key_list[2], (MODEL_DIM, HIDDEN_DIM), jnp.float32) * MODEL_DIM ** -0.5
    down_vals = jax.random.normal(key_list[3], (HIDDEN_DIM, MODEL_DIM), jnp.float32) * HIDDEN_DIM ** -0.5
    dy_vals = jax.random.normal(key_list[4], (row_count, MODEL_DIM), jnp.float32)
    return {
        'x_in': x_vals.astype(jnp.bfloat16),
        'w_gate': gate_vals.astype(jnp.bfloat16),
        'w_up': up_vals.astype(jnp.bfloat16),
        'w_down': down_vals.astype(jnp.bfloat16),
        'dy_in': dy_vals.astype(jnp.bfloat16),
    }


def reference(x_in, w_gate, w_up, w_down, dy_in):
    row_count = DATA_SHARDS * SHARD_TOKENS
    x_blocks = x_in.reshape(DATA_SHARDS, SHARD_TOKENS, MODEL_DIM)
    dy_blocks = dy_in.reshape(DATA_SHARDS, SHARD_TOKENS, MODEL_DIM)

    def shard_pass(carry, block):
        acc_gate, acc_up, acc_down = carry
        x_blk, dy_blk = block
        gate_pre = jnp.dot(x_blk, w_gate, preferred_element_type=jnp.float32)
        up_pre = jnp.dot(x_blk, w_up, preferred_element_type=jnp.float32)
        sig_gate = jax.nn.sigmoid(gate_pre)
        silu_gate = gate_pre * sig_gate
        hidden = (silu_gate * up_pre).astype(jnp.bfloat16)
        y_blk = (x_blk.astype(jnp.float32) + jnp.dot(hidden, w_down, preferred_element_type=jnp.float32)).astype(jnp.bfloat16)
        grad_h = jnp.dot(dy_blk, w_down.T, preferred_element_type=jnp.float32)
        d_gate = (grad_h * up_pre * sig_gate * (1.0 + gate_pre * (1.0 - sig_gate))).astype(jnp.bfloat16)
        d_up = (grad_h * silu_gate).astype(jnp.bfloat16)
        dx_blk = (dy_blk.astype(jnp.float32)
                  + jnp.dot(d_gate, w_gate.T, preferred_element_type=jnp.float32)
                  + jnp.dot(d_up, w_up.T, preferred_element_type=jnp.float32)).astype(jnp.bfloat16)
        acc_gate = acc_gate + jnp.dot(x_blk.T, d_gate, preferred_element_type=jnp.float32)
        acc_up = acc_up + jnp.dot(x_blk.T, d_up, preferred_element_type=jnp.float32)
        acc_down = acc_down + jnp.dot(hidden.T, dy_blk, preferred_element_type=jnp.float32)
        return (acc_gate, acc_up, acc_down), (y_blk, dx_blk)

    zero_acc = (jnp.zeros((MODEL_DIM, HIDDEN_DIM), jnp.float32),
                jnp.zeros((MODEL_DIM, HIDDEN_DIM), jnp.float32),
                jnp.zeros((HIDDEN_DIM, MODEL_DIM), jnp.float32))
    sums, outs = lax.scan(shard_pass, zero_acc, (x_blocks, dy_blocks))
    y_blocks, dx_blocks = outs
    return (y_blocks.reshape(row_count, MODEL_DIM), dx_blocks.reshape(row_count, MODEL_DIM), sums[0], sums[1], sums[2])
```

```python
import jax
import jax.numpy as jnp
from jax import lax
from jax.sharding import PartitionSpec as P

F32 = jnp.float32
BF16 = jnp.bfloat16


def dot_nn(a, b):
    return jnp.dot(a, b, preferred_element_type=F32)


def dot_nt(a, b):
    return lax.dot_general(a, b, (((1,), (1,)), ((), ())), preferred_element_type=F32)


def dot_tn(a, b):
    return lax.dot_general(a, b, (((0,), (0,)), ((), ())), preferred_element_type=F32)


def hidden_grads(x, dy, wg, wu, wd):
    a = dot_nn(x, wg)
    b = dot_nn(x, wu)
    g = dot_nn(dy, wd)
    s = jax.nn.sigmoid(a)
    silu = a * s
    h = (silu * b).astype(BF16)
    da = (g * b * s * (1.0 + a * (1.0 - s))).astype(BF16)
    db = (g * silu).astype(BF16)
    return h, da, db


def solution(mesh):
    n_tp = mesh.shape['tp']
    n_dp = mesh.shape['dp']

    def device_pass(x_rows, gate_blk, up_blk, down_blk, dy_rows):
        rows = x_rows.shape[0]
        part = rows // n_tp
        tp = lax.axis_index('tp')
        dp = lax.axis_index('dp')
        core = lax.rem(dp, 2)
        wg = lax.all_gather(gate_blk, 'dp', axis=0, tiled=True)
        wu = lax.all_gather(up_blk, 'dp', axis=0, tiled=True)
        wd = lax.all_gather(down_blk.T, 'dp', axis=0, tiled=True)
        x_part = lax.dynamic_slice_in_dim(x_rows, tp * part, part, 0)
        dy_part = lax.dynamic_slice_in_dim(dy_rows, tp * part, part, 0)
        x_all = lax.all_gather(x_part, ('tp', 'dp'), axis=0, tiled=True)
        dy_all = lax.all_gather(dy_part, ('tp', 'dp'), axis=0, tiled=True)

        h, da, db = hidden_grads(x_rows, dy_rows, wg, wu, wd)

        y_part = dot_nt(h, wd)
        dx_part = dot_nt(da, wg) + dot_nt(db, wu)
        y_part, dx_part, x_all, dy_all = lax.optimization_barrier((y_part, dx_part, x_all, dy_all))

        def finish(base, partial):
            mine = lax.psum_scatter(partial, 'tp', scatter_dimension=0, tiled=True)
            out = (base.astype(F32) + mine).astype(BF16)
            return lax.all_gather(out, 'tp', axis=0, tiled=True)

        y = finish(x_part, y_part)
        dx = finish(dy_part, dx_part)

        half = wg.shape[1] // 2
        wg_h = lax.dynamic_slice_in_dim(wg, core * half, half, 1)
        wu_h = lax.dynamic_slice_in_dim(wu, core * half, half, 1)
        wd_h = lax.dynamic_slice_in_dim(wd, core * half, half, 1)
        h, da, db = hidden_grads(x_all, dy_all, wg_h, wu_h, wd_h)
        width = gate_blk.shape[0]
        chip = lax.div(dp, 2)
        x_cols = lax.dynamic_slice_in_dim(x_all, chip * 2 * width, 2 * width, 1)
        dy_cols = lax.dynamic_slice_in_dim(dy_all, chip * 2 * width, 2 * width, 1)
        swap = [(i, i ^ 1) for i in range(n_dp)]

        def exchange(grad, axis):
            own = lax.dynamic_slice_in_dim(grad, core * width, width, axis)
            other = lax.dynamic_slice_in_dim(grad, (1 - core) * width, width, axis)
            other = lax.ppermute(other, 'dp', swap)
            low = jnp.where(core == 0, own, other)
            high = jnp.where(core == 0, other, own)
            return jnp.concatenate([low, high], axis=1 - axis)

        dw_gate = exchange(dot_tn(x_cols, da), 0)
        dw_up = exchange(dot_tn(x_cols, db), 0)
        dw_down = exchange(dot_tn(h, dy_cols), 1)
        return y, dx, dw_gate, dw_up, dw_down

    row_spec = P('dp', None)
    weight_spec = P('dp', 'tp')
    down_spec = P('tp', 'dp')
    return jax.shard_map(device_pass, mesh=mesh,
                         in_specs=(row_spec, weight_spec, weight_spec, down_spec, row_spec),
                         out_specs=(row_spec, row_spec, weight_spec, weight_spec, down_spec),
                         check_vma=False)
```

```python
import functools

import jax
import jax.numpy as jnp
from jax import lax
from jax.experimental import pallas as pl
from jax.experimental.pallas import tpu as pltpu
from jax.sharding import PartitionSpec as P

F32 = jnp.float32
BF16 = jnp.bfloat16
MESH = pl.DeviceIdType.MESH
SLOTS = 8


def dot_nn(a, b):
    return jnp.dot(a, b, preferred_element_type=F32)


def dot_nt(a, b):
    return lax.dot_general(a, b, (((1,), (1,)), ((), ())), preferred_element_type=F32)


def dot_tn(a, b):
    return lax.dot_general(a, b, (((0,), (0,)), ((), ())), preferred_element_type=F32)


def sigmoid(a):
    return 1.0 / (1.0 + jnp.exp(-a))


def kernel(x_ref, dy_ref, wg_ref, wu_ref, wd_ref,
           yd_ref, og_ref, ou_ref, od_ref, xb, dyb, xp, dyp,
           w_s, acc, yacc, pbuf, sb, xt, dyt, a_s, b_s, g_s, h_all, h_s, da_s, db_s, rbuf, fin,
           w_send, w_recv, wr_send, wr_recv, w_own, wp_send, wp_recv,
           own_send, own_recv, q_send, q_recv, rl_send, f_send, f_recv,
           sb_send, sb_recv, credit, rs_send, rs_recv, ag_send, ag_recv, fin_own, ld, out_send, out_recv, out_own):
    rows, model = x_ref.shape
    blk, width = wg_ref.shape
    half = width // 2
    hb = blk // 2
    tile = rows // 2
    piece = tile // 4
    rc = rows // 32
    steps = 16
    win = acc.shape[1]
    w_in = (wg_ref, wu_ref, wd_ref)
    outs = (og_ref, ou_ref, od_ref)
    tok = (x_ref, dy_ref)
    tok_b = (xb, dyb)
    tok_p = (xp, dyp)
    tok_t = (xt, dyt)

    t = lax.axis_index('tp')
    me = lax.axis_index('dp')
    cy = lax.div(me, 4)
    cx = lax.rem(lax.div(me, 2), 2)
    j = lax.rem(me, 2)
    partner = me + 1 - 2 * j
    chip = cy * 2 + cx

    def near(link, core):
        if link == 0:
            return cy * 4 + (1 - cx) * 2 + core
        return (1 - cy) * 4 + cx * 2 + core

    def far(core):
        return (1 - cy) * 4 + (1 - cx) * 2 + core

    def send(src, dst, s_sem, r_sem, dp=None, tp=None):
        where = {'dp': me if dp is None else dp, 'tp': t if tp is None else tp}
        return pltpu.make_async_remote_copy(src_ref=src, dst_ref=dst, send_sem=s_sem, recv_sem=r_sem,
                                            device_id=where, device_id_type=MESH)

    def wait(ref, sem):
        pltpu.make_async_copy(ref, ref, sem).wait()

    barrier = pltpu.get_barrier_semaphore()
    for peer in (partner, near(0, 0), near(0, 1), near(1, 0), near(1, 1)):
        pl.semaphore_signal(barrier, inc=1, device_id={'dp': peer, 'tp': t}, device_id_type=MESH)

    @pl.when(t > 0)
    def _():
        pl.semaphore_signal(barrier, inc=1, device_id={'dp': me, 'tp': t - 1}, device_id_type=MESH)

    @pl.when(t < 3)
    def _():
        pl.semaphore_signal(barrier, inc=1, device_id={'dp': me, 'tp': t + 1}, device_id_type=MESH)

    pl.semaphore_wait(barrier, 5 + jnp.minimum(t, 1) + jnp.minimum(3 - t, 1))

    def w_rows(k, dev, part=None):
        if part is None:
            return w_s.at[k, pl.ds(pl.multiple_of(dev * blk, 16), blk), :]
        return w_s.at[k, pl.ds(pl.multiple_of(dev * blk + part * hb, 16), hb), :]

    def w_cols(core):
        return pl.ds(pl.multiple_of(core * half, 128), half)

    def w_copy(k, link, part, core):
        return send(w_in[k].at[pl.ds(part * hb, hb), w_cols(core)], w_rows(k, me, part),
                    w_send.at[k, link, part, core], w_recv.at[k, link, part, j], dp=near(link, core))

    def w_own_copy(k):
        return pltpu.make_async_copy(w_in[k].at[:, w_cols(j)], w_rows(k, me), w_own.at[k])

    def w_partner_copy(k):
        return send(w_in[k].at[:, w_cols(1 - j)], w_rows(k, me), wp_send.at[k], wp_recv.at[k], dp=partner)

    def w_start(k):
        for first in (0, 1):
            for core in (0, 1):
                w_copy(k, 0, 1 - first, core).start()
                w_copy(k, 1, first, core).start()
        w_own_copy(k).start()
        w_partner_copy(k).start()

    def w_relay_copy(k, link_out, core):
        part = 1 if link_out == 1 else 0
        ref = w_rows(k, near(1 - link_out, core), part)
        return send(ref, ref, wr_send.at[k, link_out, core], wr_recv.at[k, link_out, core], dp=near(link_out, j))

    def w_relay(k):
        for core in (0, 1):
            wait(w_rows(k, near(0, core), 1), w_recv.at[k, 0, 1, core])
            w_relay_copy(k, 1, core).start()
            wait(w_rows(k, near(1, core), 0), w_recv.at[k, 1, 0, core])
            w_relay_copy(k, 0, core).start()

    def w_finish(k):
        for core in (0, 1):
            wait(w_rows(k, near(0, core), 0), w_recv.at[k, 0, 0, core])
            wait(w_rows(k, near(1, core), 1), w_recv.at[k, 1, 1, core])
        wait(w_rows(k, me), w_own.at[k])
        wait(w_rows(k, partner), wp_recv.at[k])
        for core in (0, 1):
            wait(w_rows(k, far(core), 0), wr_recv.at[k, 0, core])
            wait(w_rows(k, far(core), 1), wr_recv.at[k, 1, core])

    def slot_of(ten, q, link, core):
        return tok_b[ten].at[q, pl.ds(pl.multiple_of((2 * link + core) * piece, piece), piece), :]

    def q_copy(ten, q, link):
        b = lax.div(q, 4)
        sub = lax.rem(q, 4)
        first = 1 - b if link == 0 else b
        src = tok[ten].at[pl.ds(pl.multiple_of(first * tile + sub * piece, piece), piece), :]
        return send(src, slot_of(ten, q, link, j), q_send.at[q, link, ten], q_recv.at[q, link, ten], dp=near(link, j))

    def relay_copy(ten, sub, link_out):
        return send(slot_of(ten, sub, 1 - link_out, j), slot_of(ten, 8 + sub, link_out, j),
                    rl_send.at[sub, link_out, ten], q_recv.at[8 + sub, link_out, ten], dp=near(link_out, j))

    def forward_copy(ten, q, link):
        ref = slot_of(ten, q, link, j)
        return send(ref, ref, f_send.at[q, link, ten], f_recv.at[q, link, ten], dp=partner)

    def own_copy(ten):
        return send(tok[ten], tok_p[ten], own_send.at[ten], own_recv.at[ten], dp=partner)

    def chunk(ten, s, way):
        row = (lax.rem(s, steps) * 2 + way) * rc
        return ten, pl.ds(pl.multiple_of(row, rc), rc), slice(None)

    def sum_copy(s, way, nxt):
        slot = lax.rem(s, SLOTS)
        return send(yacc.at[chunk(lax.div(s, steps), s, way)], rbuf.at[way, slot],
                    rs_send.at[way, slot], rs_recv.at[way, slot], tp=nxt)

    def done_copy(s, way, prv, src):
        slot = lax.rem(s, SLOTS)
        return send(src, yd_ref.at[chunk(lax.div(s, steps), s, way)], ag_send.at[way, slot], ag_recv.at[way, slot], tp=prv)

    def tick(tau):
        for way in (0, 1):
            p = t if way == 0 else 3 - t
            nxt = t + 1 if way == 0 else t - 1
            prv = t - 1 if way == 0 else t + 1
            s = tau - p
            slot = lax.rem(jnp.maximum(s, 0), SLOTS)
            live = jnp.logical_and(s >= 0, s < 2 * steps)

            @pl.when(jnp.logical_and(live, p > 0))
            def _():
                wait(rbuf.at[way, slot], rs_recv.at[way, slot])

            @pl.when(jnp.logical_and(live, p < 3))
            def _():
                @pl.when(s >= SLOTS)
                def _():
                    sum_copy(s - SLOTS, way, nxt).wait_send()

                @pl.when(p > 0)
                def _():
                    here = chunk(lax.div(s, steps), s, way)
                    yacc[here] = yacc[here] + rbuf[way, slot]

                sum_copy(s, way, nxt).start()

            @pl.when(jnp.logical_and(live, p == 3))
            def _():
                @pl.when(s >= SLOTS)
                def _():
                    done_copy(s - SLOTS, way, prv, fin.at[way, slot]).wait_send()
                    wait(fin.at[way, slot], fin_own.at[way, slot])

                here = chunk(lax.div(s, steps), s, way)
                fin[way, slot] = (yacc[here] + rbuf[way, slot]).astype(BF16)
                pltpu.make_async_copy(fin.at[way, slot], yd_ref.at[here], fin_own.at[way, slot]).start()
                done_copy(s, way, prv, fin.at[way, slot]).start()

            s2 = tau - 6 + p
            slot2 = lax.rem(jnp.maximum(s2, 0), SLOTS)
            live2 = jnp.logical_and(jnp.logical_and(s2 >= 0, s2 < 2 * steps), p < 3)

            @pl.when(live2)
            def _():
                here = yd_ref.at[chunk(lax.div(s2, steps), s2, way)]
                wait(here, ag_recv.at[way, slot2])

                @pl.when(p > 0)
                def _():
                    @pl.when(s2 >= SLOTS)
                    def _():
                        done_copy(s2 - SLOTS, way, prv, here).wait_send()

                    done_copy(s2, way, prv, here).start()

    def drain_sums():
        def body(n, carry):
            s = 2 * steps - SLOTS + n
            for way in (0, 1):
                p = t if way == 0 else 3 - t
                slot = lax.rem(s, SLOTS)

                @pl.when(p < 3)
                def _():
                    wait(rbuf.at[way, slot], rs_send.at[way, slot])

                @pl.when(p > 0)
                def _():
                    wait(fin.at[way, slot], ag_send.at[way, slot])

                @pl.when(p == 3)
                def _():
                    wait(fin.at[way, slot], fin_own.at[way, slot])
            return carry

        lax.fori_loop(0, SLOTS, body, 0)

    w_start(0)
    w_start(1)
    for ten in (0, 1):
        own_copy(ten).start()

    def clear(n, carry):
        at = pl.ds(pl.multiple_of(n * 32, 32), 32)
        for k in range(3):
            acc[k, at, :] = jnp.zeros((32, half), F32)
        return carry

    lax.fori_loop(0, win // 32, clear, 0)
    w_relay(0)
    w_relay(1)
    w_start(2)
    w_finish(0)
    w_finish(1)

    group = min(32, tile)
    first = pl.multiple_of(lax.div(chip * 2 * blk, 128) * 128, 128)
    shift = chip * 2 * blk - first
    cols = pl.ds(first, win)
    base = jnp.where(t == 0, 1.0, 0.0).astype(F32)

    def put_partial(ten, r, own):
        at = pl.ds(pl.multiple_of(r * tile, tile), tile)

        @pl.when(own == 0)
        def _():
            if ten == 1:
                pl.semaphore_wait(credit, 1)
            send(sb.at[0], pbuf.at[at, :], sb_send.at[ten, r], sb_recv.at[ten, r], dp=partner).start()

        @pl.when(own == 1)
        def _():
            wait(pbuf.at[at, :], sb_recv.at[ten, r])
            src = tok_t[ten]

            def body(n, carry):
                lo = pl.ds(pl.multiple_of(n * group, group), group)
                there = pl.ds(pl.multiple_of(r * tile + n * group, group), group)
                yacc[ten, there, :] = sb[1, lo, :] + pbuf[there, :] + src[lo, :].astype(F32) * base
                return carry

            lax.fori_loop(0, tile // group, body, 0)
            if ten == 0:
                pl.semaphore_signal(credit, inc=1, device_id={'dp': partner, 'tp': t}, device_id_type=MESH)

    def free_sb(ten, r, own):
        if ten == 1:
            @pl.when(jnp.logical_and(own == 0, r == 0))
            def _():
                wait(sb.at[0], sb_send.at[0, 1])

        @pl.when(jnp.logical_and(own == 0, r == 1))
        def _():
            wait(sb.at[0], sb_send.at[ten, 0])

    n_block = 3
    n_cols = model // n_block

    def one_tile(i, carry):
        r = lax.div(lax.rem(i, 4), 2)
        own = lax.rem(i, 2)
        q = i - 12

        @pl.when(i == 2)
        def _():
            w_relay(2)

        @pl.when(jnp.logical_and(i >= 2, i < 10))
        def _():
            for ten in (0, 1):
                for link in (0, 1):
                    q_copy(ten, i - 2, link).start()

        @pl.when(i == 4)
        def _():
            w_finish(2)

        at = pl.ds(pl.multiple_of(r * tile, tile), tile)
        for ten in (0, 1):
            due = i < 12 if ten == 0 else jnp.logical_and(i >= 8, i < 12)

            @pl.when(jnp.logical_and(due, own == 1))
            def _():
                pltpu.make_async_copy(tok[ten].at[at, :], tok_t[ten], ld.at[ten]).start()

            @pl.when(i == 8 * ten)
            def _():
                wait(tok_p[ten], own_recv.at[ten])

            @pl.when(jnp.logical_and(due, own == 0))
            def _():
                pltpu.make_async_copy(tok_p[ten].at[at, :], tok_t[ten], ld.at[ten]).start()

        @pl.when(i >= 12)
        def _():
            for ten in (0, 1):
                for link in (0, 1):
                    wait(slot_of(ten, q, link, j), q_recv.at[q, link, ten])
                    forward_copy(ten, q, link).start()

            @pl.when(q < 4)
            def _():
                for ten in (0, 1):
                    for link in (0, 1):
                        relay_copy(ten, q, link).start()

            for ten in (0, 1):
                for link in (0, 1):
                    wait(slot_of(ten, q, link, 1 - j), f_recv.at[q, link, ten])
                pltpu.make_async_copy(tok_b[ten].at[q], tok_t[ten], ld.at[ten]).start()

        wait(xt, ld.at[0])

        @pl.when(jnp.logical_or(i < 4, i >= 8))
        def _():
            a_s[...] = dot_nn(xt[...], w_s[0])
            b_s[...] = dot_nn(xt[...], w_s[1])
            tick(jnp.where(i >= 12, 15 + 2 * (i - 12), jnp.where(i >= 8, 3 + 3 * (i - 8), -1000)))

        @pl.when(i < 4)
        def _():
            def body(n, c):
                lo = pl.ds(pl.multiple_of(n * group, group), group)
                a = a_s[lo, :]
                h_all[i, lo, :] = (a * sigmoid(a) * b_s[lo, :]).astype(BF16)
                return c

            lax.fori_loop(0, tile // group, body, 0)

        @pl.when(jnp.logical_and(i >= 4, i < 8))
        def _():
            free_sb(0, r, own)

            def block(n, c):
                to = pl.ds(pl.multiple_of(n * n_cols, n_cols), n_cols)
                sb[own, :, to] = dot_nt(h_all[lax.rem(i, 4)], w_s[2, to, :])
                return c

            lax.fori_loop(0, n_block, block, 0)
            put_partial(0, r, own)
            tick(jnp.where(i >= 5, i - 5, -1000))

        @pl.when(i >= 8)
        def _():
            wait(dyt, ld.at[1])
            g_s[...] = dot_nn(dyt[...], w_s[2])

            def body(n, c):
                lo = pl.ds(pl.multiple_of(n * group, group), group)
                a = a_s[lo, :]
                b = b_s[lo, :]
                g = g_s[lo, :]
                s = sigmoid(a)
                silu = a * s
                h_s[lo, :] = (silu * b).astype(BF16)
                da_s[lo, :] = (g * b * s * (1.0 + a * (1.0 - s))).astype(BF16)
                db_s[lo, :] = (g * silu).astype(BF16)
                return c

            lax.fori_loop(0, tile // group, body, 0)
            x_win = xt[:, cols]
            acc[0] += dot_tn(x_win, da_s[...])
            acc[1] += dot_tn(x_win, db_s[...])
            acc[2] += dot_tn(dyt[:, cols], h_s[...])

            tick(jnp.where(i >= 12, 16 + 2 * (i - 12), 4 + 3 * (i - 8)))

        @pl.when(jnp.logical_and(i >= 8, i < 12))
        def _():
            free_sb(1, r, own)

            def block(n, c):
                to = pl.ds(pl.multiple_of(n * n_cols, n_cols), n_cols)
                sb[own, :, to] = dot_nt(da_s[...], w_s[0, to, :]) + dot_nt(db_s[...], w_s[1, to, :])
                return c

            lax.fori_loop(0, n_block, block, 0)
            put_partial(1, r, own)
            tick(5 + 3 * (i - 8))

        return carry

    lax.fori_loop(0, 24, one_tile, 0)

    def w_grad(k, core):
        return acc.at[k, pl.ds(pl.multiple_of(shift + core * blk, 8), blk), :]

    for k in range(3):
        send(w_grad(k, 1 - j), outs[k].at[:, w_cols(j)], out_send.at[k], out_recv.at[k], dp=partner).start()
        pltpu.make_async_copy(w_grad(k, j), outs[k].at[:, w_cols(j)], out_own.at[k]).start()

    drain_sums()
    wait(sb.at[0], sb_send.at[1, 1])
    for k in range(3):
        for core in (0, 1):
            for link in (0, 1):
                for part in (0, 1):
                    w_copy(k, link, part, core).wait_send()
                w_relay_copy(k, link, core).wait_send()
        w_partner_copy(k).wait_send()
    for ten in (0, 1):
        own_copy(ten).wait_send()

    def drain(q, carry):
        for ten in (0, 1):
            for link in (0, 1):
                @pl.when(q < 8)
                def _():
                    wait(slot_of(ten, 0, link, j), q_send.at[lax.rem(q, 8), link, ten])

                @pl.when(q < 4)
                def _():
                    wait(slot_of(ten, 0, link, j), rl_send.at[lax.rem(q, 4), link, ten])

                wait(slot_of(ten, q, link, j), f_send.at[q, link, ten])
        return carry

    lax.fori_loop(0, 12, drain, 0)
    for k in range(3):
        wait(w_grad(k, j), out_own.at[k])
        wait(w_grad(k, 1 - j), out_send.at[k])
        wait(w_grad(k, j), out_recv.at[k])


def window(model, blk):
    starts = [(2 * blk * c) // 128 * 128 for c in range(model // (2 * blk))]
    shift = max(2 * blk * c - s for c, s in enumerate(starts))
    return -(-(shift + 2 * blk) // 128) * 128


def mega(x, dy, wg, wu, wd):
    rows, model = x.shape
    blk, width = wg.shape
    half = width // 2
    tile = rows // 2
    rc = rows // 32
    dma = pltpu.SemaphoreType.DMA
    anywhere = pl.BlockSpec(memory_space=pl.ANY)
    shape = jax.ShapeDtypeStruct
    flops = 2 * model * half * rows * 2 * 20
    return pl.pallas_call(
        kernel,
        name='mlp',
        out_shape=(shape((2, rows, model), BF16),
                   shape((blk, width), F32), shape((blk, width), F32), shape((blk, width), F32),
                   shape((12, tile, model), BF16), shape((12, tile, model), BF16),
                   shape((rows, model), BF16), shape((rows, model), BF16)),
        in_specs=[anywhere] * 5,
        out_specs=tuple([anywhere] * 8),
        scratch_shapes=[
            pltpu.VMEM((3, model, half), BF16),
            pltpu.VMEM((3, window(model, blk), half), F32),
            pltpu.VMEM((2, rows, model), F32),
            pltpu.VMEM((rows, model), F32),
            pltpu.VMEM((2, tile, model), F32),
            pltpu.VMEM((tile, model), BF16),
            pltpu.VMEM((tile, model), BF16),
            pltpu.VMEM((tile, half), F32),
            pltpu.VMEM((tile, half), F32),
            pltpu.VMEM((tile, half), F32),
            pltpu.VMEM((4, tile, half), BF16),
            pltpu.VMEM((tile, half), BF16),
            pltpu.VMEM((tile, half), BF16),
            pltpu.VMEM((tile, half), BF16),
            pltpu.VMEM((2, SLOTS, rc, model), F32),
            pltpu.VMEM((2, SLOTS, rc, model), BF16),
            dma((3, 2, 2, 2)), dma((3, 2, 2, 2)), dma((3, 2, 2)), dma((3, 2, 2)), dma((3,)), dma((3,)), dma((3,)),
            dma((2,)), dma((2,)), dma((8, 2, 2)), dma((12, 2, 2)), dma((4, 2, 2)), dma((12, 2, 2)), dma((12, 2, 2)),
            dma((2, 2)), dma((2, 2)), pltpu.SemaphoreType.REGULAR,
            dma((2, SLOTS)), dma((2, SLOTS)), dma((2, SLOTS)), dma((2, SLOTS)), dma((2, SLOTS)),
            dma((2,)), dma((3,)), dma((3,)), dma((3,)),
        ],
        compiler_params=pltpu.CompilerParams(collective_id=0, has_side_effects=True, vmem_limit_bytes=67_000_000),
        cost_estimate=pl.CostEstimate(flops=flops, bytes_accessed=100_000_000, transcendentals=0),
    )(x, dy, wg, wu, wd)


def solution(mesh):
    def device_pass(x_rows, gate_blk, up_blk, down_blk, dy_rows):
        out = mega(x_rows, dy_rows, gate_blk, up_blk, down_blk.T)
        yd, dw_gate, dw_up, dw_down = out[:4]
        return yd[0], yd[1], dw_gate, dw_up, dw_down.T

    row_spec = P('dp', None)
    weight_spec = P('dp', 'tp')
    down_spec = P('tp', 'dp')
    return jax.shard_map(device_pass, mesh=mesh,
                         in_specs=(row_spec, weight_spec, weight_spec, down_spec, row_spec),
                         out_specs=(row_spec, row_spec, weight_spec, weight_spec, down_spec),
                         check_vma=False)
```

```python
import jax
import jax.numpy as jnp
from jax import lax
from jax.experimental import pallas as pl
from jax.experimental.pallas import tpu as pltpu
from jax.sharding import PartitionSpec as P

F32 = jnp.float32
BF16 = jnp.bfloat16
MESH = pl.DeviceIdType.MESH
SLOTS = 8
LANES = 128


def dot_nn(a, b):
    return jnp.dot(a, b, preferred_element_type=F32)


def dot_nt(a, b):
    return lax.dot_general(a, b, (((1,), (1,)), ((), ())), preferred_element_type=F32)


def dot_tn(a, b):
    return lax.dot_general(a, b, (((0,), (0,)), ((), ())), preferred_element_type=F32)


def sigmoid(a):
    return 1.0 / (1.0 + jnp.exp(-a))


def kernel(x_ref, dy_ref, wg_ref, wu_ref, wd_ref,
           yd_ref, og_ref, ou_ref, od_ref, xb, dyb, xp, dyp,
           w_s, acc, yacc, pbuf, sb, xt, dyt, a_all, b_all, g_s, h_all, rbuf, fin,
           w_send, w_recv, wr_send, wr_recv, w_own, wp_send, wp_recv,
           own_send, own_recv, q_send, q_recv, rl_send, f_send, f_recv,
           y_send, y_recv, dx_send, dx_recv, credit,
           rs_send, rs_recv, ag_send, ag_recv, fin_own, ld, out_send, out_recv, out_own):
    rows, model = x_ref.shape
    blk, width = wg_ref.shape
    half = width // 2
    hb = blk // 2
    tile = rows // 2
    piece = tile // 4
    win = acc.shape[1]
    line = model // 2
    units = line // LANES
    near_units = (2 * blk - LANES // 2) // LANES if (2 * blk) % LANES else 2 * blk // LANES
    rest_units = units - near_units
    steps = 2 * units
    group = min(32, tile)
    w_in = (wg_ref, wu_ref, wd_ref)
    outs = (og_ref, ou_ref, od_ref)
    tok = (x_ref, dy_ref)
    tok_b = (xb, dyb)
    tok_p = (xp, dyp)
    tok_t = (xt, dyt)

    t = lax.axis_index('tp')
    me = lax.axis_index('dp')
    cy = lax.div(me, 4)
    cx = lax.rem(lax.div(me, 2), 2)
    j = lax.rem(me, 2)
    partner = me + 1 - 2 * j
    chip = cy * 2 + cx

    def near(link, core):
        if link == 0:
            return cy * 4 + (1 - cx) * 2 + core
        return (1 - cy) * 4 + cx * 2 + core

    def far(core):
        return (1 - cy) * 4 + (1 - cx) * 2 + core

    def send(src, dst, s_sem, r_sem, dp=None, tp=None):
        where = {'dp': me if dp is None else dp, 'tp': t if tp is None else tp}
        return pltpu.make_async_remote_copy(src_ref=src, dst_ref=dst, send_sem=s_sem, recv_sem=r_sem,
                                            device_id=where, device_id_type=MESH)

    def wait(ref, sem):
        pltpu.make_async_copy(ref, ref, sem).wait()

    barrier = pltpu.get_barrier_semaphore()
    for peer in (partner, near(0, 0), near(0, 1), near(1, 0), near(1, 1)):
        pl.semaphore_signal(barrier, inc=1, device_id={'dp': peer, 'tp': t}, device_id_type=MESH)

    @pl.when(t > 0)
    def _():
        pl.semaphore_signal(barrier, inc=1, device_id={'dp': me, 'tp': t - 1}, device_id_type=MESH)

    @pl.when(t < 3)
    def _():
        pl.semaphore_signal(barrier, inc=1, device_id={'dp': me, 'tp': t + 1}, device_id_type=MESH)

    pl.semaphore_wait(barrier, 5 + jnp.minimum(t, 1) + jnp.minimum(3 - t, 1))

    def w_rows(k, dev, part=None):
        if part is None:
            return w_s.at[k, pl.ds(pl.multiple_of(dev * blk, 16), blk), :]
        return w_s.at[k, pl.ds(pl.multiple_of(dev * blk + part * hb, 16), hb), :]

    def w_cols(core):
        return pl.ds(pl.multiple_of(core * half, LANES), half)

    def w_copy(k, link, part, core):
        return send(w_in[k].at[pl.ds(part * hb, hb), w_cols(core)], w_rows(k, me, part),
                    w_send.at[k, link, part, core], w_recv.at[k, link, part, j], dp=near(link, core))

    def w_own_copy(k):
        return pltpu.make_async_copy(w_in[k].at[:, w_cols(j)], w_rows(k, me), w_own.at[k])

    def w_partner_copy(k):
        return send(w_in[k].at[:, w_cols(1 - j)], w_rows(k, me), wp_send.at[k], wp_recv.at[k], dp=partner)

    def w_start(k):
        for first in (0, 1):
            for core in (0, 1):
                w_copy(k, 0, 1 - first, core).start()
                w_copy(k, 1, first, core).start()
        w_own_copy(k).start()
        w_partner_copy(k).start()

    def w_relay_copy(k, link_out, core):
        part = 1 if link_out == 1 else 0
        ref = w_rows(k, near(1 - link_out, core), part)
        return send(ref, ref, wr_send.at[k, link_out, core], wr_recv.at[k, link_out, core], dp=near(link_out, j))

    def w_relay(k):
        for core in (0, 1):
            wait(w_rows(k, near(0, core), 1), w_recv.at[k, 0, 1, core])
            w_relay_copy(k, 1, core).start()
            wait(w_rows(k, near(1, core), 0), w_recv.at[k, 1, 0, core])
            w_relay_copy(k, 0, core).start()

    def w_have(k, which):
        if which == 'chip':
            wait(w_rows(k, me), w_own.at[k])
            wait(w_rows(k, partner), wp_recv.at[k])
        for core in (0, 1):
            if which == 'x':
                wait(w_rows(k, near(0, core), 0), w_recv.at[k, 0, 0, core])
            if which == 'y':
                wait(w_rows(k, near(1, core), 1), w_recv.at[k, 1, 1, core])
            if which == 'far':
                wait(w_rows(k, far(core), 0), wr_recv.at[k, 0, core])
                wait(w_rows(k, far(core), 1), wr_recv.at[k, 1, core])

    def slot_of(ten, q, link, core):
        return tok_b[ten].at[q, pl.ds(pl.multiple_of((2 * link + core) * piece, piece), piece), :]

    def q_copy(ten, q, link):
        b = lax.div(q, 4)
        sub = lax.rem(q, 4)
        first = 1 - b if link == 0 else b
        src = tok[ten].at[pl.ds(pl.multiple_of(first * tile + sub * piece, piece), piece), :]
        return send(src, slot_of(ten, q, link, j), q_send.at[q, link, ten], q_recv.at[q, link, ten], dp=near(link, j))

    def q_start(q):
        for ten in (0, 1):
            for link in (0, 1):
                q_copy(ten, q, link).start()

    def relay_copy(ten, sub, link_out):
        return send(slot_of(ten, sub, 1 - link_out, j), slot_of(ten, 8 + sub, link_out, j),
                    rl_send.at[sub, link_out, ten], q_recv.at[8 + sub, link_out, ten], dp=near(link_out, j))

    def forward_copy(ten, q, link):
        ref = slot_of(ten, q, link, j)
        return send(ref, ref, f_send.at[q, link, ten], f_recv.at[q, link, ten], dp=partner)

    def own_copy(ten):
        return send(tok[ten], tok_p[ten], own_send.at[ten], own_recv.at[ten], dp=partner)

    def arrive(ten, q):
        with jax.named_scope('arrive'):
            for link in (0, 1):
                wait(slot_of(ten, q, link, j), q_recv.at[q, link, ten])
                forward_copy(ten, q, link).start()

        @pl.when(q < 4)
        def _():
            for link in (0, 1):
                relay_copy(ten, q, link).start()

    def load_b(ten, q):
        with jax.named_scope('passed'):
            for link in (0, 1):
                wait(slot_of(ten, q, link, 1 - j), f_recv.at[q, link, ten])
        pltpu.make_async_copy(tok_b[ten].at[q], tok_t[ten].at[lax.rem(q, 2)], ld.at[ten, lax.rem(q, 2)]).start()

    def rows_of(r):
        return pl.ds(pl.multiple_of(r * tile, tile), tile)

    def load_a(ten, n):
        own = lax.div(n, 2)
        slot = lax.rem(n, 2)

        @pl.when(own == 1)
        def _():
            pltpu.make_async_copy(tok[ten].at[rows_of(slot), :], tok_t[ten].at[slot], ld.at[ten, slot]).start()

        @pl.when(own == 0)
        def _():
            pltpu.make_async_copy(tok_p[ten].at[rows_of(slot), :], tok_t[ten].at[slot], ld.at[ten, slot]).start()

    def loaded(ten, slot):
        with jax.named_scope('ld'):
            wait(tok_t[ten].at[slot], ld.at[ten, slot])

    def unit_col(u):
        mine = cy * units
        other = (1 - cy) * units
        low = cx * rest_units
        high = (1 - cx) * near_units
        a = near_units
        col = jnp.where(u < a, mine + low + u,
                        jnp.where(u < units, mine + high + (u - a),
                                  jnp.where(u < units + a, other + low + (u - units), other + high + (u - units - a))))
        return pl.multiple_of(col * LANES, LANES)

    def chunk(s, way):
        return lax.div(s, steps), pl.ds(way * tile, tile), pl.ds(unit_col(lax.rem(s, steps)), LANES)

    def sum_copy(s, way, nxt):
        slot = lax.rem(s, SLOTS)
        return send(yacc.at[chunk(s, way)], rbuf.at[way, slot], rs_send.at[way, slot], rs_recv.at[way, slot], tp=nxt)

    def done_copy(s, way, prv, src):
        slot = lax.rem(s, SLOTS)
        return send(src, yd_ref.at[chunk(s, way)], ag_send.at[way, slot], ag_recv.at[way, slot], tp=prv)

    def tick(tau):
        with jax.named_scope('tick'):
            tick_body(tau)

    def tick_body(tau):
        for way in (0, 1):
            p = t if way == 0 else 3 - t
            nxt = t + 1 if way == 0 else t - 1
            prv = t - 1 if way == 0 else t + 1
            s = tau - p
            slot = lax.rem(jnp.maximum(s, 0), SLOTS)
            live = jnp.logical_and(s >= 0, s < 2 * steps)

            @pl.when(jnp.logical_and(live, p > 0))
            def _():
                wait(rbuf.at[way, slot], rs_recv.at[way, slot])

            @pl.when(jnp.logical_and(live, p < 3))
            def _():
                @pl.when(s >= SLOTS)
                def _():
                    wait(rbuf.at[way, slot], rs_send.at[way, slot])

                @pl.when(p > 0)
                def _():
                    here = chunk(s, way)
                    yacc[here] = yacc[here] + rbuf[way, slot]

                sum_copy(s, way, nxt).start()

            @pl.when(jnp.logical_and(live, p == 3))
            def _():
                @pl.when(s >= SLOTS)
                def _():
                    wait(fin.at[way, slot], ag_send.at[way, slot])
                    wait(fin.at[way, slot], fin_own.at[way, slot])

                here = chunk(s, way)
                fin[way, slot] = (yacc[here] + rbuf[way, slot]).astype(BF16)
                pltpu.make_async_copy(fin.at[way, slot], yd_ref.at[here], fin_own.at[way, slot]).start()
                done_copy(s, way, prv, fin.at[way, slot]).start()

            s2 = tau - 6 + p
            slot2 = lax.rem(jnp.maximum(s2, 0), SLOTS)
            live2 = jnp.logical_and(jnp.logical_and(s2 >= 0, s2 < 2 * steps), p < 3)

            @pl.when(live2)
            def _():
                here = yd_ref.at[chunk(s2, way)]
                wait(here, ag_recv.at[way, slot2])

                @pl.when(p > 0)
                def _():
                    @pl.when(s2 >= SLOTS)
                    def _():
                        wait(fin.at[way, slot2], ag_send.at[way, slot2])

                    done_copy(s2, way, prv, here).start()

    def ticks(lo, hi):
        def body(n, c):
            tick(n)
            return c

        lax.fori_loop(lo, hi, body, 0)

    def drain_sums():
        def body(n, carry):
            for way in (0, 1):
                p = t if way == 0 else 3 - t
                slot = n

                @pl.when(p < 3)
                def _():
                    wait(rbuf.at[way, slot], rs_send.at[way, slot])

                @pl.when(p > 0)
                def _():
                    wait(fin.at[way, slot], ag_send.at[way, slot])

                @pl.when(p == 3)
                def _():
                    wait(fin.at[way, slot], fin_own.at[way, slot])
            return carry

        lax.fori_loop(0, SLOTS, body, 0)

    for ten in (0, 1):
        own_copy(ten).start()
    w_start(0)
    w_start(1)
    base = jnp.where(t == 0, 1.0, 0.0).astype(F32)

    with jax.named_scope('clear'):
        for r in (0, 1):
            for ten in (0, 1):
                load_a(ten, 2 + r)

        def clear(n, carry):
            at = pl.ds(pl.multiple_of(n * 32, 32), 32)
            for k in range(3):
                acc[k, at, :] = jnp.zeros((32, half), F32)
            return carry

        lax.fori_loop(0, win // 32, clear, 0)

        def clear_ab(n, carry):
            lo = pl.ds(pl.multiple_of(n * group, group), group)
            for m in range(4):
                a_all[m, lo, :] = jnp.zeros((group, half), F32)
                b_all[m, lo, :] = jnp.zeros((group, half), F32)
            return carry

        lax.fori_loop(0, tile // group, clear_ab, 0)
        for r in (0, 1):
            for ten in (0, 1):
                loaded(ten, r)

                def residual(n, carry):
                    lo = pl.ds(pl.multiple_of(n * group, group), group)
                    there = pl.ds(pl.multiple_of(r * tile + n * group, group), group)
                    yacc[ten, there, :] = tok_t[ten][r, lo, :].astype(F32) * base
                    return carry

                lax.fori_loop(0, tile // group, residual, 0)
        for ten in (0, 1):
            wait(tok_p[ten], own_recv.at[ten])

    with jax.named_scope('w_relay'):
        w_relay(0)
        w_relay(1)
    w_start(2)

    def ab_pass(last):
        row = cy if last == 0 else 1 - cy
        at_k = pl.ds(pl.multiple_of(row * line, LANES), line)
        load_a(0, 0)

        def body(n, carry):
            slot = lax.rem(n, 2)

            @pl.when(n < 3)
            def _():
                load_a(0, n + 1)

            loaded(0, slot)
            with jax.named_scope('ab_half'):
                x_half = xt[slot, :, at_k]
                a_all[n] += dot_nn(x_half, w_s[0, at_k, :])
                b_all[n] += dot_nn(x_half, w_s[1, at_k, :])

            if last:
                def hidden(m, c):
                    lo = pl.ds(pl.multiple_of(m * group, group), group)
                    a = a_all[n, lo, :]
                    h_all[n, lo, :] = (a * sigmoid(a) * b_all[n, lo, :]).astype(BF16)
                    return c

                lax.fori_loop(0, tile // group, hidden, 0)
            return carry

        lax.fori_loop(0, 4, body, 0)

    with jax.named_scope('w_have'):
        for k in (0, 1):
            w_have(k, 'chip')
            w_have(k, 'x')
    ab_pass(0)
    with jax.named_scope('w_have'):
        for k in (0, 1):
            w_have(k, 'y')
            w_have(k, 'far')
    ab_pass(1)

    def y_group(g):
        u0 = (0, near_units, units, units + near_units)[g]
        n_u = (near_units, rest_units)[g % 2]
        col = unit_col(u0)
        cols = pl.ds(col, n_u * LANES)

        def theirs(r, carry):
            if g > 0:
                before = (near_units, rest_units)[(g - 1) % 2] * LANES
                wait(sb.at[r, :, pl.ds(0, before)], y_send.at[(g - 1) % 2, r])
            with jax.named_scope('y_dot'):
                sb[r, :, :n_u * LANES] = dot_nt(h_all[r], w_s[2, cols, :])
            send(sb.at[r, :, pl.ds(0, n_u * LANES)], pbuf.at[rows_of(r), cols],
                 y_send.at[g % 2, r], y_recv.at[g, r], dp=partner).start()
            return carry

        def ours(r, carry):
            with jax.named_scope('y_wait'):
                wait(pbuf.at[rows_of(r), cols], y_recv.at[g, r])
            with jax.named_scope('y_dot'):
                yacc[0, rows_of(r), cols] = (yacc[0, rows_of(r), cols] + pbuf[rows_of(r), cols]
                                             + dot_nt(h_all[2 + r], w_s[2, cols, :]))
            pl.semaphore_signal(credit, inc=1, device_id={'dp': partner, 'tp': t}, device_id_type=MESH)
            return carry

        lax.fori_loop(0, 2, theirs, 0)
        lax.fori_loop(0, 2, ours, 0)

    with jax.named_scope('w_have2'):
        w_have(2, 'chip')
    y_group(0)
    tick(0)
    with jax.named_scope('w_relay2'):
        w_relay(2)
    q_start(0)
    q_start(1)
    ticks(1, 4)
    with jax.named_scope('w_have2'):
        w_have(2, 'x')
        w_have(2, 'y')
    y_group(1)
    tick(4)
    y_group(2)
    q_start(2)
    ticks(5, 7)
    with jax.named_scope('w_have2'):
        w_have(2, 'far')
    y_group(3)
    q_start(3)
    tick(7)

    first = pl.multiple_of(lax.div(chip * 2 * blk, LANES) * LANES, LANES)
    shift = chip * 2 * blk - first
    at_win = pl.ds(first, win)
    n_block = 3
    n_cols = model // n_block

    def w_grad(k, core):
        return acc.at[k, pl.ds(pl.multiple_of(shift + core * blk, 8), blk), :]

    def put_grad(k):
        send(w_grad(k, 1 - j), outs[k].at[:, w_cols(j)], out_send.at[k], out_recv.at[k], dp=partner).start()
        pltpu.make_async_copy(w_grad(k, j), outs[k].at[:, w_cols(j)], out_own.at[k]).start()

    def dx_tile(n):
        r = lax.rem(n, 2)

        def theirs(m, carry):
            cols = pl.ds(pl.multiple_of(m * n_cols, n_cols), n_cols)
            slot = lax.rem(m + r * n_block, 2)

            @pl.when(m + r * n_block >= 2)
            def _():
                wait(sb.at[slot], dx_send.at[slot])

            with jax.named_scope('dx_dot'):
                sb[slot] = dot_nt(h_all[1], w_s[0, cols, :]) + dot_nt(h_all[2], w_s[1, cols, :])
            send(sb.at[slot], pbuf.at[rows_of(r), cols], dx_send.at[slot], dx_recv.at[r, m], dp=partner).start()
            return carry

        def ours(m, carry):
            cols = pl.ds(pl.multiple_of(m * n_cols, n_cols), n_cols)
            with jax.named_scope('dx_wait'):
                wait(pbuf.at[rows_of(r), cols], dx_recv.at[r, m])
            with jax.named_scope('dx_dot'):
                yacc[1, rows_of(r), cols] = (yacc[1, rows_of(r), cols] + pbuf[rows_of(r), cols]
                                             + (dot_nt(h_all[1], w_s[0, cols, :]) + dot_nt(h_all[2], w_s[1, cols, :])))
            return carry

        @pl.when(n == 0)
        def _():
            pl.semaphore_wait(credit, 8)
            for r_ in (0, 1):
                wait(sb.at[r_, :, pl.ds(0, rest_units * LANES)], y_send.at[1, r_])

        @pl.when(n < 2)
        def _():
            lax.fori_loop(0, n_block, theirs, 0)

        @pl.when(n >= 2)
        def _():
            lax.fori_loop(0, n_block, ours, 0)

    load_a(1, 0)
    load_a(0, 0)

    def grad_tile(n, carry):
        q = n - 4
        slot = lax.rem(n, 2)
        at = jnp.where(n < 4, n, slot)
        final = n == 15

        @pl.when(n < 4)
        def _():
            q_start(4 + n)

        loaded(0, slot)

        @pl.when(n >= 4)
        def _():
            with jax.named_scope('ab'):
                a_all[at] = dot_nn(xt[slot], w_s[0])
                b_all[at] = dot_nn(xt[slot], w_s[1])

            @pl.when(final)
            def _():
                arrive(1, q)

            load_b(1, q)
        tick(jnp.where(n < 4, 8 + 2 * n, jnp.where(q < 6, 16 + 2 * q, 28 + 3 * (q - 6))))
        loaded(1, slot)
        with jax.named_scope('g_dot'):
            g_s[...] = dot_nn(dyt[slot], w_s[2])

        with jax.named_scope('act'):
            def body(m, c):
                lo = pl.ds(pl.multiple_of(m * group, group), group)
                a = a_all[at, lo, :]
                b = b_all[at, lo, :]
                g = g_s[lo, :]
                s = sigmoid(a)
                silu = a * s
                h_all[0, lo, :] = (silu * b).astype(BF16)
                h_all[1, lo, :] = (g * b * s * (1.0 + a * (1.0 - s))).astype(BF16)
                h_all[2, lo, :] = (g * silu).astype(BF16)
                return c

            lax.fori_loop(0, tile // group, body, 0)

        @pl.when(jnp.logical_and(n >= 10, n < 15))
        def _():
            tick(29 + 3 * (q - 6))

        @pl.when(n < 3)
        def _():
            load_a(0, n + 1)
            load_a(1, n + 1)

        @pl.when(jnp.logical_and(n >= 3, n < 15))
        def _():
            arrive(0, q + 1)

        with jax.named_scope('dw_dot'):
            x_win = xt[slot, :, at_win]
            acc[0] += dot_tn(x_win, h_all[1])

            @pl.when(final)
            def _():
                put_grad(0)

            acc[1] += dot_tn(x_win, h_all[2])

            @pl.when(final)
            def _():
                put_grad(1)

            acc[2] += dot_tn(dyt[slot, :, at_win], h_all[0])

            @pl.when(final)
            def _():
                put_grad(2)

        @pl.when(n < 4)
        def _():
            dx_tile(n)

        tick(jnp.where(n < 4, 9 + 2 * n, jnp.where(q < 6, 17 + 2 * q, 30 + 3 * (q - 6))))

        @pl.when(jnp.logical_and(n >= 3, n < 15))
        def _():
            load_b(0, q + 1)

            @pl.when(n < 14)
            def _():
                arrive(1, q + 1)
        return carry

    lax.fori_loop(0, 16, grad_tile, 0)

    with jax.named_scope('drain_sums'):
        drain_sums()
    with jax.named_scope('drain'):
        for slot in (0, 1):
            wait(sb.at[slot], dx_send.at[slot])
        for k in range(3):
            for core in (0, 1):
                for link in (0, 1):
                    for part in (0, 1):
                        w_copy(k, link, part, core).wait_send()
                    w_relay_copy(k, link, core).wait_send()
            w_partner_copy(k).wait_send()
        for ten in (0, 1):
            own_copy(ten).wait_send()

        def drain(q, carry):
            for ten in (0, 1):
                for link in (0, 1):
                    @pl.when(q < 8)
                    def _():
                        wait(slot_of(ten, 0, link, j), q_send.at[lax.rem(q, 8), link, ten])

                    @pl.when(q < 4)
                    def _():
                        wait(slot_of(ten, 0, link, j), rl_send.at[lax.rem(q, 4), link, ten])

                    wait(slot_of(ten, q, link, j), f_send.at[q, link, ten])
            return carry

        lax.fori_loop(0, 12, drain, 0)
    with jax.named_scope('drain_out'):
        for k in range(3):
            wait(w_grad(k, j), out_own.at[k])
            wait(w_grad(k, 1 - j), out_send.at[k])
            wait(w_grad(k, j), out_recv.at[k])


def window(model, blk):
    starts = [(2 * blk * c) // LANES * LANES for c in range(model // (2 * blk))]
    shift = max(2 * blk * c - s for c, s in enumerate(starts))
    return -(-(shift + 2 * blk) // LANES) * LANES


def mlp(x, dy, wg, wu, wd):
    rows, model = x.shape
    blk, width = wg.shape
    half = width // 2
    tile = rows // 2
    dma = pltpu.SemaphoreType.DMA
    vmem = pltpu.VMEM
    anywhere = pl.BlockSpec(memory_space=pl.ANY)
    shape = jax.ShapeDtypeStruct
    flops = 2 * model * half * rows * 2 * 20
    return pl.pallas_call(
        kernel,
        name='mlp',
        out_shape=(shape((2, rows, model), BF16),
                   shape((blk, width), F32), shape((blk, width), F32), shape((blk, width), F32),
                   shape((12, tile, model), BF16), shape((12, tile, model), BF16),
                   shape((rows, model), BF16), shape((rows, model), BF16)),
        in_specs=[anywhere] * 5,
        out_specs=tuple([anywhere] * 8),
        scratch_shapes=[
            vmem((3, model, half), BF16),
            vmem((3, window(model, blk), half), F32),
            vmem((2, rows, model), F32),
            vmem((rows, model), F32),
            vmem((2, tile, model // 3), F32),
            vmem((2, tile, model), BF16),
            vmem((2, tile, model), BF16),
            vmem((4, tile, half), F32),
            vmem((4, tile, half), F32),
            vmem((tile, half), F32),
            vmem((4, tile, half), BF16),
            vmem((2, SLOTS, tile, LANES), F32),
            vmem((2, SLOTS, tile, LANES), BF16),
            dma((3, 2, 2, 2)), dma((3, 2, 2, 2)), dma((3, 2, 2)), dma((3, 2, 2)), dma((3,)), dma((3,)), dma((3,)),
            dma((2,)), dma((2,)), dma((8, 2, 2)), dma((12, 2, 2)), dma((4, 2, 2)), dma((12, 2, 2)), dma((12, 2, 2)),
            dma((2, 2)), dma((4, 2)), dma((2,)), dma((2, 3)), pltpu.SemaphoreType.REGULAR,
            dma((2, SLOTS)), dma((2, SLOTS)), dma((2, SLOTS)), dma((2, SLOTS)), dma((2, SLOTS)),
            dma((2, 2)), dma((3,)), dma((3,)), dma((3,)),
        ],
        compiler_params=pltpu.CompilerParams(collective_id=0, has_side_effects=True, vmem_limit_bytes=67_000_000),
        cost_estimate=pl.CostEstimate(flops=flops, bytes_accessed=100_000_000, transcendentals=0),
    )(x, dy, wg, wu, wd)


def solution(mesh):
    def device_pass(x_rows, gate_blk, up_blk, down_blk, dy_rows):
        out = mlp(x_rows, dy_rows, gate_blk, up_blk, down_blk.T)
        yd, dw_gate, dw_up, dw_down = out[:4]
        return yd[0], yd[1], dw_gate, dw_up, dw_down.T

    row_spec = P('dp', None)
    weight_spec = P('dp', 'tp')
    down_spec = P('tp', 'dp')
    return jax.shard_map(device_pass, mesh=mesh,
                         in_specs=(row_spec, weight_spec, weight_spec, down_spec, row_spec),
                         out_specs=(row_spec, row_spec, weight_spec, weight_spec, down_spec),
                         check_vma=False)
```

```python
import jax
import jax.numpy as jnp
from jax import lax
from jax.experimental import pallas as pl
from jax.experimental.pallas import tpu as pltpu
from jax.sharding import PartitionSpec as P

F32 = jnp.float32
BF16 = jnp.bfloat16
MESH = pl.DeviceIdType.MESH
SLOTS = 8
LANES = 128
EARLY = 4


def dot_nn(a, b):
    return jnp.dot(a, b, preferred_element_type=F32)


def dot_nt(a, b):
    return lax.dot_general(a, b, (((1,), (1,)), ((), ())), preferred_element_type=F32)


def dot_tn(a, b):
    return lax.dot_general(a, b, (((0,), (0,)), ((), ())), preferred_element_type=F32)


def sigmoid(a):
    return 1.0 / (1.0 + jnp.exp(-a))


def kernel(x_ref, dy_ref, wg_ref, wu_ref, wd_ref,
           yd_ref, og_ref, ou_ref, od_ref, xb, dyb, xp, dyp,
           w_s, acc, yacc, pbuf, sb, xt, dyt, a_all, b_all, g_s, h_all, rbuf, fin,
           w_send, w_recv, wr_send, wr_recv, w_own, wp_send, wp_recv,
           own_send, own_recv, q_send, q_recv, rl_send, f_send, f_recv,
           y_send, y_recv, dx_send, dx_recv, credit,
           rs_send, rs_recv, ag_send, ag_recv, fin_own, ld, out_send, out_recv, out_own):
    rows, model = x_ref.shape
    blk, width = wg_ref.shape
    half = width // 2
    hb = blk // 2
    tile = rows // 2
    piece = tile // 4
    win = acc.shape[1]
    line = model // 2
    units = line // LANES
    near_units = (2 * blk - LANES // 2) // LANES if (2 * blk) % LANES else 2 * blk // LANES
    rest_units = units - near_units
    steps = 2 * units
    group = min(32, tile)
    w_in = (wg_ref, wu_ref, wd_ref)
    outs = (og_ref, ou_ref, od_ref)
    tok = (x_ref, dy_ref)
    tok_b = (xb, dyb)
    tok_p = (xp, dyp)
    tok_t = (xt, dyt)

    t = lax.axis_index('tp')
    me = lax.axis_index('dp')
    cy = lax.div(me, 4)
    cx = lax.rem(lax.div(me, 2), 2)
    j = lax.rem(me, 2)
    partner = me + 1 - 2 * j
    chip = cy * 2 + cx

    def near(link, core):
        if link == 0:
            return cy * 4 + (1 - cx) * 2 + core
        return (1 - cy) * 4 + cx * 2 + core

    def far(core):
        return (1 - cy) * 4 + (1 - cx) * 2 + core

    def send(src, dst, s_sem, r_sem, dp=None, tp=None):
        where = {'dp': me if dp is None else dp, 'tp': t if tp is None else tp}
        return pltpu.make_async_remote_copy(src_ref=src, dst_ref=dst, send_sem=s_sem, recv_sem=r_sem,
                                            device_id=where, device_id_type=MESH)

    def wait(ref, sem):
        pltpu.make_async_copy(ref, ref, sem).wait()

    barrier = pltpu.get_barrier_semaphore()
    for peer in (partner, near(0, 0), near(0, 1), near(1, 0), near(1, 1)):
        pl.semaphore_signal(barrier, inc=1, device_id={'dp': peer, 'tp': t}, device_id_type=MESH)

    @pl.when(t > 0)
    def _():
        pl.semaphore_signal(barrier, inc=1, device_id={'dp': me, 'tp': t - 1}, device_id_type=MESH)

    @pl.when(t < 3)
    def _():
        pl.semaphore_signal(barrier, inc=1, device_id={'dp': me, 'tp': t + 1}, device_id_type=MESH)

    pl.semaphore_wait(barrier, 5 + jnp.minimum(t, 1) + jnp.minimum(3 - t, 1))

    def w_rows(k, dev, part=None):
        if part is None:
            return w_s.at[k, pl.ds(pl.multiple_of(dev * blk, 16), blk), :]
        return w_s.at[k, pl.ds(pl.multiple_of(dev * blk + part * hb, 16), hb), :]

    def w_cols(core):
        return pl.ds(pl.multiple_of(core * half, LANES), half)

    def w_copy(k, link, part, core):
        return send(w_in[k].at[pl.ds(part * hb, hb), w_cols(core)], w_rows(k, me, part),
                    w_send.at[k, link, part, core], w_recv.at[k, link, part, j], dp=near(link, core))

    def w_own_copy(k):
        return pltpu.make_async_copy(w_in[k].at[:, w_cols(j)], w_rows(k, me), w_own.at[k])

    def w_partner_copy(k):
        return send(w_in[k].at[:, w_cols(1 - j)], w_rows(k, me), wp_send.at[k], wp_recv.at[k], dp=partner)

    def w_start(k):
        for first in (0, 1):
            for core in (0, 1):
                w_copy(k, 0, 1 - first, core).start()
                w_copy(k, 1, first, core).start()
        w_own_copy(k).start()
        w_partner_copy(k).start()

    def w_relay_copy(k, link_out, core):
        part = 1 if link_out == 1 else 0
        ref = w_rows(k, near(1 - link_out, core), part)
        return send(ref, ref, wr_send.at[k, link_out, core], wr_recv.at[k, link_out, core], dp=near(link_out, j))

    def w_relay(k):
        for core in (0, 1):
            wait(w_rows(k, near(0, core), 1), w_recv.at[k, 0, 1, core])
            w_relay_copy(k, 1, core).start()
            wait(w_rows(k, near(1, core), 0), w_recv.at[k, 1, 0, core])
            w_relay_copy(k, 0, core).start()

    def w_have(k, which):
        if which == 'chip':
            wait(w_rows(k, me), w_own.at[k])
            wait(w_rows(k, partner), wp_recv.at[k])
        for core in (0, 1):
            if which == 'x':
                wait(w_rows(k, near(0, core), 0), w_recv.at[k, 0, 0, core])
            if which == 'y':
                wait(w_rows(k, near(1, core), 1), w_recv.at[k, 1, 1, core])
            if which == 'far':
                wait(w_rows(k, far(core), 0), wr_recv.at[k, 0, core])
                wait(w_rows(k, far(core), 1), wr_recv.at[k, 1, core])

    def slot_of(ten, q, link, core):
        return tok_b[ten].at[q, pl.ds(pl.multiple_of((2 * link + core) * piece, piece), piece), :]

    def q_copy(ten, q, link):
        b = lax.div(q, 4)
        sub = lax.rem(q, 4)
        first = 1 - b if link == 0 else b
        src = tok[ten].at[pl.ds(pl.multiple_of(first * tile + sub * piece, piece), piece), :]
        return send(src, slot_of(ten, q, link, j), q_send.at[q, link, ten], q_recv.at[q, link, ten], dp=near(link, j))

    def q_start(q):
        for ten in (0, 1):
            for link in (0, 1):
                q_copy(ten, q, link).start()

    def relay_copy(ten, sub, link_out):
        return send(slot_of(ten, sub, 1 - link_out, j), slot_of(ten, 8 + sub, link_out, j),
                    rl_send.at[sub, link_out, ten], q_recv.at[8 + sub, link_out, ten], dp=near(link_out, j))

    def forward_copy(ten, q, link):
        ref = slot_of(ten, q, link, j)
        return send(ref, ref, f_send.at[q, link, ten], f_recv.at[q, link, ten], dp=partner)

    def own_copy(ten):
        return send(tok[ten], tok_p[ten], own_send.at[ten], own_recv.at[ten], dp=partner)

    def arrive(ten, q):
        with jax.named_scope('arrive'):
            for link in (0, 1):
                wait(slot_of(ten, q, link, j), q_recv.at[q, link, ten])
                forward_copy(ten, q, link).start()

        @pl.when(q < 4)
        def _():
            for link in (0, 1):
                relay_copy(ten, q, link).start()

    def load_b(ten, q):
        with jax.named_scope('passed'):
            for link in (0, 1):
                wait(slot_of(ten, q, link, 1 - j), f_recv.at[q, link, ten])
        pltpu.make_async_copy(tok_b[ten].at[q], tok_t[ten].at[lax.rem(q, 2)], ld.at[ten, lax.rem(q, 2)]).start()

    def rows_of(r):
        return pl.ds(pl.multiple_of(r * tile, tile), tile)

    def load_a(ten, n):
        own = lax.div(n, 2)
        slot = lax.rem(n, 2)

        @pl.when(own == 1)
        def _():
            pltpu.make_async_copy(tok[ten].at[rows_of(slot), :], tok_t[ten].at[slot], ld.at[ten, slot]).start()

        @pl.when(own == 0)
        def _():
            pltpu.make_async_copy(tok_p[ten].at[rows_of(slot), :], tok_t[ten].at[slot], ld.at[ten, slot]).start()

    def loaded(ten, slot):
        with jax.named_scope('ld'):
            wait(tok_t[ten].at[slot], ld.at[ten, slot])

    def unit_col(u):
        mine = cy * units
        other = (1 - cy) * units
        low = cx * rest_units
        high = (1 - cx) * near_units
        a = near_units
        col = jnp.where(u < a, mine + low + u,
                        jnp.where(u < units, mine + high + (u - a),
                                  jnp.where(u < units + a, other + low + (u - units), other + high + (u - units - a))))
        return pl.multiple_of(col * LANES, LANES)

    def chunk(s, way):
        return lax.div(s, steps), pl.ds(way * tile, tile), pl.ds(unit_col(lax.rem(s, steps)), LANES)

    def sum_copy(s, way, nxt):
        slot = lax.rem(s, SLOTS)
        return send(yacc.at[chunk(s, way)], rbuf.at[way, slot], rs_send.at[way, slot], rs_recv.at[way, slot], tp=nxt)

    def done_copy(s, way, prv, src):
        slot = lax.rem(s, SLOTS)
        return send(src, yd_ref.at[chunk(s, way)], ag_send.at[way, slot], ag_recv.at[way, slot], tp=prv)

    def tick(tau):
        with jax.named_scope('tick'):
            tick_body(tau)

    def tick_body(tau):
        for way in (0, 1):
            p = t if way == 0 else 3 - t
            nxt = t + 1 if way == 0 else t - 1
            prv = t - 1 if way == 0 else t + 1
            s = tau - p
            slot = lax.rem(jnp.maximum(s, 0), SLOTS)
            live = jnp.logical_and(s >= 0, s < 2 * steps)

            @pl.when(jnp.logical_and(live, p > 0))
            def _():
                wait(rbuf.at[way, slot], rs_recv.at[way, slot])

            @pl.when(jnp.logical_and(live, p < 3))
            def _():
                @pl.when(s >= SLOTS)
                def _():
                    wait(rbuf.at[way, slot], rs_send.at[way, slot])

                @pl.when(p > 0)
                def _():
                    here = chunk(s, way)
                    yacc[here] = yacc[here] + rbuf[way, slot]

                sum_copy(s, way, nxt).start()

            @pl.when(jnp.logical_and(live, p == 3))
            def _():
                @pl.when(s >= SLOTS)
                def _():
                    wait(fin.at[way, slot], ag_send.at[way, slot])
                    wait(fin.at[way, slot], fin_own.at[way, slot])

                here = chunk(s, way)
                fin[way, slot] = (yacc[here] + rbuf[way, slot]).astype(BF16)
                pltpu.make_async_copy(fin.at[way, slot], yd_ref.at[here], fin_own.at[way, slot]).start()
                done_copy(s, way, prv, fin.at[way, slot]).start()

            s2 = tau - 6 + p
            slot2 = lax.rem(jnp.maximum(s2, 0), SLOTS)
            live2 = jnp.logical_and(jnp.logical_and(s2 >= 0, s2 < 2 * steps), p < 3)

            @pl.when(live2)
            def _():
                here = yd_ref.at[chunk(s2, way)]
                wait(here, ag_recv.at[way, slot2])

                @pl.when(p > 0)
                def _():
                    @pl.when(s2 >= SLOTS)
                    def _():
                        wait(fin.at[way, slot2], ag_send.at[way, slot2])

                    done_copy(s2, way, prv, here).start()

    def ticks(lo, hi):
        def body(n, c):
            tick(n)
            return c

        lax.fori_loop(lo, hi, body, 0)

    def drain_sums():
        def body(n, carry):
            for way in (0, 1):
                p = t if way == 0 else 3 - t
                slot = n

                @pl.when(p < 3)
                def _():
                    wait(rbuf.at[way, slot], rs_send.at[way, slot])

                @pl.when(p > 0)
                def _():
                    wait(fin.at[way, slot], ag_send.at[way, slot])

                @pl.when(p == 3)
                def _():
                    wait(fin.at[way, slot], fin_own.at[way, slot])
            return carry

        lax.fori_loop(0, SLOTS, body, 0)

    for ten in (0, 1):
        own_copy(ten).start()
    w_start(0)
    w_start(1)
    base = jnp.where(t == 0, 1.0, 0.0).astype(F32)

    with jax.named_scope('clear'):
        for r in (0, 1):
            for ten in (0, 1):
                load_a(ten, 2 + r)

        def clear(n, carry):
            at = pl.ds(pl.multiple_of(n * 32, 32), 32)
            for k in range(3):
                acc[k, at, :] = jnp.zeros((32, half), F32)
            return carry

        lax.fori_loop(0, win // 32, clear, 0)

        def clear_ab(n, carry):
            lo = pl.ds(pl.multiple_of(n * group, group), group)
            for m in range(4):
                a_all[m, lo, :] = jnp.zeros((group, half), F32)
                b_all[m, lo, :] = jnp.zeros((group, half), F32)
            return carry

        lax.fori_loop(0, tile // group, clear_ab, 0)
        for r in (0, 1):
            for ten in (0, 1):
                loaded(ten, r)

                def residual(n, carry):
                    lo = pl.ds(pl.multiple_of(n * group, group), group)
                    there = pl.ds(pl.multiple_of(r * tile + n * group, group), group)
                    yacc[ten, there, :] = tok_t[ten][r, lo, :].astype(F32) * base
                    return carry

                lax.fori_loop(0, tile // group, residual, 0)
        for ten in (0, 1):
            wait(tok_p[ten], own_recv.at[ten])

    with jax.named_scope('w_relay'):
        w_relay(0)
        w_relay(1)
    w_start(2)

    def ab_pass(last):
        row = cy if last == 0 else 1 - cy
        at_k = pl.ds(pl.multiple_of(row * line, LANES), line)
        load_a(0, 0)

        def body(n, carry):
            slot = lax.rem(n, 2)

            @pl.when(n < 3)
            def _():
                load_a(0, n + 1)

            loaded(0, slot)
            with jax.named_scope('ab_half'):
                x_half = xt[slot, :, at_k]
                a_all[n] += dot_nn(x_half, w_s[0, at_k, :])
                b_all[n] += dot_nn(x_half, w_s[1, at_k, :])

            if last:
                def hidden(m, c):
                    lo = pl.ds(pl.multiple_of(m * group, group), group)
                    a = a_all[n, lo, :]
                    h_all[n, lo, :] = (a * sigmoid(a) * b_all[n, lo, :]).astype(BF16)
                    return c

                lax.fori_loop(0, tile // group, hidden, 0)
            return carry

        lax.fori_loop(0, 4, body, 0)

    with jax.named_scope('w_have'):
        for k in (0, 1):
            w_have(k, 'chip')
            w_have(k, 'x')
    ab_pass(0)
    with jax.named_scope('w_have'):
        for k in (0, 1):
            w_have(k, 'y')
            w_have(k, 'far')
    ab_pass(1)

    def y_group(g):
        u0 = (0, near_units, units, units + near_units)[g]
        n_u = (near_units, rest_units)[g % 2]
        col = unit_col(u0)
        cols = pl.ds(col, n_u * LANES)

        def theirs(r, carry):
            if g > 0:
                before = (near_units, rest_units)[(g - 1) % 2] * LANES
                wait(sb.at[r, :, pl.ds(0, before)], y_send.at[(g - 1) % 2, r])
            with jax.named_scope('y_dot'):
                sb[r, :, :n_u * LANES] = dot_nt(h_all[r], w_s[2, cols, :])
            send(sb.at[r, :, pl.ds(0, n_u * LANES)], pbuf.at[rows_of(r), cols],
                 y_send.at[g % 2, r], y_recv.at[g, r], dp=partner).start()
            return carry

        def ours(r, carry):
            with jax.named_scope('y_wait'):
                wait(pbuf.at[rows_of(r), cols], y_recv.at[g, r])
            with jax.named_scope('y_dot'):
                yacc[0, rows_of(r), cols] = (yacc[0, rows_of(r), cols] + pbuf[rows_of(r), cols]
                                             + dot_nt(h_all[2 + r], w_s[2, cols, :]))
            pl.semaphore_signal(credit, inc=1, device_id={'dp': partner, 'tp': t}, device_id_type=MESH)
            return carry

        lax.fori_loop(0, 2, theirs, 0)
        lax.fori_loop(0, 2, ours, 0)

    load_a(1, 0)
    load_a(0, 0)
    with jax.named_scope('w_have2'):
        w_have(2, 'chip')
    y_group(0)
    tick(0)
    with jax.named_scope('w_relay2'):
        w_relay(2)
    q_start(0)
    q_start(1)
    ticks(1, 4)
    with jax.named_scope('w_have2'):
        w_have(2, 'x')
        w_have(2, 'y')
    y_group(1)
    tick(4)
    y_group(2)
    q_start(2)
    ticks(5, 7)
    with jax.named_scope('w_have2'):
        w_have(2, 'far')
    y_group(3)
    q_start(3)
    tick(7)

    first = pl.multiple_of(lax.div(chip * 2 * blk, LANES) * LANES, LANES)
    shift = chip * 2 * blk - first
    at_win = pl.ds(first, win)
    n_block = 3
    n_cols = model // n_block

    def w_grad(k, core):
        return acc.at[k, pl.ds(pl.multiple_of(shift + core * blk, 8), blk), :]

    def put_grad(k):
        send(w_grad(k, 1 - j), outs[k].at[:, w_cols(j)], out_send.at[k], out_recv.at[k], dp=partner).start()
        pltpu.make_async_copy(w_grad(k, j), outs[k].at[:, w_cols(j)], out_own.at[k]).start()

    def dx_tile(n):
        r = lax.rem(n, 2)

        @pl.when(n == 0)
        def _():
            pl.semaphore_wait(credit, 8)
            for r_ in (0, 1):
                wait(sb.at[r_, :, pl.ds(0, rest_units * LANES)], y_send.at[1, r_])

        def block(m, carry):
            cols = pl.ds(pl.multiple_of(m * n_cols, n_cols), n_cols)
            slot = lax.rem(m + r * n_block, 2)

            @pl.when(jnp.logical_and(n < 2, m + r * n_block >= 2))
            def _():
                wait(sb.at[slot], dx_send.at[slot])

            @pl.when(n < 2)
            def _():
                with jax.named_scope('dx_dot'):
                    sb[slot] = dot_nt(h_all[1], w_s[0, cols, :]) + dot_nt(h_all[2], w_s[1, cols, :])
                send(sb.at[slot], pbuf.at[rows_of(r), cols], dx_send.at[slot], dx_recv.at[r, m], dp=partner).start()

            @pl.when(n >= 2)
            def _():
                with jax.named_scope('dx_wait'):
                    wait(pbuf.at[rows_of(r), cols], dx_recv.at[r, m])
                with jax.named_scope('dx_dot'):
                    yacc[1, rows_of(r), cols] = (yacc[1, rows_of(r), cols] + pbuf[rows_of(r), cols]
                                                 + (dot_nt(h_all[1], w_s[0, cols, :]) + dot_nt(h_all[2], w_s[1, cols, :])))

            @pl.when(m == 1)
            def _():
                tick(9 + 2 * n)
            return carry

        lax.fori_loop(0, n_block, block, 0)

    def grad_tile(n, carry):
        q = n - 4
        slot = lax.rem(n, 2)
        at = jnp.where(n < 4, n, slot)
        final = n == 15
        early = jnp.logical_and(n >= 3, q + 1 <= EARLY)
        late = jnp.logical_and(n < 15, q + 1 > EARLY)
        tau = jnp.where(q < EARLY, 16 + 2 * q, 16 + 2 * EARLY + 3 * (q - EARLY))

        @pl.when(n < 4)
        def _():
            q_start(4 + n)

        loaded(0, slot)

        @pl.when(n >= 4)
        def _():
            with jax.named_scope('ab'):
                a_all[at] = dot_nn(xt[slot], w_s[0])
                b_all[at] = dot_nn(xt[slot], w_s[1])

            @pl.when(final)
            def _():
                arrive(1, q)

            @pl.when(q > EARLY)
            def _():
                load_b(1, q)

            tick(tau)

        @pl.when(early)
        def _():
            arrive(0, q + 1)
            arrive(1, q + 1)

        loaded(1, slot)
        with jax.named_scope('g_dot'):
            g_s[...] = dot_nn(dyt[slot], w_s[2])

        with jax.named_scope('act'):
            def body(m, c):
                lo = pl.ds(pl.multiple_of(m * group, group), group)
                a = a_all[at, lo, :]
                b = b_all[at, lo, :]
                g = g_s[lo, :]
                s = sigmoid(a)
                silu = a * s
                h_all[0, lo, :] = (silu * b).astype(BF16)
                h_all[1, lo, :] = (g * b * s * (1.0 + a * (1.0 - s))).astype(BF16)
                h_all[2, lo, :] = (g * silu).astype(BF16)
                return c

            lax.fori_loop(0, tile // group, body, 0)

        @pl.when(jnp.logical_or(n < 4, q >= EARLY))
        def _():
            tick(jnp.where(n < 4, 8 + 2 * n, tau + 1))

        @pl.when(n < 3)
        def _():
            load_a(0, n + 1)
            load_a(1, n + 1)

        @pl.when(early)
        def _():
            load_b(0, q + 1)
            load_b(1, q + 1)

        @pl.when(late)
        def _():
            arrive(0, q + 1)

        with jax.named_scope('dw_dot'):
            x_win = xt[slot, :, at_win]
            acc[0] += dot_tn(x_win, h_all[1])

            @pl.when(final)
            def _():
                put_grad(0)

            acc[1] += dot_tn(x_win, h_all[2])

            @pl.when(final)
            def _():
                put_grad(1)

            acc[2] += dot_tn(dyt[slot, :, at_win], h_all[0])

            @pl.when(final)
            def _():
                put_grad(2)

        @pl.when(n < 4)
        def _():
            dx_tile(n)

        @pl.when(n >= 4)
        def _():
            tick(jnp.where(q < EARLY, tau + 1, tau + 2))

        @pl.when(late)
        def _():
            load_b(0, q + 1)

            @pl.when(n < 14)
            def _():
                arrive(1, q + 1)
        return carry

    lax.fori_loop(0, 16, grad_tile, 0)

    with jax.named_scope('drain_sums'):
        drain_sums()
    with jax.named_scope('drain'):
        for slot in (0, 1):
            wait(sb.at[slot], dx_send.at[slot])
        for k in range(3):
            for core in (0, 1):
                for link in (0, 1):
                    for part in (0, 1):
                        w_copy(k, link, part, core).wait_send()
                    w_relay_copy(k, link, core).wait_send()
            w_partner_copy(k).wait_send()
        for ten in (0, 1):
            own_copy(ten).wait_send()

        def drain(q, carry):
            for ten in (0, 1):
                for link in (0, 1):
                    @pl.when(q < 8)
                    def _():
                        wait(slot_of(ten, 0, link, j), q_send.at[lax.rem(q, 8), link, ten])

                    @pl.when(q < 4)
                    def _():
                        wait(slot_of(ten, 0, link, j), rl_send.at[lax.rem(q, 4), link, ten])

                    wait(slot_of(ten, q, link, j), f_send.at[q, link, ten])
            return carry

        lax.fori_loop(0, 12, drain, 0)
    with jax.named_scope('drain_out'):
        for k in range(3):
            wait(w_grad(k, j), out_own.at[k])
            wait(w_grad(k, 1 - j), out_send.at[k])
            wait(w_grad(k, j), out_recv.at[k])


def window(model, blk):
    starts = [(2 * blk * c) // LANES * LANES for c in range(model // (2 * blk))]
    shift = max(2 * blk * c - s for c, s in enumerate(starts))
    return -(-(shift + 2 * blk) // LANES) * LANES


def mlp(x, dy, wg, wu, wd):
    rows, model = x.shape
    blk, width = wg.shape
    half = width // 2
    tile = rows // 2
    dma = pltpu.SemaphoreType.DMA
    vmem = pltpu.VMEM
    anywhere = pl.BlockSpec(memory_space=pl.ANY)
    shape = jax.ShapeDtypeStruct
    flops = 2 * model * half * rows * 2 * 20
    return pl.pallas_call(
        kernel,
        name='mlp',
        out_shape=(shape((2, rows, model), BF16),
                   shape((blk, width), F32), shape((blk, width), F32), shape((blk, width), F32),
                   shape((12, tile, model), BF16), shape((12, tile, model), BF16),
                   shape((rows, model), BF16), shape((rows, model), BF16)),
        in_specs=[anywhere] * 5,
        out_specs=tuple([anywhere] * 8),
        scratch_shapes=[
            vmem((3, model, half), BF16),
            vmem((3, window(model, blk), half), F32),
            vmem((2, rows, model), F32),
            vmem((rows, model), F32),
            vmem((2, tile, model // 3), F32),
            vmem((2, tile, model), BF16),
            vmem((2, tile, model), BF16),
            vmem((4, tile, half), F32),
            vmem((4, tile, half), F32),
            vmem((tile, half), F32),
            vmem((4, tile, half), BF16),
            vmem((2, SLOTS, tile, LANES), F32),
            vmem((2, SLOTS, tile, LANES), BF16),
            dma((3, 2, 2, 2)), dma((3, 2, 2, 2)), dma((3, 2, 2)), dma((3, 2, 2)), dma((3,)), dma((3,)), dma((3,)),
            dma((2,)), dma((2,)), dma((8, 2, 2)), dma((12, 2, 2)), dma((4, 2, 2)), dma((12, 2, 2)), dma((12, 2, 2)),
            dma((2, 2)), dma((4, 2)), dma((2,)), dma((2, 3)), pltpu.SemaphoreType.REGULAR,
            dma((2, SLOTS)), dma((2, SLOTS)), dma((2, SLOTS)), dma((2, SLOTS)), dma((2, SLOTS)),
            dma((2, 2)), dma((3,)), dma((3,)), dma((3,)),
        ],
        compiler_params=pltpu.CompilerParams(collective_id=0, has_side_effects=True, vmem_limit_bytes=67_000_000),
        cost_estimate=pl.CostEstimate(flops=flops, bytes_accessed=100_000_000, transcendentals=0),
    )(x, dy, wg, wu, wd)


def copy_kernel(yd_ref, g_ref, u_ref, d_ref, y_out, dx_out, g_out, u_out, d_out, yd_s, g_s, u_s, d_s, load, store):
    rows = yd_ref.shape[1] // 4
    blk = g_ref.shape[0] // 4
    parts = []
    for m in range(4):
        for src, dst, buf in ((g_ref, g_out, g_s), (u_ref, u_out, u_s), (d_ref, d_out, d_s)):
            at = pl.ds(m * blk, blk)
            parts.append((src.at[at, :], buf.at[at, :], dst.at[at, :]))
        for ten, dst in ((0, y_out), (1, dx_out)):
            at = pl.ds(m * rows, rows)
            parts.append((yd_ref.at[ten, at, :], yd_s.at[ten, at, :], dst.at[at, :]))
    for n, (src, buf, dst) in enumerate(parts):
        pltpu.make_async_copy(src, buf, load.at[n]).start()
    for n, (src, buf, dst) in enumerate(parts):
        pltpu.make_async_copy(src, buf, load.at[n]).wait()
        pltpu.make_async_copy(buf, dst, store.at[n]).start()
    for n, (src, buf, dst) in enumerate(parts):
        pltpu.make_async_copy(buf, dst, store.at[n]).wait()


def copy_results(yd, dwg, dwu, dwd):
    anywhere = pl.BlockSpec(memory_space=pl.ANY)
    shape = jax.ShapeDtypeStruct
    vmem = pltpu.VMEM
    return pl.pallas_call(
        copy_kernel,
        name='results',
        out_shape=(shape(yd.shape[1:], yd.dtype), shape(yd.shape[1:], yd.dtype),
                   shape(dwg.shape, F32), shape(dwu.shape, F32), shape(dwd.shape, F32)),
        in_specs=[anywhere] * 4,
        out_specs=tuple([anywhere] * 5),
        scratch_shapes=[vmem(yd.shape, yd.dtype), vmem(dwg.shape, F32), vmem(dwu.shape, F32), vmem(dwd.shape, F32),
                        pltpu.SemaphoreType.DMA((20,)), pltpu.SemaphoreType.DMA((20,))],
        compiler_params=pltpu.CompilerParams(vmem_limit_bytes=64_000_000),
    )(yd, dwg, dwu, dwd)


def solution(mesh):
    def device_pass(x_rows, gate_blk, up_blk, down_blk, dy_rows):
        out = mlp(x_rows, dy_rows, gate_blk, up_blk, down_blk.T)
        y, dx, dw_gate, dw_up, dw_down = copy_results(*out[:4])
        return y, dx, dw_gate, dw_up, dw_down.T

    row_spec = P('dp', None)
    weight_spec = P('dp', 'tp')
    down_spec = P('tp', 'dp')
    return jax.shard_map(device_pass, mesh=mesh,
                         in_specs=(row_spec, weight_spec, weight_spec, down_spec, row_spec),
                         out_specs=(row_spec, row_spec, weight_spec, weight_spec, down_spec),
                         check_vma=False)
```

```python
import jax
import jax.numpy as jnp
from jax import lax
from jax.experimental import pallas as pl
from jax.experimental.pallas import tpu as pltpu
from jax.sharding import PartitionSpec as P

F32 = jnp.float32
BF16 = jnp.bfloat16
MESH = pl.DeviceIdType.MESH
SLOTS = 8
DEPTH = 13
HOP = 2
LANES = 128
EARLY = 6
SPARSE = 3


def dot_nn(a, b):
    return jnp.dot(a, b, preferred_element_type=F32)


def dot_nt(a, b):
    return lax.dot_general(a, b, (((1,), (1,)), ((), ())), preferred_element_type=F32)


def dot_tn(a, b):
    return lax.dot_general(a, b, (((0,), (0,)), ((), ())), preferred_element_type=F32)


def sigmoid(a):
    return 1.0 / (1.0 + jnp.exp(-a))


def kernel(x_ref, dy_ref, wg_ref, wu_ref, wd_ref,
           yd_ref, og_ref, ou_ref, od_ref, xb, dyb, xp, dyp,
           w_s, acc, yacc, pbuf, sb, xt, dyt, a_all, b_all, g_s, h_all, rbuf, fin,
           w_send, w_recv, wr_send, wr_recv, w_own, wp_send, wp_recv,
           own_send, own_recv, q_send, q_recv, rl_send, f_send, f_recv,
           y_send, y_recv, dx_send, dx_recv, credit,
           rs_send, rs_recv, ag_send, ag_recv, fin_own, ld, out_send, out_recv, out_own):
    rows, model = x_ref.shape
    blk, width = wg_ref.shape
    half = width // 2
    hb = blk // 2
    tile = rows // 2
    piece = tile // 4
    win = acc.shape[1]
    line = model // 2
    units = line // LANES
    near_units = (2 * blk - LANES // 2) // LANES if (2 * blk) % LANES else 2 * blk // LANES
    rest_units = units - near_units
    steps = 2 * units
    group = min(32, tile)
    w_in = (wg_ref, wu_ref, wd_ref)
    outs = (og_ref, ou_ref, od_ref)
    tok = (x_ref, dy_ref)
    tok_b = (xb, dyb)
    tok_p = (xp, dyp)
    tok_t = (xt, dyt)

    t = lax.axis_index('tp')
    me = lax.axis_index('dp')
    cy = lax.div(me, 4)
    cx = lax.rem(lax.div(me, 2), 2)
    j = lax.rem(me, 2)
    partner = me + 1 - 2 * j
    chip = cy * 2 + cx

    def near(link, core):
        if link == 0:
            return cy * 4 + (1 - cx) * 2 + core
        return (1 - cy) * 4 + cx * 2 + core

    def far(core):
        return (1 - cy) * 4 + (1 - cx) * 2 + core

    def send(src, dst, s_sem, r_sem, dp=None, tp=None):
        where = {'dp': me if dp is None else dp, 'tp': t if tp is None else tp}
        return pltpu.make_async_remote_copy(src_ref=src, dst_ref=dst, send_sem=s_sem, recv_sem=r_sem,
                                            device_id=where, device_id_type=MESH)

    def wait(ref, sem):
        pltpu.make_async_copy(ref, ref, sem).wait()

    barrier = pltpu.get_barrier_semaphore()
    for peer in (partner, near(0, 0), near(0, 1), near(1, 0), near(1, 1)):
        pl.semaphore_signal(barrier, inc=1, device_id={'dp': peer, 'tp': t}, device_id_type=MESH)

    @pl.when(t > 0)
    def _():
        pl.semaphore_signal(barrier, inc=1, device_id={'dp': me, 'tp': t - 1}, device_id_type=MESH)

    @pl.when(t < 3)
    def _():
        pl.semaphore_signal(barrier, inc=1, device_id={'dp': me, 'tp': t + 1}, device_id_type=MESH)

    pl.semaphore_wait(barrier, 5 + jnp.minimum(t, 1) + jnp.minimum(3 - t, 1))

    def w_rows(k, dev, part=None):
        if part is None:
            return w_s.at[k, pl.ds(pl.multiple_of(dev * blk, 16), blk), :]
        return w_s.at[k, pl.ds(pl.multiple_of(dev * blk + part * hb, 16), hb), :]

    def w_cols(core):
        return pl.ds(pl.multiple_of(core * half, LANES), half)

    def w_copy(k, link, part, core):
        return send(w_in[k].at[pl.ds(part * hb, hb), w_cols(core)], w_rows(k, me, part),
                    w_send.at[k, link, part, core], w_recv.at[k, link, part, j], dp=near(link, core))

    def w_own_copy(k):
        return pltpu.make_async_copy(w_in[k].at[:, w_cols(j)], w_rows(k, me), w_own.at[k])

    def w_partner_copy(k):
        return send(w_in[k].at[:, w_cols(1 - j)], w_rows(k, me), wp_send.at[k], wp_recv.at[k], dp=partner)

    def w_start(k):
        for first in (0, 1):
            for core in (0, 1):
                w_copy(k, 0, 1 - first, core).start()
                w_copy(k, 1, first, core).start()
        w_own_copy(k).start()
        w_partner_copy(k).start()

    def w_relay_copy(k, link_out, core):
        part = 1 if link_out == 1 else 0
        ref = w_rows(k, near(1 - link_out, core), part)
        return send(ref, ref, wr_send.at[k, link_out, core], wr_recv.at[k, link_out, core], dp=near(link_out, j))

    def w_relay(k):
        for core in (0, 1):
            wait(w_rows(k, near(0, core), 1), w_recv.at[k, 0, 1, core])
            w_relay_copy(k, 1, core).start()
            wait(w_rows(k, near(1, core), 0), w_recv.at[k, 1, 0, core])
            w_relay_copy(k, 0, core).start()

    def w_have(k, which):
        if which == 'chip':
            wait(w_rows(k, me), w_own.at[k])
            wait(w_rows(k, partner), wp_recv.at[k])
        for core in (0, 1):
            if which == 'x':
                wait(w_rows(k, near(0, core), 0), w_recv.at[k, 0, 0, core])
            if which == 'y':
                wait(w_rows(k, near(1, core), 1), w_recv.at[k, 1, 1, core])
            if which == 'far':
                wait(w_rows(k, far(core), 0), wr_recv.at[k, 0, core])
                wait(w_rows(k, far(core), 1), wr_recv.at[k, 1, core])

    def slot_of(ten, q, link, core):
        return tok_b[ten].at[q, pl.ds(pl.multiple_of((2 * link + core) * piece, piece), piece), :]

    def q_copy(ten, q, link):
        b = lax.div(q, 4)
        sub = lax.rem(q, 4)
        first = 1 - b if link == 0 else b
        src = tok[ten].at[pl.ds(pl.multiple_of(first * tile + sub * piece, piece), piece), :]
        return send(src, slot_of(ten, q, link, j), q_send.at[q, link, ten], q_recv.at[q, link, ten], dp=near(link, j))

    def q_start(q):
        for ten in (0, 1):
            for link in (0, 1):
                q_copy(ten, q, link).start()

    def relay_copy(ten, sub, link_out):
        return send(slot_of(ten, sub, 1 - link_out, j), slot_of(ten, 8 + sub, link_out, j),
                    rl_send.at[sub, link_out, ten], q_recv.at[8 + sub, link_out, ten], dp=near(link_out, j))

    def forward_copy(ten, q, link):
        ref = slot_of(ten, q, link, j)
        return send(ref, ref, f_send.at[q, link, ten], f_recv.at[q, link, ten], dp=partner)

    def own_copy(ten):
        return send(tok[ten], tok_p[ten], own_send.at[ten], own_recv.at[ten], dp=partner)

    def arrive(ten, q):
        with jax.named_scope('arrive'):
            for link in (0, 1):
                wait(slot_of(ten, q, link, j), q_recv.at[q, link, ten])
                forward_copy(ten, q, link).start()

        @pl.when(q < 4)
        def _():
            for link in (0, 1):
                relay_copy(ten, q, link).start()

    def load_b(ten, q):
        with jax.named_scope('passed'):
            for link in (0, 1):
                wait(slot_of(ten, q, link, 1 - j), f_recv.at[q, link, ten])
        pltpu.make_async_copy(tok_b[ten].at[q], tok_t[ten].at[lax.rem(q, 2)], ld.at[ten, lax.rem(q, 2)]).start()

    def rows_of(r):
        return pl.ds(pl.multiple_of(r * tile, tile), tile)

    def load_a(ten, n):
        own = lax.div(n, 2)
        slot = lax.rem(n, 2)

        @pl.when(own == 1)
        def _():
            pltpu.make_async_copy(tok[ten].at[rows_of(slot), :], tok_t[ten].at[slot], ld.at[ten, slot]).start()

        @pl.when(own == 0)
        def _():
            pltpu.make_async_copy(tok_p[ten].at[rows_of(slot), :], tok_t[ten].at[slot], ld.at[ten, slot]).start()

    def loaded(ten, slot):
        with jax.named_scope('ld'):
            wait(tok_t[ten].at[slot], ld.at[ten, slot])

    def unit_col(u):
        mine = cy * units
        other = (1 - cy) * units
        low = cx * rest_units
        high = (1 - cx) * near_units
        a = near_units
        col = jnp.where(u < a, mine + low + u,
                        jnp.where(u < units, mine + high + (u - a),
                                  jnp.where(u < units + a, other + low + (u - units), other + high + (u - units - a))))
        return pl.multiple_of(col * LANES, LANES)

    def chunk(s, way):
        return lax.div(s, steps), pl.ds(way * tile, tile), pl.ds(unit_col(lax.rem(s, steps)), LANES)

    def sum_copy(s, way, nxt):
        land = lax.rem(s, DEPTH)
        return send(yacc.at[chunk(s, way)], rbuf.at[way, land], rs_send.at[way, lax.rem(s, SLOTS)], rs_recv.at[way, land], tp=nxt)

    def done_copy(s, way, prv, src):
        return send(src, yd_ref.at[chunk(s, way)], ag_send.at[way, lax.rem(s, SLOTS)], ag_recv.at[way, lax.rem(s, DEPTH)], tp=prv)

    def tick(tau):
        with jax.named_scope('tick'):
            tick_body(tau)

    def tick_body(tau):
        for way in (0, 1):
            p = t if way == 0 else 3 - t
            nxt = t + 1 if way == 0 else t - 1
            prv = t - 1 if way == 0 else t + 1
            s = tau - HOP * p
            slot = lax.rem(jnp.maximum(s, 0), SLOTS)
            land = lax.rem(jnp.maximum(s, 0), DEPTH)
            live = jnp.logical_and(s >= 0, s < 2 * steps)

            @pl.when(jnp.logical_and(live, p > 0))
            def _():
                wait(rbuf.at[way, land], rs_recv.at[way, land])

            @pl.when(jnp.logical_and(live, p < 3))
            def _():
                @pl.when(s >= SLOTS)
                def _():
                    wait(rbuf.at[way, slot], rs_send.at[way, slot])

                @pl.when(p > 0)
                def _():
                    here = chunk(s, way)
                    yacc[here] = yacc[here] + rbuf[way, land]

                sum_copy(s, way, nxt).start()

            @pl.when(jnp.logical_and(live, p == 3))
            def _():
                @pl.when(s >= SLOTS)
                def _():
                    wait(fin.at[slot], ag_send.at[way, slot])
                    wait(fin.at[slot], fin_own.at[way, slot])

                here = chunk(s, way)
                fin[slot] = (yacc[here] + rbuf[way, land]).astype(BF16)
                pltpu.make_async_copy(fin.at[slot], yd_ref.at[here], fin_own.at[way, slot]).start()
                done_copy(s, way, prv, fin.at[slot]).start()

            s2 = tau - HOP * (6 - p)
            slot2 = lax.rem(jnp.maximum(s2, 0), SLOTS)
            land2 = lax.rem(jnp.maximum(s2, 0), DEPTH)
            live2 = jnp.logical_and(jnp.logical_and(s2 >= 0, s2 < 2 * steps), p < 3)

            @pl.when(live2)
            def _():
                here = yd_ref.at[chunk(s2, way)]
                wait(here, ag_recv.at[way, land2])

                @pl.when(p > 0)
                def _():
                    @pl.when(s2 >= SLOTS)
                    def _():
                        wait(fin.at[slot2], ag_send.at[way, slot2])

                    done_copy(s2, way, prv, here).start()

    def ticks(lo, hi):
        def body(n, c):
            tick(n)
            return c

        lax.fori_loop(lo, hi, body, 0)

    def drain_sums():
        def body(n, carry):
            for way in (0, 1):
                p = t if way == 0 else 3 - t
                slot = n

                @pl.when(p < 3)
                def _():
                    wait(rbuf.at[way, slot], rs_send.at[way, slot])

                @pl.when(p > 0)
                def _():
                    wait(fin.at[slot], ag_send.at[way, slot])

                @pl.when(p == 3)
                def _():
                    wait(fin.at[slot], fin_own.at[way, slot])
            return carry

        lax.fori_loop(0, SLOTS, body, 0)

    for ten in (0, 1):
        own_copy(ten).start()
    w_start(0)
    w_start(1)
    base = jnp.where(t == 0, 1.0, 0.0).astype(F32)

    with jax.named_scope('clear'):
        for r in (0, 1):
            for ten in (0, 1):
                load_a(ten, 2 + r)

        def clear(n, carry):
            at = pl.ds(pl.multiple_of(n * 32, 32), 32)
            for k in range(3):
                acc[k, at, :] = jnp.zeros((32, half), F32)
            return carry

        lax.fori_loop(0, win // 32, clear, 0)

        def clear_ab(n, carry):
            lo = pl.ds(pl.multiple_of(n * group, group), group)
            for m in range(4):
                a_all[m, lo, :] = jnp.zeros((group, half), F32)
                b_all[m, lo, :] = jnp.zeros((group, half), F32)
            return carry

        lax.fori_loop(0, tile // group, clear_ab, 0)
        for r in (0, 1):
            for ten in (0, 1):
                loaded(ten, r)

                def residual(n, carry):
                    lo = pl.ds(pl.multiple_of(n * group, group), group)
                    there = pl.ds(pl.multiple_of(r * tile + n * group, group), group)
                    yacc[ten, there, :] = tok_t[ten][r, lo, :].astype(F32) * base
                    return carry

                lax.fori_loop(0, tile // group, residual, 0)
        for ten in (0, 1):
            wait(tok_p[ten], own_recv.at[ten])

    with jax.named_scope('w_relay'):
        w_relay(0)
        w_relay(1)
    w_start(2)

    def ab_pass(last):
        row = cy if last == 0 else 1 - cy
        at_k = pl.ds(pl.multiple_of(row * line, LANES), line)
        load_a(0, 0)

        def body(n, carry):
            slot = lax.rem(n, 2)

            @pl.when(n < 3)
            def _():
                load_a(0, n + 1)

            loaded(0, slot)
            with jax.named_scope('ab_half'):
                x_half = xt[slot, :, at_k]
                a_all[n] += dot_nn(x_half, w_s[0, at_k, :])
                b_all[n] += dot_nn(x_half, w_s[1, at_k, :])

            if last:
                def hidden(m, c):
                    lo = pl.ds(pl.multiple_of(m * group, group), group)
                    a = a_all[n, lo, :]
                    h_all[n, lo, :] = (a * sigmoid(a) * b_all[n, lo, :]).astype(BF16)
                    return c

                lax.fori_loop(0, tile // group, hidden, 0)
            return carry

        lax.fori_loop(0, 4, body, 0)

    with jax.named_scope('w_have'):
        for k in (0, 1):
            w_have(k, 'chip')
            w_have(k, 'x')
    ab_pass(0)
    with jax.named_scope('w_have'):
        for k in (0, 1):
            w_have(k, 'y')
            w_have(k, 'far')
    ab_pass(1)

    def y_group(g):
        u0 = (0, near_units, units, units + near_units)[g]
        n_u = (near_units, rest_units)[g % 2]
        col = unit_col(u0)
        cols = pl.ds(col, n_u * LANES)

        def theirs(r, carry):
            if g > 0:
                before = (near_units, rest_units)[(g - 1) % 2] * LANES
                wait(sb.at[r, :, pl.ds(0, before)], y_send.at[(g - 1) % 2, r])
            with jax.named_scope('y_dot'):
                sb[r, :, :n_u * LANES] = dot_nt(h_all[r], w_s[2, cols, :])
            send(sb.at[r, :, pl.ds(0, n_u * LANES)], pbuf.at[rows_of(r), cols],
                 y_send.at[g % 2, r], y_recv.at[g, r], dp=partner).start()
            return carry

        def ours(r, carry):
            with jax.named_scope('y_wait'):
                wait(pbuf.at[rows_of(r), cols], y_recv.at[g, r])
            with jax.named_scope('y_dot'):
                yacc[0, rows_of(r), cols] = (yacc[0, rows_of(r), cols] + pbuf[rows_of(r), cols]
                                             + dot_nt(h_all[2 + r], w_s[2, cols, :]))
            pl.semaphore_signal(credit, inc=1, device_id={'dp': partner, 'tp': t}, device_id_type=MESH)
            return carry

        lax.fori_loop(0, 2, theirs, 0)
        lax.fori_loop(0, 2, ours, 0)

    load_a(1, 0)
    load_a(0, 0)
    with jax.named_scope('w_have2'):
        w_have(2, 'chip')
    y_group(0)
    tick(0)
    with jax.named_scope('w_relay2'):
        w_relay(2)
    q_start(0)
    q_start(1)
    ticks(1, 4)
    with jax.named_scope('w_have2'):
        w_have(2, 'x')
        w_have(2, 'y')
    y_group(1)
    tick(4)
    y_group(2)
    q_start(2)
    ticks(5, 7)
    with jax.named_scope('w_have2'):
        w_have(2, 'far')
    y_group(3)
    q_start(3)
    tick(7)

    first = pl.multiple_of(lax.div(chip * 2 * blk, LANES) * LANES, LANES)
    shift = chip * 2 * blk - first
    at_win = pl.ds(first, win)
    n_block = 3
    n_cols = model // n_block

    def w_grad(k, core):
        return acc.at[k, pl.ds(pl.multiple_of(shift + core * blk, 8), blk), :]

    def put_grad(k):
        send(w_grad(k, 1 - j), outs[k].at[:, w_cols(j)], out_send.at[k], out_recv.at[k], dp=partner).start()
        pltpu.make_async_copy(w_grad(k, j), outs[k].at[:, w_cols(j)], out_own.at[k]).start()

    def dx_tile(n):
        r = lax.rem(n, 2)

        @pl.when(n == 0)
        def _():
            pl.semaphore_wait(credit, 8)
            for r_ in (0, 1):
                wait(sb.at[r_, :, pl.ds(0, rest_units * LANES)], y_send.at[1, r_])

        def block(m, carry):
            cols = pl.ds(pl.multiple_of(m * n_cols, n_cols), n_cols)
            slot = lax.rem(m + r * n_block, 2)

            @pl.when(jnp.logical_and(n < 2, m + r * n_block >= 2))
            def _():
                wait(sb.at[slot], dx_send.at[slot])

            @pl.when(n < 2)
            def _():
                with jax.named_scope('dx_dot'):
                    sb[slot] = dot_nt(h_all[1], w_s[0, cols, :]) + dot_nt(h_all[2], w_s[1, cols, :])
                send(sb.at[slot], pbuf.at[rows_of(r), cols], dx_send.at[slot], dx_recv.at[r, m], dp=partner).start()

            @pl.when(n >= 2)
            def _():
                with jax.named_scope('dx_wait'):
                    wait(pbuf.at[rows_of(r), cols], dx_recv.at[r, m])
                with jax.named_scope('dx_dot'):
                    yacc[1, rows_of(r), cols] = (yacc[1, rows_of(r), cols] + pbuf[rows_of(r), cols]
                                                 + (dot_nt(h_all[1], w_s[0, cols, :]) + dot_nt(h_all[2], w_s[1, cols, :])))

            @pl.when(m == 1)
            def _():
                tick(9 + 2 * n)
            return carry

        lax.fori_loop(0, n_block, block, 0)

    def grad_tile(n, carry):
        q = n - 4
        slot = lax.rem(n, 2)
        at = jnp.where(n < 4, n, slot)
        final = n == 15
        early = jnp.logical_and(n >= 3, q + 1 <= EARLY)
        late = jnp.logical_and(n < 15, q + 1 > EARLY)
        tau = jnp.where(q < SPARSE, 16 + 2 * q, 16 + 2 * SPARSE + 3 * (q - SPARSE))

        @pl.when(n < 4)
        def _():
            q_start(4 + n)

        loaded(0, slot)

        @pl.when(n >= 4)
        def _():
            with jax.named_scope('ab'):
                a_all[at] = dot_nn(xt[slot], w_s[0])
                b_all[at] = dot_nn(xt[slot], w_s[1])

            @pl.when(final)
            def _():
                arrive(1, q)

            @pl.when(q > EARLY)
            def _():
                load_b(1, q)

            tick(tau)

        @pl.when(early)
        def _():
            arrive(0, q + 1)
            arrive(1, q + 1)

        loaded(1, slot)
        with jax.named_scope('g_dot'):
            g_s[...] = dot_nn(dyt[slot], w_s[2])

        with jax.named_scope('act'):
            def body(m, c):
                lo = pl.ds(pl.multiple_of(m * group, group), group)
                a = a_all[at, lo, :]
                b = b_all[at, lo, :]
                g = g_s[lo, :]
                s = sigmoid(a)
                silu = a * s
                h_all[0, lo, :] = (silu * b).astype(BF16)
                h_all[1, lo, :] = (g * b * s * (1.0 + a * (1.0 - s))).astype(BF16)
                h_all[2, lo, :] = (g * silu).astype(BF16)
                return c

            lax.fori_loop(0, tile // group, body, 0)

        @pl.when(jnp.logical_or(n < 4, q >= SPARSE))
        def _():
            tick(jnp.where(n < 4, 8 + 2 * n, tau + 1))

        @pl.when(n < 3)
        def _():
            load_a(0, n + 1)
            load_a(1, n + 1)

        @pl.when(early)
        def _():
            load_b(0, q + 1)
            load_b(1, q + 1)

        @pl.when(late)
        def _():
            arrive(0, q + 1)

        with jax.named_scope('dw_dot'):
            x_win = xt[slot, :, at_win]
            acc[0] += dot_tn(x_win, h_all[1])

            @pl.when(final)
            def _():
                put_grad(0)

            acc[1] += dot_tn(x_win, h_all[2])

            @pl.when(final)
            def _():
                put_grad(1)

            acc[2] += dot_tn(dyt[slot, :, at_win], h_all[0])

            @pl.when(final)
            def _():
                put_grad(2)

        @pl.when(n < 4)
        def _():
            dx_tile(n)

        @pl.when(n >= 4)
        def _():
            tick(jnp.where(q < SPARSE, tau + 1, tau + 2))

        @pl.when(late)
        def _():
            load_b(0, q + 1)

            @pl.when(n < 14)
            def _():
                arrive(1, q + 1)
        return carry

    lax.fori_loop(0, 16, grad_tile, 0)

    with jax.named_scope('drain_sums'):
        drain_sums()
    with jax.named_scope('drain'):
        for slot in (0, 1):
            wait(sb.at[slot], dx_send.at[slot])
        for k in range(3):
            for core in (0, 1):
                for link in (0, 1):
                    for part in (0, 1):
                        w_copy(k, link, part, core).wait_send()
                    w_relay_copy(k, link, core).wait_send()
            w_partner_copy(k).wait_send()
        for ten in (0, 1):
            own_copy(ten).wait_send()

        def drain(q, carry):
            for ten in (0, 1):
                for link in (0, 1):
                    @pl.when(q < 8)
                    def _():
                        wait(slot_of(ten, 0, link, j), q_send.at[lax.rem(q, 8), link, ten])

                    @pl.when(q < 4)
                    def _():
                        wait(slot_of(ten, 0, link, j), rl_send.at[lax.rem(q, 4), link, ten])

                    wait(slot_of(ten, q, link, j), f_send.at[q, link, ten])
            return carry

        lax.fori_loop(0, 12, drain, 0)
    with jax.named_scope('drain_out'):
        for k in range(3):
            wait(w_grad(k, j), out_own.at[k])
            wait(w_grad(k, 1 - j), out_send.at[k])
            wait(w_grad(k, j), out_recv.at[k])


def window(model, blk):
    starts = [(2 * blk * c) // LANES * LANES for c in range(model // (2 * blk))]
    shift = max(2 * blk * c - s for c, s in enumerate(starts))
    return -(-(shift + 2 * blk) // LANES) * LANES


def mlp(x, dy, wg, wu, wd):
    rows, model = x.shape
    blk, width = wg.shape
    half = width // 2
    tile = rows // 2
    dma = pltpu.SemaphoreType.DMA
    vmem = pltpu.VMEM
    anywhere = pl.BlockSpec(memory_space=pl.ANY)
    shape = jax.ShapeDtypeStruct
    flops = 2 * model * half * rows * 2 * 20
    return pl.pallas_call(
        kernel,
        name='mlp',
        out_shape=(shape((2, rows, model), BF16),
                   shape((blk, width), F32), shape((blk, width), F32), shape((blk, width), F32),
                   shape((12, tile, model), BF16), shape((12, tile, model), BF16),
                   shape((rows, model), BF16), shape((rows, model), BF16)),
        in_specs=[anywhere] * 5,
        out_specs=tuple([anywhere] * 8),
        scratch_shapes=[
            vmem((3, model, half), BF16),
            vmem((3, window(model, blk), half), F32),
            vmem((2, rows, model), F32),
            vmem((rows, model), F32),
            vmem((2, tile, model // 3), F32),
            vmem((2, tile, model), BF16),
            vmem((2, tile, model), BF16),
            vmem((4, tile, half), F32),
            vmem((4, tile, half), F32),
            vmem((tile, half), F32),
            vmem((4, tile, half), BF16),
            vmem((2, DEPTH, tile, LANES), F32),
            vmem((SLOTS, tile, LANES), BF16),
            dma((3, 2, 2, 2)), dma((3, 2, 2, 2)), dma((3, 2, 2)), dma((3, 2, 2)), dma((3,)), dma((3,)), dma((3,)),
            dma((2,)), dma((2,)), dma((8, 2, 2)), dma((12, 2, 2)), dma((4, 2, 2)), dma((12, 2, 2)), dma((12, 2, 2)),
            dma((2, 2)), dma((4, 2)), dma((2,)), dma((2, 3)), pltpu.SemaphoreType.REGULAR,
            dma((2, SLOTS)), dma((2, DEPTH)), dma((2, SLOTS)), dma((2, DEPTH)), dma((2, SLOTS)),
            dma((2, 2)), dma((3,)), dma((3,)), dma((3,)),
        ],
        compiler_params=pltpu.CompilerParams(collective_id=0, has_side_effects=True, vmem_limit_bytes=67_000_000),
        cost_estimate=pl.CostEstimate(flops=flops, bytes_accessed=100_000_000, transcendentals=0),
    )(x, dy, wg, wu, wd)


def copy_kernel(yd_ref, g_ref, u_ref, d_ref, y_out, dx_out, g_out, u_out, d_out, yd_s, g_s, u_s, d_s, load, store):
    rows = yd_ref.shape[1] // 4
    blk = g_ref.shape[0] // 4
    parts = []
    for m in range(4):
        for src, dst, buf in ((g_ref, g_out, g_s), (u_ref, u_out, u_s), (d_ref, d_out, d_s)):
            at = pl.ds(m * blk, blk)
            parts.append((src.at[at, :], buf.at[at, :], dst.at[at, :]))
        for ten, dst in ((0, y_out), (1, dx_out)):
            at = pl.ds(m * rows, rows)
            parts.append((yd_ref.at[ten, at, :], yd_s.at[ten, at, :], dst.at[at, :]))
    for n, (src, buf, dst) in enumerate(parts):
        pltpu.make_async_copy(src, buf, load.at[n]).start()
    for n, (src, buf, dst) in enumerate(parts):
        pltpu.make_async_copy(src, buf, load.at[n]).wait()
        pltpu.make_async_copy(buf, dst, store.at[n]).start()
    for n, (src, buf, dst) in enumerate(parts):
        pltpu.make_async_copy(buf, dst, store.at[n]).wait()


def copy_results(yd, dwg, dwu, dwd):
    anywhere = pl.BlockSpec(memory_space=pl.ANY)
    shape = jax.ShapeDtypeStruct
    vmem = pltpu.VMEM
    return pl.pallas_call(
        copy_kernel,
        name='results',
        out_shape=(shape(yd.shape[1:], yd.dtype), shape(yd.shape[1:], yd.dtype),
                   shape(dwg.shape, F32), shape(dwu.shape, F32), shape(dwd.shape, F32)),
        in_specs=[anywhere] * 4,
        out_specs=tuple([anywhere] * 5),
        scratch_shapes=[vmem(yd.shape, yd.dtype), vmem(dwg.shape, F32), vmem(dwu.shape, F32), vmem(dwd.shape, F32),
                        pltpu.SemaphoreType.DMA((20,)), pltpu.SemaphoreType.DMA((20,))],
        compiler_params=pltpu.CompilerParams(vmem_limit_bytes=64_000_000),
    )(yd, dwg, dwu, dwd)


def solution(mesh):
    def device_pass(x_rows, gate_blk, up_blk, down_blk, dy_rows):
        out = mlp(x_rows, dy_rows, gate_blk, up_blk, down_blk.T)
        y, dx, dw_gate, dw_up, dw_down = copy_results(*out[:4])
        return y, dx, dw_gate, dw_up, dw_down.T

    row_spec = P('dp', None)
    weight_spec = P('dp', 'tp')
    down_spec = P('tp', 'dp')
    return jax.shard_map(device_pass, mesh=mesh,
                         in_specs=(row_spec, weight_spec, weight_spec, down_spec, row_spec),
                         out_specs=(row_spec, row_spec, weight_spec, weight_spec, down_spec),
                         check_vma=False)
```

```python
import jax
import jax.numpy as jnp
from jax import lax
from jax.experimental import pallas as pl
from jax.experimental.pallas import tpu as pltpu
from jax.sharding import PartitionSpec as P

F32 = jnp.float32
BF16 = jnp.bfloat16
MESH = pl.DeviceIdType.MESH
SLOTS = 8
DEPTH = 13
HOP = 2
LANES = 128
EARLY = 6
SPARSE = 3


def dot_nn(a, b):
    return jnp.dot(a, b, preferred_element_type=F32)


def dot_nt(a, b):
    return lax.dot_general(a, b, (((1,), (1,)), ((), ())), preferred_element_type=F32)


def dot_tn(a, b):
    return lax.dot_general(a, b, (((0,), (0,)), ((), ())), preferred_element_type=F32)


def sigmoid(a):
    return 1.0 / (1.0 + jnp.exp(-a))


def kernel(x_ref, dy_ref, wg_ref, wu_ref, wd_ref,
           yd_ref, og_ref, ou_ref, od_ref, xb, dyb, xp, dyp,
           w_s, acc, yacc, pbuf, sb, xt, dyt, a_all, b_all, g_s, h_all, rbuf, fin,
           w_send, w_recv, wr_send, wr_recv, w_own, wp_send, wp_recv,
           own_send, own_recv, q_send, q_recv, rl_send, f_send, f_recv,
           y_send, y_recv, dx_send, dx_recv, credit, room,
           rs_send, rs_recv, ag_send, ag_recv, fin_own, ld, out_send, out_recv, out_own):
    rows, model = x_ref.shape
    blk, width = wg_ref.shape
    half = width // 2
    hb = blk // 2
    tile = rows // 2
    piece = tile // 4
    win = acc.shape[1]
    line = model // 2
    units = line // LANES
    near_units = (2 * blk - LANES // 2) // LANES if (2 * blk) % LANES else 2 * blk // LANES
    rest_units = units - near_units
    steps = 4 * units
    part_rows = tile // 2
    group = min(32, tile)
    w_in = (wg_ref, wu_ref, wd_ref)
    outs = (og_ref, ou_ref, od_ref)
    tok = (x_ref, dy_ref)
    tok_b = (xb, dyb)
    tok_p = (xp, dyp)
    tok_t = (xt, dyt)

    t = lax.axis_index('tp')
    me = lax.axis_index('dp')
    cy = lax.div(me, 4)
    cx = lax.rem(lax.div(me, 2), 2)
    j = lax.rem(me, 2)
    partner = me + 1 - 2 * j
    chip = cy * 2 + cx

    def near(link, core):
        if link == 0:
            return cy * 4 + (1 - cx) * 2 + core
        return (1 - cy) * 4 + cx * 2 + core

    def far(core):
        return (1 - cy) * 4 + (1 - cx) * 2 + core

    def send(src, dst, s_sem, r_sem, dp=None, tp=None):
        where = {'dp': me if dp is None else dp, 'tp': t if tp is None else tp}
        return pltpu.make_async_remote_copy(src_ref=src, dst_ref=dst, send_sem=s_sem, recv_sem=r_sem,
                                            device_id=where, device_id_type=MESH)

    def wait(ref, sem):
        pltpu.make_async_copy(ref, ref, sem).wait()

    barrier = pltpu.get_barrier_semaphore()
    for peer in (partner, near(0, 0), near(0, 1), near(1, 0), near(1, 1)):
        pl.semaphore_signal(barrier, inc=1, device_id={'dp': peer, 'tp': t}, device_id_type=MESH)

    @pl.when(t > 0)
    def _():
        pl.semaphore_signal(barrier, inc=1, device_id={'dp': me, 'tp': t - 1}, device_id_type=MESH)

    @pl.when(t < 3)
    def _():
        pl.semaphore_signal(barrier, inc=1, device_id={'dp': me, 'tp': t + 1}, device_id_type=MESH)

    pl.semaphore_wait(barrier, 5 + jnp.minimum(t, 1) + jnp.minimum(3 - t, 1))

    def w_rows(k, dev, part=None):
        if part is None:
            return w_s.at[k, pl.ds(pl.multiple_of(dev * blk, 16), blk), :]
        return w_s.at[k, pl.ds(pl.multiple_of(dev * blk + part * hb, 16), hb), :]

    def w_cols(core):
        return pl.ds(pl.multiple_of(core * half, LANES), half)

    def w_copy(k, link, part, core):
        return send(w_in[k].at[pl.ds(part * hb, hb), w_cols(core)], w_rows(k, me, part),
                    w_send.at[k, link, part, core], w_recv.at[k, link, part, j], dp=near(link, core))

    def w_own_copy(k):
        return pltpu.make_async_copy(w_in[k].at[:, w_cols(j)], w_rows(k, me), w_own.at[k])

    def w_partner_copy(k):
        return send(w_in[k].at[:, w_cols(1 - j)], w_rows(k, me), wp_send.at[k], wp_recv.at[k], dp=partner)

    def w_start(k):
        for first in (0, 1):
            for core in (0, 1):
                w_copy(k, 0, 1 - first, core).start()
                w_copy(k, 1, first, core).start()
        w_own_copy(k).start()
        w_partner_copy(k).start()

    def w_relay_copy(k, link_out, core):
        part = 1 if link_out == 1 else 0
        ref = w_rows(k, near(1 - link_out, core), part)
        return send(ref, ref, wr_send.at[k, link_out, core], wr_recv.at[k, link_out, core], dp=near(link_out, j))

    def w_relay(k):
        for core in (0, 1):
            wait(w_rows(k, near(0, core), 1), w_recv.at[k, 0, 1, core])
            w_relay_copy(k, 1, core).start()
            wait(w_rows(k, near(1, core), 0), w_recv.at[k, 1, 0, core])
            w_relay_copy(k, 0, core).start()

    def w_have(k, which):
        if which == 'chip':
            wait(w_rows(k, me), w_own.at[k])
            wait(w_rows(k, partner), wp_recv.at[k])
        for core in (0, 1):
            if which == 'x':
                wait(w_rows(k, near(0, core), 0), w_recv.at[k, 0, 0, core])
            if which == 'y':
                wait(w_rows(k, near(1, core), 1), w_recv.at[k, 1, 1, core])
            if which == 'far':
                wait(w_rows(k, far(core), 0), wr_recv.at[k, 0, core])
                wait(w_rows(k, far(core), 1), wr_recv.at[k, 1, core])

    def slot_of(ten, q, link):
        return tok_b[ten].at[q, pl.ds(link * piece, piece), :]

    def q_copy(ten, q, link):
        b = lax.div(q, 4)
        sub = lax.rem(q, 4)
        first = 1 - b if link == 0 else b
        src = tok[ten].at[pl.ds(pl.multiple_of(first * tile + sub * piece, piece), piece), :]
        return send(src, slot_of(ten, q, link), q_send.at[q, link, ten], q_recv.at[q, link, ten], dp=near(link, j))

    def q_start(q):
        for ten in (0, 1):
            for link in (0, 1):
                q_copy(ten, q, link).start()

    def relay_copy(ten, sub, link_out):
        return send(slot_of(ten, sub, 1 - link_out), slot_of(ten, 8 + sub, link_out),
                    rl_send.at[sub, link_out, ten], q_recv.at[8 + sub, link_out, ten], dp=near(link_out, j))

    def tile_part(ten, q, core):
        return tok_t[ten].at[lax.rem(q, 2), pl.ds(pl.multiple_of(core * 2 * piece, 2 * piece), 2 * piece), :]

    def forward_copy(ten, q):
        return send(tok_b[ten].at[q], tile_part(ten, q, j), f_send.at[q, ten], f_recv.at[q, ten], dp=partner)

    def own_copy(ten):
        return send(tok[ten], tok_p[ten], own_send.at[ten], own_recv.at[ten], dp=partner)

    def arrive(ten, q):
        with jax.named_scope('arrive'):
            for link in (0, 1):
                wait(slot_of(ten, q, link), q_recv.at[q, link, ten])
            pl.semaphore_wait(room.at[ten], 1)
            forward_copy(ten, q).start()
            pltpu.make_async_copy(tok_b[ten].at[q], tile_part(ten, q, j), ld.at[ten, lax.rem(q, 2)]).start()

        @pl.when(q < 4)
        def _():
            for link in (0, 1):
                relay_copy(ten, q, link).start()

    def landed(ten, q):
        with jax.named_scope('landed'):
            wait(tile_part(ten, q, j), ld.at[ten, lax.rem(q, 2)])
            wait(tile_part(ten, q, 1 - j), f_recv.at[q, ten])

    def rows_of(r):
        return pl.ds(pl.multiple_of(r * tile, tile), tile)

    def load_a(ten, n):
        own = lax.div(n, 2)
        slot = lax.rem(n, 2)

        @pl.when(own == 1)
        def _():
            pltpu.make_async_copy(tok[ten].at[rows_of(slot), :], tok_t[ten].at[slot], ld.at[ten, slot]).start()

        @pl.when(own == 0)
        def _():
            pltpu.make_async_copy(tok_p[ten].at[rows_of(slot), :], tok_t[ten].at[slot], ld.at[ten, slot]).start()

    def loaded(ten, slot):
        with jax.named_scope('ld'):
            wait(tok_t[ten].at[slot], ld.at[ten, slot])

    def unit_col(u):
        mine = cy * units
        other = (1 - cy) * units
        low = cx * rest_units
        high = (1 - cx) * near_units
        a = near_units
        col = jnp.where(u < a, mine + low + u,
                        jnp.where(u < units, mine + high + (u - a),
                                  jnp.where(u < units + a, other + low + (u - units), other + high + (u - units - a))))
        return pl.multiple_of(col * LANES, LANES)

    def chunk(s, way):
        n = lax.rem(s, steps)
        row = pl.multiple_of(way * tile + lax.rem(n, 2) * part_rows, part_rows)
        return lax.div(s, steps), pl.ds(row, part_rows), pl.ds(unit_col(lax.div(n, 2)), LANES)

    def sum_copy(s, way, nxt):
        land = lax.rem(s, DEPTH)
        return send(yacc.at[chunk(s, way)], rbuf.at[way, land], rs_send.at[way, lax.rem(s, SLOTS)], rs_recv.at[way, land], tp=nxt)

    def done_copy(s, way, prv, src):
        return send(src, yd_ref.at[chunk(s, way)], ag_send.at[way, lax.rem(s, SLOTS)], ag_recv.at[way, lax.rem(s, DEPTH)], tp=prv)

    def tick(tau):
        with jax.named_scope('tick'):
            tick_body(tau)

    def tick_body(tau):
        for way in (0, 1):
            p = t if way == 0 else 3 - t
            nxt = t + 1 if way == 0 else t - 1
            prv = t - 1 if way == 0 else t + 1
            s = tau - HOP * p
            slot = lax.rem(jnp.maximum(s, 0), SLOTS)
            land = lax.rem(jnp.maximum(s, 0), DEPTH)
            live = jnp.logical_and(s >= 0, s < 2 * steps)

            @pl.when(jnp.logical_and(live, p > 0))
            def _():
                wait(rbuf.at[way, land], rs_recv.at[way, land])

            @pl.when(jnp.logical_and(live, p < 3))
            def _():
                @pl.when(s >= SLOTS)
                def _():
                    wait(rbuf.at[way, slot], rs_send.at[way, slot])

                @pl.when(p > 0)
                def _():
                    here = chunk(s, way)
                    yacc[here] = yacc[here] + rbuf[way, land]

                sum_copy(s, way, nxt).start()

            @pl.when(jnp.logical_and(live, p == 3))
            def _():
                @pl.when(s >= SLOTS)
                def _():
                    wait(fin.at[slot], ag_send.at[way, slot])
                    wait(fin.at[slot], fin_own.at[way, slot])

                here = chunk(s, way)
                fin[slot] = (yacc[here] + rbuf[way, land]).astype(BF16)
                pltpu.make_async_copy(fin.at[slot], yd_ref.at[here], fin_own.at[way, slot]).start()
                done_copy(s, way, prv, fin.at[slot]).start()

            s2 = tau - HOP * (6 - p)
            slot2 = lax.rem(jnp.maximum(s2, 0), SLOTS)
            land2 = lax.rem(jnp.maximum(s2, 0), DEPTH)
            live2 = jnp.logical_and(jnp.logical_and(s2 >= 0, s2 < 2 * steps), p < 3)

            @pl.when(live2)
            def _():
                here = yd_ref.at[chunk(s2, way)]
                wait(here, ag_recv.at[way, land2])

                @pl.when(p > 0)
                def _():
                    @pl.when(s2 >= SLOTS)
                    def _():
                        wait(fin.at[slot2], ag_send.at[way, slot2])

                    done_copy(s2, way, prv, here).start()

    def ticks(lo, hi):
        def body(n, c):
            tick(n)
            return c

        lax.fori_loop(lo, hi, body, 0)

    def drain_sums():
        def body(n, carry):
            for way in (0, 1):
                p = t if way == 0 else 3 - t
                slot = n

                @pl.when(p < 3)
                def _():
                    wait(rbuf.at[way, slot], rs_send.at[way, slot])

                @pl.when(p > 0)
                def _():
                    wait(fin.at[slot], ag_send.at[way, slot])

                @pl.when(p == 3)
                def _():
                    wait(fin.at[slot], fin_own.at[way, slot])
            return carry

        lax.fori_loop(0, SLOTS, body, 0)

    for ten in (0, 1):
        own_copy(ten).start()
    w_start(0)
    w_start(1)
    base = jnp.where(t == 0, 1.0, 0.0).astype(F32)

    with jax.named_scope('clear'):
        for r in (0, 1):
            for ten in (0, 1):
                load_a(ten, 2 + r)

        def clear(n, carry):
            at = pl.ds(pl.multiple_of(n * 32, 32), 32)
            for k in range(3):
                acc[k, at, :] = jnp.zeros((32, half), F32)
            return carry

        lax.fori_loop(0, win // 32, clear, 0)

        def clear_ab(n, carry):
            lo = pl.ds(pl.multiple_of(n * group, group), group)
            for m in range(4):
                a_all[m, lo, :] = jnp.zeros((group, half), F32)
                b_all[m, lo, :] = jnp.zeros((group, half), F32)
            return carry

        lax.fori_loop(0, tile // group, clear_ab, 0)
        for r in (0, 1):
            for ten in (0, 1):
                loaded(ten, r)

                def residual(n, carry):
                    lo = pl.ds(pl.multiple_of(n * group, group), group)
                    there = pl.ds(pl.multiple_of(r * tile + n * group, group), group)
                    yacc[ten, there, :] = tok_t[ten][r, lo, :].astype(F32) * base
                    return carry

                lax.fori_loop(0, tile // group, residual, 0)
        for ten in (0, 1):
            wait(tok_p[ten], own_recv.at[ten])

    with jax.named_scope('w_relay'):
        w_relay(0)
        w_relay(1)
    w_start(2)

    def ab_pass(last):
        row = cy if last == 0 else 1 - cy
        at_k = pl.ds(pl.multiple_of(row * line, LANES), line)
        load_a(0, 0)

        def body(n, carry):
            slot = lax.rem(n, 2)

            @pl.when(n < 3)
            def _():
                load_a(0, n + 1)

            loaded(0, slot)
            with jax.named_scope('ab_half'):
                x_half = xt[slot, :, at_k]
                a_all[n] += dot_nn(x_half, w_s[0, at_k, :])
                b_all[n] += dot_nn(x_half, w_s[1, at_k, :])

            if last:
                def hidden(m, c):
                    lo = pl.ds(pl.multiple_of(m * group, group), group)
                    a = a_all[n, lo, :]
                    h_all[n, lo, :] = (a * sigmoid(a) * b_all[n, lo, :]).astype(BF16)
                    return c

                lax.fori_loop(0, tile // group, hidden, 0)
            return carry

        lax.fori_loop(0, 4, body, 0)

    with jax.named_scope('w_have'):
        for k in (0, 1):
            w_have(k, 'chip')
            w_have(k, 'x')
    ab_pass(0)
    with jax.named_scope('w_have'):
        for k in (0, 1):
            w_have(k, 'y')
            w_have(k, 'far')
    ab_pass(1)

    def y_group(g, tau):
        u0 = (0, near_units, units, units + near_units)[g]
        n_u = (near_units, rest_units)[g % 2]
        col = unit_col(u0)
        cols = pl.ds(col, n_u * LANES)

        def theirs(r, carry):
            if g > 0:
                before = (near_units, rest_units)[(g - 1) % 2] * LANES
                wait(sb.at[r, :, pl.ds(0, before)], y_send.at[(g - 1) % 2, r])
            with jax.named_scope('y_dot'):
                sb[r, :, :n_u * LANES] = dot_nt(h_all[r], w_s[2, cols, :])
            send(sb.at[r, :, pl.ds(0, n_u * LANES)], pbuf.at[rows_of(r), cols],
                 y_send.at[g % 2, r], y_recv.at[g, r], dp=partner).start()
            return carry

        def ours(r, carry):
            with jax.named_scope('y_wait'):
                wait(pbuf.at[rows_of(r), cols], y_recv.at[g, r])
            with jax.named_scope('y_dot'):
                yacc[0, rows_of(r), cols] = (yacc[0, rows_of(r), cols] + pbuf[rows_of(r), cols]
                                             + dot_nt(h_all[2 + r], w_s[2, cols, :]))
            pl.semaphore_signal(credit, inc=1, device_id={'dp': partner, 'tp': t}, device_id_type=MESH)
            return carry

        lax.fori_loop(0, 2, theirs, 0)
        if g > 0:
            tick(tau)
        lax.fori_loop(0, 2, ours, 0)
        if g > 0:
            tick(tau + 1)

    load_a(1, 0)
    load_a(0, 0)
    with jax.named_scope('w_have2'):
        w_have(2, 'chip')
    y_group(0, 0)
    tick(0)
    with jax.named_scope('w_relay2'):
        w_relay(2)
    q_start(0)
    q_start(1)
    ticks(1, 6)
    with jax.named_scope('w_have2'):
        w_have(2, 'x')
        w_have(2, 'y')
    y_group(1, 6)
    y_group(2, 8)
    q_start(2)
    ticks(10, 14)
    with jax.named_scope('w_have2'):
        w_have(2, 'far')
    y_group(3, 14)
    q_start(3)
    tick(16)

    first = pl.multiple_of(lax.div(chip * 2 * blk, LANES) * LANES, LANES)
    shift = chip * 2 * blk - first
    at_win = pl.ds(first, win)
    n_block = 3
    n_cols = model // n_block

    def w_grad(k, core):
        return acc.at[k, pl.ds(pl.multiple_of(shift + core * blk, 8), blk), :]

    def put_grad(k):
        send(w_grad(k, 1 - j), outs[k].at[:, w_cols(j)], out_send.at[k], out_recv.at[k], dp=partner).start()
        pltpu.make_async_copy(w_grad(k, j), outs[k].at[:, w_cols(j)], out_own.at[k]).start()

    def dx_tile(n):
        r = lax.rem(n, 2)

        @pl.when(n == 0)
        def _():
            pl.semaphore_wait(credit, 8)
            for r_ in (0, 1):
                wait(sb.at[r_, :, pl.ds(0, rest_units * LANES)], y_send.at[1, r_])

        def block(m, carry):
            cols = pl.ds(pl.multiple_of(m * n_cols, n_cols), n_cols)
            slot = lax.rem(m + r * n_block, 2)

            @pl.when(jnp.logical_and(n < 2, m + r * n_block >= 2))
            def _():
                wait(sb.at[slot], dx_send.at[slot])

            @pl.when(n < 2)
            def _():
                with jax.named_scope('dx_dot'):
                    sb[slot] = dot_nt(h_all[1], w_s[0, cols, :]) + dot_nt(h_all[2], w_s[1, cols, :])
                send(sb.at[slot], pbuf.at[rows_of(r), cols], dx_send.at[slot], dx_recv.at[r, m], dp=partner).start()

            @pl.when(n >= 2)
            def _():
                with jax.named_scope('dx_wait'):
                    wait(pbuf.at[rows_of(r), cols], dx_recv.at[r, m])
                with jax.named_scope('dx_dot'):
                    yacc[1, rows_of(r), cols] = (yacc[1, rows_of(r), cols] + pbuf[rows_of(r), cols]
                                                 + (dot_nt(h_all[1], w_s[0, cols, :]) + dot_nt(h_all[2], w_s[1, cols, :])))

            @pl.when(m >= 1)
            def _():
                tick(18 + 4 * n + m)
            return carry

        lax.fori_loop(0, n_block, block, 0)

    def grad_tile(n, carry):
        q = n - 4
        slot = lax.rem(n, 2)
        at = jnp.where(n < 4, n, slot)
        final = n == 15
        early = jnp.logical_and(n >= 3, q + 1 <= EARLY)
        late = jnp.logical_and(n < 15, q + 1 > EARLY)
        few = q < SPARSE
        tau = jnp.where(n < 4, 17 + 4 * n, jnp.where(few, 33 + 4 * q, 33 + 4 * SPARSE + 6 * (q - SPARSE)))

        @pl.when(n < 4)
        def _():
            q_start(4 + n)
            loaded(0, slot)

        @pl.when(n >= 4)
        def _():
            landed(0, q)
            with jax.named_scope('a_dot'):
                a_all[at] = dot_nn(xt[slot], w_s[0])
            tick(tau)
            with jax.named_scope('b_dot'):
                b_all[at] = dot_nn(xt[slot], w_s[1])

            @pl.when(final)
            def _():
                arrive(1, q)

            tick(tau + 1)

        @pl.when(early)
        def _():
            arrive(0, q + 1)
            arrive(1, q + 1)

        @pl.when(n < 4)
        def _():
            loaded(1, slot)

        @pl.when(n >= 4)
        def _():
            landed(1, q)

        with jax.named_scope('g_dot'):
            g_s[...] = dot_nn(dyt[slot], w_s[2])

        @pl.when(q >= SPARSE)
        def _():
            tick(tau + 2)

        with jax.named_scope('act'):
            def body(m, c):
                lo = pl.ds(pl.multiple_of(m * group, group), group)
                a = a_all[at, lo, :]
                b = b_all[at, lo, :]
                g = g_s[lo, :]
                s = sigmoid(a)
                silu = a * s
                h_all[0, lo, :] = (silu * b).astype(BF16)
                h_all[1, lo, :] = (g * b * s * (1.0 + a * (1.0 - s))).astype(BF16)
                h_all[2, lo, :] = (g * silu).astype(BF16)
                return c

            lax.fori_loop(0, tile // group, body, 0)
        tick(tau + jnp.where(n < 4, 0, jnp.where(few, 2, 3)))

        @pl.when(n < 3)
        def _():
            load_a(0, n + 1)
            load_a(1, n + 1)

        @pl.when(late)
        def _():
            arrive(0, q + 1)

        with jax.named_scope('dw_dot'):
            x_win = xt[slot, :, at_win]
            acc[0] += dot_tn(x_win, h_all[1])

            @pl.when(final)
            def _():
                put_grad(0)

            acc[1] += dot_tn(x_win, h_all[2])

        @pl.when(final)
        def _():
            put_grad(1)

        @pl.when(q >= SPARSE)
        def _():
            tick(tau + 4)

        with jax.named_scope('dw_dot2'):
            acc[2] += dot_tn(dyt[slot, :, at_win], h_all[0])

        @pl.when(final)
        def _():
            put_grad(2)

        @pl.when(jnp.logical_and(n >= 2, n < 14))
        def _():
            for ten in (0, 1):
                pl.semaphore_signal(room.at[ten], inc=1, device_id={'dp': partner, 'tp': t}, device_id_type=MESH)

        tick(tau + jnp.where(n < 4, 1, jnp.where(few, 3, 5)))

        @pl.when(n < 4)
        def _():
            dx_tile(n)

        @pl.when(jnp.logical_and(late, n < 14))
        def _():
            arrive(1, q + 1)
        return carry

    lax.fori_loop(0, 16, grad_tile, 0)

    with jax.named_scope('drain_sums'):
        drain_sums()
    with jax.named_scope('drain'):
        for slot in (0, 1):
            wait(sb.at[slot], dx_send.at[slot])
        for k in range(3):
            for core in (0, 1):
                for link in (0, 1):
                    for part in (0, 1):
                        w_copy(k, link, part, core).wait_send()
                    w_relay_copy(k, link, core).wait_send()
            w_partner_copy(k).wait_send()
        for ten in (0, 1):
            own_copy(ten).wait_send()

        def drain(q, carry):
            for ten in (0, 1):
                wait(tok_b[ten].at[0], f_send.at[q, ten])
                for link in (0, 1):
                    @pl.when(q < 8)
                    def _():
                        wait(slot_of(ten, 0, link), q_send.at[lax.rem(q, 8), link, ten])

                    @pl.when(q < 4)
                    def _():
                        wait(slot_of(ten, 0, link), rl_send.at[lax.rem(q, 4), link, ten])

            return carry

        lax.fori_loop(0, 12, drain, 0)
    with jax.named_scope('drain_out'):
        for k in range(3):
            wait(w_grad(k, j), out_own.at[k])
            wait(w_grad(k, 1 - j), out_send.at[k])
            wait(w_grad(k, j), out_recv.at[k])


def window(model, blk):
    starts = [(2 * blk * c) // LANES * LANES for c in range(model // (2 * blk))]
    shift = max(2 * blk * c - s for c, s in enumerate(starts))
    return -(-(shift + 2 * blk) // LANES) * LANES


def mlp(x, dy, wg, wu, wd):
    rows, model = x.shape
    blk, width = wg.shape
    half = width // 2
    tile = rows // 2
    dma = pltpu.SemaphoreType.DMA
    vmem = pltpu.VMEM
    anywhere = pl.BlockSpec(memory_space=pl.ANY)
    shape = jax.ShapeDtypeStruct
    flops = 2 * model * half * rows * 2 * 20
    return pl.pallas_call(
        kernel,
        name='mlp',
        out_shape=(shape((2, rows, model), BF16),
                   shape((blk, width), F32), shape((blk, width), F32), shape((blk, width), F32),
                   shape((12, tile // 2, model), BF16), shape((12, tile // 2, model), BF16),
                   shape((rows, model), BF16), shape((rows, model), BF16)),
        in_specs=[anywhere] * 5,
        out_specs=tuple([anywhere] * 8),
        scratch_shapes=[
            vmem((3, model, half), BF16),
            vmem((3, window(model, blk), half), F32),
            vmem((2, rows, model), F32),
            vmem((rows, model), F32),
            vmem((2, tile, model // 3), F32),
            vmem((2, tile, model), BF16),
            vmem((2, tile, model), BF16),
            vmem((4, tile, half), F32),
            vmem((4, tile, half), F32),
            vmem((tile, half), F32),
            vmem((4, tile, half), BF16),
            vmem((2, DEPTH, tile // 2, LANES), F32),
            vmem((SLOTS, tile // 2, LANES), BF16),
            dma((3, 2, 2, 2)), dma((3, 2, 2, 2)), dma((3, 2, 2)), dma((3, 2, 2)), dma((3,)), dma((3,)), dma((3,)),
            dma((2,)), dma((2,)), dma((8, 2, 2)), dma((12, 2, 2)), dma((4, 2, 2)), dma((12, 2)), dma((12, 2)),
            dma((2, 2)), dma((4, 2)), dma((2,)), dma((2, 3)), pltpu.SemaphoreType.REGULAR, pltpu.SemaphoreType.REGULAR((2,)),
            dma((2, SLOTS)), dma((2, DEPTH)), dma((2, SLOTS)), dma((2, DEPTH)), dma((2, SLOTS)),
            dma((2, 2)), dma((3,)), dma((3,)), dma((3,)),
        ],
        compiler_params=pltpu.CompilerParams(collective_id=0, has_side_effects=True, vmem_limit_bytes=67_000_000),
        cost_estimate=pl.CostEstimate(flops=flops, bytes_accessed=100_000_000, transcendentals=0),
    )(x, dy, wg, wu, wd)


def copy_kernel(yd_ref, g_ref, u_ref, d_ref, y_out, dx_out, g_out, u_out, d_out, yd_s, g_s, u_s, d_s, load, store):
    rows = yd_ref.shape[1] // 4
    blk = g_ref.shape[0] // 4
    parts = []
    for m in range(4):
        for src, dst, buf in ((g_ref, g_out, g_s), (u_ref, u_out, u_s), (d_ref, d_out, d_s)):
            at = pl.ds(m * blk, blk)
            parts.append((src.at[at, :], buf.at[at, :], dst.at[at, :]))
        for ten, dst in ((0, y_out), (1, dx_out)):
            at = pl.ds(m * rows, rows)
            parts.append((yd_ref.at[ten, at, :], yd_s.at[ten, at, :], dst.at[at, :]))
    for n, (src, buf, dst) in enumerate(parts):
        pltpu.make_async_copy(src, buf, load.at[n]).start()
    for n, (src, buf, dst) in enumerate(parts):
        pltpu.make_async_copy(src, buf, load.at[n]).wait()
        pltpu.make_async_copy(buf, dst, store.at[n]).start()
    for n, (src, buf, dst) in enumerate(parts):
        pltpu.make_async_copy(buf, dst, store.at[n]).wait()


def copy_results(yd, dwg, dwu, dwd):
    anywhere = pl.BlockSpec(memory_space=pl.ANY)
    shape = jax.ShapeDtypeStruct
    vmem = pltpu.VMEM
    return pl.pallas_call(
        copy_kernel,
        name='results',
        out_shape=(shape(yd.shape[1:], yd.dtype), shape(yd.shape[1:], yd.dtype),
                   shape(dwg.shape, F32), shape(dwu.shape, F32), shape(dwd.shape, F32)),
        in_specs=[anywhere] * 4,
        out_specs=tuple([anywhere] * 5),
        scratch_shapes=[vmem(yd.shape, yd.dtype), vmem(dwg.shape, F32), vmem(dwu.shape, F32), vmem(dwd.shape, F32),
                        pltpu.SemaphoreType.DMA((20,)), pltpu.SemaphoreType.DMA((20,))],
        compiler_params=pltpu.CompilerParams(vmem_limit_bytes=64_000_000),
    )(yd, dwg, dwu, dwd)


def solution(mesh):
    def device_pass(x_rows, gate_blk, up_blk, down_blk, dy_rows):
        out = mlp(x_rows, dy_rows, gate_blk, up_blk, down_blk.T)
        y, dx, dw_gate, dw_up, dw_down = copy_results(*out[:4])
        return y, dx, dw_gate, dw_up, dw_down.T

    row_spec = P('dp', None)
    weight_spec = P('dp', 'tp')
    down_spec = P('tp', 'dp')
    return jax.shard_map(device_pass, mesh=mesh,
                         in_specs=(row_spec, weight_spec, weight_spec, down_spec, row_spec),
                         out_specs=(row_spec, row_spec, weight_spec, weight_spec, down_spec),
                         check_vma=False)
```

```python
import jax
import jax.numpy as jnp
from jax import lax
from jax.experimental import pallas as pl
from jax.experimental.pallas import tpu as pltpu
from jax.sharding import PartitionSpec as P

F32 = jnp.float32
BF16 = jnp.bfloat16
MESH = pl.DeviceIdType.MESH
SLOTS = 8
DEPTH = 13
HOP = 2
LANES = 128
EARLY = 6


def dot_nn(a, b):
    return jnp.dot(a, b, preferred_element_type=F32)


def dot_nt(a, b):
    return lax.dot_general(a, b, (((1,), (1,)), ((), ())), preferred_element_type=F32)


def dot_tn(a, b):
    return lax.dot_general(a, b, (((0,), (0,)), ((), ())), preferred_element_type=F32)


def sigmoid(a):
    return 1.0 / (1.0 + jnp.exp(-a))


def kernel(x_ref, dy_ref, wg_ref, wu_ref, wd_ref,
           yd_ref, og_ref, ou_ref, od_ref, xb, dyb, xp, dyp,
           w_s, acc, yacc, pbuf, sb, xt, dyt, a_all, b_all, g_s, h_all, rbuf, fin,
           w_send, w_recv, wr_send, wr_recv, w_own, wp_send, wp_recv,
           own_send, own_recv, q_send, q_recv, rl_send, f_send, f_recv,
           y_send, y_recv, dx_send, dx_recv, credit, room,
           rs_send, rs_recv, ag_send, ag_recv, fin_own, ld, out_send, out_recv, out_own):
    rows, model = x_ref.shape
    blk, width = wg_ref.shape
    half = width // 2
    hb = blk // 2
    tile = rows // 2
    piece = tile // 4
    win = acc.shape[1]
    line = model // 2
    units = line // LANES
    near_units = (2 * blk - LANES // 2) // LANES if (2 * blk) % LANES else 2 * blk // LANES
    rest_units = units - near_units
    steps = 4 * units
    part_rows = tile // 2
    group = min(32, tile)
    w_in = (wg_ref, wu_ref, wd_ref)
    outs = (og_ref, ou_ref, od_ref)
    tok = (x_ref, dy_ref)
    tok_b = (xb, dyb)
    tok_p = (xp, dyp)
    tok_t = (xt, dyt)

    t = lax.axis_index('tp')
    me = lax.axis_index('dp')
    cy = lax.div(me, 4)
    cx = lax.rem(lax.div(me, 2), 2)
    j = lax.rem(me, 2)
    partner = me + 1 - 2 * j
    chip = cy * 2 + cx

    def near(link, core):
        if link == 0:
            return cy * 4 + (1 - cx) * 2 + core
        return (1 - cy) * 4 + cx * 2 + core

    def far(core):
        return (1 - cy) * 4 + (1 - cx) * 2 + core

    def send(src, dst, s_sem, r_sem, dp=None, tp=None):
        where = {'dp': me if dp is None else dp, 'tp': t if tp is None else tp}
        return pltpu.make_async_remote_copy(src_ref=src, dst_ref=dst, send_sem=s_sem, recv_sem=r_sem,
                                            device_id=where, device_id_type=MESH)

    def wait(ref, sem):
        pltpu.make_async_copy(ref, ref, sem).wait()

    barrier = pltpu.get_barrier_semaphore()
    for peer in (partner, near(0, 0), near(0, 1), near(1, 0), near(1, 1)):
        pl.semaphore_signal(barrier, inc=1, device_id={'dp': peer, 'tp': t}, device_id_type=MESH)

    @pl.when(t > 0)
    def _():
        pl.semaphore_signal(barrier, inc=1, device_id={'dp': me, 'tp': t - 1}, device_id_type=MESH)

    @pl.when(t < 3)
    def _():
        pl.semaphore_signal(barrier, inc=1, device_id={'dp': me, 'tp': t + 1}, device_id_type=MESH)

    pl.semaphore_wait(barrier, 5 + jnp.minimum(t, 1) + jnp.minimum(3 - t, 1))

    def w_rows(k, dev, part=None):
        if part is None:
            return w_s.at[k, pl.ds(pl.multiple_of(dev * blk, 16), blk), :]
        return w_s.at[k, pl.ds(pl.multiple_of(dev * blk + part * hb, 16), hb), :]

    def w_cols(core):
        return pl.ds(pl.multiple_of(core * half, LANES), half)

    def w_copy(k, link, part, core):
        return send(w_in[k].at[pl.ds(part * hb, hb), w_cols(core)], w_rows(k, me, part),
                    w_send.at[k, link, part, core], w_recv.at[k, link, part, j], dp=near(link, core))

    def w_own_copy(k):
        return pltpu.make_async_copy(w_in[k].at[:, w_cols(j)], w_rows(k, me), w_own.at[k])

    def w_partner_copy(k):
        return send(w_in[k].at[:, w_cols(1 - j)], w_rows(k, me), wp_send.at[k], wp_recv.at[k], dp=partner)

    def w_start(k):
        for first in (0, 1):
            for core in (0, 1):
                w_copy(k, 0, 1 - first, core).start()
                w_copy(k, 1, first, core).start()
        w_own_copy(k).start()
        w_partner_copy(k).start()

    def w_relay_copy(k, link_out, core):
        part = 1 if link_out == 1 else 0
        ref = w_rows(k, near(1 - link_out, core), part)
        return send(ref, ref, wr_send.at[k, link_out, core], wr_recv.at[k, link_out, core], dp=near(link_out, j))

    def w_relay(k):
        for core in (0, 1):
            wait(w_rows(k, near(0, core), 1), w_recv.at[k, 0, 1, core])
            w_relay_copy(k, 1, core).start()
            wait(w_rows(k, near(1, core), 0), w_recv.at[k, 1, 0, core])
            w_relay_copy(k, 0, core).start()

    def w_have(k, which):
        if which == 'chip':
            wait(w_rows(k, me), w_own.at[k])
            wait(w_rows(k, partner), wp_recv.at[k])
        for core in (0, 1):
            if which == 'x':
                wait(w_rows(k, near(0, core), 0), w_recv.at[k, 0, 0, core])
            if which == 'y':
                wait(w_rows(k, near(1, core), 1), w_recv.at[k, 1, 1, core])
            if which == 'far':
                wait(w_rows(k, far(core), 0), wr_recv.at[k, 0, core])
                wait(w_rows(k, far(core), 1), wr_recv.at[k, 1, core])

    def slot_of(ten, q, link):
        return tok_b[ten].at[q, pl.ds(link * piece, piece), :]

    def q_copy(ten, q, link):
        b = lax.div(q, 4)
        sub = lax.rem(q, 4)
        first = 1 - b if link == 0 else b
        src = tok[ten].at[pl.ds(pl.multiple_of(first * tile + sub * piece, piece), piece), :]
        return send(src, slot_of(ten, q, link), q_send.at[q, link, ten], q_recv.at[q, link, ten], dp=near(link, j))

    def q_start(q):
        for ten in (0, 1):
            for link in (0, 1):
                q_copy(ten, q, link).start()

    def relay_copy(ten, sub, link_out):
        return send(slot_of(ten, sub, 1 - link_out), slot_of(ten, 8 + sub, link_out),
                    rl_send.at[sub, link_out, ten], q_recv.at[8 + sub, link_out, ten], dp=near(link_out, j))

    def tile_part(ten, q, core):
        return tok_t[ten].at[lax.rem(q, 2), pl.ds(pl.multiple_of(core * 2 * piece, 2 * piece), 2 * piece), :]

    def forward_copy(ten, q):
        return send(tok_b[ten].at[q], tile_part(ten, q, j), f_send.at[q, ten], f_recv.at[q, ten], dp=partner)

    def own_copy(ten):
        return send(tok[ten], tok_p[ten], own_send.at[ten], own_recv.at[ten], dp=partner)

    def arrive(ten, q):
        with jax.named_scope('arrive'):
            for link in (0, 1):
                wait(slot_of(ten, q, link), q_recv.at[q, link, ten])
            pl.semaphore_wait(room.at[ten], 1)
            forward_copy(ten, q).start()
            pltpu.make_async_copy(tok_b[ten].at[q], tile_part(ten, q, j), ld.at[ten, lax.rem(q, 2)]).start()

        @pl.when(q < 4)
        def _():
            for link in (0, 1):
                relay_copy(ten, q, link).start()

    def landed(ten, q):
        with jax.named_scope('landed'):
            wait(tile_part(ten, q, j), ld.at[ten, lax.rem(q, 2)])
            wait(tile_part(ten, q, 1 - j), f_recv.at[q, ten])

    def rows_of(r):
        return pl.ds(pl.multiple_of(r * tile, tile), tile)

    def load_a(ten, n):
        own = lax.div(n, 2)
        slot = lax.rem(n, 2)

        @pl.when(own == 1)
        def _():
            pltpu.make_async_copy(tok[ten].at[rows_of(slot), :], tok_t[ten].at[slot], ld.at[ten, slot]).start()

        @pl.when(own == 0)
        def _():
            pltpu.make_async_copy(tok_p[ten].at[rows_of(slot), :], tok_t[ten].at[slot], ld.at[ten, slot]).start()

    def loaded(ten, slot):
        with jax.named_scope('ld'):
            wait(tok_t[ten].at[slot], ld.at[ten, slot])

    def unit_col(u):
        mine = cy * units
        other = (1 - cy) * units
        low = cx * rest_units
        high = (1 - cx) * near_units
        a = near_units
        col = jnp.where(u < a, mine + low + u,
                        jnp.where(u < units, mine + high + (u - a),
                                  jnp.where(u < units + a, other + low + (u - units), other + high + (u - units - a))))
        return pl.multiple_of(col * LANES, LANES)

    def chunk(s, way):
        n = lax.rem(s, steps)
        row = pl.multiple_of(way * tile + lax.rem(n, 2) * part_rows, part_rows)
        return lax.div(s, steps), pl.ds(row, part_rows), pl.ds(unit_col(lax.div(n, 2)), LANES)

    def sum_copy(s, way, nxt):
        land = lax.rem(s, DEPTH)
        return send(yacc.at[chunk(s, way)], rbuf.at[way, land], rs_send.at[way, lax.rem(s, SLOTS)], rs_recv.at[way, land], tp=nxt)

    def done_copy(s, way, prv, src):
        return send(src, yd_ref.at[chunk(s, way)], ag_send.at[way, lax.rem(s, SLOTS)], ag_recv.at[way, lax.rem(s, DEPTH)], tp=prv)

    def tick(tau):
        with jax.named_scope('tick'):
            tick_body(tau)

    def tick_body(tau):
        for way in (0, 1):
            p = t if way == 0 else 3 - t
            nxt = t + 1 if way == 0 else t - 1
            prv = t - 1 if way == 0 else t + 1
            s = tau - HOP * p
            slot = lax.rem(jnp.maximum(s, 0), SLOTS)
            land = lax.rem(jnp.maximum(s, 0), DEPTH)
            live = jnp.logical_and(s >= 0, s < 2 * steps)

            @pl.when(jnp.logical_and(live, p > 0))
            def _():
                wait(rbuf.at[way, land], rs_recv.at[way, land])

            @pl.when(jnp.logical_and(live, p < 3))
            def _():
                @pl.when(s >= SLOTS)
                def _():
                    wait(rbuf.at[way, slot], rs_send.at[way, slot])

                @pl.when(p > 0)
                def _():
                    here = chunk(s, way)
                    yacc[here] = yacc[here] + rbuf[way, land]

                sum_copy(s, way, nxt).start()

            @pl.when(jnp.logical_and(live, p == 3))
            def _():
                @pl.when(s >= SLOTS)
                def _():
                    wait(fin.at[slot], ag_send.at[way, slot])
                    wait(fin.at[slot], fin_own.at[way, slot])

                here = chunk(s, way)
                fin[slot] = (yacc[here] + rbuf[way, land]).astype(BF16)
                pltpu.make_async_copy(fin.at[slot], yd_ref.at[here], fin_own.at[way, slot]).start()
                done_copy(s, way, prv, fin.at[slot]).start()

            s2 = tau - HOP * (6 - p)
            slot2 = lax.rem(jnp.maximum(s2, 0), SLOTS)
            land2 = lax.rem(jnp.maximum(s2, 0), DEPTH)
            live2 = jnp.logical_and(jnp.logical_and(s2 >= 0, s2 < 2 * steps), p < 3)

            @pl.when(live2)
            def _():
                here = yd_ref.at[chunk(s2, way)]
                wait(here, ag_recv.at[way, land2])

                @pl.when(p > 0)
                def _():
                    @pl.when(s2 >= SLOTS)
                    def _():
                        wait(fin.at[slot2], ag_send.at[way, slot2])

                    done_copy(s2, way, prv, here).start()

    def ticks(lo, hi):
        def body(n, c):
            tick(n)
            return c

        lax.fori_loop(lo, hi, body, 0)

    def drain_sums():
        def body(n, carry):
            for way in (0, 1):
                p = t if way == 0 else 3 - t
                slot = n

                @pl.when(p < 3)
                def _():
                    wait(rbuf.at[way, slot], rs_send.at[way, slot])

                @pl.when(p > 0)
                def _():
                    wait(fin.at[slot], ag_send.at[way, slot])

                @pl.when(p == 3)
                def _():
                    wait(fin.at[slot], fin_own.at[way, slot])
            return carry

        lax.fori_loop(0, SLOTS, body, 0)

    for ten in (0, 1):
        own_copy(ten).start()
    w_start(0)
    w_start(1)
    base = jnp.where(t == 0, 1.0, 0.0).astype(F32)

    with jax.named_scope('clear'):
        for r in (0, 1):
            for ten in (0, 1):
                load_a(ten, 2 + r)

        def clear(n, carry):
            at = pl.ds(pl.multiple_of(n * 32, 32), 32)
            for k in range(3):
                acc[k, at, :] = jnp.zeros((32, half), F32)
            return carry

        lax.fori_loop(0, win // 32, clear, 0)

        def clear_ab(n, carry):
            lo = pl.ds(pl.multiple_of(n * group, group), group)
            for m in range(4):
                a_all[m, lo, :] = jnp.zeros((group, half), F32)
                b_all[m, lo, :] = jnp.zeros((group, half), F32)
            return carry

        lax.fori_loop(0, tile // group, clear_ab, 0)
        for r in (0, 1):
            for ten in (0, 1):
                loaded(ten, r)

                def residual(n, carry):
                    lo = pl.ds(pl.multiple_of(n * group, group), group)
                    there = pl.ds(pl.multiple_of(r * tile + n * group, group), group)
                    yacc[ten, there, :] = tok_t[ten][r, lo, :].astype(F32) * base
                    return carry

                lax.fori_loop(0, tile // group, residual, 0)
        for ten in (0, 1):
            wait(tok_p[ten], own_recv.at[ten])

    with jax.named_scope('w_relay'):
        w_relay(0)
        w_relay(1)
    w_start(2)

    def ab_pass(last):
        row = cy if last == 0 else 1 - cy
        at_k = pl.ds(pl.multiple_of(row * line, LANES), line)
        load_a(0, 0)

        def body(n, carry):
            slot = lax.rem(n, 2)

            @pl.when(n < 3)
            def _():
                load_a(0, n + 1)

            loaded(0, slot)
            with jax.named_scope('ab_half'):
                x_half = xt[slot, :, at_k]
                a_all[n] += dot_nn(x_half, w_s[0, at_k, :])
                b_all[n] += dot_nn(x_half, w_s[1, at_k, :])

            if last:
                def hidden(m, c):
                    lo = pl.ds(pl.multiple_of(m * group, group), group)
                    a = a_all[n, lo, :]
                    h_all[n, lo, :] = (a * sigmoid(a) * b_all[n, lo, :]).astype(BF16)
                    return c

                lax.fori_loop(0, tile // group, hidden, 0)
            return carry

        lax.fori_loop(0, 4, body, 0)

    with jax.named_scope('w_have'):
        for k in (0, 1):
            w_have(k, 'chip')
            w_have(k, 'x')
    ab_pass(0)
    with jax.named_scope('w_have'):
        for k in (0, 1):
            w_have(k, 'y')
            w_have(k, 'far')
    ab_pass(1)

    def y_group(g, tau):
        u0 = (0, near_units, units, units + near_units)[g]
        n_u = (near_units, rest_units)[g % 2]
        col = unit_col(u0)
        cols = pl.ds(col, n_u * LANES)

        def theirs(r, carry):
            if g > 0:
                before = (near_units, rest_units)[(g - 1) % 2] * LANES
                wait(sb.at[r, :, pl.ds(0, before)], y_send.at[(g - 1) % 2, r])
            with jax.named_scope('y_dot'):
                sb[r, :, :n_u * LANES] = dot_nt(h_all[r], w_s[2, cols, :])
            send(sb.at[r, :, pl.ds(0, n_u * LANES)], pbuf.at[rows_of(r), cols],
                 y_send.at[g % 2, r], y_recv.at[g, r], dp=partner).start()
            return carry

        def ours(r, carry):
            with jax.named_scope('y_wait'):
                wait(pbuf.at[rows_of(r), cols], y_recv.at[g, r])
            with jax.named_scope('y_dot'):
                yacc[0, rows_of(r), cols] = (yacc[0, rows_of(r), cols] + pbuf[rows_of(r), cols]
                                             + dot_nt(h_all[2 + r], w_s[2, cols, :]))
            pl.semaphore_signal(credit, inc=1, device_id={'dp': partner, 'tp': t}, device_id_type=MESH)
            return carry

        lax.fori_loop(0, 2, theirs, 0)
        if g > 0:
            tick(tau)
        lax.fori_loop(0, 2, ours, 0)
        if g > 0:
            tick(tau + 1)

    load_a(1, 0)
    load_a(0, 0)
    with jax.named_scope('w_have2'):
        w_have(2, 'chip')
    y_group(0, 0)
    tick(0)
    with jax.named_scope('w_relay2'):
        w_relay(2)
    q_start(0)
    q_start(1)
    ticks(1, 7)
    with jax.named_scope('w_have2'):
        w_have(2, 'x')
        w_have(2, 'y')
    y_group(1, 7)
    y_group(2, 9)
    q_start(2)
    ticks(11, 16)
    with jax.named_scope('w_have2'):
        w_have(2, 'far')
    y_group(3, 16)
    q_start(3)
    tick(18)

    first = pl.multiple_of(lax.div(chip * 2 * blk, LANES) * LANES, LANES)
    shift = chip * 2 * blk - first
    at_win = pl.ds(first, win)
    n_block = 3
    n_cols = model // n_block

    def w_grad(k, core):
        return acc.at[k, pl.ds(pl.multiple_of(shift + core * blk, 8), blk), :]

    def put_grad(k):
        send(w_grad(k, 1 - j), outs[k].at[:, w_cols(j)], out_send.at[k], out_recv.at[k], dp=partner).start()
        pltpu.make_async_copy(w_grad(k, j), outs[k].at[:, w_cols(j)], out_own.at[k]).start()

    def dx_tile(n):
        r = lax.rem(n, 2)

        @pl.when(n == 0)
        def _():
            pl.semaphore_wait(credit, 8)
            for r_ in (0, 1):
                wait(sb.at[r_, :, pl.ds(0, rest_units * LANES)], y_send.at[1, r_])

        def block(m, carry):
            cols = pl.ds(pl.multiple_of(m * n_cols, n_cols), n_cols)
            slot = lax.rem(m + r * n_block, 2)

            @pl.when(jnp.logical_and(n < 2, m + r * n_block >= 2))
            def _():
                wait(sb.at[slot], dx_send.at[slot])

            @pl.when(n < 2)
            def _():
                with jax.named_scope('dx_dot'):
                    sb[slot] = dot_nt(h_all[1], w_s[0, cols, :]) + dot_nt(h_all[2], w_s[1, cols, :])
                send(sb.at[slot], pbuf.at[rows_of(r), cols], dx_send.at[slot], dx_recv.at[r, m], dp=partner).start()

            @pl.when(n >= 2)
            def _():
                with jax.named_scope('dx_wait'):
                    wait(pbuf.at[rows_of(r), cols], dx_recv.at[r, m])
                with jax.named_scope('dx_dot'):
                    yacc[1, rows_of(r), cols] = (yacc[1, rows_of(r), cols] + pbuf[rows_of(r), cols]
                                                 + (dot_nt(h_all[1], w_s[0, cols, :]) + dot_nt(h_all[2], w_s[1, cols, :])))

            @pl.when(m >= 1)
            def _():
                tick(20 + 4 * n + m)
            return carry

        lax.fori_loop(0, n_block, block, 0)

    def grad_tile(n, carry):
        q = n - 4
        slot = lax.rem(n, 2)
        at = jnp.where(n < 4, n, slot)
        final = n == 15
        early = jnp.logical_and(n >= 3, q + 1 <= EARLY)
        late = jnp.logical_and(n < 15, q + 1 > EARLY)
        tau = 19 + 4 * n

        @pl.when(n < 4)
        def _():
            q_start(4 + n)
            loaded(0, slot)

        @pl.when(n >= 4)
        def _():
            landed(0, q)
            with jax.named_scope('a_dot'):
                a_all[at] = dot_nn(xt[slot], w_s[0])
            tick(tau)
            with jax.named_scope('b_dot'):
                b_all[at] = dot_nn(xt[slot], w_s[1])

            @pl.when(final)
            def _():
                arrive(1, q)

            tick(tau + 1)

        @pl.when(early)
        def _():
            arrive(0, q + 1)
            arrive(1, q + 1)

        @pl.when(n < 4)
        def _():
            loaded(1, slot)

        @pl.when(n >= 4)
        def _():
            landed(1, q)

        with jax.named_scope('g_dot'):
            g_s[...] = dot_nn(dyt[slot], w_s[2])

        with jax.named_scope('act'):
            def body(m, c):
                lo = pl.ds(pl.multiple_of(m * group, group), group)
                a = a_all[at, lo, :]
                b = b_all[at, lo, :]
                g = g_s[lo, :]
                s = sigmoid(a)
                silu = a * s
                h_all[0, lo, :] = (silu * b).astype(BF16)
                h_all[1, lo, :] = (g * b * s * (1.0 + a * (1.0 - s))).astype(BF16)
                h_all[2, lo, :] = (g * silu).astype(BF16)
                return c

            lax.fori_loop(0, tile // group, body, 0)
        tick(tau + jnp.where(n < 4, 0, 2))

        @pl.when(n < 3)
        def _():
            load_a(0, n + 1)
            load_a(1, n + 1)

        @pl.when(late)
        def _():
            arrive(0, q + 1)

        with jax.named_scope('dw_dot'):
            x_win = xt[slot, :, at_win]
            acc[0] += dot_tn(x_win, h_all[1])

            @pl.when(final)
            def _():
                put_grad(0)

            acc[1] += dot_tn(x_win, h_all[2])

        @pl.when(final)
        def _():
            put_grad(1)

        with jax.named_scope('dw_dot2'):
            acc[2] += dot_tn(dyt[slot, :, at_win], h_all[0])

        @pl.when(final)
        def _():
            put_grad(2)

        @pl.when(jnp.logical_and(n >= 2, n < 14))
        def _():
            for ten in (0, 1):
                pl.semaphore_signal(room.at[ten], inc=1, device_id={'dp': partner, 'tp': t}, device_id_type=MESH)

        tick(tau + jnp.where(n < 4, 1, 3))

        @pl.when(n < 4)
        def _():
            dx_tile(n)

        @pl.when(jnp.logical_and(late, n < 14))
        def _():
            arrive(1, q + 1)
        return carry

    lax.fori_loop(0, 16, grad_tile, 0)
    tick(83)

    with jax.named_scope('drain_sums'):
        drain_sums()
    with jax.named_scope('drain'):
        for slot in (0, 1):
            wait(sb.at[slot], dx_send.at[slot])
        for k in range(3):
            for core in (0, 1):
                for link in (0, 1):
                    for part in (0, 1):
                        w_copy(k, link, part, core).wait_send()
                    w_relay_copy(k, link, core).wait_send()
            w_partner_copy(k).wait_send()
        for ten in (0, 1):
            own_copy(ten).wait_send()

        def drain(q, carry):
            for ten in (0, 1):
                wait(tok_b[ten].at[0], f_send.at[q, ten])
                for link in (0, 1):
                    @pl.when(q < 8)
                    def _():
                        wait(slot_of(ten, 0, link), q_send.at[lax.rem(q, 8), link, ten])

                    @pl.when(q < 4)
                    def _():
                        wait(slot_of(ten, 0, link), rl_send.at[lax.rem(q, 4), link, ten])

            return carry

        lax.fori_loop(0, 12, drain, 0)
    with jax.named_scope('drain_out'):
        for k in range(3):
            wait(w_grad(k, j), out_own.at[k])
            wait(w_grad(k, 1 - j), out_send.at[k])
            wait(w_grad(k, j), out_recv.at[k])


def window(model, blk):
    starts = [(2 * blk * c) // LANES * LANES for c in range(model // (2 * blk))]
    shift = max(2 * blk * c - s for c, s in enumerate(starts))
    return -(-(shift + 2 * blk) // LANES) * LANES


def mlp(x, dy, wg, wu, wd):
    rows, model = x.shape
    blk, width = wg.shape
    half = width // 2
    tile = rows // 2
    dma = pltpu.SemaphoreType.DMA
    vmem = pltpu.VMEM
    anywhere = pl.BlockSpec(memory_space=pl.ANY)
    shape = jax.ShapeDtypeStruct
    flops = 2 * model * half * rows * 2 * 20
    return pl.pallas_call(
        kernel,
        name='mlp',
        out_shape=(shape((2, rows, model), BF16),
                   shape((blk, width), F32), shape((blk, width), F32), shape((blk, width), F32),
                   shape((12, tile // 2, model), BF16), shape((12, tile // 2, model), BF16),
                   shape((rows, model), BF16), shape((rows, model), BF16)),
        in_specs=[anywhere] * 5,
        out_specs=tuple([anywhere] * 8),
        scratch_shapes=[
            vmem((3, model, half), BF16),
            vmem((3, window(model, blk), half), F32),
            vmem((2, rows, model), F32),
            vmem((rows, model), F32),
            vmem((2, tile, model // 3), F32),
            vmem((2, tile, model), BF16),
            vmem((2, tile, model), BF16),
            vmem((4, tile, half), F32),
            vmem((4, tile, half), F32),
            vmem((tile, half), F32),
            vmem((4, tile, half), BF16),
            vmem((2, DEPTH, tile // 2, LANES), F32),
            vmem((SLOTS, tile // 2, LANES), BF16),
            dma((3, 2, 2, 2)), dma((3, 2, 2, 2)), dma((3, 2, 2)), dma((3, 2, 2)), dma((3,)), dma((3,)), dma((3,)),
            dma((2,)), dma((2,)), dma((8, 2, 2)), dma((12, 2, 2)), dma((4, 2, 2)), dma((12, 2)), dma((12, 2)),
            dma((2, 2)), dma((4, 2)), dma((2,)), dma((2, 3)), pltpu.SemaphoreType.REGULAR, pltpu.SemaphoreType.REGULAR((2,)),
            dma((2, SLOTS)), dma((2, DEPTH)), dma((2, SLOTS)), dma((2, DEPTH)), dma((2, SLOTS)),
            dma((2, 2)), dma((3,)), dma((3,)), dma((3,)),
        ],
        compiler_params=pltpu.CompilerParams(collective_id=0, has_side_effects=True, vmem_limit_bytes=67_000_000),
        cost_estimate=pl.CostEstimate(flops=flops, bytes_accessed=100_000_000, transcendentals=0),
    )(x, dy, wg, wu, wd)


def copy_kernel(yd_ref, g_ref, u_ref, d_ref, y_out, dx_out, g_out, u_out, d_out, yd_s, g_s, u_s, d_s, load, store):
    rows = yd_ref.shape[1] // 4
    blk = g_ref.shape[0] // 4
    parts = []
    for m in range(4):
        for src, dst, buf in ((g_ref, g_out, g_s), (u_ref, u_out, u_s), (d_ref, d_out, d_s)):
            at = pl.ds(m * blk, blk)
            parts.append((src.at[at, :], buf.at[at, :], dst.at[at, :]))
        for ten, dst in ((0, y_out), (1, dx_out)):
            at = pl.ds(m * rows, rows)
            parts.append((yd_ref.at[ten, at, :], yd_s.at[ten, at, :], dst.at[at, :]))
    for n, (src, buf, dst) in enumerate(parts):
        pltpu.make_async_copy(src, buf, load.at[n]).start()
    for n, (src, buf, dst) in enumerate(parts):
        pltpu.make_async_copy(src, buf, load.at[n]).wait()
        pltpu.make_async_copy(buf, dst, store.at[n]).start()
    for n, (src, buf, dst) in enumerate(parts):
        pltpu.make_async_copy(buf, dst, store.at[n]).wait()


def copy_results(yd, dwg, dwu, dwd):
    anywhere = pl.BlockSpec(memory_space=pl.ANY)
    shape = jax.ShapeDtypeStruct
    vmem = pltpu.VMEM
    return pl.pallas_call(
        copy_kernel,
        name='results',
        out_shape=(shape(yd.shape[1:], yd.dtype), shape(yd.shape[1:], yd.dtype),
                   shape(dwg.shape, F32), shape(dwu.shape, F32), shape(dwd.shape, F32)),
        in_specs=[anywhere] * 4,
        out_specs=tuple([anywhere] * 5),
        scratch_shapes=[vmem(yd.shape, yd.dtype), vmem(dwg.shape, F32), vmem(dwu.shape, F32), vmem(dwd.shape, F32),
                        pltpu.SemaphoreType.DMA((20,)), pltpu.SemaphoreType.DMA((20,))],
        compiler_params=pltpu.CompilerParams(vmem_limit_bytes=64_000_000),
    )(yd, dwg, dwu, dwd)


def solution(mesh):
    def device_pass(x_rows, gate_blk, up_blk, down_blk, dy_rows):
        out = mlp(x_rows, dy_rows, gate_blk, up_blk, down_blk.T)
        y, dx, dw_gate, dw_up, dw_down = copy_results(*out[:4])
        return y, dx, dw_gate, dw_up, dw_down.T

    row_spec = P('dp', None)
    weight_spec = P('dp', 'tp')
    down_spec = P('tp', 'dp')
    return jax.shard_map(device_pass, mesh=mesh,
                         in_specs=(row_spec, weight_spec, weight_spec, down_spec, row_spec),
                         out_specs=(row_spec, row_spec, weight_spec, weight_spec, down_spec),
                         check_vma=False)
```

```python
import jax
import jax.numpy as jnp
from jax import lax
from jax.experimental import pallas as pl
from jax.experimental.pallas import tpu as pltpu
from jax.sharding import PartitionSpec as P

F32 = jnp.float32
BF16 = jnp.bfloat16
MESH = pl.DeviceIdType.MESH
SLOTS = 8
DEPTH = 13
HOP = 2
LANES = 128
EARLY = 4


def dot_nn(a, b):
    return jnp.dot(a, b, preferred_element_type=F32)


def dot_nt(a, b):
    return lax.dot_general(a, b, (((1,), (1,)), ((), ())), preferred_element_type=F32)


def dot_tn(a, b):
    return lax.dot_general(a, b, (((0,), (0,)), ((), ())), preferred_element_type=F32)


def sigmoid(a):
    return 1.0 / (1.0 + jnp.exp(-a))


def kernel(x_ref, dy_ref, wg_ref, wu_ref, wd_ref,
           yd_ref, og_ref, ou_ref, od_ref, xb, dyb, xp, dyp,
           w_gu, w_d, acc_gu, acc_d, yacc, pbuf, sb, xt, dyt, ab_all, g_s, h_all, rbuf, fin,
           w_send, w_recv, wr_send, wr_recv, w_own, wp_send, wp_recv,
           own_send, own_recv, q_send, q_recv, rl_send, f_send, f_recv,
           y_send, y_recv, dx_send, dx_recv, credit, room,
           rs_send, rs_recv, ag_send, ag_recv, fin_own, ld, out_send, out_recv, out_own):
    rows, model = x_ref.shape
    blk, width = wg_ref.shape
    half = width // 2
    hb = blk // 2
    tile = rows // 2
    piece = tile // 4
    win = acc_d.shape[0]
    line = model // 2
    units = line // LANES
    near_units = (2 * blk - LANES // 2) // LANES if (2 * blk) % LANES else 2 * blk // LANES
    rest_units = units - near_units
    steps = 4 * units
    part_rows = tile // 2
    group = min(32, tile)
    w_in = (wg_ref, wu_ref, wd_ref)
    outs = (og_ref, ou_ref, od_ref)
    tok = (x_ref, dy_ref)
    tok_b = (xb, dyb)
    tok_p = (xp, dyp)
    tok_t = (xt, dyt)

    t = lax.axis_index('tp')
    me = lax.axis_index('dp')
    cy = lax.div(me, 4)
    cx = lax.rem(lax.div(me, 2), 2)
    j = lax.rem(me, 2)
    partner = me + 1 - 2 * j
    chip = cy * 2 + cx

    def near(link, core):
        if link == 0:
            return cy * 4 + (1 - cx) * 2 + core
        return (1 - cy) * 4 + cx * 2 + core

    def far(core):
        return (1 - cy) * 4 + (1 - cx) * 2 + core

    def send(src, dst, s_sem, r_sem, dp=None, tp=None):
        where = {'dp': me if dp is None else dp, 'tp': t if tp is None else tp}
        return pltpu.make_async_remote_copy(src_ref=src, dst_ref=dst, send_sem=s_sem, recv_sem=r_sem,
                                            device_id=where, device_id_type=MESH)

    def wait(ref, sem):
        pltpu.make_async_copy(ref, ref, sem).wait()

    barrier = pltpu.get_barrier_semaphore()
    for peer in (partner, near(0, 0), near(0, 1), near(1, 0), near(1, 1)):
        pl.semaphore_signal(barrier, inc=1, device_id={'dp': peer, 'tp': t}, device_id_type=MESH)

    @pl.when(t > 0)
    def _():
        pl.semaphore_signal(barrier, inc=1, device_id={'dp': me, 'tp': t - 1}, device_id_type=MESH)

    @pl.when(t < 3)
    def _():
        pl.semaphore_signal(barrier, inc=1, device_id={'dp': me, 'tp': t + 1}, device_id_type=MESH)

    pl.semaphore_wait(barrier, 5 + jnp.minimum(t, 1) + jnp.minimum(3 - t, 1))

    def w_rows(k, dev, part=None):
        if part is None:
            at = pl.ds(pl.multiple_of(dev * blk, 16), blk)
        else:
            at = pl.ds(pl.multiple_of(dev * blk + part * hb, 16), hb)
        if k == 2:
            return w_d.at[at, :]
        return w_gu.at[at, pl.ds(k * half, half)]

    def w_cols(core):
        return pl.ds(pl.multiple_of(core * half, LANES), half)

    def w_copy(k, link, part, core):
        return send(w_in[k].at[pl.ds(part * hb, hb), w_cols(core)], w_rows(k, me, part),
                    w_send.at[k, link, part, core], w_recv.at[k, link, part, j], dp=near(link, core))

    def w_own_copy(k):
        return pltpu.make_async_copy(w_in[k].at[:, w_cols(j)], w_rows(k, me), w_own.at[k])

    def w_partner_copy(k):
        return send(w_in[k].at[:, w_cols(1 - j)], w_rows(k, me), wp_send.at[k], wp_recv.at[k], dp=partner)

    def w_start(k):
        for first in (0, 1):
            for core in (0, 1):
                w_copy(k, 0, 1 - first, core).start()
                w_copy(k, 1, first, core).start()
        w_own_copy(k).start()
        w_partner_copy(k).start()

    def w_relay_copy(k, link_out, core):
        part = 1 if link_out == 1 else 0
        ref = w_rows(k, near(1 - link_out, core), part)
        return send(ref, ref, wr_send.at[k, link_out, core], wr_recv.at[k, link_out, core], dp=near(link_out, j))

    def w_relay(k):
        for core in (0, 1):
            wait(w_rows(k, near(0, core), 1), w_recv.at[k, 0, 1, core])
            w_relay_copy(k, 1, core).start()
            wait(w_rows(k, near(1, core), 0), w_recv.at[k, 1, 0, core])
            w_relay_copy(k, 0, core).start()

    def w_have(k, which):
        if which == 'chip':
            wait(w_rows(k, me), w_own.at[k])
            wait(w_rows(k, partner), wp_recv.at[k])
        for core in (0, 1):
            if which == 'x':
                wait(w_rows(k, near(0, core), 0), w_recv.at[k, 0, 0, core])
            if which == 'y':
                wait(w_rows(k, near(1, core), 1), w_recv.at[k, 1, 1, core])
            if which == 'far':
                wait(w_rows(k, far(core), 0), wr_recv.at[k, 0, core])
                wait(w_rows(k, far(core), 1), wr_recv.at[k, 1, core])

    def slot_of(ten, q, link):
        return tok_b[ten].at[q, pl.ds(link * piece, piece), :]

    def q_copy(ten, q, link):
        b = lax.div(q, 4)
        sub = lax.rem(q, 4)
        first = 1 - b if link == 0 else b
        src = tok[ten].at[pl.ds(pl.multiple_of(first * tile + sub * piece, piece), piece), :]
        return send(src, slot_of(ten, q, link), q_send.at[q, link, ten], q_recv.at[q, link, ten], dp=near(link, j))

    def q_start(q):
        for ten in (0, 1):
            for link in (0, 1):
                q_copy(ten, q, link).start()

    def relay_copy(ten, sub, link_out):
        return send(slot_of(ten, sub, 1 - link_out), slot_of(ten, 8 + sub, link_out),
                    rl_send.at[sub, link_out, ten], q_recv.at[8 + sub, link_out, ten], dp=near(link_out, j))

    def tile_part(ten, q, core):
        return tok_t[ten].at[lax.rem(q, 2), pl.ds(pl.multiple_of(core * 2 * piece, 2 * piece), 2 * piece), :]

    def forward_copy(ten, q):
        return send(tok_b[ten].at[q], tile_part(ten, q, j), f_send.at[q, ten], f_recv.at[q, ten], dp=partner)

    def own_copy(ten):
        return send(tok[ten], tok_p[ten], own_send.at[ten], own_recv.at[ten], dp=partner)

    def arrive(ten, q):
        with jax.named_scope('arrive'):
            for link in (0, 1):
                wait(slot_of(ten, q, link), q_recv.at[q, link, ten])
            pl.semaphore_wait(room.at[ten], 1)
            forward_copy(ten, q).start()
            pltpu.make_async_copy(tok_b[ten].at[q], tile_part(ten, q, j), ld.at[ten, lax.rem(q, 2)]).start()

        @pl.when(q < 4)
        def _():
            for link in (0, 1):
                relay_copy(ten, q, link).start()

    def landed(ten, q):
        with jax.named_scope('landed'):
            wait(tile_part(ten, q, j), ld.at[ten, lax.rem(q, 2)])
            wait(tile_part(ten, q, 1 - j), f_recv.at[q, ten])

    def rows_of(r):
        return pl.ds(pl.multiple_of(r * tile, tile), tile)

    def load_a(ten, n):
        own = lax.div(n, 2)
        slot = lax.rem(n, 2)

        @pl.when(own == 1)
        def _():
            pltpu.make_async_copy(tok[ten].at[rows_of(slot), :], tok_t[ten].at[slot], ld.at[ten, slot]).start()

        @pl.when(own == 0)
        def _():
            pltpu.make_async_copy(tok_p[ten].at[rows_of(slot), :], tok_t[ten].at[slot], ld.at[ten, slot]).start()

    def loaded(ten, slot):
        with jax.named_scope('ld'):
            wait(tok_t[ten].at[slot], ld.at[ten, slot])

    def unit_col(u):
        mine = cy * units
        other = (1 - cy) * units
        low = cx * rest_units
        high = (1 - cx) * near_units
        a = near_units
        col = jnp.where(u < a, mine + low + u,
                        jnp.where(u < units, mine + high + (u - a),
                                  jnp.where(u < units + a, other + low + (u - units), other + high + (u - units - a))))
        return pl.multiple_of(col * LANES, LANES)

    def chunk(s, way):
        n = lax.rem(s, steps)
        row = pl.multiple_of(way * tile + lax.rem(n, 2) * part_rows, part_rows)
        return lax.div(s, steps), pl.ds(row, part_rows), pl.ds(unit_col(lax.div(n, 2)), LANES)

    def sum_copy(s, way, nxt):
        land = lax.rem(s, DEPTH)
        return send(yacc.at[chunk(s, way)], rbuf.at[way, land], rs_send.at[way, lax.rem(s, SLOTS)], rs_recv.at[way, land], tp=nxt)

    def done_copy(s, way, prv, src):
        return send(src, yd_ref.at[chunk(s, way)], ag_send.at[way, lax.rem(s, SLOTS)], ag_recv.at[way, lax.rem(s, DEPTH)], tp=prv)

    def tick(tau):
        with jax.named_scope('tick'):
            tick_body(tau)

    def tick_body(tau):
        for way in (0, 1):
            p = t if way == 0 else 3 - t
            nxt = t + 1 if way == 0 else t - 1
            prv = t - 1 if way == 0 else t + 1
            s = tau - HOP * p
            slot = lax.rem(jnp.maximum(s, 0), SLOTS)
            land = lax.rem(jnp.maximum(s, 0), DEPTH)
            live = jnp.logical_and(s >= 0, s < 2 * steps)

            @pl.when(jnp.logical_and(live, p > 0))
            def _():
                wait(rbuf.at[way, land], rs_recv.at[way, land])

            @pl.when(jnp.logical_and(live, p < 3))
            def _():
                @pl.when(s >= SLOTS)
                def _():
                    wait(rbuf.at[way, slot], rs_send.at[way, slot])

                @pl.when(p > 0)
                def _():
                    here = chunk(s, way)
                    yacc[here] = yacc[here] + rbuf[way, land]

                sum_copy(s, way, nxt).start()

            @pl.when(jnp.logical_and(live, p == 3))
            def _():
                @pl.when(s >= SLOTS)
                def _():
                    wait(fin.at[slot], ag_send.at[way, slot])
                    wait(fin.at[slot], fin_own.at[way, slot])

                here = chunk(s, way)
                fin[slot] = (yacc[here] + rbuf[way, land]).astype(BF16)
                pltpu.make_async_copy(fin.at[slot], yd_ref.at[here], fin_own.at[way, slot]).start()
                done_copy(s, way, prv, fin.at[slot]).start()

            s2 = tau - HOP * (6 - p)
            slot2 = lax.rem(jnp.maximum(s2, 0), SLOTS)
            land2 = lax.rem(jnp.maximum(s2, 0), DEPTH)
            live2 = jnp.logical_and(jnp.logical_and(s2 >= 0, s2 < 2 * steps), p < 3)

            @pl.when(live2)
            def _():
                here = yd_ref.at[chunk(s2, way)]
                wait(here, ag_recv.at[way, land2])

                @pl.when(p > 0)
                def _():
                    @pl.when(s2 >= SLOTS)
                    def _():
                        wait(fin.at[slot2], ag_send.at[way, slot2])

                    done_copy(s2, way, prv, here).start()

    def ticks(lo, hi):
        def body(n, c):
            tick(n)
            return c

        lax.fori_loop(lo, hi, body, 0)

    def drain_sums():
        def body(n, carry):
            for way in (0, 1):
                p = t if way == 0 else 3 - t
                slot = n

                @pl.when(p < 3)
                def _():
                    wait(rbuf.at[way, slot], rs_send.at[way, slot])

                @pl.when(p > 0)
                def _():
                    wait(fin.at[slot], ag_send.at[way, slot])

                @pl.when(p == 3)
                def _():
                    wait(fin.at[slot], fin_own.at[way, slot])
            return carry

        lax.fori_loop(0, SLOTS, body, 0)

    for ten in (0, 1):
        own_copy(ten).start()
    w_start(0)
    w_start(1)
    base = jnp.where(t == 0, 1.0, 0.0).astype(F32)

    with jax.named_scope('clear'):
        for r in (0, 1):
            for ten in (0, 1):
                load_a(ten, 2 + r)

        def clear(n, carry):
            at = pl.ds(pl.multiple_of(n * 32, 32), 32)
            acc_gu[at, :] = jnp.zeros((32, 2 * half), F32)
            acc_d[at, :] = jnp.zeros((32, half), F32)
            return carry

        lax.fori_loop(0, win // 32, clear, 0)

        def clear_ab(n, carry):
            lo = pl.ds(pl.multiple_of(n * group, group), group)
            for m in range(4):
                ab_all[m, lo, :] = jnp.zeros((group, 2 * half), F32)
            return carry

        lax.fori_loop(0, tile // group, clear_ab, 0)
        for r in (0, 1):
            for ten in (0, 1):
                loaded(ten, r)

                def residual(n, carry):
                    lo = pl.ds(pl.multiple_of(n * group, group), group)
                    there = pl.ds(pl.multiple_of(r * tile + n * group, group), group)
                    yacc[ten, there, :] = tok_t[ten][r, lo, :].astype(F32) * base
                    return carry

                lax.fori_loop(0, tile // group, residual, 0)
        for ten in (0, 1):
            wait(tok_p[ten], own_recv.at[ten])

    with jax.named_scope('w_relay'):
        w_relay(0)
        w_relay(1)
    w_start(2)

    def side(n):
        return pl.ds(pl.multiple_of(lax.rem(n, 2) * half, LANES), half)

    def ab_pass(last):
        other = (1 - cy) * line
        if last:
            parts = ((other + (1 - cx) * near_units * LANES, rest_units * LANES),)
        else:
            parts = ((cy * line, line), (other + cx * rest_units * LANES, near_units * LANES))
        load_a(0, 0)

        def body(n, carry):
            slot = lax.rem(n, 2)

            @pl.when(n < 3)
            def _():
                load_a(0, n + 1)

            loaded(0, slot)
            for at, size in parts:
                at_k = pl.ds(pl.multiple_of(at, LANES), size)
                with jax.named_scope('ab_part'):
                    ab_all[n] += dot_nn(xt[slot, :, at_k], w_gu[at_k, :])

            if last:
                def hidden(m, c):
                    lo = pl.ds(pl.multiple_of(m * group, group), group)
                    a = ab_all[n, lo, :half]
                    h_all[lax.div(n, 2), lo, side(n)] = (a * sigmoid(a) * ab_all[n, lo, half:]).astype(BF16)
                    return c

                lax.fori_loop(0, tile // group, hidden, 0)
            return carry

        lax.fori_loop(0, 4, body, 0)

    with jax.named_scope('w_have'):
        for k in (0, 1):
            w_have(k, 'chip')
            w_have(k, 'x')
            w_have(k, 'y')
    ab_pass(0)
    with jax.named_scope('w_have'):
        for k in (0, 1):
            w_have(k, 'far')
    ab_pass(1)

    def y_group(g, tau):
        u0 = (0, near_units, units, units + near_units)[g]
        n_u = (near_units, rest_units)[g % 2]
        col = unit_col(u0)
        cols = pl.ds(col, n_u * LANES)

        def theirs(r, carry):
            if g > 0:
                before = (near_units, rest_units)[(g - 1) % 2] * LANES
                wait(sb.at[r, :, pl.ds(0, before)], y_send.at[(g - 1) % 2, r])
            with jax.named_scope('y_dot'):
                sb[r, :, :n_u * LANES] = dot_nt(h_all[0, :, side(r)], w_d[cols, :])
            send(sb.at[r, :, pl.ds(0, n_u * LANES)], pbuf.at[rows_of(r), cols],
                 y_send.at[g % 2, r], y_recv.at[g, r], dp=partner).start()
            return carry

        def ours(r, carry):
            with jax.named_scope('y_wait'):
                wait(pbuf.at[rows_of(r), cols], y_recv.at[g, r])
            with jax.named_scope('y_dot'):
                yacc[0, rows_of(r), cols] = (yacc[0, rows_of(r), cols] + pbuf[rows_of(r), cols]
                                             + dot_nt(h_all[1, :, side(r)], w_d[cols, :]))
            pl.semaphore_signal(credit, inc=1, device_id={'dp': partner, 'tp': t}, device_id_type=MESH)
            return carry

        lax.fori_loop(0, 2, theirs, 0)
        if g > 0:
            tick(tau)
        lax.fori_loop(0, 2, ours, 0)
        if g > 0:
            tick(tau + 1)

    load_a(1, 0)
    load_a(0, 0)
    with jax.named_scope('w_have2'):
        w_have(2, 'chip')
    y_group(0, 0)
    tick(0)
    with jax.named_scope('w_relay2'):
        w_relay(2)
    q_start(0)
    q_start(1)
    ticks(1, 7)
    with jax.named_scope('w_have2'):
        w_have(2, 'x')
        w_have(2, 'y')
    y_group(1, 7)
    y_group(2, 9)
    q_start(2)
    ticks(11, 14)
    with jax.named_scope('w_have2'):
        w_have(2, 'far')
    y_group(3, 14)
    q_start(3)

    first = pl.multiple_of(lax.div(chip * 2 * blk, LANES) * LANES, LANES)
    shift = chip * 2 * blk - first
    at_win = pl.ds(first, win)
    n_block = 3
    n_cols = model // n_block

    def w_grad(k, core):
        at = pl.ds(pl.multiple_of(shift + core * blk, 8), blk)
        if k == 2:
            return acc_d.at[at, :]
        return acc_gu.at[at, pl.ds(k * half, half)]

    def put_grad(k):
        send(w_grad(k, 1 - j), outs[k].at[:, w_cols(j)], out_send.at[k], out_recv.at[k], dp=partner).start()
        pltpu.make_async_copy(w_grad(k, j), outs[k].at[:, w_cols(j)], out_own.at[k]).start()

    def dx_tile(n):
        r = lax.rem(n, 2)

        @pl.when(n == 0)
        def _():
            pl.semaphore_wait(credit, 8)
            for r_ in (0, 1):
                wait(sb.at[r_, :, pl.ds(0, rest_units * LANES)], y_send.at[1, r_])

        def block(m, carry):
            cols = pl.ds(pl.multiple_of(m * n_cols, n_cols), n_cols)
            slot = lax.rem(m + r * n_block, 2)

            @pl.when(jnp.logical_and(n < 2, m + r * n_block >= 2))
            def _():
                wait(sb.at[slot], dx_send.at[slot])

            @pl.when(n < 2)
            def _():
                with jax.named_scope('dx_dot'):
                    sb[slot] = dot_nt(h_all[1], w_gu[cols, :])
                send(sb.at[slot], pbuf.at[rows_of(r), cols], dx_send.at[slot], dx_recv.at[r, m], dp=partner).start()

            @pl.when(n >= 2)
            def _():
                with jax.named_scope('dx_wait'):
                    wait(pbuf.at[rows_of(r), cols], dx_recv.at[r, m])
                with jax.named_scope('dx_dot'):
                    yacc[1, rows_of(r), cols] = (yacc[1, rows_of(r), cols] + pbuf[rows_of(r), cols]
                                                 + dot_nt(h_all[1], w_gu[cols, :]))

            @pl.when(m >= 1)
            def _():
                tick(17 + 4 * n + m)
            return carry

        lax.fori_loop(0, n_block, block, 0)

    def grad_tile(n, carry):
        q = n - 4
        slot = lax.rem(n, 2)
        at = jnp.where(n < 4, n, slot)
        final = n == 15
        cut = (half + 255) // 256 * 256
        early = jnp.logical_and(n >= 3, q + 1 <= EARLY)
        late = jnp.logical_and(n < 15, q + 1 > EARLY)
        dense = q >= 8
        tau = jnp.where(dense, 64 + 5 * (q - 8), 16 + 4 * n)

        @pl.when(n < 4)
        def _():
            q_start(4 + n)
            loaded(0, slot)

        @pl.when(n >= 4)
        def _():
            landed(0, q)
            with jax.named_scope('ab_dot'):
                ab_all[at, :, :cut] = dot_nn(xt[slot], w_gu[:, :cut])
            tick(tau)
            with jax.named_scope('ab_dot'):
                ab_all[at, :, cut:] = dot_nn(xt[slot], w_gu[:, cut:])

            @pl.when(final)
            def _():
                arrive(1, q)

            tick(tau + 1)

        @pl.when(early)
        def _():
            arrive(0, q + 1)
            arrive(1, q + 1)

        @pl.when(n < 4)
        def _():
            loaded(1, slot)

        @pl.when(n >= 4)
        def _():
            landed(1, q)

        with jax.named_scope('g_dot'):
            g_s[...] = dot_nn(dyt[slot], w_d[...])

        @pl.when(dense)
        def _():
            tick(tau + 2)

        with jax.named_scope('act'):
            def body(m, c):
                lo = pl.ds(pl.multiple_of(m * group, group), group)
                a = ab_all[at, lo, :half]
                b = ab_all[at, lo, half:]
                g = g_s[lo, :]
                s = sigmoid(a)
                silu = a * s
                h_all[0, lo, :half] = (silu * b).astype(BF16)
                h_all[1, lo, :half] = (g * b * s * (1.0 + a * (1.0 - s))).astype(BF16)
                h_all[1, lo, half:] = (g * silu).astype(BF16)
                return c

            lax.fori_loop(0, tile // group, body, 0)
        tick(tau + jnp.where(n < 4, 0, jnp.where(dense, 3, 2)))

        @pl.when(n < 3)
        def _():
            load_a(0, n + 1)
            load_a(1, n + 1)

        @pl.when(late)
        def _():
            arrive(0, q + 1)

        with jax.named_scope('dw_dot'):
            for lo, hi in ((0, cut), (cut, 2 * half)):
                acc_gu[:, lo:hi] += dot_tn(xt[slot, :, at_win], h_all[1, :, lo:hi])

        @pl.when(final)
        def _():
            put_grad(0)
            put_grad(1)

        with jax.named_scope('dw_dot2'):
            acc_d[...] += dot_tn(dyt[slot, :, at_win], h_all[0, :, :half])

        @pl.when(final)
        def _():
            put_grad(2)

        @pl.when(jnp.logical_and(n >= 2, n < 14))
        def _():
            for ten in (0, 1):
                pl.semaphore_signal(room.at[ten], inc=1, device_id={'dp': partner, 'tp': t}, device_id_type=MESH)

        tick(tau + jnp.where(n < 4, 1, jnp.where(dense, 4, 3)))

        @pl.when(n < 4)
        def _():
            dx_tile(n)

        @pl.when(jnp.logical_and(late, n < 14))
        def _():
            arrive(1, q + 1)
        return carry

    lax.fori_loop(0, 16, grad_tile, 0)

    with jax.named_scope('drain_sums'):
        drain_sums()
    with jax.named_scope('drain'):
        for slot in (0, 1):
            wait(sb.at[slot], dx_send.at[slot])
        for k in range(3):
            for core in (0, 1):
                for link in (0, 1):
                    for part in (0, 1):
                        w_copy(k, link, part, core).wait_send()
                    w_relay_copy(k, link, core).wait_send()
            w_partner_copy(k).wait_send()
        for ten in (0, 1):
            own_copy(ten).wait_send()

        def drain(q, carry):
            for ten in (0, 1):
                wait(tok_b[ten].at[0], f_send.at[q, ten])
                for link in (0, 1):
                    @pl.when(q < 8)
                    def _():
                        wait(slot_of(ten, 0, link), q_send.at[lax.rem(q, 8), link, ten])

                    @pl.when(q < 4)
                    def _():
                        wait(slot_of(ten, 0, link), rl_send.at[lax.rem(q, 4), link, ten])

            return carry

        lax.fori_loop(0, 12, drain, 0)
    with jax.named_scope('drain_out'):
        for k in range(3):
            wait(w_grad(k, j), out_own.at[k])
            wait(w_grad(k, 1 - j), out_send.at[k])
            wait(w_grad(k, j), out_recv.at[k])


def window(model, blk):
    starts = [(2 * blk * c) // LANES * LANES for c in range(model // (2 * blk))]
    shift = max(2 * blk * c - s for c, s in enumerate(starts))
    return -(-(shift + 2 * blk) // LANES) * LANES


def mlp(x, dy, wg, wu, wd):
    rows, model = x.shape
    blk, width = wg.shape
    half = width // 2
    tile = rows // 2
    dma = pltpu.SemaphoreType.DMA
    vmem = pltpu.VMEM
    anywhere = pl.BlockSpec(memory_space=pl.ANY)
    shape = jax.ShapeDtypeStruct
    flops = 2 * model * half * rows * 2 * 20
    return pl.pallas_call(
        kernel,
        name='mlp',
        out_shape=(shape((2, rows, model), BF16),
                   shape((blk, width), F32), shape((blk, width), F32), shape((blk, width), F32),
                   shape((12, tile // 2, model), BF16), shape((12, tile // 2, model), BF16),
                   shape((rows, model), BF16), shape((rows, model), BF16)),
        in_specs=[anywhere] * 5,
        out_specs=tuple([anywhere] * 8),
        scratch_shapes=[
            vmem((model, 2 * half), BF16),
            vmem((model, half), BF16),
            vmem((window(model, blk), 2 * half), F32),
            vmem((window(model, blk), half), F32),
            vmem((2, rows, model), F32),
            vmem((rows, model), F32),
            vmem((2, tile, model // 3), F32),
            vmem((2, tile, model), BF16),
            vmem((2, tile, model), BF16),
            vmem((4, tile, 2 * half), F32),
            vmem((tile, half), F32),
            vmem((2, tile, 2 * half), BF16),
            vmem((2, DEPTH, tile // 2, LANES), F32),
            vmem((SLOTS, tile // 2, LANES), BF16),
            dma((3, 2, 2, 2)), dma((3, 2, 2, 2)), dma((3, 2, 2)), dma((3, 2, 2)), dma((3,)), dma((3,)), dma((3,)),
            dma((2,)), dma((2,)), dma((8, 2, 2)), dma((12, 2, 2)), dma((4, 2, 2)), dma((12, 2)), dma((12, 2)),
            dma((2, 2)), dma((4, 2)), dma((2,)), dma((2, 3)), pltpu.SemaphoreType.REGULAR, pltpu.SemaphoreType.REGULAR((2,)),
            dma((2, SLOTS)), dma((2, DEPTH)), dma((2, SLOTS)), dma((2, DEPTH)), dma((2, SLOTS)),
            dma((2, 2)), dma((3,)), dma((3,)), dma((3,)),
        ],
        compiler_params=pltpu.CompilerParams(collective_id=0, has_side_effects=True, vmem_limit_bytes=67_000_000),
        cost_estimate=pl.CostEstimate(flops=flops, bytes_accessed=100_000_000, transcendentals=0),
    )(x, dy, wg, wu, wd)


def copy_kernel(yd_ref, g_ref, u_ref, d_ref, y_out, dx_out, g_out, u_out, d_out, yd_s, g_s, u_s, d_s, load, store):
    rows = yd_ref.shape[1] // 4
    blk = g_ref.shape[0] // 4
    parts = []
    for m in range(4):
        for src, dst, buf in ((g_ref, g_out, g_s), (u_ref, u_out, u_s), (d_ref, d_out, d_s)):
            at = pl.ds(m * blk, blk)
            parts.append((src.at[at, :], buf.at[at, :], dst.at[at, :]))
        for ten, dst in ((0, y_out), (1, dx_out)):
            at = pl.ds(m * rows, rows)
            parts.append((yd_ref.at[ten, at, :], yd_s.at[ten, at, :], dst.at[at, :]))
    for n, (src, buf, dst) in enumerate(parts):
        pltpu.make_async_copy(src, buf, load.at[n]).start()
    for n, (src, buf, dst) in enumerate(parts):
        pltpu.make_async_copy(src, buf, load.at[n]).wait()
        pltpu.make_async_copy(buf, dst, store.at[n]).start()
    for n, (src, buf, dst) in enumerate(parts):
        pltpu.make_async_copy(buf, dst, store.at[n]).wait()


def copy_results(yd, dwg, dwu, dwd):
    anywhere = pl.BlockSpec(memory_space=pl.ANY)
    shape = jax.ShapeDtypeStruct
    vmem = pltpu.VMEM
    return pl.pallas_call(
        copy_kernel,
        name='results',
        out_shape=(shape(yd.shape[1:], yd.dtype), shape(yd.shape[1:], yd.dtype),
                   shape(dwg.shape, F32), shape(dwu.shape, F32), shape(dwd.shape, F32)),
        in_specs=[anywhere] * 4,
        out_specs=tuple([anywhere] * 5),
        scratch_shapes=[vmem(yd.shape, yd.dtype), vmem(dwg.shape, F32), vmem(dwu.shape, F32), vmem(dwd.shape, F32),
                        pltpu.SemaphoreType.DMA((20,)), pltpu.SemaphoreType.DMA((20,))],
        compiler_params=pltpu.CompilerParams(vmem_limit_bytes=64_000_000),
    )(yd, dwg, dwu, dwd)


def solution(mesh):
    def device_pass(x_rows, gate_blk, up_blk, down_blk, dy_rows):
        out = mlp(x_rows, dy_rows, gate_blk, up_blk, down_blk.T)
        y, dx, dw_gate, dw_up, dw_down = copy_results(*out[:4])
        return y, dx, dw_gate, dw_up, dw_down.T

    row_spec = P('dp', None)
    weight_spec = P('dp', 'tp')
    down_spec = P('tp', 'dp')
    return jax.shard_map(device_pass, mesh=mesh,
                         in_specs=(row_spec, weight_spec, weight_spec, down_spec, row_spec),
                         out_specs=(row_spec, row_spec, weight_spec, weight_spec, down_spec),
                         check_vma=False)
```

```python
import functools
import math

import jax
import jax.numpy as jnp
from jax import lax
from jax.experimental import pallas as pl
from jax.experimental.pallas import tpu as pltpu
from jax.sharding import PartitionSpec as P

F32 = jnp.float32
BF16 = jnp.bfloat16
MESH = pl.DeviceIdType.MESH
SLOTS = 8
DEPTH = 13
HOP = 2
LANES = 128
EARLY = 4


def dot_nn(a, b):
    return jnp.dot(a, b, preferred_element_type=F32)


def dot_nt(a, b):
    return lax.dot_general(a, b, (((1,), (1,)), ((), ())), preferred_element_type=F32)


def dot_tn(a, b):
    return lax.dot_general(a, b, (((0,), (0,)), ((), ())), preferred_element_type=F32)


def sigmoid(a):
    return 1.0 / (1.0 + jnp.exp(-a))


def kernel(x_ref, dy_ref, wg_ref, wu_ref, wd_ref,
           yd_ref, acc_gu, acc_d, pbuf, yacc, xb, dyb, xp, dyp,
           w_gu, w_d, sb, xt, dyt, ab_all, g_s, h_all, rbuf, fin,
           w_send, w_recv, wr_send, wr_recv, w_own, wp_send, wp_recv,
           own_send, own_recv, q_send, q_recv, rl_send, f_send, f_recv,
           y_send, y_recv, dx_send, dx_recv, credit, room,
           rs_send, rs_recv, ag_send, ag_recv, fin_own, ld, out_send, out_recv, h_send, h_recv):
    rows, model = x_ref.shape
    blk, width = wg_ref.shape
    half = width // 2
    hb = blk // 2
    tile = rows // 2
    piece = tile // 4
    win = acc_d.shape[0]
    line = model // 2
    units = line // LANES
    near_units = (2 * blk - LANES // 2) // LANES if (2 * blk) % LANES else 2 * blk // LANES
    rest_units = units - near_units
    steps = 4 * units
    part_rows = tile // 2
    group = min(32, tile)
    w_in = (wg_ref, wu_ref, wd_ref)
    tok = (x_ref, dy_ref)
    tok_b = (xb, dyb)
    tok_p = (xp, dyp)
    tok_t = (xt, dyt)

    t = lax.axis_index('tp')
    me = lax.axis_index('dp')
    cy = lax.div(me, 4)
    cx = lax.rem(lax.div(me, 2), 2)
    j = lax.rem(me, 2)
    partner = me + 1 - 2 * j
    chip = cy * 2 + cx

    def near(link, core):
        if link == 0:
            return cy * 4 + (1 - cx) * 2 + core
        return (1 - cy) * 4 + cx * 2 + core

    def far(core):
        return (1 - cy) * 4 + (1 - cx) * 2 + core

    def send(src, dst, s_sem, r_sem, dp=None, tp=None):
        where = {'dp': me if dp is None else dp, 'tp': t if tp is None else tp}
        return pltpu.make_async_remote_copy(src_ref=src, dst_ref=dst, send_sem=s_sem, recv_sem=r_sem,
                                            device_id=where, device_id_type=MESH)

    def wait(ref, sem):
        pltpu.make_async_copy(ref, ref, sem).wait()

    barrier = pltpu.get_barrier_semaphore()
    for peer in (partner, near(0, 0), near(0, 1), near(1, 0), near(1, 1)):
        pl.semaphore_signal(barrier, inc=1, device_id={'dp': peer, 'tp': t}, device_id_type=MESH)

    @pl.when(t > 0)
    def _():
        pl.semaphore_signal(barrier, inc=1, device_id={'dp': me, 'tp': t - 1}, device_id_type=MESH)

    @pl.when(t < 3)
    def _():
        pl.semaphore_signal(barrier, inc=1, device_id={'dp': me, 'tp': t + 1}, device_id_type=MESH)

    pl.semaphore_wait(barrier, 5 + jnp.minimum(t, 1) + jnp.minimum(3 - t, 1))

    def w_rows(k, dev, part=None):
        if part is None:
            at = pl.ds(pl.multiple_of(dev * blk, 16), blk)
        else:
            at = pl.ds(pl.multiple_of(dev * blk + part * hb, 16), hb)
        if k == 2:
            return w_d.at[at, :]
        return w_gu.at[at, pl.ds(k * half, half)]

    def w_cols(core):
        return pl.ds(pl.multiple_of(core * half, LANES), half)

    def w_copy(k, link, part, core):
        return send(w_in[k].at[pl.ds(part * hb, hb), w_cols(core)], w_rows(k, me, part),
                    w_send.at[k, link, part, core], w_recv.at[k, link, part, j], dp=near(link, core))

    def w_own_copy(k):
        return pltpu.make_async_copy(w_in[k].at[:, w_cols(j)], w_rows(k, me), w_own.at[k])

    def w_partner_copy(k):
        return send(w_in[k].at[:, w_cols(1 - j)], w_rows(k, me), wp_send.at[k], wp_recv.at[k], dp=partner)

    def w_start(k):
        for first in (0, 1):
            for core in (0, 1):
                w_copy(k, 0, 1 - first, core).start()
                w_copy(k, 1, first, core).start()
        w_own_copy(k).start()
        w_partner_copy(k).start()

    def w_relay_copy(k, link_out, core):
        part = 1 if link_out == 1 else 0
        ref = w_rows(k, near(1 - link_out, core), part)
        return send(ref, ref, wr_send.at[k, link_out, core], wr_recv.at[k, link_out, core], dp=near(link_out, j))

    def w_relay(k):
        for core in (0, 1):
            wait(w_rows(k, near(0, core), 1), w_recv.at[k, 0, 1, core])
            w_relay_copy(k, 1, core).start()
            wait(w_rows(k, near(1, core), 0), w_recv.at[k, 1, 0, core])
            w_relay_copy(k, 0, core).start()

    def w_have(k, which):
        if which == 'chip':
            wait(w_rows(k, me), w_own.at[k])
            wait(w_rows(k, partner), wp_recv.at[k])
        for core in (0, 1):
            if which == 'x':
                wait(w_rows(k, near(0, core), 0), w_recv.at[k, 0, 0, core])
            if which == 'y':
                wait(w_rows(k, near(1, core), 1), w_recv.at[k, 1, 1, core])
            if which == 'far':
                wait(w_rows(k, far(core), 0), wr_recv.at[k, 0, core])
                wait(w_rows(k, far(core), 1), wr_recv.at[k, 1, core])

    def slot_of(ten, q, link):
        return tok_b[ten].at[q, pl.ds(link * piece, piece), :]

    def q_copy(ten, q, link):
        b = lax.div(q, 4)
        sub = lax.rem(q, 4)
        first = 1 - b if link == 0 else b
        src = tok[ten].at[pl.ds(pl.multiple_of(first * tile + sub * piece, piece), piece), :]
        return send(src, slot_of(ten, q, link), q_send.at[q, link, ten], q_recv.at[q, link, ten], dp=near(link, j))

    def q_start(q):
        for ten in (0, 1):
            for link in (0, 1):
                q_copy(ten, q, link).start()

    def relay_copy(ten, sub, link_out):
        return send(slot_of(ten, sub, 1 - link_out), slot_of(ten, 8 + sub, link_out),
                    rl_send.at[sub, link_out, ten], q_recv.at[8 + sub, link_out, ten], dp=near(link_out, j))

    def tile_part(ten, q, core):
        return tok_t[ten].at[lax.rem(q, 2), pl.ds(pl.multiple_of(core * 2 * piece, 2 * piece), 2 * piece), :]

    def forward_copy(ten, q):
        return send(tok_b[ten].at[q], tile_part(ten, q, j), f_send.at[q, ten], f_recv.at[q, ten], dp=partner)

    def own_copy(ten):
        return send(tok[ten], tok_p[ten], own_send.at[ten], own_recv.at[ten], dp=partner)

    def arrive(ten, q):
        with jax.named_scope('arrive'):
            for link in (0, 1):
                wait(slot_of(ten, q, link), q_recv.at[q, link, ten])
            pl.semaphore_wait(room.at[ten], 1)
            forward_copy(ten, q).start()
            pltpu.make_async_copy(tok_b[ten].at[q], tile_part(ten, q, j), ld.at[ten, lax.rem(q, 2)]).start()

        @pl.when(q < 4)
        def _():
            for link in (0, 1):
                relay_copy(ten, q, link).start()

    def landed(ten, q):
        with jax.named_scope('landed'):
            wait(tile_part(ten, q, j), ld.at[ten, lax.rem(q, 2)])
            wait(tile_part(ten, q, 1 - j), f_recv.at[q, ten])

    def rows_of(r):
        return pl.ds(pl.multiple_of(r * tile, tile), tile)

    def load_a(ten, n):
        own = lax.div(n, 2)
        slot = lax.rem(n, 2)

        @pl.when(own == 1)
        def _():
            pltpu.make_async_copy(tok[ten].at[rows_of(slot), :], tok_t[ten].at[slot], ld.at[ten, slot]).start()

        @pl.when(own == 0)
        def _():
            pltpu.make_async_copy(tok_p[ten].at[rows_of(slot), :], tok_t[ten].at[slot], ld.at[ten, slot]).start()

    def loaded(ten, slot):
        with jax.named_scope('ld'):
            wait(tok_t[ten].at[slot], ld.at[ten, slot])

    def unit_col(u):
        mine = cy * units
        other = (1 - cy) * units
        low = cx * rest_units
        high = (1 - cx) * near_units
        a = near_units
        col = jnp.where(u < a, mine + low + u,
                        jnp.where(u < units, mine + high + (u - a),
                                  jnp.where(u < units + a, other + low + (u - units), other + high + (u - units - a))))
        return pl.multiple_of(col * LANES, LANES)

    def chunk(s, way):
        n = lax.rem(s, steps)
        row = pl.multiple_of(way * tile + lax.rem(n, 2) * part_rows, part_rows)
        return lax.div(s, steps), pl.ds(row, part_rows), pl.ds(unit_col(lax.div(n, 2)), LANES)

    def sum_copy(s, way, nxt):
        land = lax.rem(s, DEPTH)
        return send(yacc.at[chunk(s, way)], rbuf.at[way, land], rs_send.at[way, lax.rem(s, SLOTS)], rs_recv.at[way, land], tp=nxt)

    def done_copy(s, way, prv, src):
        return send(src, yd_ref.at[chunk(s, way)], ag_send.at[way, lax.rem(s, SLOTS)], ag_recv.at[way, lax.rem(s, DEPTH)], tp=prv)

    def tick(tau):
        with jax.named_scope('tick'):
            tick_body(tau)

    def tick_body(tau):
        for way in (0, 1):
            p = t if way == 0 else 3 - t
            nxt = t + 1 if way == 0 else t - 1
            prv = t - 1 if way == 0 else t + 1
            s = tau - HOP * p
            slot = lax.rem(jnp.maximum(s, 0), SLOTS)
            land = lax.rem(jnp.maximum(s, 0), DEPTH)
            live = jnp.logical_and(s >= 0, s < 2 * steps)

            @pl.when(jnp.logical_and(live, p > 0))
            def _():
                wait(rbuf.at[way, land], rs_recv.at[way, land])

            @pl.when(jnp.logical_and(live, p < 3))
            def _():
                @pl.when(s >= SLOTS)
                def _():
                    wait(rbuf.at[way, slot], rs_send.at[way, slot])

                @pl.when(p > 0)
                def _():
                    here = chunk(s, way)
                    yacc[here] = yacc[here] + rbuf[way, land]

                sum_copy(s, way, nxt).start()

            @pl.when(jnp.logical_and(live, p == 3))
            def _():
                @pl.when(s >= SLOTS)
                def _():
                    wait(fin.at[slot], ag_send.at[way, slot])
                    wait(fin.at[slot], fin_own.at[way, slot])

                here = chunk(s, way)
                fin[slot] = (yacc[here] + rbuf[way, land]).astype(BF16)
                pltpu.make_async_copy(fin.at[slot], yd_ref.at[here], fin_own.at[way, slot]).start()
                done_copy(s, way, prv, fin.at[slot]).start()

            s2 = tau - HOP * (6 - p)
            slot2 = lax.rem(jnp.maximum(s2, 0), SLOTS)
            land2 = lax.rem(jnp.maximum(s2, 0), DEPTH)
            live2 = jnp.logical_and(jnp.logical_and(s2 >= 0, s2 < 2 * steps), p < 3)

            @pl.when(live2)
            def _():
                here = yd_ref.at[chunk(s2, way)]
                wait(here, ag_recv.at[way, land2])

                @pl.when(p > 0)
                def _():
                    @pl.when(s2 >= SLOTS)
                    def _():
                        wait(fin.at[slot2], ag_send.at[way, slot2])

                    done_copy(s2, way, prv, here).start()

    def ticks(lo, hi):
        def body(n, c):
            tick(n)
            return c

        lax.fori_loop(lo, hi, body, 0)

    def drain_sums():
        def body(n, carry):
            for way in (0, 1):
                p = t if way == 0 else 3 - t
                slot = n

                @pl.when(p < 3)
                def _():
                    wait(rbuf.at[way, slot], rs_send.at[way, slot])

                @pl.when(p > 0)
                def _():
                    wait(fin.at[slot], ag_send.at[way, slot])

                @pl.when(p == 3)
                def _():
                    wait(fin.at[slot], fin_own.at[way, slot])
            return carry

        lax.fori_loop(0, SLOTS, body, 0)

    w_start(0)
    w_start(1)
    for ten in (0, 1):
        own_copy(ten).start()
    base = jnp.where(t == 0, 1.0, 0.0).astype(F32)

    with jax.named_scope('clear'):
        for r in (0, 1):
            for ten in (0, 1):
                load_a(ten, 2 + r)

        def clear(n, carry):
            at = pl.ds(pl.multiple_of(n * 32, 32), 32)
            acc_gu[at, :] = jnp.zeros((32, 2 * half), F32)
            acc_d[at, :] = jnp.zeros((32, half), F32)
            return carry

        lax.fori_loop(0, win // 32, clear, 0)

        def clear_ab(n, carry):
            lo = pl.ds(pl.multiple_of(n * group, group), group)
            for m in range(4):
                ab_all[m, lo, :] = jnp.zeros((group, 2 * half), F32)
            return carry

        lax.fori_loop(0, tile // group, clear_ab, 0)
        for r in (0, 1):
            for ten in (0, 1):
                loaded(ten, r)

                def residual(n, carry):
                    lo = pl.ds(pl.multiple_of(n * group, group), group)
                    there = pl.ds(pl.multiple_of(r * tile + n * group, group), group)
                    yacc[ten, there, :] = tok_t[ten][r, lo, :].astype(F32) * base
                    return carry

                lax.fori_loop(0, tile // group, residual, 0)
        for ten in (0, 1):
            wait(tok_p[ten], own_recv.at[ten])

    with jax.named_scope('w_relay'):
        w_relay(0)
        w_relay(1)
    w_start(2)

    def side(n):
        return pl.ds(pl.multiple_of(lax.rem(n, 2) * half, LANES), half)

    def ab_pass(last):
        other = (1 - cy) * line
        if last:
            parts = ((other + (1 - cx) * near_units * LANES, rest_units * LANES),)
        else:
            parts = ((cy * line, line), (other + cx * rest_units * LANES, near_units * LANES))
        load_a(0, 0)

        def body(n, carry):
            slot = lax.rem(n, 2)

            @pl.when(n < 3)
            def _():
                load_a(0, n + 1)

            loaded(0, slot)
            for at, size in parts:
                at_k = pl.ds(pl.multiple_of(at, LANES), size)
                with jax.named_scope('ab_part'):
                    ab_all[n] += dot_nn(xt[slot, :, at_k], w_gu[at_k, :])

            if last:
                def hidden(m, c):
                    lo = pl.ds(pl.multiple_of(m * group, group), group)
                    a = ab_all[n, lo, :half]
                    h_all[lax.div(n, 2), lo, side(n)] = (a * sigmoid(a) * ab_all[n, lo, half:]).astype(BF16)
                    return c

                lax.fori_loop(0, tile // group, hidden, 0)
            return carry

        lax.fori_loop(0, 4, body, 0)

    with jax.named_scope('w_have'):
        for k in (0, 1):
            w_have(k, 'chip')
            w_have(k, 'x')
            w_have(k, 'y')
    ab_pass(0)
    with jax.named_scope('w_have'):
        for k in (0, 1):
            w_have(k, 'far')
    ab_pass(1)

    def y_group(g, tau):
        u0 = (0, near_units, units, units + near_units)[g]
        n_u = (near_units, rest_units)[g % 2]
        col = unit_col(u0)
        cols = pl.ds(col, n_u * LANES)

        def theirs(r, carry):
            if g > 0:
                before = (near_units, rest_units)[(g - 1) % 2] * LANES
                wait(sb.at[r, :, pl.ds(0, before)], y_send.at[(g - 1) % 2, r])
            with jax.named_scope('y_dot'):
                sb[r, :, :n_u * LANES] = dot_nt(h_all[0, :, side(r)], w_d[cols, :])
            send(sb.at[r, :, pl.ds(0, n_u * LANES)], pbuf.at[rows_of(r), cols],
                 y_send.at[g % 2, r], y_recv.at[g, r], dp=partner).start()
            return carry

        def ours(r, carry):
            with jax.named_scope('y_wait'):
                wait(pbuf.at[rows_of(r), cols], y_recv.at[g, r])
            with jax.named_scope('y_dot'):
                yacc[0, rows_of(r), cols] = (yacc[0, rows_of(r), cols] + pbuf[rows_of(r), cols]
                                             + dot_nt(h_all[1, :, side(r)], w_d[cols, :]))
            pl.semaphore_signal(credit, inc=1, device_id={'dp': partner, 'tp': t}, device_id_type=MESH)
            return carry

        lax.fori_loop(0, 2, theirs, 0)
        if g > 0:
            tick(tau)
        lax.fori_loop(0, 2, ours, 0)
        if g > 0:
            tick(tau + 1)

    load_a(1, 0)
    load_a(0, 0)
    with jax.named_scope('w_have2'):
        w_have(2, 'chip')
    y_group(0, 0)
    tick(0)
    with jax.named_scope('w_relay2'):
        w_relay(2)
    q_start(0)
    q_start(1)
    ticks(1, 7)
    with jax.named_scope('w_have2'):
        w_have(2, 'x')
        w_have(2, 'y')
    y_group(1, 7)
    y_group(2, 9)
    q_start(2)
    ticks(11, 14)
    with jax.named_scope('w_have2'):
        w_have(2, 'far')
    y_group(3, 14)
    q_start(3)

    at_win, shift = window_of(chip * 2 * blk, win)
    own = own_window(blk)
    at_own, _ = window_of(me * blk, own)
    in_acc = pl.ds(pl.multiple_of(window_of(me * blk, own)[0].start - at_win.start, 8), own)
    n_block = 3
    n_cols = model // n_block

    def grad_copies():
        rows_ = pl.ds(pl.multiple_of(shift + (1 - j) * blk, 8), blk)
        there = pl.ds(pl.multiple_of(window_of(partner * blk, own)[1], 8), blk)
        return (send(acc_gu.at[rows_, :], pbuf.at[there, pl.ds(0, 2 * half)], out_send.at[0], out_recv.at[0], dp=partner),
                send(acc_d.at[rows_, :], yacc.at[0, there, pl.ds(0, half)], out_send.at[1], out_recv.at[1], dp=partner))

    def last_copies():
        return (send(h_all.at[1], xt.at[0, :, pl.ds(0, 2 * half)], h_send.at[0], h_recv.at[0], dp=partner),
                send(h_all.at[0, :, pl.ds(0, half)], dyt.at[0, :, pl.ds(0, half)], h_send.at[1], h_recv.at[1], dp=partner))

    def dx_tile(n):
        r = lax.rem(n, 2)

        @pl.when(n == 0)
        def _():
            pl.semaphore_wait(credit, 8)
            for r_ in (0, 1):
                wait(sb.at[r_, :, pl.ds(0, rest_units * LANES)], y_send.at[1, r_])

        def block(m, carry):
            cols = pl.ds(pl.multiple_of(m * n_cols, n_cols), n_cols)
            slot = lax.rem(m + r * n_block, 2)

            @pl.when(jnp.logical_and(n < 2, m + r * n_block >= 2))
            def _():
                wait(sb.at[slot], dx_send.at[slot])

            @pl.when(n < 2)
            def _():
                with jax.named_scope('dx_dot'):
                    sb[slot] = dot_nt(h_all[1], w_gu[cols, :])
                send(sb.at[slot], pbuf.at[rows_of(r), cols], dx_send.at[slot], dx_recv.at[r, m], dp=partner).start()

            @pl.when(n >= 2)
            def _():
                with jax.named_scope('dx_wait'):
                    wait(pbuf.at[rows_of(r), cols], dx_recv.at[r, m])
                with jax.named_scope('dx_dot'):
                    yacc[1, rows_of(r), cols] = (yacc[1, rows_of(r), cols] + pbuf[rows_of(r), cols]
                                                 + dot_nt(h_all[1], w_gu[cols, :]))

            @pl.when(m >= 1)
            def _():
                tick(17 + 4 * n + m)
            return carry

        lax.fori_loop(0, n_block, block, 0)

    def grad_tile(n, carry):
        q = n - 4
        slot = lax.rem(n, 2)
        at = jnp.where(n < 4, n, slot)
        final = n == 15
        cut = (half + 255) // 256 * 256
        early = jnp.logical_and(n >= 3, q + 1 <= EARLY)
        late = jnp.logical_and(n < 15, q + 1 > EARLY)
        dense = q >= 8
        tau = jnp.where(dense, 64 + 5 * (q - 8), 16 + 4 * n)

        @pl.when(n < 4)
        def _():
            q_start(4 + n)
            loaded(0, slot)

        @pl.when(n >= 4)
        def _():
            landed(0, q)
            with jax.named_scope('ab_dot'):
                ab_all[at, :, :cut] = dot_nn(xt[slot], w_gu[:, :cut])
            tick(tau)
            with jax.named_scope('ab_dot'):
                ab_all[at, :, cut:] = dot_nn(xt[slot], w_gu[:, cut:])

            @pl.when(final)
            def _():
                arrive(1, q)

            tick(tau + 1)

        @pl.when(early)
        def _():
            arrive(0, q + 1)
            arrive(1, q + 1)

        @pl.when(n < 4)
        def _():
            loaded(1, slot)

        @pl.when(n >= 4)
        def _():
            landed(1, q)

        with jax.named_scope('g_dot'):
            g_s[...] = dot_nn(dyt[slot], w_d[...])

        @pl.when(dense)
        def _():
            tick(tau + 2)

        with jax.named_scope('act'):
            def body(m, c):
                lo = pl.ds(pl.multiple_of(m * group, group), group)
                a = ab_all[at, lo, :half]
                b = ab_all[at, lo, half:]
                g = g_s[lo, :]
                s = sigmoid(a)
                silu = a * s
                h_all[0, lo, :half] = (silu * b).astype(BF16)
                h_all[1, lo, :half] = (g * b * s * (1.0 + a * (1.0 - s))).astype(BF16)
                h_all[1, lo, half:] = (g * silu).astype(BF16)
                return c

            lax.fori_loop(0, tile // group, body, 0)
        tick(tau + jnp.where(n < 4, 0, jnp.where(dense, 3, 2)))

        @pl.when(n < 3)
        def _():
            load_a(0, n + 1)
            load_a(1, n + 1)

        @pl.when(late)
        def _():
            arrive(0, q + 1)

        @pl.when(jnp.logical_not(final))
        def _():
            with jax.named_scope('dw_dot'):
                for lo, hi in ((0, cut), (cut, 2 * half)):
                    acc_gu[:, lo:hi] += dot_tn(xt[slot, :, at_win], h_all[1, :, lo:hi])
            with jax.named_scope('dw_dot2'):
                acc_d[...] += dot_tn(dyt[slot, :, at_win], h_all[0, :, :half])

        @pl.when(n == 14)
        def _():
            for copy in grad_copies():
                copy.start()

        @pl.when(final)
        def _():
            for ten in (0, 1):
                pl.semaphore_wait(room.at[ten], 1)
            for copy in last_copies():
                copy.start()
            with jax.named_scope('grads_sent'):
                for copy in grad_copies():
                    copy.wait_send()
            with jax.named_scope('dw_own'):
                for lo, hi in ((0, cut), (cut, 2 * half)):
                    acc_gu[in_acc, lo:hi] += dot_tn(xt[1, :, at_own], h_all[1, :, lo:hi])
                acc_d[in_acc, :] += dot_tn(dyt[1, :, at_own], h_all[0, :, :half])

        @pl.when(jnp.logical_and(n >= 2, n < 15))
        def _():
            for ten in (0, 1):
                pl.semaphore_signal(room.at[ten], inc=1, device_id={'dp': partner, 'tp': t}, device_id_type=MESH)

        tick(tau + jnp.where(n < 4, 1, jnp.where(dense, 4, 3)))

        @pl.when(n < 4)
        def _():
            dx_tile(n)

        @pl.when(jnp.logical_and(late, n < 14))
        def _():
            arrive(1, q + 1)
        return carry

    lax.fori_loop(0, 16, grad_tile, 0)

    with jax.named_scope('last_wait'):
        theirs = pl.ds(pl.multiple_of(window_of(me * blk, own)[1], 8), blk)
        wait(pbuf.at[theirs, pl.ds(0, 2 * half)], out_recv.at[0])
        wait(yacc.at[0, theirs, pl.ds(0, half)], out_recv.at[1])
        wait(xt.at[0, :, pl.ds(0, 2 * half)], h_recv.at[0])
        wait(dyt.at[0, :, pl.ds(0, half)], h_recv.at[1])
    with jax.named_scope('dw_other'):
        cut = (half + 255) // 256 * 256
        for lo, hi in ((0, cut), (cut, 2 * half)):
            pbuf[:own, lo:hi] += dot_tn(xt[1, :, at_own], xt[0, :, lo:hi])
        yacc[0, :own, :half] += dot_tn(dyt[1, :, at_own], dyt[0, :, :half])

    with jax.named_scope('drain_sums'):
        drain_sums()
    with jax.named_scope('drain'):
        for slot in (0, 1):
            wait(sb.at[slot], dx_send.at[slot])
        for k in range(3):
            for core in (0, 1):
                for link in (0, 1):
                    for part in (0, 1):
                        w_copy(k, link, part, core).wait_send()
                    w_relay_copy(k, link, core).wait_send()
            w_partner_copy(k).wait_send()
        for ten in (0, 1):
            own_copy(ten).wait_send()

        def drain(q, carry):
            for ten in (0, 1):
                wait(tok_b[ten].at[0], f_send.at[q, ten])
                for link in (0, 1):
                    @pl.when(q < 8)
                    def _():
                        wait(slot_of(ten, 0, link), q_send.at[lax.rem(q, 8), link, ten])

                    @pl.when(q < 4)
                    def _():
                        wait(slot_of(ten, 0, link), rl_send.at[lax.rem(q, 4), link, ten])

            return carry

        lax.fori_loop(0, 12, drain, 0)
        for copy in last_copies():
            copy.wait_send()


def window_of(start, size):
    first = lax.div(start, LANES) * LANES
    return pl.ds(pl.multiple_of(first, LANES), size), start - first


def own_window(blk):
    return -(-(blk + LANES - 32) // LANES) * LANES


def window(model, blk):
    starts = [(2 * blk * c) // LANES * LANES for c in range(model // (2 * blk))]
    shift = max(2 * blk * c - s for c, s in enumerate(starts))
    return -(-(shift + 2 * blk) // LANES) * LANES


def mlp(x, dy, wg, wu, wd):
    rows, model = x.shape
    blk, width = wg.shape
    half = width // 2
    tile = rows // 2
    dma = pltpu.SemaphoreType.DMA
    vmem = pltpu.VMEM
    anywhere = pl.BlockSpec(memory_space=pl.ANY)
    shape = jax.ShapeDtypeStruct
    flops = 2 * model * half * rows * 2 * 20
    win = window(model, blk)
    most = max(rows, own_window(blk))
    kept = (vmem((win, 2 * half), F32), vmem((win, half), F32), vmem((most, model), F32), vmem((2, most, model), F32))
    held = sum(4 * math.prod(k.shape) for k in kept)
    in_vmem = pl.BlockSpec(memory_space=pltpu.VMEM)
    return pl.pallas_call(
        kernel,
        name='mlp',
        out_shape=(shape((2, rows, model), BF16), *kept,
                   shape((12, tile // 2, model), BF16), shape((12, tile // 2, model), BF16),
                   shape((rows, model), BF16), shape((rows, model), BF16)),
        in_specs=[anywhere] * 5,
        out_specs=(anywhere, *[in_vmem] * 4, *[anywhere] * 4),
        scratch_shapes=[
            vmem((model, 2 * half), BF16),
            vmem((model, half), BF16),
            vmem((2, tile, model // 3), F32),
            vmem((2, tile, model), BF16),
            vmem((2, tile, model), BF16),
            vmem((4, tile, 2 * half), F32),
            vmem((tile, half), F32),
            vmem((2, tile, 2 * half), BF16),
            vmem((2, DEPTH, tile // 2, LANES), F32),
            vmem((SLOTS, tile // 2, LANES), BF16),
            dma((3, 2, 2, 2)), dma((3, 2, 2, 2)), dma((3, 2, 2)), dma((3, 2, 2)), dma((3,)), dma((3,)), dma((3,)),
            dma((2,)), dma((2,)), dma((8, 2, 2)), dma((12, 2, 2)), dma((4, 2, 2)), dma((12, 2)), dma((12, 2)),
            dma((2, 2)), dma((4, 2)), dma((2,)), dma((2, 3)), pltpu.SemaphoreType.REGULAR, pltpu.SemaphoreType.REGULAR((2,)),
            dma((2, SLOTS)), dma((2, DEPTH)), dma((2, SLOTS)), dma((2, DEPTH)), dma((2, SLOTS)),
            dma((2, 2)), dma((2,)), dma((2,)), dma((2,)), dma((2,)),
        ],
        compiler_params=pltpu.CompilerParams(collective_id=0, has_side_effects=True, vmem_limit_bytes=67_000_000 - held),
        cost_estimate=pl.CostEstimate(flops=flops, bytes_accessed=100_000_000, transcendentals=0),
    )(x, dy, wg, wu, wd)


def results_kernel(blk, half, yd_ref, acc_gu, acc_d, pbuf, yacc, y_out, dx_out, g_out, u_out, d_out, yd_s, load, store, grad):
    me = lax.axis_index('dp')
    j = lax.rem(me, 2)
    chip = lax.div(me, 2)
    mine = pl.ds(pl.multiple_of(window_of(chip * 2 * blk, 128)[1] + j * blk, 8), blk)
    other = pl.ds(pl.multiple_of(window_of(me * blk, 128)[1], 8), blk)
    own_cols = pl.ds(pl.multiple_of(j * half, LANES), half)
    other_cols = pl.ds(pl.multiple_of((1 - j) * half, LANES), half)
    low, high = pl.ds(0, half), pl.ds(half, half)
    rows = yd_ref.shape[1] // 4
    parts = []
    for m in range(4):
        for ten, dst in ((0, y_out), (1, dx_out)):
            at = pl.ds(m * rows, rows)
            parts.append((yd_ref.at[ten, at, :], yd_s.at[ten, at, :], dst.at[at, :]))
    grads = ((acc_gu.at[mine, low], g_out.at[:, own_cols]), (acc_gu.at[mine, high], u_out.at[:, own_cols]),
             (acc_d.at[mine, :], d_out.at[:, own_cols]),
             (pbuf.at[other, low], g_out.at[:, other_cols]), (pbuf.at[other, high], u_out.at[:, other_cols]),
             (yacc.at[0, other, low], d_out.at[:, other_cols]))
    for n, (src, buf, dst) in enumerate(parts):
        pltpu.make_async_copy(src, buf, load.at[n]).start()
    for n, (src, dst) in enumerate(grads):
        pltpu.make_async_copy(src, dst, grad.at[n]).start()
    for n, (src, buf, dst) in enumerate(parts):
        pltpu.make_async_copy(src, buf, load.at[n]).wait()
        pltpu.make_async_copy(buf, dst, store.at[n]).start()
    for n, (src, buf, dst) in enumerate(parts):
        pltpu.make_async_copy(buf, dst, store.at[n]).wait()
    for n, (src, dst) in enumerate(grads):
        pltpu.make_async_copy(src, dst, grad.at[n]).wait()


def results(blk, width, yd, *kept):
    anywhere = pl.BlockSpec(memory_space=pl.ANY)
    in_vmem = pl.BlockSpec(memory_space=pltpu.VMEM)
    shape = jax.ShapeDtypeStruct
    dma = pltpu.SemaphoreType.DMA
    yd = pltpu.with_memory_space_constraint(yd, pltpu.HBM)
    kept = [pltpu.with_memory_space_constraint(k, pltpu.VMEM) for k in kept]
    return pl.pallas_call(
        functools.partial(results_kernel, blk, width // 2),
        name='results',
        out_shape=(shape(yd.shape[1:], yd.dtype), shape(yd.shape[1:], yd.dtype),
                   shape((blk, width), F32), shape((blk, width), F32), shape((blk, width), F32)),
        in_specs=[pl.BlockSpec(memory_space=pltpu.HBM), *[in_vmem] * 4],
        out_specs=tuple([anywhere] * 5),
        scratch_shapes=[pltpu.VMEM(yd.shape, yd.dtype), dma((8,)), dma((8,)), dma((6,))],
        compiler_params=pltpu.CompilerParams(vmem_limit_bytes=12_000_000),
    )(yd, *kept)


def solution(mesh):
    def device_pass(x_rows, gate_blk, up_blk, down_blk, dy_rows):
        out = mlp(x_rows, dy_rows, gate_blk, up_blk, down_blk.T)
        y, dx, dw_gate, dw_up, dw_down = results(*gate_blk.shape, *out[:5])
        return y, dx, dw_gate, dw_up, dw_down.T

    row_spec = P('dp', None)
    weight_spec = P('dp', 'tp')
    down_spec = P('tp', 'dp')
    return jax.shard_map(device_pass, mesh=mesh,
                         in_specs=(row_spec, weight_spec, weight_spec, down_spec, row_spec),
                         out_specs=(row_spec, row_spec, weight_spec, weight_spec, down_spec),
                         check_vma=False)
```

```python
import functools
import math

import jax
import jax.numpy as jnp
from jax import lax
from jax.experimental import pallas as pl
from jax.experimental.pallas import tpu as pltpu
from jax.sharding import PartitionSpec as P

F32 = jnp.float32
BF16 = jnp.bfloat16
MESH = pl.DeviceIdType.MESH
SLOTS = 8
DEPTH = 13
KEEP = 16
LAG = 3
HOP = 2
LANES = 128
EARLY = 4


def dot_nn(a, b):
    return jnp.dot(a, b, preferred_element_type=F32)


def dot_nt(a, b):
    return lax.dot_general(a, b, (((1,), (1,)), ((), ())), preferred_element_type=F32)


def dot_tn(a, b):
    return lax.dot_general(a, b, (((0,), (0,)), ((), ())), preferred_element_type=F32)


def sigmoid(a):
    return 1.0 / (1.0 + jnp.exp(-a))


def kernel(x_ref, dy_ref, wg_ref, wu_ref, wd_ref,
           yd_ref, acc_gu, acc_d, pbuf, yacc, xb, dyb, xp, dyp,
           w_gu, w_d, sb, xt, dyt, ab_all, g_s, h_all, rbuf, back,
           w_send, w_recv, wr_send, wr_recv, w_own, wp_send, wp_recv,
           own_send, own_recv, q_send, q_recv, rl_send, f_send, f_recv,
           y_send, y_recv, dx_send, dx_recv, credit, room,
           rs_send, rs_recv, ag_send, ag_recv, fin_own, ld, out_send, out_recv, h_send, h_recv):
    rows, model = x_ref.shape
    blk, width = wg_ref.shape
    half = width // 2
    hb = blk // 2
    tile = rows // 2
    piece = tile // 4
    win = acc_d.shape[0]
    line = model // 2
    units = line // LANES
    near_units = (2 * blk - LANES // 2) // LANES if (2 * blk) % LANES else 2 * blk // LANES
    rest_units = units - near_units
    steps = 4 * units
    part_rows = tile // 2
    group = min(32, tile)
    w_in = (wg_ref, wu_ref, wd_ref)
    cut = (half + 255) // 256 * 256
    pieces = ((0, cut), (cut, 2 * half))
    tok = (x_ref, dy_ref)
    tok_b = (xb, dyb)
    tok_p = (xp, dyp)
    tok_t = (xt, dyt)

    t = lax.axis_index('tp')
    me = lax.axis_index('dp')
    cy = lax.div(me, 4)
    cx = lax.rem(lax.div(me, 2), 2)
    j = lax.rem(me, 2)
    partner = me + 1 - 2 * j
    chip = cy * 2 + cx

    def near(link, core):
        if link == 0:
            return cy * 4 + (1 - cx) * 2 + core
        return (1 - cy) * 4 + cx * 2 + core

    def far(core):
        return (1 - cy) * 4 + (1 - cx) * 2 + core

    def send(src, dst, s_sem, r_sem, dp=None, tp=None):
        where = {'dp': me if dp is None else dp, 'tp': t if tp is None else tp}
        return pltpu.make_async_remote_copy(src_ref=src, dst_ref=dst, send_sem=s_sem, recv_sem=r_sem,
                                            device_id=where, device_id_type=MESH)

    def wait(ref, sem):
        pltpu.make_async_copy(ref, ref, sem).wait()

    barrier = pltpu.get_barrier_semaphore()
    for peer in (partner, near(0, 0), near(0, 1), near(1, 0), near(1, 1)):
        pl.semaphore_signal(barrier, inc=1, device_id={'dp': peer, 'tp': t}, device_id_type=MESH)

    @pl.when(t > 0)
    def _():
        pl.semaphore_signal(barrier, inc=1, device_id={'dp': me, 'tp': t - 1}, device_id_type=MESH)

    @pl.when(t < 3)
    def _():
        pl.semaphore_signal(barrier, inc=1, device_id={'dp': me, 'tp': t + 1}, device_id_type=MESH)

    pl.semaphore_wait(barrier, 5 + jnp.minimum(t, 1) + jnp.minimum(3 - t, 1))

    def w_rows(k, dev, part=None):
        if part is None:
            at = pl.ds(pl.multiple_of(dev * blk, 16), blk)
        else:
            at = pl.ds(pl.multiple_of(dev * blk + part * hb, 16), hb)
        if k == 2:
            return w_d.at[at, :]
        return w_gu.at[at, pl.ds(k * half, half)]

    def w_cols(core):
        return pl.ds(pl.multiple_of(core * half, LANES), half)

    def w_copy(k, link, part, core):
        return send(w_in[k].at[pl.ds(part * hb, hb), w_cols(core)], w_rows(k, me, part),
                    w_send.at[k, link, part, core], w_recv.at[k, link, part, j], dp=near(link, core))

    def w_own_copy(k):
        return pltpu.make_async_copy(w_in[k].at[:, w_cols(j)], w_rows(k, me), w_own.at[k])

    def w_partner_copy(k):
        return send(w_in[k].at[:, w_cols(1 - j)], w_rows(k, me), wp_send.at[k], wp_recv.at[k], dp=partner)

    def w_start(k):
        for first in (0, 1):
            for core in (0, 1):
                w_copy(k, 0, 1 - first, core).start()
                w_copy(k, 1, first, core).start()
        w_own_copy(k).start()
        w_partner_copy(k).start()

    def w_relay_copy(k, link_out, core):
        part = 1 if link_out == 1 else 0
        ref = w_rows(k, near(1 - link_out, core), part)
        return send(ref, ref, wr_send.at[k, link_out, core], wr_recv.at[k, link_out, core], dp=near(link_out, j))

    def w_relay(k):
        for core in (0, 1):
            wait(w_rows(k, near(0, core), 1), w_recv.at[k, 0, 1, core])
            w_relay_copy(k, 1, core).start()
            wait(w_rows(k, near(1, core), 0), w_recv.at[k, 1, 0, core])
            w_relay_copy(k, 0, core).start()

    def w_have(k, which):
        if which == 'chip':
            wait(w_rows(k, me), w_own.at[k])
            wait(w_rows(k, partner), wp_recv.at[k])
        for core in (0, 1):
            if which == 'x':
                wait(w_rows(k, near(0, core), 0), w_recv.at[k, 0, 0, core])
            if which == 'y':
                wait(w_rows(k, near(1, core), 1), w_recv.at[k, 1, 1, core])
            if which == 'far':
                wait(w_rows(k, far(core), 0), wr_recv.at[k, 0, core])
                wait(w_rows(k, far(core), 1), wr_recv.at[k, 1, core])

    def slot_of(ten, q, link):
        return tok_b[ten].at[q, pl.ds(link * piece, piece), :]

    def q_copy(ten, q, link):
        b = lax.div(q, 4)
        sub = lax.rem(q, 4)
        first = 1 - b if link == 0 else b
        src = tok[ten].at[pl.ds(pl.multiple_of(first * tile + sub * piece, piece), piece), :]
        return send(src, slot_of(ten, q, link), q_send.at[q, link, ten], q_recv.at[q, link, ten], dp=near(link, j))

    def q_start(q):
        for ten in (0, 1):
            for link in (0, 1):
                q_copy(ten, q, link).start()

    def relay_copy(ten, sub, link_out):
        return send(slot_of(ten, sub, 1 - link_out), slot_of(ten, 8 + sub, link_out),
                    rl_send.at[sub, link_out, ten], q_recv.at[8 + sub, link_out, ten], dp=near(link_out, j))

    def tile_part(ten, q, core):
        return tok_t[ten].at[lax.rem(q, 2), pl.ds(pl.multiple_of(core * 2 * piece, 2 * piece), 2 * piece), :]

    def forward_copy(ten, q):
        return send(tok_b[ten].at[q], tile_part(ten, q, j), f_send.at[q, ten], f_recv.at[q, ten], dp=partner)

    def own_copy(ten):
        return send(tok[ten], tok_p[ten], own_send.at[ten], own_recv.at[ten], dp=partner)

    def arrive(ten, q):
        with jax.named_scope('arrive'):
            for link in (0, 1):
                wait(slot_of(ten, q, link), q_recv.at[q, link, ten])
            pl.semaphore_wait(room.at[ten], 1)
            forward_copy(ten, q).start()
            pltpu.make_async_copy(tok_b[ten].at[q], tile_part(ten, q, j), ld.at[ten, lax.rem(q, 2)]).start()

        @pl.when(q < 4)
        def _():
            for link in (0, 1):
                relay_copy(ten, q, link).start()

    def landed(ten, q):
        with jax.named_scope('landed'):
            wait(tile_part(ten, q, j), ld.at[ten, lax.rem(q, 2)])
            wait(tile_part(ten, q, 1 - j), f_recv.at[q, ten])

    def rows_of(r):
        return pl.ds(pl.multiple_of(r * tile, tile), tile)

    def load_a(ten, n):
        own = lax.div(n, 2)
        slot = lax.rem(n, 2)

        @pl.when(own == 1)
        def _():
            pltpu.make_async_copy(tok[ten].at[rows_of(slot), :], tok_t[ten].at[slot], ld.at[ten, slot]).start()

        @pl.when(own == 0)
        def _():
            pltpu.make_async_copy(tok_p[ten].at[rows_of(slot), :], tok_t[ten].at[slot], ld.at[ten, slot]).start()

    def loaded(ten, slot):
        with jax.named_scope('ld'):
            wait(tok_t[ten].at[slot], ld.at[ten, slot])

    def unit_col(u):
        mine = cy * units
        other = (1 - cy) * units
        low = cx * rest_units
        high = (1 - cx) * near_units
        a = near_units
        col = jnp.where(u < a, mine + low + u,
                        jnp.where(u < units, mine + high + (u - a),
                                  jnp.where(u < units + a, other + low + (u - units), other + high + (u - units - a))))
        return pl.multiple_of(col * LANES, LANES)

    def chunk(s, way):
        n = lax.rem(s, steps)
        row = pl.multiple_of(way * tile + lax.rem(n, 2) * part_rows, part_rows)
        return lax.div(s, steps), pl.ds(row, part_rows), pl.ds(unit_col(lax.div(n, 2)), LANES)

    def sum_copy(s, way, nxt):
        land = lax.rem(s, DEPTH)
        return send(yacc.at[chunk(s, way)], rbuf.at[way, land], rs_send.at[way, lax.rem(s, SLOTS)], rs_recv.at[way, land], tp=nxt)

    def done_copy(s, way, prv):
        ref = back.at[way, lax.rem(s, KEEP)]
        return send(ref, ref, ag_send.at[way, lax.rem(s, LAG + 1)], ag_recv.at[way, lax.rem(s, KEEP)], tp=prv)

    def store_copy(s, way):
        return pltpu.make_async_copy(back.at[way, lax.rem(s, KEEP)], yd_ref.at[chunk(s, way)],
                                     fin_own.at[way, lax.rem(s, LAG + 1)])

    def tick(tau):
        with jax.named_scope('tick'):
            tick_body(tau)

    def give(s, way, p, prv):
        @pl.when(s >= LAG)
        def _():
            store_copy(s - LAG, way).wait()

            @pl.when(p > 0)
            def _():
                wait(back.at[way, 0], ag_send.at[way, lax.rem(s - LAG, LAG + 1)])

        store_copy(s, way).start()

        @pl.when(p > 0)
        def _():
            done_copy(s, way, prv).start()

    def tick_body(tau):
        for way in (0, 1):
            p = t if way == 0 else 3 - t
            nxt = t + 1 if way == 0 else t - 1
            prv = t - 1 if way == 0 else t + 1
            s = tau - HOP * p
            slot = lax.rem(jnp.maximum(s, 0), SLOTS)
            land = lax.rem(jnp.maximum(s, 0), DEPTH)
            live = jnp.logical_and(s >= 0, s < 2 * steps)

            @pl.when(jnp.logical_and(live, p > 0))
            def _():
                wait(rbuf.at[way, land], rs_recv.at[way, land])

            @pl.when(jnp.logical_and(live, p < 3))
            def _():
                @pl.when(s >= SLOTS)
                def _():
                    wait(rbuf.at[way, 0], rs_send.at[way, slot])

                @pl.when(p > 0)
                def _():
                    here = chunk(s, way)
                    yacc[here] = yacc[here] + rbuf[way, land]

                sum_copy(s, way, nxt).start()

            @pl.when(jnp.logical_and(live, p == 3))
            def _():
                back[way, lax.rem(s, KEEP)] = (yacc[chunk(s, way)] + rbuf[way, land]).astype(BF16)
                give(s, way, p, prv)

        for way in (0, 1):
            p = t if way == 0 else 3 - t
            prv = t - 1 if way == 0 else t + 1
            s = tau - HOP * (6 - p)

            @pl.when(jnp.logical_and(jnp.logical_and(s >= 0, s < 2 * steps), p < 3))
            def _():
                keep = lax.rem(s, KEEP)
                wait(back.at[way, keep], ag_recv.at[way, keep])
                give(s, way, p, prv)

    def ticks(lo, hi):
        def body(n, c):
            tick(n)
            return c

        lax.fori_loop(lo, hi, body, 0)

    def drain_sums():
        for way in (0, 1):
            p = t if way == 0 else 3 - t

            @pl.when(p < 3)
            def _():
                for slot in range(SLOTS):
                    wait(rbuf.at[way, 0], rs_send.at[way, slot])

            for m in range(LAG):
                s = 2 * steps - LAG + m
                wait(back.at[way, 0], fin_own.at[way, s % (LAG + 1)])

                @pl.when(p > 0)
                def _():
                    wait(back.at[way, 0], ag_send.at[way, s % (LAG + 1)])

    w_start(0)
    w_start(1)
    for ten in (0, 1):
        own_copy(ten).start()
    base = jnp.where(t == 0, 1.0, 0.0).astype(F32)

    with jax.named_scope('clear'):
        for r in (0, 1):
            for ten in (0, 1):
                load_a(ten, 2 + r)

        def clear(n, carry):
            at = pl.ds(pl.multiple_of(n * 32, 32), 32)
            acc_gu[at, :] = jnp.zeros((32, 2 * half), F32)
            acc_d[at, :] = jnp.zeros((32, half), F32)
            return carry

        lax.fori_loop(0, win // 32, clear, 0)

        def clear_ab(n, carry):
            lo = pl.ds(pl.multiple_of(n * group, group), group)
            for m in range(4):
                ab_all[m, lo, :] = jnp.zeros((group, 2 * half), F32)
            return carry

        lax.fori_loop(0, tile // group, clear_ab, 0)
        for r in (0, 1):
            for ten in (0, 1):
                loaded(ten, r)

                def residual(n, carry):
                    lo = pl.ds(pl.multiple_of(n * group, group), group)
                    there = pl.ds(pl.multiple_of(r * tile + n * group, group), group)
                    yacc[ten, there, :] = tok_t[ten][r, lo, :].astype(F32) * base
                    return carry

                lax.fori_loop(0, tile // group, residual, 0)
        for ten in (0, 1):
            wait(tok_p[ten], own_recv.at[ten])

    with jax.named_scope('w_relay'):
        w_relay(0)
        w_relay(1)
    w_start(2)

    def side(n):
        return pl.ds(pl.multiple_of(lax.rem(n, 2) * half, LANES), half)

    def ab_pass(last):
        other = (1 - cy) * line
        if last:
            parts = ((other + (1 - cx) * near_units * LANES, rest_units * LANES),)
        else:
            parts = ((cy * line, line), (other + cx * rest_units * LANES, near_units * LANES))
        load_a(0, 0)

        def body(n, carry):
            slot = lax.rem(n, 2)

            @pl.when(n < 3)
            def _():
                load_a(0, n + 1)

            loaded(0, slot)
            for at, size in parts:
                at_k = pl.ds(pl.multiple_of(at, LANES), size)
                with jax.named_scope('ab_part'):
                    for lo, hi in pieces:
                        ab_all[n, :, lo:hi] += dot_nn(xt[slot, :, at_k], w_gu[at_k, lo:hi])

            if last:
                def hidden(m, c):
                    lo = pl.ds(pl.multiple_of(m * group, group), group)
                    a = ab_all[n, lo, :half]
                    h_all[lax.div(n, 2), lo, side(n)] = (a * sigmoid(a) * ab_all[n, lo, half:]).astype(BF16)
                    return c

                lax.fori_loop(0, tile // group, hidden, 0)
            return carry

        lax.fori_loop(0, 4, body, 0)

    with jax.named_scope('w_have'):
        for k in (0, 1):
            w_have(k, 'chip')
            w_have(k, 'x')
            w_have(k, 'y')
    ab_pass(0)
    with jax.named_scope('w_have'):
        for k in (0, 1):
            w_have(k, 'far')
    ab_pass(1)

    def y_group(g, tau):
        u0 = (0, near_units, units, units + near_units)[g]
        n_u = (near_units, rest_units)[g % 2]
        col = unit_col(u0)
        cols = pl.ds(col, n_u * LANES)

        def theirs(r, carry):
            if g > 0:
                before = (near_units, rest_units)[(g - 1) % 2] * LANES
                wait(sb.at[r, :, pl.ds(0, before)], y_send.at[(g - 1) % 2, r])
            with jax.named_scope('y_dot'):
                sb[r, :, :n_u * LANES] = dot_nt(h_all[0, :, side(r)], w_d[cols, :])
            send(sb.at[r, :, pl.ds(0, n_u * LANES)], pbuf.at[rows_of(r), cols],
                 y_send.at[g % 2, r], y_recv.at[g, r], dp=partner).start()
            return carry

        def ours(r, carry):
            with jax.named_scope('y_wait'):
                wait(pbuf.at[rows_of(r), cols], y_recv.at[g, r])
            with jax.named_scope('y_dot'):
                yacc[0, rows_of(r), cols] = (yacc[0, rows_of(r), cols] + pbuf[rows_of(r), cols]
                                             + dot_nt(h_all[1, :, side(r)], w_d[cols, :]))
            pl.semaphore_signal(credit, inc=1, device_id={'dp': partner, 'tp': t}, device_id_type=MESH)
            return carry

        lax.fori_loop(0, 2, theirs, 0)
        if g > 0:
            tick(tau)
        lax.fori_loop(0, 2, ours, 0)
        if g > 0:
            tick(tau + 1)

    load_a(1, 0)
    load_a(0, 0)
    with jax.named_scope('w_have2'):
        w_have(2, 'chip')
    y_group(0, 0)
    tick(0)
    with jax.named_scope('w_relay2'):
        w_relay(2)
    q_start(0)
    q_start(1)
    ticks(1, 7)
    with jax.named_scope('w_have2'):
        w_have(2, 'x')
        w_have(2, 'y')
    y_group(1, 7)
    y_group(2, 9)
    q_start(2)
    ticks(11, 14)
    with jax.named_scope('w_have2'):
        w_have(2, 'far')
    y_group(3, 14)
    q_start(3)

    at_win, shift = window_of(chip * 2 * blk, win)
    own = own_window(blk)
    at_own, _ = window_of(me * blk, own)
    in_acc = pl.ds(pl.multiple_of(window_of(me * blk, own)[0].start - at_win.start, 8), own)
    n_block = 3
    n_cols = model // n_block

    def grad_copies():
        rows_ = pl.ds(pl.multiple_of(shift + (1 - j) * blk, 8), blk)
        there = pl.ds(pl.multiple_of(window_of(partner * blk, own)[1], 8), blk)
        return (send(acc_gu.at[rows_, :], pbuf.at[there, pl.ds(0, 2 * half)], out_send.at[0], out_recv.at[0], dp=partner),
                send(acc_d.at[rows_, :], yacc.at[0, there, pl.ds(0, half)], out_send.at[1], out_recv.at[1], dp=partner))

    def last_copies():
        return (send(h_all.at[1], xt.at[0, :, pl.ds(0, 2 * half)], h_send.at[0], h_recv.at[0], dp=partner),
                send(h_all.at[0, :, pl.ds(0, half)], dyt.at[0, :, pl.ds(0, half)], h_send.at[1], h_recv.at[1], dp=partner))

    def dx_tile(n):
        r = lax.rem(n, 2)

        @pl.when(n == 0)
        def _():
            pl.semaphore_wait(credit, 8)
            for r_ in (0, 1):
                wait(sb.at[r_, :, pl.ds(0, rest_units * LANES)], y_send.at[1, r_])

        def block(m, carry):
            cols = pl.ds(pl.multiple_of(m * n_cols, n_cols), n_cols)
            slot = lax.rem(m + r * n_block, 2)

            @pl.when(jnp.logical_and(n < 2, m + r * n_block >= 2))
            def _():
                wait(sb.at[slot], dx_send.at[slot])

            @pl.when(n < 2)
            def _():
                with jax.named_scope('dx_dot'):
                    sb[slot] = dot_nt(h_all[1], w_gu[cols, :])
                send(sb.at[slot], pbuf.at[rows_of(r), cols], dx_send.at[slot], dx_recv.at[r, m], dp=partner).start()

            @pl.when(n >= 2)
            def _():
                with jax.named_scope('dx_wait'):
                    wait(pbuf.at[rows_of(r), cols], dx_recv.at[r, m])
                with jax.named_scope('dx_dot'):
                    yacc[1, rows_of(r), cols] = (yacc[1, rows_of(r), cols] + pbuf[rows_of(r), cols]
                                                 + dot_nt(h_all[1], w_gu[cols, :]))

            @pl.when(m >= 1)
            def _():
                tick(17 + 4 * n + m)
            return carry

        lax.fori_loop(0, n_block, block, 0)

    def grad_tile(n, carry):
        q = n - 4
        slot = lax.rem(n, 2)
        at = jnp.where(n < 4, n, slot)
        final = n == 15
        early = jnp.logical_and(n >= 3, q + 1 <= EARLY)
        late = jnp.logical_and(n < 15, q + 1 > EARLY)
        dense = q >= 8
        tau = jnp.where(dense, 64 + 5 * (q - 8), 16 + 4 * n)

        @pl.when(n < 4)
        def _():
            q_start(4 + n)
            loaded(0, slot)

        @pl.when(n >= 4)
        def _():
            landed(0, q)
            with jax.named_scope('ab_dot'):
                ab_all[at, :, :cut] = dot_nn(xt[slot], w_gu[:, :cut])
            tick(tau)
            with jax.named_scope('ab_dot'):
                ab_all[at, :, cut:] = dot_nn(xt[slot], w_gu[:, cut:])

            @pl.when(final)
            def _():
                arrive(1, q)

            tick(tau + 1)

        @pl.when(early)
        def _():
            arrive(0, q + 1)
            arrive(1, q + 1)

        @pl.when(n < 4)
        def _():
            loaded(1, slot)

        @pl.when(n >= 4)
        def _():
            landed(1, q)

        with jax.named_scope('g_dot'):
            g_s[...] = dot_nn(dyt[slot], w_d[...])

        @pl.when(dense)
        def _():
            tick(tau + 2)

        with jax.named_scope('act'):
            def body(m, c):
                lo = pl.ds(pl.multiple_of(m * group, group), group)
                a = ab_all[at, lo, :half]
                b = ab_all[at, lo, half:]
                g = g_s[lo, :]
                s = sigmoid(a)
                silu = a * s
                h_all[0, lo, :half] = (silu * b).astype(BF16)
                h_all[1, lo, :half] = (g * b * s * (1.0 + a * (1.0 - s))).astype(BF16)
                h_all[1, lo, half:] = (g * silu).astype(BF16)
                return c

            lax.fori_loop(0, tile // group, body, 0)
        tick(tau + jnp.where(n < 4, 0, jnp.where(dense, 3, 2)))

        @pl.when(n < 3)
        def _():
            load_a(0, n + 1)
            load_a(1, n + 1)

        @pl.when(late)
        def _():
            arrive(0, q + 1)

        @pl.when(jnp.logical_not(final))
        def _():
            with jax.named_scope('dw_dot'):
                for lo in range(0, 2 * half, 2 * half // 3):
                    hi = lo + 2 * half // 3
                    acc_gu[:, lo:hi] += dot_tn(xt[slot, :, at_win], h_all[1, :, lo:hi])
            with jax.named_scope('dw_dot2'):
                for lo, hi in ((0, half // 2 // 128 * 128), (half // 2 // 128 * 128, half)):
                    acc_d[:, lo:hi] += dot_tn(dyt[slot, :, at_win], h_all[0, :, lo:hi])

        @pl.when(n == 14)
        def _():
            for copy in grad_copies():
                copy.start()

        @pl.when(final)
        def _():
            for ten in (0, 1):
                pl.semaphore_wait(room.at[ten], 1)
            for copy in last_copies():
                copy.start()
            with jax.named_scope('grads_sent'):
                for copy in grad_copies():
                    copy.wait_send()
            with jax.named_scope('dw_own'):
                for lo, hi in pieces:
                    acc_gu[in_acc, lo:hi] += dot_tn(xt[1, :, at_own], h_all[1, :, lo:hi])
                acc_d[in_acc, :] += dot_tn(dyt[1, :, at_own], h_all[0, :, :half])

        @pl.when(jnp.logical_and(n >= 2, n < 15))
        def _():
            for ten in (0, 1):
                pl.semaphore_signal(room.at[ten], inc=1, device_id={'dp': partner, 'tp': t}, device_id_type=MESH)

        tick(tau + jnp.where(n < 4, 1, jnp.where(dense, 4, 3)))

        @pl.when(n < 4)
        def _():
            dx_tile(n)

        @pl.when(jnp.logical_and(late, n < 14))
        def _():
            arrive(1, q + 1)
        return carry

    lax.fori_loop(0, 16, grad_tile, 0)

    with jax.named_scope('last_wait'):
        theirs = pl.ds(pl.multiple_of(window_of(me * blk, own)[1], 8), blk)
        wait(pbuf.at[theirs, pl.ds(0, 2 * half)], out_recv.at[0])
        wait(yacc.at[0, theirs, pl.ds(0, half)], out_recv.at[1])
        wait(xt.at[0, :, pl.ds(0, 2 * half)], h_recv.at[0])
        wait(dyt.at[0, :, pl.ds(0, half)], h_recv.at[1])
    with jax.named_scope('dw_other'):
        for lo, hi in pieces:
            pbuf[:own, lo:hi] += dot_tn(xt[1, :, at_own], xt[0, :, lo:hi])
        yacc[0, :own, :half] += dot_tn(dyt[1, :, at_own], dyt[0, :, :half])

    with jax.named_scope('drain_sums'):
        drain_sums()
    with jax.named_scope('drain'):
        for slot in (0, 1):
            wait(sb.at[slot], dx_send.at[slot])
        for k in range(3):
            for core in (0, 1):
                for link in (0, 1):
                    for part in (0, 1):
                        w_copy(k, link, part, core).wait_send()
                    w_relay_copy(k, link, core).wait_send()
            w_partner_copy(k).wait_send()
        for ten in (0, 1):
            own_copy(ten).wait_send()

        def drain(q, carry):
            for ten in (0, 1):
                wait(tok_b[ten].at[0], f_send.at[q, ten])
                for link in (0, 1):
                    @pl.when(q < 8)
                    def _():
                        wait(slot_of(ten, 0, link), q_send.at[lax.rem(q, 8), link, ten])

                    @pl.when(q < 4)
                    def _():
                        wait(slot_of(ten, 0, link), rl_send.at[lax.rem(q, 4), link, ten])

            return carry

        lax.fori_loop(0, 12, drain, 0)
        for copy in last_copies():
            copy.wait_send()


def window_of(start, size):
    first = lax.div(start, LANES) * LANES
    return pl.ds(pl.multiple_of(first, LANES), size), start - first


def own_window(blk):
    return -(-(blk + LANES - 32) // LANES) * LANES


def window(model, blk):
    starts = [(2 * blk * c) // LANES * LANES for c in range(model // (2 * blk))]
    shift = max(2 * blk * c - s for c, s in enumerate(starts))
    return -(-(shift + 2 * blk) // LANES) * LANES


def mlp(x, dy, wg, wu, wd):
    rows, model = x.shape
    blk, width = wg.shape
    half = width // 2
    tile = rows // 2
    dma = pltpu.SemaphoreType.DMA
    vmem = pltpu.VMEM
    anywhere = pl.BlockSpec(memory_space=pl.ANY)
    shape = jax.ShapeDtypeStruct
    flops = 2 * model * half * rows * 2 * 20
    win = window(model, blk)
    most = max(rows, own_window(blk))
    kept = (vmem((win, 2 * half), F32), vmem((win, half), F32), vmem((most, model), F32), vmem((2, most, model), F32))
    held = sum(4 * math.prod(k.shape) for k in kept)
    in_vmem = pl.BlockSpec(memory_space=pltpu.VMEM)
    return pl.pallas_call(
        kernel,
        name='mlp',
        out_shape=(shape((2, rows, model), BF16), *kept,
                   shape((12, tile // 2, model), BF16), shape((12, tile // 2, model), BF16),
                   shape((rows, model), BF16), shape((rows, model), BF16)),
        in_specs=[anywhere] * 5,
        out_specs=(anywhere, *[in_vmem] * 4, *[anywhere] * 4),
        scratch_shapes=[
            vmem((model, 2 * half), BF16),
            vmem((model, half), BF16),
            vmem((2, tile, model // 3), F32),
            vmem((2, tile, model), BF16),
            vmem((2, tile, model), BF16),
            vmem((4, tile, 2 * half), F32),
            vmem((tile, half), F32),
            vmem((2, tile, 2 * half), BF16),
            vmem((2, DEPTH, tile // 2, LANES), F32),
            vmem((2, KEEP, tile // 2, LANES), BF16),
            dma((3, 2, 2, 2)), dma((3, 2, 2, 2)), dma((3, 2, 2)), dma((3, 2, 2)), dma((3,)), dma((3,)), dma((3,)),
            dma((2,)), dma((2,)), dma((8, 2, 2)), dma((12, 2, 2)), dma((4, 2, 2)), dma((12, 2)), dma((12, 2)),
            dma((2, 2)), dma((4, 2)), dma((2,)), dma((2, 3)), pltpu.SemaphoreType.REGULAR, pltpu.SemaphoreType.REGULAR((2,)),
            dma((2, SLOTS)), dma((2, DEPTH)), dma((2, LAG + 1)), dma((2, KEEP)), dma((2, LAG + 1)),
            dma((2, 2)), dma((2,)), dma((2,)), dma((2,)), dma((2,)),
        ],
        compiler_params=pltpu.CompilerParams(collective_id=0, has_side_effects=True, vmem_limit_bytes=67_000_000 - held),
        cost_estimate=pl.CostEstimate(flops=flops, bytes_accessed=100_000_000, transcendentals=0),
    )(x, dy, wg, wu, wd)


def results_kernel(blk, half, yd_ref, acc_gu, acc_d, pbuf, yacc, y_out, dx_out, g_out, u_out, d_out, yd_s, load, store, grad):
    me = lax.axis_index('dp')
    j = lax.rem(me, 2)
    chip = lax.div(me, 2)
    mine = pl.ds(pl.multiple_of(window_of(chip * 2 * blk, 128)[1] + j * blk, 8), blk)
    other = pl.ds(pl.multiple_of(window_of(me * blk, 128)[1], 8), blk)
    own_cols = pl.ds(pl.multiple_of(j * half, LANES), half)
    other_cols = pl.ds(pl.multiple_of((1 - j) * half, LANES), half)
    low, high = pl.ds(0, half), pl.ds(half, half)
    rows = yd_ref.shape[1] // 4
    parts = []
    for m in range(4):
        for ten, dst in ((0, y_out), (1, dx_out)):
            at = pl.ds(m * rows, rows)
            parts.append((yd_ref.at[ten, at, :], yd_s.at[ten, at, :], dst.at[at, :]))
    grads = ((acc_gu.at[mine, low], g_out.at[:, own_cols]), (acc_gu.at[mine, high], u_out.at[:, own_cols]),
             (acc_d.at[mine, :], d_out.at[:, own_cols]),
             (pbuf.at[other, low], g_out.at[:, other_cols]), (pbuf.at[other, high], u_out.at[:, other_cols]),
             (yacc.at[0, other, low], d_out.at[:, other_cols]))
    for n, (src, buf, dst) in enumerate(parts):
        pltpu.make_async_copy(src, buf, load.at[n]).start()
    for n, (src, dst) in enumerate(grads):
        pltpu.make_async_copy(src, dst, grad.at[n]).start()
    for n, (src, buf, dst) in enumerate(parts):
        pltpu.make_async_copy(src, buf, load.at[n]).wait()
        pltpu.make_async_copy(buf, dst, store.at[n]).start()
    for n, (src, buf, dst) in enumerate(parts):
        pltpu.make_async_copy(buf, dst, store.at[n]).wait()
    for n, (src, dst) in enumerate(grads):
        pltpu.make_async_copy(src, dst, grad.at[n]).wait()


def results(blk, width, yd, *kept):
    anywhere = pl.BlockSpec(memory_space=pl.ANY)
    in_vmem = pl.BlockSpec(memory_space=pltpu.VMEM)
    shape = jax.ShapeDtypeStruct
    dma = pltpu.SemaphoreType.DMA
    yd = pltpu.with_memory_space_constraint(yd, pltpu.HBM)
    kept = [pltpu.with_memory_space_constraint(k, pltpu.VMEM) for k in kept]
    return pl.pallas_call(
        functools.partial(results_kernel, blk, width // 2),
        name='results',
        out_shape=(shape(yd.shape[1:], yd.dtype), shape(yd.shape[1:], yd.dtype),
                   shape((blk, width), F32), shape((blk, width), F32), shape((blk, width), F32)),
        in_specs=[pl.BlockSpec(memory_space=pltpu.HBM), *[in_vmem] * 4],
        out_specs=tuple([anywhere] * 5),
        scratch_shapes=[pltpu.VMEM(yd.shape, yd.dtype), dma((8,)), dma((8,)), dma((6,))],
        compiler_params=pltpu.CompilerParams(vmem_limit_bytes=12_000_000),
    )(yd, *kept)


def solution(mesh):
    def device_pass(x_rows, gate_blk, up_blk, down_blk, dy_rows):
        out = mlp(x_rows, dy_rows, gate_blk, up_blk, down_blk.T)
        y, dx, dw_gate, dw_up, dw_down = results(*gate_blk.shape, *out[:5])
        return y, dx, dw_gate, dw_up, dw_down.T

    row_spec = P('dp', None)
    weight_spec = P('dp', 'tp')
    down_spec = P('tp', 'dp')
    return jax.shard_map(device_pass, mesh=mesh,
                         in_specs=(row_spec, weight_spec, weight_spec, down_spec, row_spec),
                         out_specs=(row_spec, row_spec, weight_spec, weight_spec, down_spec),
                         check_vma=False)
```

```python
import functools
import math

import jax
import jax.numpy as jnp
from jax import lax
from jax.experimental import pallas as pl
from jax.experimental.pallas import tpu as pltpu
from jax.sharding import PartitionSpec as P

F32 = jnp.float32
BF16 = jnp.bfloat16
MESH = pl.DeviceIdType.MESH
SLOTS = 8
DEPTH = 13
KEEP = 16
LAG = 3
HOP = 2
LANES = 128
EARLY = 6
MIDDLE = 7


def dot_nn(a, b):
    return jnp.dot(a, b, preferred_element_type=F32)


def dot_nt(a, b):
    return lax.dot_general(a, b, (((1,), (1,)), ((), ())), preferred_element_type=F32)


def dot_tn(a, b):
    return lax.dot_general(a, b, (((0,), (0,)), ((), ())), preferred_element_type=F32)


def sigmoid(a):
    return 1.0 / (1.0 + jnp.exp(-a))


def kernel(x_ref, dy_ref, wg_ref, wu_ref, wd_ref,
           yd_ref, acc_gu, acc_d, pbuf, yacc, xb, dyb, xp, dyp,
           w_gu, w_d, sb, xt, dyt, ab_all, g_s, h_all, rbuf, back,
           w_send, w_recv, wr_send, wr_recv, w_own, wp_send, wp_recv,
           own_send, own_recv, q_send, q_recv, rl_send, f_send, f_recv,
           y_send, y_recv, dx_send, dx_recv, credit, room,
           rs_send, rs_recv, ag_send, ag_recv, fin_own, ld, out_send, out_recv, h_send, h_recv):
    rows, model = x_ref.shape
    blk, width = wg_ref.shape
    half = width // 2
    hb = blk // 2
    tile = rows // 2
    piece = tile // 4
    win = acc_d.shape[0]
    line = model // 2
    units = line // LANES
    near_units = (2 * blk - LANES // 2) // LANES if (2 * blk) % LANES else 2 * blk // LANES
    rest_units = units - near_units
    steps = 4 * units
    part_rows = tile // 2
    group = min(32, tile)
    w_in = (wg_ref, wu_ref, wd_ref)
    cut = (half + 255) // 256 * 256
    pieces = ((0, cut), (cut, 2 * half))
    tok = (x_ref, dy_ref)
    tok_b = (xb, dyb)
    tok_p = (xp, dyp)
    tok_t = (xt, dyt)

    t = lax.axis_index('tp')
    me = lax.axis_index('dp')
    cy = lax.div(me, 4)
    cx = lax.rem(lax.div(me, 2), 2)
    j = lax.rem(me, 2)
    partner = me + 1 - 2 * j
    chip = cy * 2 + cx

    def near(link, core):
        if link == 0:
            return cy * 4 + (1 - cx) * 2 + core
        return (1 - cy) * 4 + cx * 2 + core

    def far(core):
        return (1 - cy) * 4 + (1 - cx) * 2 + core

    def send(src, dst, s_sem, r_sem, dp=None, tp=None):
        where = {'dp': me if dp is None else dp, 'tp': t if tp is None else tp}
        return pltpu.make_async_remote_copy(src_ref=src, dst_ref=dst, send_sem=s_sem, recv_sem=r_sem,
                                            device_id=where, device_id_type=MESH)

    def wait(ref, sem):
        pltpu.make_async_copy(ref, ref, sem).wait()

    barrier = pltpu.get_barrier_semaphore()
    for peer in (partner, near(0, 0), near(0, 1), near(1, 0), near(1, 1)):
        pl.semaphore_signal(barrier, inc=1, device_id={'dp': peer, 'tp': t}, device_id_type=MESH)

    @pl.when(t > 0)
    def _():
        pl.semaphore_signal(barrier, inc=1, device_id={'dp': me, 'tp': t - 1}, device_id_type=MESH)

    @pl.when(t < 3)
    def _():
        pl.semaphore_signal(barrier, inc=1, device_id={'dp': me, 'tp': t + 1}, device_id_type=MESH)

    pl.semaphore_wait(barrier, 5 + jnp.minimum(t, 1) + jnp.minimum(3 - t, 1))

    def w_rows(k, dev, part=None):
        if part is None:
            at = pl.ds(pl.multiple_of(dev * blk, 16), blk)
        else:
            at = pl.ds(pl.multiple_of(dev * blk + part * hb, 16), hb)
        if k == 2:
            return w_d.at[at, :]
        return w_gu.at[at, pl.ds(k * half, half)]

    def w_cols(core):
        return pl.ds(pl.multiple_of(core * half, LANES), half)

    def w_copy(k, link, part, core):
        return send(w_in[k].at[pl.ds(part * hb, hb), w_cols(core)], w_rows(k, me, part),
                    w_send.at[k, link, part, core], w_recv.at[k, link, part, j], dp=near(link, core))

    def w_own_copy(k):
        return pltpu.make_async_copy(w_in[k].at[:, w_cols(j)], w_rows(k, me), w_own.at[k])

    def w_partner_copy(k):
        return send(w_in[k].at[:, w_cols(1 - j)], w_rows(k, me), wp_send.at[k], wp_recv.at[k], dp=partner)

    def w_start(k):
        for first in (0, 1):
            for core in (0, 1):
                w_copy(k, 0, 1 - first, core).start()
                w_copy(k, 1, first, core).start()
        w_own_copy(k).start()
        w_partner_copy(k).start()

    def w_relay_copy(k, link_out, core):
        part = 1 if link_out == 1 else 0
        ref = w_rows(k, near(1 - link_out, core), part)
        return send(ref, ref, wr_send.at[k, link_out, core], wr_recv.at[k, link_out, core], dp=near(link_out, j))

    def w_relay(k):
        for core in (0, 1):
            wait(w_rows(k, near(0, core), 1), w_recv.at[k, 0, 1, core])
            w_relay_copy(k, 1, core).start()
            wait(w_rows(k, near(1, core), 0), w_recv.at[k, 1, 0, core])
            w_relay_copy(k, 0, core).start()

    def w_have(k, which):
        if which == 'chip':
            wait(w_rows(k, me), w_own.at[k])
            wait(w_rows(k, partner), wp_recv.at[k])
        for core in (0, 1):
            if which == 'x':
                wait(w_rows(k, near(0, core), 0), w_recv.at[k, 0, 0, core])
            if which == 'y':
                wait(w_rows(k, near(1, core), 1), w_recv.at[k, 1, 1, core])
            if which == 'far':
                wait(w_rows(k, far(core), 0), wr_recv.at[k, 0, core])
                wait(w_rows(k, far(core), 1), wr_recv.at[k, 1, core])

    def slot_of(ten, q, link):
        return tok_b[ten].at[q, pl.ds(link * piece, piece), :]

    def q_copy(ten, q, link):
        b = lax.div(q, 4)
        sub = lax.rem(q, 4)
        first = 1 - b if link == 0 else b
        src = tok[ten].at[pl.ds(pl.multiple_of(first * tile + sub * piece, piece), piece), :]
        return send(src, slot_of(ten, q, link), q_send.at[q, link, ten], q_recv.at[q, link, ten], dp=near(link, j))

    def q_start(q):
        for ten in (0, 1):
            for link in (0, 1):
                q_copy(ten, q, link).start()

    def relay_copy(ten, sub, link_out):
        return send(slot_of(ten, sub, 1 - link_out), slot_of(ten, 8 + sub, link_out),
                    rl_send.at[sub, link_out, ten], q_recv.at[8 + sub, link_out, ten], dp=near(link_out, j))

    def tile_part(ten, q, core):
        return tok_t[ten].at[lax.rem(q, 2), pl.ds(pl.multiple_of(core * 2 * piece, 2 * piece), 2 * piece), :]

    def forward_copy(ten, q):
        return send(tok_b[ten].at[q], tile_part(ten, q, j), f_send.at[q, ten], f_recv.at[q, ten], dp=partner)

    def own_copy(ten):
        return send(tok[ten], tok_p[ten], own_send.at[ten], own_recv.at[ten], dp=partner)

    def arrive(ten, q):
        with jax.named_scope('arrive'):
            for link in (0, 1):
                wait(slot_of(ten, q, link), q_recv.at[q, link, ten])
            if ten == 0:
                pl.semaphore_wait(room.at[0], 1)
            else:
                @pl.when(q < 11)
                def _():
                    pl.semaphore_wait(room.at[1], 1)

            forward_copy(ten, q).start()
            pltpu.make_async_copy(tok_b[ten].at[q], tile_part(ten, q, j), ld.at[ten, lax.rem(q, 2)]).start()

        @pl.when(q < 4)
        def _():
            for link in (0, 1):
                relay_copy(ten, q, link).start()

    def landed(ten, q):
        with jax.named_scope('landed'):
            wait(tile_part(ten, q, j), ld.at[ten, lax.rem(q, 2)])
            wait(tile_part(ten, q, 1 - j), f_recv.at[q, ten])

    def rows_of(r):
        return pl.ds(pl.multiple_of(r * tile, tile), tile)

    def load_a(ten, n):
        own = lax.div(n, 2)
        slot = lax.rem(n, 2)

        @pl.when(own == 1)
        def _():
            pltpu.make_async_copy(tok[ten].at[rows_of(slot), :], tok_t[ten].at[slot], ld.at[ten, slot]).start()

        @pl.when(own == 0)
        def _():
            pltpu.make_async_copy(tok_p[ten].at[rows_of(slot), :], tok_t[ten].at[slot], ld.at[ten, slot]).start()

    def loaded(ten, slot):
        with jax.named_scope('ld'):
            wait(tok_t[ten].at[slot], ld.at[ten, slot])

    def unit_col(u):
        mine = cy * units
        other = (1 - cy) * units
        low = cx * rest_units
        high = (1 - cx) * near_units
        a = near_units
        col = jnp.where(u < a, mine + low + u,
                        jnp.where(u < units, mine + high + (u - a),
                                  jnp.where(u < units + a, other + low + (u - units), other + high + (u - units - a))))
        return pl.multiple_of(col * LANES, LANES)

    def chunk(s, way):
        n = lax.rem(s, steps)
        row = pl.multiple_of(way * tile + lax.rem(n, 2) * part_rows, part_rows)
        return lax.div(s, steps), pl.ds(row, part_rows), pl.ds(unit_col(lax.div(n, 2)), LANES)

    def sum_copy(s, way, nxt):
        land = lax.rem(s, DEPTH)
        return send(yacc.at[chunk(s, way)], rbuf.at[way, land], rs_send.at[way, lax.rem(s, SLOTS)], rs_recv.at[way, land], tp=nxt)

    def done_copy(s, way, prv):
        ref = back.at[way, lax.rem(s, KEEP)]
        return send(ref, ref, ag_send.at[way, lax.rem(s, LAG + 1)], ag_recv.at[way, lax.rem(s, KEEP)], tp=prv)

    def store_copy(s, way):
        return pltpu.make_async_copy(back.at[way, lax.rem(s, KEEP)], yd_ref.at[chunk(s, way)],
                                     fin_own.at[way, lax.rem(s, LAG + 1)])

    def tick(tau):
        with jax.named_scope('tick'):
            tick_body(tau)

    def give(s, way, p, prv):
        @pl.when(s >= LAG)
        def _():
            store_copy(s - LAG, way).wait()

            @pl.when(p > 0)
            def _():
                wait(back.at[way, 0], ag_send.at[way, lax.rem(s - LAG, LAG + 1)])

        store_copy(s, way).start()

        @pl.when(p > 0)
        def _():
            done_copy(s, way, prv).start()

    def tick_body(tau):
        for way in (0, 1):
            p = t if way == 0 else 3 - t
            nxt = t + 1 if way == 0 else t - 1
            prv = t - 1 if way == 0 else t + 1
            s = tau - HOP * p
            slot = lax.rem(jnp.maximum(s, 0), SLOTS)
            land = lax.rem(jnp.maximum(s, 0), DEPTH)
            live = jnp.logical_and(s >= 0, s < 2 * steps)

            @pl.when(jnp.logical_and(live, p > 0))
            def _():
                wait(rbuf.at[way, land], rs_recv.at[way, land])

            @pl.when(jnp.logical_and(live, p < 3))
            def _():
                @pl.when(s >= SLOTS)
                def _():
                    wait(rbuf.at[way, 0], rs_send.at[way, slot])

                @pl.when(p > 0)
                def _():
                    here = chunk(s, way)
                    yacc[here] = yacc[here] + rbuf[way, land]

                sum_copy(s, way, nxt).start()

            @pl.when(jnp.logical_and(live, p == 3))
            def _():
                back[way, lax.rem(s, KEEP)] = (yacc[chunk(s, way)] + rbuf[way, land]).astype(BF16)
                give(s, way, p, prv)

        for way in (0, 1):
            p = t if way == 0 else 3 - t
            prv = t - 1 if way == 0 else t + 1
            s = tau - HOP * (6 - p)

            @pl.when(jnp.logical_and(jnp.logical_and(s >= 0, s < 2 * steps), p < 3))
            def _():
                keep = lax.rem(s, KEEP)
                wait(back.at[way, keep], ag_recv.at[way, keep])
                give(s, way, p, prv)

    def ticks(lo, hi):
        def body(n, c):
            tick(n)
            return c

        lax.fori_loop(lo, hi, body, 0)

    def drain_sums():
        for way in (0, 1):
            p = t if way == 0 else 3 - t

            @pl.when(p < 3)
            def _():
                for slot in range(SLOTS):
                    wait(rbuf.at[way, 0], rs_send.at[way, slot])

            for m in range(LAG):
                s = 2 * steps - LAG + m
                wait(back.at[way, 0], fin_own.at[way, s % (LAG + 1)])

                @pl.when(p > 0)
                def _():
                    wait(back.at[way, 0], ag_send.at[way, s % (LAG + 1)])

    w_start(0)
    w_start(1)
    for ten in (0, 1):
        own_copy(ten).start()
    base = jnp.where(t == 0, 1.0, 0.0).astype(F32)

    with jax.named_scope('clear'):
        for r in (0, 1):
            for ten in (0, 1):
                load_a(ten, 2 + r)

        def clear(n, carry):
            at = pl.ds(pl.multiple_of(n * 32, 32), 32)
            acc_gu[at, :] = jnp.zeros((32, 2 * half), F32)
            acc_d[at, :] = jnp.zeros((32, half), F32)
            return carry

        lax.fori_loop(0, win // 32, clear, 0)

        def clear_ab(n, carry):
            lo = pl.ds(pl.multiple_of(n * group, group), group)
            for m in range(4):
                ab_all[m, lo, :] = jnp.zeros((group, 2 * half), F32)
            return carry

        lax.fori_loop(0, tile // group, clear_ab, 0)
        for r in (0, 1):
            for ten in (0, 1):
                loaded(ten, r)

                def residual(n, carry):
                    lo = pl.ds(pl.multiple_of(n * group, group), group)
                    there = pl.ds(pl.multiple_of(r * tile + n * group, group), group)
                    yacc[ten, there, :] = tok_t[ten][r, lo, :].astype(F32) * base
                    return carry

                lax.fori_loop(0, tile // group, residual, 0)
        for ten in (0, 1):
            wait(tok_p[ten], own_recv.at[ten])

    with jax.named_scope('w_relay'):
        w_relay(0)
        w_relay(1)
    w_start(2)

    def side(n):
        return pl.ds(pl.multiple_of(lax.rem(n, 2) * half, LANES), half)

    def ab_pass(last):
        other = (1 - cy) * line
        if last:
            parts = ((other + (1 - cx) * near_units * LANES, rest_units * LANES),)
        else:
            parts = ((cy * line, line), (other + cx * rest_units * LANES, near_units * LANES))
        load_a(0, 0)

        def body(n, carry):
            slot = lax.rem(n, 2)

            @pl.when(n < 3)
            def _():
                load_a(0, n + 1)

            loaded(0, slot)
            for at, size in parts:
                at_k = pl.ds(pl.multiple_of(at, LANES), size)
                with jax.named_scope('ab_part'):
                    for lo, hi in pieces:
                        ab_all[n, :, lo:hi] += dot_nn(xt[slot, :, at_k], w_gu[at_k, lo:hi])

            if last:
                def hidden(m, c):
                    lo = pl.ds(pl.multiple_of(m * group, group), group)
                    a = ab_all[n, lo, :half]
                    h_all[lax.div(n, 2), lo, side(n)] = (a * sigmoid(a) * ab_all[n, lo, half:]).astype(BF16)
                    return c

                lax.fori_loop(0, tile // group, hidden, 0)
            return carry

        lax.fori_loop(0, 4, body, 0)

    with jax.named_scope('w_have'):
        for k in (0, 1):
            w_have(k, 'chip')
            w_have(k, 'x')
            w_have(k, 'y')
    ab_pass(0)
    with jax.named_scope('w_have'):
        for k in (0, 1):
            w_have(k, 'far')
    ab_pass(1)

    def y_group(g, tau):
        u0 = (0, near_units, units, units + near_units)[g]
        n_u = (near_units, rest_units)[g % 2]
        col = unit_col(u0)
        cols = pl.ds(col, n_u * LANES)

        def theirs(r, carry):
            if g > 0:
                before = (near_units, rest_units)[(g - 1) % 2] * LANES
                wait(sb.at[r, :, pl.ds(0, before)], y_send.at[(g - 1) % 2, r])
            with jax.named_scope('y_dot'):
                sb[r, :, :n_u * LANES] = dot_nt(h_all[0, :, side(r)], w_d[cols, :])
            send(sb.at[r, :, pl.ds(0, n_u * LANES)], pbuf.at[rows_of(r), cols],
                 y_send.at[g % 2, r], y_recv.at[g, r], dp=partner).start()
            return carry

        def ours(r, carry):
            with jax.named_scope('y_wait'):
                wait(pbuf.at[rows_of(r), cols], y_recv.at[g, r])
            with jax.named_scope('y_dot'):
                yacc[0, rows_of(r), cols] = (yacc[0, rows_of(r), cols] + pbuf[rows_of(r), cols]
                                             + dot_nt(h_all[1, :, side(r)], w_d[cols, :]))
            pl.semaphore_signal(credit, inc=1, device_id={'dp': partner, 'tp': t}, device_id_type=MESH)
            return carry

        lax.fori_loop(0, 2, theirs, 0)
        if g > 0:
            tick(tau)
        lax.fori_loop(0, 2, ours, 0)
        if g > 0:
            tick(tau + 1)

    load_a(1, 0)
    load_a(0, 0)
    with jax.named_scope('w_have2'):
        w_have(2, 'chip')
    y_group(0, 0)
    tick(0)
    with jax.named_scope('w_relay2'):
        w_relay(2)
    q_start(0)
    q_start(1)
    ticks(1, 7)
    with jax.named_scope('w_have2'):
        w_have(2, 'x')
        w_have(2, 'y')
    y_group(1, 7)
    y_group(2, 9)
    q_start(2)
    ticks(11, 14)
    with jax.named_scope('w_have2'):
        w_have(2, 'far')
    y_group(3, 14)
    q_start(3)

    at_win, shift = window_of(chip * 2 * blk, win)
    own = own_window(blk)
    at_own, _ = window_of(me * blk, own)
    in_acc = pl.ds(pl.multiple_of(window_of(me * blk, own)[0].start - at_win.start, 8), own)
    n_block = 3
    n_cols = model // n_block

    def grad_copy(m):
        rows_ = pl.ds(pl.multiple_of(shift + (1 - j) * blk, 8), blk)
        there = pl.ds(pl.multiple_of(window_of(partner * blk, own)[1], 8), blk)
        if m == 0:
            return send(acc_gu.at[rows_, :], pbuf.at[there, pl.ds(0, 2 * half)], out_send.at[0], out_recv.at[0], dp=partner)
        return send(acc_d.at[rows_, :], yacc.at[0, there, pl.ds(0, half)], out_send.at[1], out_recv.at[1], dp=partner)

    def last_copy(m):
        if m == 0:
            return send(h_all.at[1], xt.at[0, :, pl.ds(0, 2 * half)], h_send.at[0], h_recv.at[0], dp=partner)
        return send(h_all.at[0, :, pl.ds(0, half)], dyt.at[0, :, pl.ds(0, half)], h_send.at[1], h_recv.at[1], dp=partner)

    def dx_tile(n):
        r = lax.rem(n, 2)

        @pl.when(n == 0)
        def _():
            pl.semaphore_wait(credit, 8)
            for r_ in (0, 1):
                wait(sb.at[r_, :, pl.ds(0, rest_units * LANES)], y_send.at[1, r_])

        def block(m, carry):
            cols = pl.ds(pl.multiple_of(m * n_cols, n_cols), n_cols)
            slot = lax.rem(m + r * n_block, 2)

            @pl.when(jnp.logical_and(n < 2, m + r * n_block >= 2))
            def _():
                wait(sb.at[slot], dx_send.at[slot])

            @pl.when(n < 2)
            def _():
                with jax.named_scope('dx_dot'):
                    sb[slot] = dot_nt(h_all[1], w_gu[cols, :])
                send(sb.at[slot], pbuf.at[rows_of(r), cols], dx_send.at[slot], dx_recv.at[r, m], dp=partner).start()

            @pl.when(n >= 2)
            def _():
                with jax.named_scope('dx_wait'):
                    wait(pbuf.at[rows_of(r), cols], dx_recv.at[r, m])
                with jax.named_scope('dx_dot'):
                    yacc[1, rows_of(r), cols] = (yacc[1, rows_of(r), cols] + pbuf[rows_of(r), cols]
                                                 + dot_nt(h_all[1], w_gu[cols, :]))

            @pl.when(m >= 1)
            def _():
                tick(17 + 4 * n + m)
            return carry

        lax.fori_loop(0, n_block, block, 0)

    def grad_tile(n, carry):
        q = n - 4
        slot = lax.rem(n, 2)
        at = jnp.where(n < 4, n, slot)
        final = n == 15
        early = jnp.logical_and(n >= 3, q + 1 <= EARLY)
        late = jnp.logical_and(n < 15, q + 1 > EARLY)
        dense = q >= 8
        tau = jnp.where(dense, 64 + 5 * (q - 8), 16 + 4 * n)

        @pl.when(n < 4)
        def _():
            q_start(4 + n)
            loaded(0, slot)

        @pl.when(dense)
        def _():
            tick(tau)

        step = jnp.where(dense, tau + 1, tau)

        @pl.when(n >= 4)
        def _():
            landed(0, q)
            with jax.named_scope('ab_dot'):
                ab_all[at, :, :cut] = dot_nn(xt[slot], w_gu[:, :cut])
            tick(step)
            with jax.named_scope('ab_dot'):
                ab_all[at, :, cut:] = dot_nn(xt[slot], w_gu[:, cut:])

            @pl.when(final)
            def _():
                with jax.named_scope('h_last'):
                    def body(m, c):
                        lo = pl.ds(pl.multiple_of(m * group, group), group)
                        a = ab_all[at, lo, :half]
                        h_all[0, lo, :half] = (a * sigmoid(a) * ab_all[at, lo, half:]).astype(BF16)
                        return c

                    lax.fori_loop(0, tile // group, body, 0)
                    pl.semaphore_wait(room.at[1], 2)
                    last_copy(1).start()

            @pl.when(q > MIDDLE)
            def _():
                arrive(1, q)

            tick(step + 1)

        @pl.when(early)
        def _():
            arrive(0, q + 1)
            arrive(1, q + 1)

        @pl.when(n < 4)
        def _():
            loaded(1, slot)

        @pl.when(n >= 4)
        def _():
            landed(1, q)

        with jax.named_scope('g_dot'):
            g_s[...] = dot_nn(dyt[slot], w_d[...])

        with jax.named_scope('act'):
            def body(m, c):
                lo = pl.ds(pl.multiple_of(m * group, group), group)
                a = ab_all[at, lo, :half]
                b = ab_all[at, lo, half:]
                g = g_s[lo, :]
                s = sigmoid(a)
                silu = a * s
                @pl.when(jnp.logical_not(final))
                def _():
                    h_all[0, lo, :half] = (silu * b).astype(BF16)

                h_all[1, lo, :half] = (g * b * s * (1.0 + a * (1.0 - s))).astype(BF16)
                h_all[1, lo, half:] = (g * silu).astype(BF16)
                return c

            lax.fori_loop(0, tile // group, body, 0)
        tick(step + jnp.where(n < 4, 0, 2))

        @pl.when(n < 3)
        def _():
            load_a(0, n + 1)
            load_a(1, n + 1)

        @pl.when(late)
        def _():
            arrive(0, q + 1)

        @pl.when(jnp.logical_not(final))
        def _():
            with jax.named_scope('dw_dot'):
                for lo in range(0, 2 * half, 2 * half // 3):
                    hi = lo + 2 * half // 3
                    acc_gu[:, lo:hi] += dot_tn(xt[slot, :, at_win], h_all[1, :, lo:hi])

            @pl.when(n == 14)
            def _():
                grad_copy(0).start()

            with jax.named_scope('dw_dot2'):
                for lo, hi in ((0, half // 2 // 128 * 128), (half // 2 // 128 * 128, half)):
                    acc_d[:, lo:hi] += dot_tn(dyt[slot, :, at_win], h_all[0, :, lo:hi])

            @pl.when(n == 14)
            def _():
                grad_copy(1).start()

        @pl.when(final)
        def _():
            pl.semaphore_wait(room.at[0], 1)
            last_copy(0).start()
            with jax.named_scope('grads_sent'):
                for m in (0, 1):
                    grad_copy(m).wait_send()
            with jax.named_scope('dw_own'):
                for lo, hi in pieces:
                    acc_gu[in_acc, lo:hi] += dot_tn(xt[1, :, at_own], h_all[1, :, lo:hi])
                acc_d[in_acc, :] += dot_tn(dyt[1, :, at_own], h_all[0, :, :half])

        @pl.when(jnp.logical_and(n >= 2, n < 15))
        def _():
            for ten in (0, 1):
                pl.semaphore_signal(room.at[ten], inc=1, device_id={'dp': partner, 'tp': t}, device_id_type=MESH)

        tick(step + jnp.where(n < 4, 1, 3))

        @pl.when(n < 4)
        def _():
            dx_tile(n)

        @pl.when(jnp.logical_and(late, q + 1 <= MIDDLE))
        def _():
            arrive(1, q + 1)
        return carry

    lax.fori_loop(0, 16, grad_tile, 0)

    theirs = pl.ds(pl.multiple_of(window_of(me * blk, own)[1], 8), blk)
    with jax.named_scope('last_wait_h'):
        wait(yacc.at[0, theirs, pl.ds(0, half)], out_recv.at[1])
        wait(dyt.at[0, :, pl.ds(0, half)], h_recv.at[1])
    with jax.named_scope('dw_other'):
        yacc[0, :own, :half] += dot_tn(dyt[1, :, at_own], dyt[0, :, :half])
    with jax.named_scope('last_wait'):
        wait(pbuf.at[theirs, pl.ds(0, 2 * half)], out_recv.at[0])
        wait(xt.at[0, :, pl.ds(0, 2 * half)], h_recv.at[0])
    with jax.named_scope('dw_other'):
        for lo, hi in pieces:
            pbuf[:own, lo:hi] += dot_tn(xt[1, :, at_own], xt[0, :, lo:hi])

    with jax.named_scope('drain_sums'):
        drain_sums()
    with jax.named_scope('drain'):
        for slot in (0, 1):
            wait(sb.at[slot], dx_send.at[slot])
        for k in range(3):
            for core in (0, 1):
                for link in (0, 1):
                    for part in (0, 1):
                        w_copy(k, link, part, core).wait_send()
                    w_relay_copy(k, link, core).wait_send()
            w_partner_copy(k).wait_send()
        for ten in (0, 1):
            own_copy(ten).wait_send()

        def drain(q, carry):
            for ten in (0, 1):
                wait(tok_b[ten].at[0], f_send.at[q, ten])
                for link in (0, 1):
                    @pl.when(q < 8)
                    def _():
                        wait(slot_of(ten, 0, link), q_send.at[lax.rem(q, 8), link, ten])

                    @pl.when(q < 4)
                    def _():
                        wait(slot_of(ten, 0, link), rl_send.at[lax.rem(q, 4), link, ten])

            return carry

        lax.fori_loop(0, 12, drain, 0)
        for m in (0, 1):
            last_copy(m).wait_send()


def window_of(start, size):
    first = lax.div(start, LANES) * LANES
    return pl.ds(pl.multiple_of(first, LANES), size), start - first


def own_window(blk):
    return -(-(blk + LANES - 32) // LANES) * LANES


def window(model, blk):
    starts = [(2 * blk * c) // LANES * LANES for c in range(model // (2 * blk))]
    shift = max(2 * blk * c - s for c, s in enumerate(starts))
    return -(-(shift + 2 * blk) // LANES) * LANES


def mlp(x, dy, wg, wu, wd):
    rows, model = x.shape
    blk, width = wg.shape
    half = width // 2
    tile = rows // 2
    dma = pltpu.SemaphoreType.DMA
    vmem = pltpu.VMEM
    anywhere = pl.BlockSpec(memory_space=pl.ANY)
    shape = jax.ShapeDtypeStruct
    flops = 2 * model * half * rows * 2 * 20
    win = window(model, blk)
    most = max(rows, own_window(blk))
    kept = (vmem((win, 2 * half), F32), vmem((win, half), F32), vmem((most, model), F32), vmem((2, most, model), F32))
    held = sum(4 * math.prod(k.shape) for k in kept)
    in_vmem = pl.BlockSpec(memory_space=pltpu.VMEM)
    return pl.pallas_call(
        kernel,
        name='mlp',
        out_shape=(shape((2, rows, model), BF16), *kept,
                   shape((12, tile // 2, model), BF16), shape((12, tile // 2, model), BF16),
                   shape((rows, model), BF16), shape((rows, model), BF16)),
        in_specs=[anywhere] * 5,
        out_specs=(anywhere, *[in_vmem] * 4, *[anywhere] * 4),
        scratch_shapes=[
            vmem((model, 2 * half), BF16),
            vmem((model, half), BF16),
            vmem((2, tile, model // 3), F32),
            vmem((2, tile, model), BF16),
            vmem((2, tile, model), BF16),
            vmem((4, tile, 2 * half), F32),
            vmem((tile, half), F32),
            vmem((2, tile, 2 * half), BF16),
            vmem((2, DEPTH, tile // 2, LANES), F32),
            vmem((2, KEEP, tile // 2, LANES), BF16),
            dma((3, 2, 2, 2)), dma((3, 2, 2, 2)), dma((3, 2, 2)), dma((3, 2, 2)), dma((3,)), dma((3,)), dma((3,)),
            dma((2,)), dma((2,)), dma((8, 2, 2)), dma((12, 2, 2)), dma((4, 2, 2)), dma((12, 2)), dma((12, 2)),
            dma((2, 2)), dma((4, 2)), dma((2,)), dma((2, 3)), pltpu.SemaphoreType.REGULAR, pltpu.SemaphoreType.REGULAR((2,)),
            dma((2, SLOTS)), dma((2, DEPTH)), dma((2, LAG + 1)), dma((2, KEEP)), dma((2, LAG + 1)),
            dma((2, 2)), dma((2,)), dma((2,)), dma((2,)), dma((2,)),
        ],
        compiler_params=pltpu.CompilerParams(collective_id=0, has_side_effects=True, vmem_limit_bytes=67_000_000 - held),
        cost_estimate=pl.CostEstimate(flops=flops, bytes_accessed=100_000_000, transcendentals=0),
    )(x, dy, wg, wu, wd)


def results_kernel(blk, half, yd_ref, acc_gu, acc_d, pbuf, yacc, y_out, dx_out, g_out, u_out, d_out, yd_s, load, store, grad):
    me = lax.axis_index('dp')
    j = lax.rem(me, 2)
    chip = lax.div(me, 2)
    mine = pl.ds(pl.multiple_of(window_of(chip * 2 * blk, 128)[1] + j * blk, 8), blk)
    other = pl.ds(pl.multiple_of(window_of(me * blk, 128)[1], 8), blk)
    own_cols = pl.ds(pl.multiple_of(j * half, LANES), half)
    other_cols = pl.ds(pl.multiple_of((1 - j) * half, LANES), half)
    low, high = pl.ds(0, half), pl.ds(half, half)
    rows = yd_ref.shape[1] // 4
    parts = []
    for m in range(4):
        for ten, dst in ((0, y_out), (1, dx_out)):
            at = pl.ds(m * rows, rows)
            parts.append((yd_ref.at[ten, at, :], yd_s.at[ten, at, :], dst.at[at, :]))
    grads = ((acc_gu.at[mine, low], g_out.at[:, own_cols]), (acc_gu.at[mine, high], u_out.at[:, own_cols]),
             (acc_d.at[mine, :], d_out.at[:, own_cols]),
             (pbuf.at[other, low], g_out.at[:, other_cols]), (pbuf.at[other, high], u_out.at[:, other_cols]),
             (yacc.at[0, other, low], d_out.at[:, other_cols]))
    for n, (src, buf, dst) in enumerate(parts):
        pltpu.make_async_copy(src, buf, load.at[n]).start()
    for n, (src, dst) in enumerate(grads):
        pltpu.make_async_copy(src, dst, grad.at[n]).start()
    for n, (src, buf, dst) in enumerate(parts):
        pltpu.make_async_copy(src, buf, load.at[n]).wait()
        pltpu.make_async_copy(buf, dst, store.at[n]).start()
    for n, (src, buf, dst) in enumerate(parts):
        pltpu.make_async_copy(buf, dst, store.at[n]).wait()
    for n, (src, dst) in enumerate(grads):
        pltpu.make_async_copy(src, dst, grad.at[n]).wait()


def results(blk, width, yd, *kept):
    anywhere = pl.BlockSpec(memory_space=pl.ANY)
    in_vmem = pl.BlockSpec(memory_space=pltpu.VMEM)
    shape = jax.ShapeDtypeStruct
    dma = pltpu.SemaphoreType.DMA
    yd = pltpu.with_memory_space_constraint(yd, pltpu.HBM)
    kept = [pltpu.with_memory_space_constraint(k, pltpu.VMEM) for k in kept]
    return pl.pallas_call(
        functools.partial(results_kernel, blk, width // 2),
        name='results',
        out_shape=(shape(yd.shape[1:], yd.dtype), shape(yd.shape[1:], yd.dtype),
                   shape((blk, width), F32), shape((blk, width), F32), shape((blk, width), F32)),
        in_specs=[pl.BlockSpec(memory_space=pltpu.HBM), *[in_vmem] * 4],
        out_specs=tuple([anywhere] * 5),
        scratch_shapes=[pltpu.VMEM(yd.shape, yd.dtype), dma((8,)), dma((8,)), dma((6,))],
        compiler_params=pltpu.CompilerParams(vmem_limit_bytes=12_000_000),
    )(yd, *kept)


def solution(mesh):
    def device_pass(x_rows, gate_blk, up_blk, down_blk, dy_rows):
        out = mlp(x_rows, dy_rows, gate_blk, up_blk, down_blk.T)
        y, dx, dw_gate, dw_up, dw_down = results(*gate_blk.shape, *out[:5])
        return y, dx, dw_gate, dw_up, dw_down.T

    row_spec = P('dp', None)
    weight_spec = P('dp', 'tp')
    down_spec = P('tp', 'dp')
    return jax.shard_map(device_pass, mesh=mesh,
                         in_specs=(row_spec, weight_spec, weight_spec, down_spec, row_spec),
                         out_specs=(row_spec, row_spec, weight_spec, weight_spec, down_spec),
                         check_vma=False)
```

```python
import functools
import math

import jax
import jax.numpy as jnp
from jax import lax
from jax.experimental import pallas as pl
from jax.experimental.pallas import tpu as pltpu
from jax.sharding import PartitionSpec as P

F32 = jnp.float32
BF16 = jnp.bfloat16
MESH = pl.DeviceIdType.MESH
SLOTS = 8
DEPTH = 13
KEEP = 16
LAG = 3
HOP = 2
LANES = 128
EARLY = 4
MIDDLE = 8


def dot_nn(a, b):
    return jnp.dot(a, b, preferred_element_type=F32)


def dot_nt(a, b):
    return lax.dot_general(a, b, (((1,), (1,)), ((), ())), preferred_element_type=F32)


def dot_tn(a, b):
    return lax.dot_general(a, b, (((0,), (0,)), ((), ())), preferred_element_type=F32)


def sigmoid(a):
    return 1.0 / (1.0 + jnp.exp(-a))


def kernel(x_ref, dy_ref, wg_ref, wu_ref, wd_ref,
           yd_ref, acc_gu, acc_d, pbuf, yacc, xb, dyb, xp, dyp,
           w_gu, w_d, sb, xt, dyt, ab_all, g_s, h_all, rbuf, back,
           w_send, w_recv, wr_send, wr_recv, w_own, wp_send, wp_recv,
           own_send, own_recv, q_send, q_recv, rl_send, f_send, f_recv,
           y_send, y_recv, dx_send, dx_recv, credit, room,
           rs_send, rs_recv, ag_send, ag_recv, fin_own, ld, out_send, out_recv, h_send, h_recv):
    rows, model = x_ref.shape
    blk, width = wg_ref.shape
    half = width // 2
    hb = blk // 2
    tile = rows // 2
    piece = tile // 4
    win = acc_d.shape[0]
    line = model // 2
    units = line // LANES
    near_units = (2 * blk - LANES // 2) // LANES if (2 * blk) % LANES else 2 * blk // LANES
    rest_units = units - near_units
    steps = 4 * units
    part_rows = tile // 2
    group = min(32, tile)
    w_in = (wg_ref, wu_ref, wd_ref)
    cut = (half + 255) // 256 * 256
    pieces = ((0, cut), (cut, 2 * half))
    tok = (x_ref, dy_ref)
    tok_b = (xb, dyb)
    tok_p = (xp, dyp)
    tok_t = (xt, dyt)

    t = lax.axis_index('tp')
    me = lax.axis_index('dp')
    cy = lax.div(me, 4)
    cx = lax.rem(lax.div(me, 2), 2)
    j = lax.rem(me, 2)
    partner = me + 1 - 2 * j
    chip = cy * 2 + cx

    def near(link, core):
        if link == 0:
            return cy * 4 + (1 - cx) * 2 + core
        return (1 - cy) * 4 + cx * 2 + core

    def far(core):
        return (1 - cy) * 4 + (1 - cx) * 2 + core

    def send(src, dst, s_sem, r_sem, dp=None, tp=None):
        where = {'dp': me if dp is None else dp, 'tp': t if tp is None else tp}
        return pltpu.make_async_remote_copy(src_ref=src, dst_ref=dst, send_sem=s_sem, recv_sem=r_sem,
                                            device_id=where, device_id_type=MESH)

    def wait(ref, sem):
        pltpu.make_async_copy(ref, ref, sem).wait()

    barrier = pltpu.get_barrier_semaphore()
    for peer in (partner, near(0, 0), near(0, 1), near(1, 0), near(1, 1)):
        pl.semaphore_signal(barrier, inc=1, device_id={'dp': peer, 'tp': t}, device_id_type=MESH)

    @pl.when(t > 0)
    def _():
        pl.semaphore_signal(barrier, inc=1, device_id={'dp': me, 'tp': t - 1}, device_id_type=MESH)

    @pl.when(t < 3)
    def _():
        pl.semaphore_signal(barrier, inc=1, device_id={'dp': me, 'tp': t + 1}, device_id_type=MESH)

    pl.semaphore_wait(barrier, 5 + jnp.minimum(t, 1) + jnp.minimum(3 - t, 1))

    def w_rows(k, dev, part=None):
        if part is None:
            at = pl.ds(pl.multiple_of(dev * blk, 16), blk)
        else:
            at = pl.ds(pl.multiple_of(dev * blk + part * hb, 16), hb)
        if k == 2:
            return w_d.at[at, :]
        return w_gu.at[at, pl.ds(k * half, half)]

    def w_cols(core):
        return pl.ds(pl.multiple_of(core * half, LANES), half)

    def w_copy(k, link, part, core):
        return send(w_in[k].at[pl.ds(part * hb, hb), w_cols(core)], w_rows(k, me, part),
                    w_send.at[k, link, part, core], w_recv.at[k, link, part, j], dp=near(link, core))

    def w_own_copy(k):
        return pltpu.make_async_copy(w_in[k].at[:, w_cols(j)], w_rows(k, me), w_own.at[k])

    def w_partner_copy(k):
        return send(w_in[k].at[:, w_cols(1 - j)], w_rows(k, me), wp_send.at[k], wp_recv.at[k], dp=partner)

    def w_start(k):
        for first in (0, 1):
            for core in (0, 1):
                w_copy(k, 0, 1 - first, core).start()
                w_copy(k, 1, first, core).start()
        w_own_copy(k).start()
        w_partner_copy(k).start()

    def w_relay_copy(k, link_out, core):
        part = 1 if link_out == 1 else 0
        ref = w_rows(k, near(1 - link_out, core), part)
        return send(ref, ref, wr_send.at[k, link_out, core], wr_recv.at[k, link_out, core], dp=near(link_out, j))

    def w_relay(k):
        for core in (0, 1):
            wait(w_rows(k, near(0, core), 1), w_recv.at[k, 0, 1, core])
            w_relay_copy(k, 1, core).start()
            wait(w_rows(k, near(1, core), 0), w_recv.at[k, 1, 0, core])
            w_relay_copy(k, 0, core).start()

    def w_have(k, which):
        if which == 'chip':
            wait(w_rows(k, me), w_own.at[k])
            wait(w_rows(k, partner), wp_recv.at[k])
        for core in (0, 1):
            if which == 'x':
                wait(w_rows(k, near(0, core), 0), w_recv.at[k, 0, 0, core])
            if which == 'y':
                wait(w_rows(k, near(1, core), 1), w_recv.at[k, 1, 1, core])
            if which == 'far':
                wait(w_rows(k, far(core), 0), wr_recv.at[k, 0, core])
                wait(w_rows(k, far(core), 1), wr_recv.at[k, 1, core])

    def slot_of(ten, q, link):
        return tok_b[ten].at[q, pl.ds(link * piece, piece), :]

    def q_copy(ten, q, link):
        b = lax.div(q, 4)
        sub = lax.rem(q, 4)
        first = 1 - b if link == 0 else b
        src = tok[ten].at[pl.ds(pl.multiple_of(first * tile + sub * piece, piece), piece), :]
        return send(src, slot_of(ten, q, link), q_send.at[q, link, ten], q_recv.at[q, link, ten], dp=near(link, j))

    def q_start(q):
        for ten in (0, 1):
            for link in (0, 1):
                q_copy(ten, q, link).start()

    def relay_copy(ten, sub, link_out):
        return send(slot_of(ten, sub, 1 - link_out), slot_of(ten, 8 + sub, link_out),
                    rl_send.at[sub, link_out, ten], q_recv.at[8 + sub, link_out, ten], dp=near(link_out, j))

    def tile_part(ten, q, core):
        return tok_t[ten].at[lax.rem(q, 2), pl.ds(pl.multiple_of(core * 2 * piece, 2 * piece), 2 * piece), :]

    def forward_copy(ten, q):
        return send(tok_b[ten].at[q], tile_part(ten, q, j), f_send.at[q, ten], f_recv.at[q, ten], dp=partner)

    def own_copy(ten):
        return send(tok[ten], tok_p[ten], own_send.at[ten], own_recv.at[ten], dp=partner)

    def arrive(ten, q):
        with jax.named_scope('arrive'):
            for link in (0, 1):
                wait(slot_of(ten, q, link), q_recv.at[q, link, ten])
            if ten == 0:
                pl.semaphore_wait(room.at[0], 1)
            else:
                @pl.when(q < 11)
                def _():
                    pl.semaphore_wait(room.at[1], 1)

            forward_copy(ten, q).start()
            pltpu.make_async_copy(tok_b[ten].at[q], tile_part(ten, q, j), ld.at[ten, lax.rem(q, 2)]).start()

        @pl.when(q < 4)
        def _():
            for link in (0, 1):
                relay_copy(ten, q, link).start()

    def landed(ten, q):
        with jax.named_scope('landed'):
            wait(tile_part(ten, q, j), ld.at[ten, lax.rem(q, 2)])
            wait(tile_part(ten, q, 1 - j), f_recv.at[q, ten])

    def rows_of(r):
        return pl.ds(pl.multiple_of(r * tile, tile), tile)

    def load_a(ten, n):
        own = lax.div(n, 2)
        slot = lax.rem(n, 2)

        @pl.when(own == 1)
        def _():
            pltpu.make_async_copy(tok[ten].at[rows_of(slot), :], tok_t[ten].at[slot], ld.at[ten, slot]).start()

        @pl.when(own == 0)
        def _():
            pltpu.make_async_copy(tok_p[ten].at[rows_of(slot), :], tok_t[ten].at[slot], ld.at[ten, slot]).start()

    def loaded(ten, slot):
        with jax.named_scope('ld'):
            wait(tok_t[ten].at[slot], ld.at[ten, slot])

    def unit_col(u):
        mine = cy * units
        other = (1 - cy) * units
        low = cx * rest_units
        high = (1 - cx) * near_units
        a = near_units
        col = jnp.where(u < a, mine + low + u,
                        jnp.where(u < units, mine + high + (u - a),
                                  jnp.where(u < units + a, other + low + (u - units), other + high + (u - units - a))))
        return pl.multiple_of(col * LANES, LANES)

    def chunk(s, way):
        n = lax.rem(s, steps)
        row = pl.multiple_of(way * tile + lax.rem(n, 2) * part_rows, part_rows)
        return lax.div(s, steps), pl.ds(row, part_rows), pl.ds(unit_col(lax.div(n, 2)), LANES)

    def sum_copy(s, way, nxt):
        land = lax.rem(s, DEPTH)
        return send(yacc.at[chunk(s, way)], rbuf.at[way, land], rs_send.at[way, lax.rem(s, SLOTS)], rs_recv.at[way, land], tp=nxt)

    def done_copy(s, way, prv):
        ref = back.at[way, lax.rem(s, KEEP)]
        return send(ref, ref, ag_send.at[way, lax.rem(s, LAG + 1)], ag_recv.at[way, lax.rem(s, KEEP)], tp=prv)

    def store_copy(s, way):
        return pltpu.make_async_copy(back.at[way, lax.rem(s, KEEP)], yd_ref.at[chunk(s, way)],
                                     fin_own.at[way, lax.rem(s, LAG + 1)])

    def tick(tau):
        with jax.named_scope('tick'):
            tick_body(tau)

    def give(s, way, p, prv):
        @pl.when(s >= LAG)
        def _():
            store_copy(s - LAG, way).wait()

            @pl.when(p > 0)
            def _():
                wait(back.at[way, 0], ag_send.at[way, lax.rem(s - LAG, LAG + 1)])

        store_copy(s, way).start()

        @pl.when(p > 0)
        def _():
            done_copy(s, way, prv).start()

    def tick_body(tau):
        for way in (0, 1):
            p = t if way == 0 else 3 - t
            nxt = t + 1 if way == 0 else t - 1
            prv = t - 1 if way == 0 else t + 1
            s = tau - HOP * p
            slot = lax.rem(jnp.maximum(s, 0), SLOTS)
            land = lax.rem(jnp.maximum(s, 0), DEPTH)
            live = jnp.logical_and(s >= 0, s < 2 * steps)

            @pl.when(jnp.logical_and(live, p > 0))
            def _():
                wait(rbuf.at[way, land], rs_recv.at[way, land])

            @pl.when(jnp.logical_and(live, p < 3))
            def _():
                @pl.when(s >= SLOTS)
                def _():
                    wait(rbuf.at[way, 0], rs_send.at[way, slot])

                @pl.when(p > 0)
                def _():
                    here = chunk(s, way)
                    yacc[here] = yacc[here] + rbuf[way, land]

                sum_copy(s, way, nxt).start()

            @pl.when(jnp.logical_and(live, p == 3))
            def _():
                back[way, lax.rem(s, KEEP)] = (yacc[chunk(s, way)] + rbuf[way, land]).astype(BF16)
                give(s, way, p, prv)

        for way in (0, 1):
            p = t if way == 0 else 3 - t
            prv = t - 1 if way == 0 else t + 1
            s = tau - HOP * (6 - p)

            @pl.when(jnp.logical_and(jnp.logical_and(s >= 0, s < 2 * steps), p < 3))
            def _():
                keep = lax.rem(s, KEEP)
                wait(back.at[way, keep], ag_recv.at[way, keep])
                give(s, way, p, prv)

    def ticks(lo, hi):
        def body(n, c):
            tick(n)
            return c

        lax.fori_loop(lo, hi, body, 0)

    def drain_sums():
        for way in (0, 1):
            p = t if way == 0 else 3 - t

            @pl.when(p < 3)
            def _():
                for slot in range(SLOTS):
                    wait(rbuf.at[way, 0], rs_send.at[way, slot])

            for m in range(LAG):
                s = 2 * steps - LAG + m
                wait(back.at[way, 0], fin_own.at[way, s % (LAG + 1)])

                @pl.when(p > 0)
                def _():
                    wait(back.at[way, 0], ag_send.at[way, s % (LAG + 1)])

    w_start(0)
    w_start(1)
    for ten in (0, 1):
        own_copy(ten).start()
    base = jnp.where(t == 0, 1.0, 0.0).astype(F32)

    with jax.named_scope('clear'):
        for r in (0, 1):
            for ten in (0, 1):
                load_a(ten, 2 + r)

        def clear(n, carry):
            at = pl.ds(pl.multiple_of(n * 32, 32), 32)
            acc_gu[at, :] = jnp.zeros((32, 2 * half), F32)
            acc_d[at, :] = jnp.zeros((32, half), F32)
            return carry

        lax.fori_loop(0, win // 32, clear, 0)

        def clear_ab(n, carry):
            lo = pl.ds(pl.multiple_of(n * group, group), group)
            for m in range(4):
                ab_all[m, lo, :] = jnp.zeros((group, 2 * half), F32)
            return carry

        lax.fori_loop(0, tile // group, clear_ab, 0)
        for r in (0, 1):
            for ten in (0, 1):
                loaded(ten, r)

                def residual(n, carry):
                    lo = pl.ds(pl.multiple_of(n * group, group), group)
                    there = pl.ds(pl.multiple_of(r * tile + n * group, group), group)
                    yacc[ten, there, :] = tok_t[ten][r, lo, :].astype(F32) * base
                    return carry

                lax.fori_loop(0, tile // group, residual, 0)
        for ten in (0, 1):
            wait(tok_p[ten], own_recv.at[ten])

    with jax.named_scope('w_relay'):
        w_relay(0)
        w_relay(1)
    w_start(2)

    def side(n):
        return pl.ds(pl.multiple_of(lax.rem(n, 2) * half, LANES), half)

    def ab_pass(last):
        other = (1 - cy) * line
        if last:
            parts = ((other + (1 - cx) * near_units * LANES, rest_units * LANES),)
        else:
            parts = ((cy * line, line), (other + cx * rest_units * LANES, near_units * LANES))
        load_a(0, 0)

        def body(n, carry):
            slot = lax.rem(n, 2)

            @pl.when(n < 3)
            def _():
                load_a(0, n + 1)

            loaded(0, slot)
            for at, size in parts:
                at_k = pl.ds(pl.multiple_of(at, LANES), size)
                with jax.named_scope('ab_part'):
                    for lo, hi in pieces:
                        ab_all[n, :, lo:hi] += dot_nn(xt[slot, :, at_k], w_gu[at_k, lo:hi])

            if last:
                def hidden(m, c):
                    lo = pl.ds(pl.multiple_of(m * group, group), group)
                    a = ab_all[n, lo, :half]
                    h_all[lax.div(n, 2), lo, side(n)] = (a * sigmoid(a) * ab_all[n, lo, half:]).astype(BF16)
                    return c

                lax.fori_loop(0, tile // group, hidden, 0)
            return carry

        lax.fori_loop(0, 4, body, 0)

    with jax.named_scope('w_have'):
        for k in (0, 1):
            w_have(k, 'chip')
            w_have(k, 'x')
            w_have(k, 'y')
    ab_pass(0)
    with jax.named_scope('w_have'):
        for k in (0, 1):
            w_have(k, 'far')
    ab_pass(1)

    def y_group(g, tau):
        u0 = (0, near_units, units, units + near_units)[g]
        n_u = (near_units, rest_units)[g % 2]
        col = unit_col(u0)
        cols = pl.ds(col, n_u * LANES)

        def theirs(r, carry):
            if g > 0:
                before = (near_units, rest_units)[(g - 1) % 2] * LANES
                wait(sb.at[r, :, pl.ds(0, before)], y_send.at[(g - 1) % 2, r])
            with jax.named_scope('y_dot'):
                sb[r, :, :n_u * LANES] = dot_nt(h_all[0, :, side(r)], w_d[cols, :])
            send(sb.at[r, :, pl.ds(0, n_u * LANES)], pbuf.at[rows_of(r), cols],
                 y_send.at[g % 2, r], y_recv.at[g, r], dp=partner).start()
            return carry

        def ours(r, carry):
            with jax.named_scope('y_wait'):
                wait(pbuf.at[rows_of(r), cols], y_recv.at[g, r])
            with jax.named_scope('y_dot'):
                yacc[0, rows_of(r), cols] = (yacc[0, rows_of(r), cols] + pbuf[rows_of(r), cols]
                                             + dot_nt(h_all[1, :, side(r)], w_d[cols, :]))
            pl.semaphore_signal(credit, inc=1, device_id={'dp': partner, 'tp': t}, device_id_type=MESH)
            return carry

        lax.fori_loop(0, 2, theirs, 0)
        if g > 0:
            tick(tau)
        lax.fori_loop(0, 2, ours, 0)
        if g > 0:
            tick(tau + 1)

    load_a(1, 0)
    load_a(0, 0)
    with jax.named_scope('w_have2'):
        w_have(2, 'chip')
    y_group(0, 0)
    tick(0)
    with jax.named_scope('w_relay2'):
        w_relay(2)
    q_start(0)
    q_start(1)
    ticks(1, 7)
    with jax.named_scope('w_have2'):
        w_have(2, 'x')
        w_have(2, 'y')
    y_group(1, 7)
    y_group(2, 9)
    q_start(2)
    ticks(11, 14)
    with jax.named_scope('w_have2'):
        w_have(2, 'far')
    y_group(3, 14)
    q_start(3)

    at_win, shift = window_of(chip * 2 * blk, win)
    own = own_window(blk)
    at_own, _ = window_of(me * blk, own)
    in_acc = pl.ds(pl.multiple_of(window_of(me * blk, own)[0].start - at_win.start, 8), own)
    n_block = 3
    n_cols = model // n_block

    def grad_copy(m):
        rows_ = pl.ds(pl.multiple_of(shift + (1 - j) * blk, 8), blk)
        there = pl.ds(pl.multiple_of(window_of(partner * blk, own)[1], 8), blk)
        if m == 0:
            return send(acc_gu.at[rows_, :], pbuf.at[there, pl.ds(0, 2 * half)], out_send.at[0], out_recv.at[0], dp=partner)
        return send(acc_d.at[rows_, :], yacc.at[0, there, pl.ds(0, half)], out_send.at[1], out_recv.at[1], dp=partner)

    def last_copy(m):
        if m == 0:
            return send(h_all.at[1], xt.at[0, :, pl.ds(0, 2 * half)], h_send.at[0], h_recv.at[0], dp=partner)
        return send(h_all.at[0, :, pl.ds(0, half)], dyt.at[0, :, pl.ds(0, half)], h_send.at[1], h_recv.at[1], dp=partner)

    def dx_tile(n):
        r = lax.rem(n, 2)

        @pl.when(n == 0)
        def _():
            pl.semaphore_wait(credit, 8)
            for r_ in (0, 1):
                wait(sb.at[r_, :, pl.ds(0, rest_units * LANES)], y_send.at[1, r_])

        def block(m, carry):
            cols = pl.ds(pl.multiple_of(m * n_cols, n_cols), n_cols)
            slot = lax.rem(m + r * n_block, 2)

            @pl.when(jnp.logical_and(n < 2, m + r * n_block >= 2))
            def _():
                wait(sb.at[slot], dx_send.at[slot])

            @pl.when(n < 2)
            def _():
                with jax.named_scope('dx_dot'):
                    sb[slot] = dot_nt(h_all[1], w_gu[cols, :])
                send(sb.at[slot], pbuf.at[rows_of(r), cols], dx_send.at[slot], dx_recv.at[r, m], dp=partner).start()

            @pl.when(n >= 2)
            def _():
                with jax.named_scope('dx_wait'):
                    wait(pbuf.at[rows_of(r), cols], dx_recv.at[r, m])
                with jax.named_scope('dx_dot'):
                    yacc[1, rows_of(r), cols] = (yacc[1, rows_of(r), cols] + pbuf[rows_of(r), cols]
                                                 + dot_nt(h_all[1], w_gu[cols, :]))

            @pl.when(m >= 1)
            def _():
                tick(17 + 4 * n + m)
            return carry

        lax.fori_loop(0, n_block, block, 0)

    def grad_tile(n, carry):
        q = n - 4
        slot = lax.rem(n, 2)
        at = jnp.where(n < 4, n, slot)
        final = n == 15
        early = jnp.logical_and(n >= 3, q + 1 <= EARLY)
        late = jnp.logical_and(n < 15, q + 1 > EARLY)
        dense = q >= 8
        tau = jnp.where(dense, 64 + 5 * (q - 8), 16 + 4 * n)

        @pl.when(n < 4)
        def _():
            q_start(4 + n)
            loaded(0, slot)

        @pl.when(dense)
        def _():
            tick(tau)

        step = jnp.where(dense, tau + 1, tau)

        @pl.when(n >= 4)
        def _():
            landed(0, q)
            with jax.named_scope('ab_dot'):
                ab_all[at, :, :cut] = dot_nn(xt[slot], w_gu[:, :cut])
            tick(step)

            @pl.when(jnp.logical_and(q > MIDDLE, n < 15))
            def _():
                arrive(1, q)

            with jax.named_scope('ab_dot'):
                ab_all[at, :, cut:] = dot_nn(xt[slot], w_gu[:, cut:])

            @pl.when(final)
            def _():
                pl.semaphore_wait(room.at[1], 2)
                arrive(1, q)
                with jax.named_scope('h_last'):
                    def body(m, c):
                        lo = pl.ds(pl.multiple_of(m * group, group), group)
                        a = ab_all[at, lo, :half]
                        h_all[0, lo, :half] = (a * sigmoid(a) * ab_all[at, lo, half:]).astype(BF16)
                        return c

                    lax.fori_loop(0, tile // group, body, 0)
                    last_copy(1).start()

            tick(step + 1)

        @pl.when(early)
        def _():
            arrive(0, q + 1)
            arrive(1, q + 1)

        @pl.when(n < 4)
        def _():
            loaded(1, slot)

        @pl.when(n >= 4)
        def _():
            landed(1, q)

        with jax.named_scope('g_dot'):
            g_s[...] = dot_nn(dyt[slot], w_d[...])

        def activate(with_h):
            def body(m, c):
                lo = pl.ds(pl.multiple_of(m * group, group), group)
                a = ab_all[at, lo, :half]
                b = ab_all[at, lo, half:]
                g = g_s[lo, :]
                s = sigmoid(a)
                silu = a * s
                if with_h:
                    h_all[0, lo, :half] = (silu * b).astype(BF16)
                h_all[1, lo, :half] = (g * b * s * (1.0 + a * (1.0 - s))).astype(BF16)
                h_all[1, lo, half:] = (g * silu).astype(BF16)
                return c

            with jax.named_scope('act'):
                lax.fori_loop(0, tile // group, body, 0)

        @pl.when(final)
        def _():
            activate(False)

        @pl.when(jnp.logical_not(final))
        def _():
            activate(True)

        tick(step + jnp.where(n < 4, 0, 2))

        @pl.when(n < 3)
        def _():
            load_a(0, n + 1)
            load_a(1, n + 1)

        @pl.when(late)
        def _():
            arrive(0, q + 1)

        @pl.when(jnp.logical_not(final))
        def _():
            with jax.named_scope('dw_dot'):
                for lo in range(0, 2 * half, 2 * half // 3):
                    hi = lo + 2 * half // 3
                    acc_gu[:, lo:hi] += dot_tn(xt[slot, :, at_win], h_all[1, :, lo:hi])

            @pl.when(n == 14)
            def _():
                grad_copy(0).start()

            with jax.named_scope('dw_dot2'):
                for lo, hi in ((0, half // 2 // 128 * 128), (half // 2 // 128 * 128, half)):
                    acc_d[:, lo:hi] += dot_tn(dyt[slot, :, at_win], h_all[0, :, lo:hi])

            @pl.when(n == 14)
            def _():
                grad_copy(1).start()

        @pl.when(final)
        def _():
            pl.semaphore_wait(room.at[0], 1)
            last_copy(0).start()
            with jax.named_scope('grads_sent'):
                for m in (0, 1):
                    grad_copy(m).wait_send()
            with jax.named_scope('dw_own'):
                for lo, hi in pieces:
                    acc_gu[in_acc, lo:hi] += dot_tn(xt[1, :, at_own], h_all[1, :, lo:hi])
                acc_d[in_acc, :] += dot_tn(dyt[1, :, at_own], h_all[0, :, :half])

        @pl.when(jnp.logical_and(n >= 2, n < 15))
        def _():
            for ten in (0, 1):
                pl.semaphore_signal(room.at[ten], inc=1, device_id={'dp': partner, 'tp': t}, device_id_type=MESH)

        tick(step + jnp.where(n < 4, 1, 3))

        @pl.when(n < 4)
        def _():
            dx_tile(n)

        @pl.when(jnp.logical_and(late, q + 1 <= MIDDLE))
        def _():
            arrive(1, q + 1)
        return carry

    lax.fori_loop(0, 16, grad_tile, 0)

    theirs = pl.ds(pl.multiple_of(window_of(me * blk, own)[1], 8), blk)
    with jax.named_scope('last_wait_h'):
        wait(yacc.at[0, theirs, pl.ds(0, half)], out_recv.at[1])
        wait(dyt.at[0, :, pl.ds(0, half)], h_recv.at[1])
    with jax.named_scope('dw_other'):
        yacc[0, :own, :half] += dot_tn(dyt[1, :, at_own], dyt[0, :, :half])
    with jax.named_scope('last_wait'):
        wait(pbuf.at[theirs, pl.ds(0, 2 * half)], out_recv.at[0])
        wait(xt.at[0, :, pl.ds(0, 2 * half)], h_recv.at[0])
    with jax.named_scope('dw_other'):
        for lo, hi in pieces:
            pbuf[:own, lo:hi] += dot_tn(xt[1, :, at_own], xt[0, :, lo:hi])

    with jax.named_scope('drain_sums'):
        drain_sums()
    with jax.named_scope('drain'):
        for slot in (0, 1):
            wait(sb.at[slot], dx_send.at[slot])
        for k in range(3):
            for core in (0, 1):
                for link in (0, 1):
                    for part in (0, 1):
                        w_copy(k, link, part, core).wait_send()
                    w_relay_copy(k, link, core).wait_send()
            w_partner_copy(k).wait_send()
        for ten in (0, 1):
            own_copy(ten).wait_send()

        def drain(q, carry):
            for ten in (0, 1):
                wait(tok_b[ten].at[0], f_send.at[q, ten])
                for link in (0, 1):
                    @pl.when(q < 8)
                    def _():
                        wait(slot_of(ten, 0, link), q_send.at[lax.rem(q, 8), link, ten])

                    @pl.when(q < 4)
                    def _():
                        wait(slot_of(ten, 0, link), rl_send.at[lax.rem(q, 4), link, ten])

            return carry

        lax.fori_loop(0, 12, drain, 0)
        for m in (0, 1):
            last_copy(m).wait_send()


def window_of(start, size):
    first = lax.div(start, LANES) * LANES
    return pl.ds(pl.multiple_of(first, LANES), size), start - first


def own_window(blk):
    return -(-(blk + LANES - 32) // LANES) * LANES


def window(model, blk):
    starts = [(2 * blk * c) // LANES * LANES for c in range(model // (2 * blk))]
    shift = max(2 * blk * c - s for c, s in enumerate(starts))
    return -(-(shift + 2 * blk) // LANES) * LANES


def mlp(x, dy, wg, wu, wd):
    rows, model = x.shape
    blk, width = wg.shape
    half = width // 2
    tile = rows // 2
    dma = pltpu.SemaphoreType.DMA
    vmem = pltpu.VMEM
    anywhere = pl.BlockSpec(memory_space=pl.ANY)
    shape = jax.ShapeDtypeStruct
    flops = 2 * model * half * rows * 2 * 20
    win = window(model, blk)
    most = max(rows, own_window(blk))
    kept = (vmem((win, 2 * half), F32), vmem((win, half), F32), vmem((most, model), F32), vmem((2, most, model), F32))
    held = sum(4 * math.prod(k.shape) for k in kept)
    in_vmem = pl.BlockSpec(memory_space=pltpu.VMEM)
    return pl.pallas_call(
        kernel,
        name='mlp',
        out_shape=(shape((2, rows, model), BF16), *kept,
                   shape((12, tile // 2, model), BF16), shape((12, tile // 2, model), BF16),
                   shape((rows, model), BF16), shape((rows, model), BF16)),
        in_specs=[anywhere] * 5,
        out_specs=(anywhere, *[in_vmem] * 4, *[anywhere] * 4),
        scratch_shapes=[
            vmem((model, 2 * half), BF16),
            vmem((model, half), BF16),
            vmem((2, tile, model // 3), F32),
            vmem((2, tile, model), BF16),
            vmem((2, tile, model), BF16),
            vmem((4, tile, 2 * half), F32),
            vmem((tile, half), F32),
            vmem((2, tile, 2 * half), BF16),
            vmem((2, DEPTH, tile // 2, LANES), F32),
            vmem((2, KEEP, tile // 2, LANES), BF16),
            dma((3, 2, 2, 2)), dma((3, 2, 2, 2)), dma((3, 2, 2)), dma((3, 2, 2)), dma((3,)), dma((3,)), dma((3,)),
            dma((2,)), dma((2,)), dma((8, 2, 2)), dma((12, 2, 2)), dma((4, 2, 2)), dma((12, 2)), dma((12, 2)),
            dma((2, 2)), dma((4, 2)), dma((2,)), dma((2, 3)), pltpu.SemaphoreType.REGULAR, pltpu.SemaphoreType.REGULAR((2,)),
            dma((2, SLOTS)), dma((2, DEPTH)), dma((2, LAG + 1)), dma((2, KEEP)), dma((2, LAG + 1)),
            dma((2, 2)), dma((2,)), dma((2,)), dma((2,)), dma((2,)),
        ],
        compiler_params=pltpu.CompilerParams(collective_id=0, has_side_effects=True, vmem_limit_bytes=67_000_000 - held),
        cost_estimate=pl.CostEstimate(flops=flops, bytes_accessed=100_000_000, transcendentals=0),
    )(x, dy, wg, wu, wd)


def results_kernel(blk, half, yd_ref, acc_gu, acc_d, pbuf, yacc, y_out, dx_out, g_out, u_out, d_out, yd_s, load, store, grad):
    me = lax.axis_index('dp')
    j = lax.rem(me, 2)
    chip = lax.div(me, 2)
    mine = pl.ds(pl.multiple_of(window_of(chip * 2 * blk, 128)[1] + j * blk, 8), blk)
    other = pl.ds(pl.multiple_of(window_of(me * blk, 128)[1], 8), blk)
    own_cols = pl.ds(pl.multiple_of(j * half, LANES), half)
    other_cols = pl.ds(pl.multiple_of((1 - j) * half, LANES), half)
    low, high = pl.ds(0, half), pl.ds(half, half)
    rows = yd_ref.shape[1] // 4
    parts = []
    for m in range(4):
        for ten, dst in ((0, y_out), (1, dx_out)):
            at = pl.ds(m * rows, rows)
            parts.append((yd_ref.at[ten, at, :], yd_s.at[ten, at, :], dst.at[at, :]))
    grads = ((acc_gu.at[mine, low], g_out.at[:, own_cols]), (acc_gu.at[mine, high], u_out.at[:, own_cols]),
             (acc_d.at[mine, :], d_out.at[:, own_cols]),
             (pbuf.at[other, low], g_out.at[:, other_cols]), (pbuf.at[other, high], u_out.at[:, other_cols]),
             (yacc.at[0, other, low], d_out.at[:, other_cols]))
    for n, (src, buf, dst) in enumerate(parts):
        pltpu.make_async_copy(src, buf, load.at[n]).start()
    for n, (src, dst) in enumerate(grads):
        pltpu.make_async_copy(src, dst, grad.at[n]).start()
    for n, (src, buf, dst) in enumerate(parts):
        pltpu.make_async_copy(src, buf, load.at[n]).wait()
        pltpu.make_async_copy(buf, dst, store.at[n]).start()
    for n, (src, buf, dst) in enumerate(parts):
        pltpu.make_async_copy(buf, dst, store.at[n]).wait()
    for n, (src, dst) in enumerate(grads):
        pltpu.make_async_copy(src, dst, grad.at[n]).wait()


def results(blk, width, yd, *kept):
    anywhere = pl.BlockSpec(memory_space=pl.ANY)
    in_vmem = pl.BlockSpec(memory_space=pltpu.VMEM)
    shape = jax.ShapeDtypeStruct
    dma = pltpu.SemaphoreType.DMA
    yd = pltpu.with_memory_space_constraint(yd, pltpu.HBM)
    kept = [pltpu.with_memory_space_constraint(k, pltpu.VMEM) for k in kept]
    return pl.pallas_call(
        functools.partial(results_kernel, blk, width // 2),
        name='results',
        out_shape=(shape(yd.shape[1:], yd.dtype), shape(yd.shape[1:], yd.dtype),
                   shape((blk, width), F32), shape((blk, width), F32), shape((blk, width), F32)),
        in_specs=[pl.BlockSpec(memory_space=pltpu.HBM), *[in_vmem] * 4],
        out_specs=tuple([anywhere] * 5),
        scratch_shapes=[pltpu.VMEM(yd.shape, yd.dtype), dma((8,)), dma((8,)), dma((6,))],
        compiler_params=pltpu.CompilerParams(vmem_limit_bytes=12_000_000),
    )(yd, *kept)


def solution(mesh):
    def device_pass(x_rows, gate_blk, up_blk, down_blk, dy_rows):
        out = mlp(x_rows, dy_rows, gate_blk, up_blk, down_blk.T)
        y, dx, dw_gate, dw_up, dw_down = results(*gate_blk.shape, *out[:5])
        return y, dx, dw_gate, dw_up, dw_down.T

    row_spec = P('dp', None)
    weight_spec = P('dp', 'tp')
    down_spec = P('tp', 'dp')
    return jax.shard_map(device_pass, mesh=mesh,
                         in_specs=(row_spec, weight_spec, weight_spec, down_spec, row_spec),
                         out_specs=(row_spec, row_spec, weight_spec, weight_spec, down_spec),
                         check_vma=False)
```

```python
import functools
import math

import jax
import jax.numpy as jnp
from jax import lax
from jax.experimental import pallas as pl
from jax.experimental.pallas import tpu as pltpu
from jax.sharding import PartitionSpec as P

F32 = jnp.float32
BF16 = jnp.bfloat16
MESH = pl.DeviceIdType.MESH
SLOTS = 8
DEPTH = 13
KEEP = 16
LAG = 3
HOP = 2
LANES = 128
EARLY = 4
MIDDLE = 8


def dot_nn(a, b):
    return jnp.dot(a, b, preferred_element_type=F32)


def dot_nt(a, b):
    return lax.dot_general(a, b, (((1,), (1,)), ((), ())), preferred_element_type=F32)


def dot_tn(a, b):
    return lax.dot_general(a, b, (((0,), (0,)), ((), ())), preferred_element_type=F32)


def sigmoid(a):
    return 1.0 / (1.0 + jnp.exp(-a))


def kernel(x_ref, dy_ref, wg_ref, wu_ref, wd_ref,
           yd_ref, acc_gu, acc_d, pbuf, yacc, w_gu, xb, dyb, xp, dyp,
           w_d, sb, xt, dyt, ab_all, g_s, h_all, rbuf, back,
           w_send, w_recv, wr_send, wr_recv, w_own, wp_send, wp_recv,
           own_send, own_recv, q_send, q_recv, rl_send, f_send, f_recv,
           y_send, y_recv, dx_send, dx_recv, credit, room,
           rs_send, rs_recv, ag_send, ag_recv, fin_own, ld, out_send, out_recv, h_send, h_recv, back_in):
    rows, model = x_ref.shape
    blk, width = wg_ref.shape
    half = width // 2
    hb = blk // 2
    tile = rows // 2
    piece = tile // 4
    win = acc_d.shape[0]
    line = model // 2
    units = line // LANES
    near_units = (2 * blk - LANES // 2) // LANES if (2 * blk) % LANES else 2 * blk // LANES
    rest_units = units - near_units
    steps = 4 * units
    part_rows = tile // 2
    group = min(32, tile)
    w_in = (wg_ref, wu_ref, wd_ref)
    cut = (half + 255) // 256 * 256
    pieces = ((0, cut), (cut, 2 * half))
    tok = (x_ref, dy_ref)
    tok_b = (xb, dyb)
    tok_p = (xp, dyp)
    tok_t = (xt, dyt)

    t = lax.axis_index('tp')
    me = lax.axis_index('dp')
    cy = lax.div(me, 4)
    cx = lax.rem(lax.div(me, 2), 2)
    j = lax.rem(me, 2)
    partner = me + 1 - 2 * j
    chip = cy * 2 + cx

    def near(link, core):
        if link == 0:
            return cy * 4 + (1 - cx) * 2 + core
        return (1 - cy) * 4 + cx * 2 + core

    def far(core):
        return (1 - cy) * 4 + (1 - cx) * 2 + core

    def send(src, dst, s_sem, r_sem, dp=None, tp=None):
        where = {'dp': me if dp is None else dp, 'tp': t if tp is None else tp}
        return pltpu.make_async_remote_copy(src_ref=src, dst_ref=dst, send_sem=s_sem, recv_sem=r_sem,
                                            device_id=where, device_id_type=MESH)

    def wait(ref, sem):
        pltpu.make_async_copy(ref, ref, sem).wait()

    barrier = pltpu.get_barrier_semaphore()
    for peer in (partner, near(0, 0), near(0, 1), near(1, 0), near(1, 1)):
        pl.semaphore_signal(barrier, inc=1, device_id={'dp': peer, 'tp': t}, device_id_type=MESH)

    @pl.when(t > 0)
    def _():
        pl.semaphore_signal(barrier, inc=1, device_id={'dp': me, 'tp': t - 1}, device_id_type=MESH)

    @pl.when(t < 3)
    def _():
        pl.semaphore_signal(barrier, inc=1, device_id={'dp': me, 'tp': t + 1}, device_id_type=MESH)

    pl.semaphore_wait(barrier, 5 + jnp.minimum(t, 1) + jnp.minimum(3 - t, 1))

    def w_rows(k, dev, part=None):
        if part is None:
            at = pl.ds(pl.multiple_of(dev * blk, 16), blk)
        else:
            at = pl.ds(pl.multiple_of(dev * blk + part * hb, 16), hb)
        if k == 2:
            return w_d.at[at, :]
        return w_gu.at[at, pl.ds(k * half, half)]

    def w_cols(core):
        return pl.ds(pl.multiple_of(core * half, LANES), half)

    def w_copy(k, link, part, core):
        return send(w_in[k].at[pl.ds(part * hb, hb), w_cols(core)], w_rows(k, me, part),
                    w_send.at[k, link, part, core], w_recv.at[k, link, part, j], dp=near(link, core))

    def w_own_copy(k):
        return pltpu.make_async_copy(w_in[k].at[:, w_cols(j)], w_rows(k, me), w_own.at[k])

    def w_partner_copy(k):
        return send(w_in[k].at[:, w_cols(1 - j)], w_rows(k, me), wp_send.at[k], wp_recv.at[k], dp=partner)

    def w_start(k):
        for first in (0, 1):
            for core in (0, 1):
                w_copy(k, 0, 1 - first, core).start()
                w_copy(k, 1, first, core).start()
        w_own_copy(k).start()
        w_partner_copy(k).start()

    def w_relay_copy(k, link_out, core):
        part = 1 if link_out == 1 else 0
        ref = w_rows(k, near(1 - link_out, core), part)
        return send(ref, ref, wr_send.at[k, link_out, core], wr_recv.at[k, link_out, core], dp=near(link_out, j))

    def w_relay(k):
        for core in (0, 1):
            wait(w_rows(k, near(0, core), 1), w_recv.at[k, 0, 1, core])
            w_relay_copy(k, 1, core).start()
            wait(w_rows(k, near(1, core), 0), w_recv.at[k, 1, 0, core])
            w_relay_copy(k, 0, core).start()

    def w_relayed(which):
        for k in which:
            for link in (0, 1):
                for core in (0, 1):
                    w_relay_copy(k, link, core).wait_send()

    def w_have(k, which):
        if which == 'chip':
            wait(w_rows(k, me), w_own.at[k])
            wait(w_rows(k, partner), wp_recv.at[k])
        for core in (0, 1):
            if which == 'x':
                wait(w_rows(k, near(0, core), 0), w_recv.at[k, 0, 0, core])
            if which == 'y':
                wait(w_rows(k, near(1, core), 1), w_recv.at[k, 1, 1, core])
            if which == 'far':
                wait(w_rows(k, far(core), 0), wr_recv.at[k, 0, core])
                wait(w_rows(k, far(core), 1), wr_recv.at[k, 1, core])

    def slot_of(ten, q, link):
        return tok_b[ten].at[q, pl.ds(link * piece, piece), :]

    def q_copy(ten, q, link):
        b = lax.div(q, 4)
        sub = lax.rem(q, 4)
        first = 1 - b if link == 0 else b
        src = tok[ten].at[pl.ds(pl.multiple_of(first * tile + sub * piece, piece), piece), :]
        return send(src, slot_of(ten, q, link), q_send.at[q, link, ten], q_recv.at[q, link, ten], dp=near(link, j))

    def q_start(q):
        for ten in (0, 1):
            for link in (0, 1):
                q_copy(ten, q, link).start()

    def relay_copy(ten, sub, link_out):
        return send(slot_of(ten, sub, 1 - link_out), slot_of(ten, 8 + sub, link_out),
                    rl_send.at[sub, link_out, ten], q_recv.at[8 + sub, link_out, ten], dp=near(link_out, j))

    def tile_part(ten, q, core):
        return tok_t[ten].at[lax.rem(q, 2), pl.ds(pl.multiple_of(core * 2 * piece, 2 * piece), 2 * piece), :]

    def forward_copy(ten, q):
        return send(tok_b[ten].at[q], tile_part(ten, q, j), f_send.at[q, ten], f_recv.at[q, ten], dp=partner)

    def own_copy(ten):
        return send(tok[ten], tok_p[ten], own_send.at[ten], own_recv.at[ten], dp=partner)

    def arrive(ten, q):
        with jax.named_scope('arrive'):
            for link in (0, 1):
                wait(slot_of(ten, q, link), q_recv.at[q, link, ten])
            if ten == 0:
                pl.semaphore_wait(room.at[0], 1)
            else:
                @pl.when(q < 11)
                def _():
                    pl.semaphore_wait(room.at[1], 1)

            forward_copy(ten, q).start()
            pltpu.make_async_copy(tok_b[ten].at[q], tile_part(ten, q, j), ld.at[ten, lax.rem(q, 2)]).start()

        @pl.when(q < 4)
        def _():
            for link in (0, 1):
                relay_copy(ten, q, link).start()

    def landed(ten, q):
        with jax.named_scope('landed'):
            wait(tile_part(ten, q, j), ld.at[ten, lax.rem(q, 2)])
            wait(tile_part(ten, q, 1 - j), f_recv.at[q, ten])

    def rows_of(r):
        return pl.ds(pl.multiple_of(r * tile, tile), tile)

    def load_a(ten, n):
        own = lax.div(n, 2)
        slot = lax.rem(n, 2)

        @pl.when(own == 1)
        def _():
            pltpu.make_async_copy(tok[ten].at[rows_of(slot), :], tok_t[ten].at[slot], ld.at[ten, slot]).start()

        @pl.when(own == 0)
        def _():
            pltpu.make_async_copy(tok_p[ten].at[rows_of(slot), :], tok_t[ten].at[slot], ld.at[ten, slot]).start()

    def loaded(ten, slot):
        with jax.named_scope('ld'):
            wait(tok_t[ten].at[slot], ld.at[ten, slot])

    def unit_col(u):
        mine = cy * units
        other = (1 - cy) * units
        low = cx * rest_units
        high = (1 - cx) * near_units
        a = near_units
        col = jnp.where(u < a, mine + low + u,
                        jnp.where(u < units, mine + high + (u - a),
                                  jnp.where(u < units + a, other + low + (u - units), other + high + (u - units - a))))
        return pl.multiple_of(col * LANES, LANES)

    def chunk(s, way):
        n = lax.rem(s, steps)
        row = pl.multiple_of(way * tile + lax.rem(n, 2) * part_rows, part_rows)
        return lax.div(s, steps), pl.ds(row, part_rows), pl.ds(unit_col(lax.div(n, 2)), LANES)

    def sum_copy(s, way, nxt):
        land = lax.rem(s, DEPTH)
        return send(yacc.at[chunk(s, way)], rbuf.at[way, land], rs_send.at[way, lax.rem(s, SLOTS)], rs_recv.at[way, land], tp=nxt)

    def done_copy(s, way, prv):
        ref = back.at[way, lax.rem(s, KEEP)]
        return send(ref, ref, ag_send.at[way, lax.rem(s, LAG + 1)], ag_recv.at[way, lax.rem(s, KEEP)], tp=prv)

    def store_copy(s, way):
        return pltpu.make_async_copy(back.at[way, lax.rem(s, KEEP)], yd_ref.at[chunk(s, way)],
                                     fin_own.at[way, lax.rem(s, LAG + 1)])

    def tick(tau):
        with jax.named_scope('tick'):
            tick_body(tau)

    def give(s, way, p, prv):
        @pl.when(s >= LAG)
        def _():
            store_copy(s - LAG, way).wait()

            @pl.when(p > 0)
            def _():
                wait(back.at[way, 0], ag_send.at[way, lax.rem(s - LAG, LAG + 1)])

        store_copy(s, way).start()

        @pl.when(p > 0)
        def _():
            done_copy(s, way, prv).start()

    def tick_body(tau):
        for way in (0, 1):
            p = t if way == 0 else 3 - t
            nxt = t + 1 if way == 0 else t - 1
            prv = t - 1 if way == 0 else t + 1
            s = tau - HOP * p
            slot = lax.rem(jnp.maximum(s, 0), SLOTS)
            land = lax.rem(jnp.maximum(s, 0), DEPTH)
            live = jnp.logical_and(s >= 0, s < 2 * steps)

            @pl.when(jnp.logical_and(live, p > 0))
            def _():
                wait(rbuf.at[way, land], rs_recv.at[way, land])

            @pl.when(jnp.logical_and(live, p < 3))
            def _():
                @pl.when(s >= SLOTS)
                def _():
                    wait(rbuf.at[way, 0], rs_send.at[way, slot])

                @pl.when(p > 0)
                def _():
                    here = chunk(s, way)
                    yacc[here] = yacc[here] + rbuf[way, land]

                sum_copy(s, way, nxt).start()

            @pl.when(jnp.logical_and(live, p == 3))
            def _():
                back[way, lax.rem(s, KEEP)] = (yacc[chunk(s, way)] + rbuf[way, land]).astype(BF16)
                give(s, way, p, prv)

        for way in (0, 1):
            p = t if way == 0 else 3 - t
            prv = t - 1 if way == 0 else t + 1
            s = tau - HOP * (6 - p)

            @pl.when(jnp.logical_and(jnp.logical_and(s >= 0, s < 2 * steps), p < 3))
            def _():
                keep = lax.rem(s, KEEP)
                wait(back.at[way, keep], ag_recv.at[way, keep])
                give(s, way, p, prv)

    def ticks(lo, hi):
        def body(n, c):
            tick(n)
            return c

        lax.fori_loop(lo, hi, body, 0)

    def drain_sums():
        for way in (0, 1):
            p = t if way == 0 else 3 - t

            @pl.when(p < 3)
            def _():
                for slot in range(SLOTS):
                    wait(rbuf.at[way, 0], rs_send.at[way, slot])

            for m in range(LAG):
                s = 2 * steps - LAG + m
                wait(back.at[way, 0], fin_own.at[way, s % (LAG + 1)])

                @pl.when(p > 0)
                def _():
                    wait(back.at[way, 0], ag_send.at[way, s % (LAG + 1)])

    w_start(0)
    w_start(1)
    for ten in (0, 1):
        own_copy(ten).start()
    base = jnp.where(t == 0, 1.0, 0.0).astype(F32)

    with jax.named_scope('clear'):
        for r in (0, 1):
            for ten in (0, 1):
                load_a(ten, 2 + r)

        def clear(n, carry):
            at = pl.ds(pl.multiple_of(n * 32, 32), 32)
            acc_gu[at, :] = jnp.zeros((32, 2 * half), F32)
            acc_d[at, :] = jnp.zeros((32, half), F32)
            return carry

        lax.fori_loop(0, win // 32, clear, 0)

        def clear_ab(n, carry):
            lo = pl.ds(pl.multiple_of(n * group, group), group)
            for m in range(4):
                ab_all[m, lo, :] = jnp.zeros((group, 2 * half), F32)
            return carry

        lax.fori_loop(0, tile // group, clear_ab, 0)
        for r in (0, 1):
            for ten in (0, 1):
                loaded(ten, r)

                def residual(n, carry):
                    lo = pl.ds(pl.multiple_of(n * group, group), group)
                    there = pl.ds(pl.multiple_of(r * tile + n * group, group), group)
                    yacc[ten, there, :] = tok_t[ten][r, lo, :].astype(F32) * base
                    return carry

                lax.fori_loop(0, tile // group, residual, 0)
        for ten in (0, 1):
            wait(tok_p[ten], own_recv.at[ten])

    with jax.named_scope('w_relay'):
        w_relay(0)
        w_relay(1)
    w_start(2)

    def side(n):
        return pl.ds(pl.multiple_of(lax.rem(n, 2) * half, LANES), half)

    def ab_pass(last):
        other = (1 - cy) * line
        if last:
            parts = ((other + (1 - cx) * near_units * LANES, rest_units * LANES),)
        else:
            parts = ((cy * line, line), (other + cx * rest_units * LANES, near_units * LANES))
        def body(n, carry):
            slot = lax.rem(n, 2)

            @pl.when(n < 3)
            def _():
                load_a(0, n + 1)

            loaded(0, slot)
            for at, size in parts:
                at_k = pl.ds(pl.multiple_of(at, LANES), size)
                with jax.named_scope('ab_part'):
                    for lo, hi in pieces:
                        ab_all[n, :, lo:hi] += dot_nn(xt[slot, :, at_k], w_gu[at_k, lo:hi])

            if last:
                def hidden(m, c):
                    lo = pl.ds(pl.multiple_of(m * group, group), group)
                    a = ab_all[n, lo, :half]
                    h_all[lax.div(n, 2), lo, side(n)] = (a * sigmoid(a) * ab_all[n, lo, half:]).astype(BF16)
                    return c

                lax.fori_loop(0, tile // group, hidden, 0)
            return carry

        lax.fori_loop(0, 4, body, 0)

    load_a(0, 0)
    with jax.named_scope('w_have'):
        for k in (0, 1):
            w_have(k, 'chip')
            w_have(k, 'x')
            w_have(k, 'y')
    ab_pass(0)
    load_a(0, 0)
    with jax.named_scope('w_have'):
        for k in (0, 1):
            w_have(k, 'far')
    ab_pass(1)

    def y_group(g, tau):
        u0 = (0, near_units, units, units + near_units)[g]
        n_u = (near_units, rest_units)[g % 2]
        col = unit_col(u0)
        cols = pl.ds(col, n_u * LANES)

        def theirs(r, carry):
            if g > 0:
                before = (near_units, rest_units)[(g - 1) % 2] * LANES
                wait(sb.at[r, :, pl.ds(0, before)], y_send.at[(g - 1) % 2, r])
            with jax.named_scope('y_dot'):
                sb[r, :, :n_u * LANES] = dot_nt(h_all[0, :, side(r)], w_d[cols, :])
            send(sb.at[r, :, pl.ds(0, n_u * LANES)], pbuf.at[rows_of(r), cols],
                 y_send.at[g % 2, r], y_recv.at[g, r], dp=partner).start()
            return carry

        def ours(r, carry):
            with jax.named_scope('y_wait'):
                wait(pbuf.at[rows_of(r), cols], y_recv.at[g, r])
            with jax.named_scope('y_dot'):
                yacc[0, rows_of(r), cols] = (yacc[0, rows_of(r), cols] + pbuf[rows_of(r), cols]
                                             + dot_nt(h_all[1, :, side(r)], w_d[cols, :]))
            pl.semaphore_signal(credit, inc=1, device_id={'dp': partner, 'tp': t}, device_id_type=MESH)
            return carry

        lax.fori_loop(0, 2, theirs, 0)
        if g > 0:
            tick(tau)
        lax.fori_loop(0, 2, ours, 0)
        if g > 0:
            tick(tau + 1)

    load_a(1, 0)
    load_a(0, 0)
    with jax.named_scope('w_have2'):
        w_have(2, 'chip')
    y_group(0, 0)
    tick(0)
    with jax.named_scope('w_relay2'):
        w_relay(2)
    q_start(0)
    q_start(1)
    ticks(1, 7)
    with jax.named_scope('w_have2'):
        w_have(2, 'x')
        w_have(2, 'y')
    y_group(1, 7)
    y_group(2, 9)
    q_start(2)
    ticks(11, 14)
    with jax.named_scope('w_have2'):
        w_have(2, 'far')
    y_group(3, 14)
    q_start(3)

    at_win, shift = window_of(chip * 2 * blk, win)
    own = own_window(blk)
    at_own, _ = window_of(me * blk, own)
    in_acc = pl.ds(pl.multiple_of(window_of(me * blk, own)[0].start - at_win.start, 8), own)
    n_block = 3
    n_cols = model // n_block

    def grad_copy(m):
        rows_ = pl.ds(pl.multiple_of(shift + (1 - j) * blk, 8), blk)
        there = pl.ds(pl.multiple_of(window_of(partner * blk, own)[1], 8), blk)
        if m == 0:
            return send(acc_gu.at[rows_, :], pbuf.at[there, pl.ds(0, 2 * half)], out_send.at[0], out_recv.at[0], dp=partner)
        return send(acc_d.at[rows_, :], yacc.at[0, there, pl.ds(0, half)], out_send.at[1], out_recv.at[1], dp=partner)

    def result_copy(ten):
        return pltpu.make_async_copy(yd_ref.at[ten], w_gu.at[pl.ds(ten * rows, rows), :], back_in.at[ten])

    def last_copy(m):
        if m == 0:
            return send(h_all.at[1], xt.at[0, :, pl.ds(0, 2 * half)], h_send.at[0], h_recv.at[0], dp=partner)
        return send(h_all.at[0, :, pl.ds(0, half)], dyt.at[0, :, pl.ds(0, half)], h_send.at[1], h_recv.at[1], dp=partner)

    def dx_tile(n):
        r = lax.rem(n, 2)

        @pl.when(n == 0)
        def _():
            pl.semaphore_wait(credit, 8)
            for r_ in (0, 1):
                wait(sb.at[r_, :, pl.ds(0, rest_units * LANES)], y_send.at[1, r_])

        def block(m, carry):
            cols = pl.ds(pl.multiple_of(m * n_cols, n_cols), n_cols)
            slot = lax.rem(m + r * n_block, 2)

            @pl.when(jnp.logical_and(n < 2, m + r * n_block >= 2))
            def _():
                wait(sb.at[slot], dx_send.at[slot])

            @pl.when(n < 2)
            def _():
                with jax.named_scope('dx_dot'):
                    sb[slot] = dot_nt(h_all[1], w_gu[cols, :])
                send(sb.at[slot], pbuf.at[rows_of(r), cols], dx_send.at[slot], dx_recv.at[r, m], dp=partner).start()

            @pl.when(n >= 2)
            def _():
                with jax.named_scope('dx_wait'):
                    wait(pbuf.at[rows_of(r), cols], dx_recv.at[r, m])
                with jax.named_scope('dx_dot'):
                    yacc[1, rows_of(r), cols] = (yacc[1, rows_of(r), cols] + pbuf[rows_of(r), cols]
                                                 + dot_nt(h_all[1], w_gu[cols, :]))

            @pl.when(m >= 1)
            def _():
                tick(17 + 4 * n + m)
            return carry

        lax.fori_loop(0, n_block, block, 0)

    def grad_tile(n, carry):
        q = n - 4
        slot = lax.rem(n, 2)
        at = jnp.where(n < 4, n, slot)
        final = n == 15
        early = jnp.logical_and(n >= 3, q + 1 <= EARLY)
        late = jnp.logical_and(n < 15, q + 1 > EARLY)
        dense = q >= 8
        extra = jnp.logical_and(dense, q < 10)
        tau = jnp.where(dense, jnp.where(q < 10, 64 + 5 * (q - 8), 74 + 4 * (q - 10)), 16 + 4 * n)

        @pl.when(n < 4)
        def _():
            q_start(4 + n)
            loaded(0, slot)

        @pl.when(extra)
        def _():
            tick(tau)

        step = jnp.where(extra, tau + 1, tau)

        @pl.when(n >= 4)
        def _():
            landed(0, q)
            with jax.named_scope('ab_dot'):
                ab_all[at, :, :cut] = dot_nn(xt[slot], w_gu[:, :cut])
            tick(step)

            @pl.when(jnp.logical_and(q > MIDDLE, n < 15))
            def _():
                arrive(1, q)

            with jax.named_scope('ab_dot'):
                ab_all[at, :, cut:] = dot_nn(xt[slot], w_gu[:, cut:])

            @pl.when(final)
            def _():
                pl.semaphore_wait(room.at[1], 2)
                arrive(1, q)
                with jax.named_scope('h_last'):
                    def body(m, c):
                        lo = pl.ds(pl.multiple_of(m * group, group), group)
                        a = ab_all[at, lo, :half]
                        h_all[0, lo, :half] = (a * sigmoid(a) * ab_all[at, lo, half:]).astype(BF16)
                        return c

                    lax.fori_loop(0, tile // group, body, 0)
                    last_copy(1).start()
                    grad_copy(1).start()
                    w_relayed((0, 1))
                    result_copy(0).start()

            tick(step + 1)

        @pl.when(early)
        def _():
            arrive(0, q + 1)
            arrive(1, q + 1)

        @pl.when(n < 4)
        def _():
            loaded(1, slot)

        @pl.when(n >= 4)
        def _():
            landed(1, q)

        with jax.named_scope('g_dot'):
            g_s[...] = dot_nn(dyt[slot], w_d[...])

        def activate(with_h):
            def body(m, c):
                lo = pl.ds(pl.multiple_of(m * group, group), group)
                a = ab_all[at, lo, :half]
                b = ab_all[at, lo, half:]
                g = g_s[lo, :]
                s = sigmoid(a)
                silu = a * s
                if with_h:
                    h_all[0, lo, :half] = (silu * b).astype(BF16)
                h_all[1, lo, :half] = (g * b * s * (1.0 + a * (1.0 - s))).astype(BF16)
                h_all[1, lo, half:] = (g * silu).astype(BF16)
                return c

            with jax.named_scope('act'):
                lax.fori_loop(0, tile // group, body, 0)

        @pl.when(final)
        def _():
            activate(False)

        @pl.when(jnp.logical_not(final))
        def _():
            activate(True)

        tick(step + jnp.where(n < 4, 0, 2))

        @pl.when(n < 3)
        def _():
            load_a(0, n + 1)
            load_a(1, n + 1)

        @pl.when(late)
        def _():
            arrive(0, q + 1)

        @pl.when(jnp.logical_not(final))
        def _():
            with jax.named_scope('dw_dot'):
                for lo in range(0, 2 * half, 2 * half // 3):
                    hi = lo + 2 * half // 3
                    acc_gu[:, lo:hi] += dot_tn(xt[slot, :, at_win], h_all[1, :, lo:hi])

            @pl.when(n == 14)
            def _():
                grad_copy(0).start()

            with jax.named_scope('dw_dot2'):
                for lo, hi in ((0, half // 2 // 128 * 128), (half // 2 // 128 * 128, half)):
                    acc_d[:, lo:hi] += dot_tn(dyt[slot, :, at_win], h_all[0, :, lo:hi])

        @pl.when(final)
        def _():
            pl.semaphore_wait(room.at[0], 1)
            last_copy(0).start()
            with jax.named_scope('grads_sent'):
                for m in (0, 1):
                    grad_copy(m).wait_send()
            with jax.named_scope('dw_own'):
                for lo, hi in pieces:
                    acc_gu[in_acc, lo:hi] += dot_tn(xt[1, :, at_own], h_all[1, :, lo:hi])
                acc_d[in_acc, :] += dot_tn(dyt[1, :, at_own], h_all[0, :, :half])

        @pl.when(jnp.logical_and(n >= 2, n < 15))
        def _():
            for ten in (0, 1):
                pl.semaphore_signal(room.at[ten], inc=1, device_id={'dp': partner, 'tp': t}, device_id_type=MESH)

        tick(step + jnp.where(n < 4, 1, 3))

        @pl.when(n < 4)
        def _():
            dx_tile(n)

        @pl.when(jnp.logical_and(late, q + 1 <= MIDDLE))
        def _():
            arrive(1, q + 1)
        return carry

    lax.fori_loop(0, 16, grad_tile, 0)

    tick(82)
    theirs = pl.ds(pl.multiple_of(window_of(me * blk, own)[1], 8), blk)
    with jax.named_scope('last_wait_h'):
        wait(yacc.at[0, theirs, pl.ds(0, half)], out_recv.at[1])
        wait(dyt.at[0, :, pl.ds(0, half)], h_recv.at[1])
    with jax.named_scope('dw_other'):
        yacc[0, :own, :half] += dot_tn(dyt[1, :, at_own], dyt[0, :, :half])
    tick(83)
    with jax.named_scope('drain_sums'):
        drain_sums()
    result_copy(1).start()
    with jax.named_scope('last_wait'):
        wait(pbuf.at[theirs, pl.ds(0, 2 * half)], out_recv.at[0])
        wait(xt.at[0, :, pl.ds(0, 2 * half)], h_recv.at[0])
    with jax.named_scope('dw_other'):
        for lo, hi in pieces:
            pbuf[:own, lo:hi] += dot_tn(xt[1, :, at_own], xt[0, :, lo:hi])

    with jax.named_scope('drain'):
        for ten in (0, 1):
            result_copy(ten).wait()
        for slot in (0, 1):
            wait(sb.at[slot], dx_send.at[slot])
        for k in range(3):
            for core in (0, 1):
                for link in (0, 1):
                    for part in (0, 1):
                        w_copy(k, link, part, core).wait_send()
            w_partner_copy(k).wait_send()
        w_relayed((2,))
        for ten in (0, 1):
            own_copy(ten).wait_send()

        def drain(q, carry):
            for ten in (0, 1):
                wait(tok_b[ten].at[0], f_send.at[q, ten])
                for link in (0, 1):
                    @pl.when(q < 8)
                    def _():
                        wait(slot_of(ten, 0, link), q_send.at[lax.rem(q, 8), link, ten])

                    @pl.when(q < 4)
                    def _():
                        wait(slot_of(ten, 0, link), rl_send.at[lax.rem(q, 4), link, ten])

            return carry

        lax.fori_loop(0, 12, drain, 0)
        for m in (0, 1):
            last_copy(m).wait_send()


def window_of(start, size):
    first = lax.div(start, LANES) * LANES
    return pl.ds(pl.multiple_of(first, LANES), size), start - first


def own_window(blk):
    return -(-(blk + LANES - 32) // LANES) * LANES


def window(model, blk):
    starts = [(2 * blk * c) // LANES * LANES for c in range(model // (2 * blk))]
    shift = max(2 * blk * c - s for c, s in enumerate(starts))
    return -(-(shift + 2 * blk) // LANES) * LANES


def mlp(x, dy, wg, wu, wd):
    rows, model = x.shape
    blk, width = wg.shape
    half = width // 2
    tile = rows // 2
    dma = pltpu.SemaphoreType.DMA
    vmem = pltpu.VMEM
    anywhere = pl.BlockSpec(memory_space=pl.ANY)
    shape = jax.ShapeDtypeStruct
    flops = 2 * model * half * rows * 2 * 20
    win = window(model, blk)
    most = max(rows, own_window(blk))
    kept = (vmem((win, 2 * half), F32), vmem((win, half), F32), vmem((most, model), F32), vmem((2, most, model), F32))
    kept = (*kept, vmem((model, 2 * half), BF16))
    held = sum(k.dtype.itemsize * math.prod(k.shape) for k in kept)
    in_vmem = pl.BlockSpec(memory_space=pltpu.VMEM)
    return pl.pallas_call(
        kernel,
        name='mlp',
        out_shape=(shape((2, rows, model), BF16), *kept,
                   shape((12, tile // 2, model), BF16), shape((12, tile // 2, model), BF16),
                   shape((rows, model), BF16), shape((rows, model), BF16)),
        in_specs=[anywhere] * 5,
        out_specs=(anywhere, *[in_vmem] * 5, *[anywhere] * 4),
        scratch_shapes=[
            vmem((model, half), BF16),
            vmem((2, tile, model // 3), F32),
            vmem((2, tile, model), BF16),
            vmem((2, tile, model), BF16),
            vmem((4, tile, 2 * half), F32),
            vmem((tile, half), F32),
            vmem((2, tile, 2 * half), BF16),
            vmem((2, DEPTH, tile // 2, LANES), F32),
            vmem((2, KEEP, tile // 2, LANES), BF16),
            dma((3, 2, 2, 2)), dma((3, 2, 2, 2)), dma((3, 2, 2)), dma((3, 2, 2)), dma((3,)), dma((3,)), dma((3,)),
            dma((2,)), dma((2,)), dma((8, 2, 2)), dma((12, 2, 2)), dma((4, 2, 2)), dma((12, 2)), dma((12, 2)),
            dma((2, 2)), dma((4, 2)), dma((2,)), dma((2, 3)), pltpu.SemaphoreType.REGULAR, pltpu.SemaphoreType.REGULAR((2,)),
            dma((2, SLOTS)), dma((2, DEPTH)), dma((2, LAG + 1)), dma((2, KEEP)), dma((2, LAG + 1)),
            dma((2, 2)), dma((2,)), dma((2,)), dma((2,)), dma((2,)), dma((2,)),
        ],
        compiler_params=pltpu.CompilerParams(collective_id=0, has_side_effects=True, vmem_limit_bytes=67_000_000 - held),
        cost_estimate=pl.CostEstimate(flops=flops, bytes_accessed=100_000_000, transcendentals=0),
    )(x, dy, wg, wu, wd)


def results_kernel(blk, half, acc_gu, acc_d, pbuf, yacc, w_gu, y_out, dx_out, g_out, u_out, d_out, sem):
    me = lax.axis_index('dp')
    j = lax.rem(me, 2)
    chip = lax.div(me, 2)
    rows = y_out.shape[0]
    mine = pl.ds(pl.multiple_of(window_of(chip * 2 * blk, LANES)[1] + j * blk, 8), blk)
    other = pl.ds(pl.multiple_of(window_of(me * blk, LANES)[1], 8), blk)
    own_cols = pl.ds(pl.multiple_of(j * half, LANES), half)
    other_cols = pl.ds(pl.multiple_of((1 - j) * half, LANES), half)
    low, high = pl.ds(0, half), pl.ds(half, half)
    copies = [pltpu.make_async_copy(src, dst, sem.at[n]) for n, (src, dst) in enumerate((
        (acc_gu.at[mine, low], g_out.at[:, own_cols]), (acc_gu.at[mine, high], u_out.at[:, own_cols]),
        (acc_d.at[mine, :], d_out.at[:, own_cols]),
        (pbuf.at[other, low], g_out.at[:, other_cols]), (pbuf.at[other, high], u_out.at[:, other_cols]),
        (yacc.at[0, other, low], d_out.at[:, other_cols]),
        (w_gu.at[pl.ds(0, rows), :], y_out), (w_gu.at[pl.ds(rows, rows), :], dx_out)))]
    for copy in copies:
        copy.start()
    for copy in copies:
        copy.wait()


def results(blk, width, rows, *kept):
    anywhere = pl.BlockSpec(memory_space=pl.ANY)
    in_vmem = pl.BlockSpec(memory_space=pltpu.VMEM)
    shape = jax.ShapeDtypeStruct
    model = kept[-1].shape[0]
    kept = [pltpu.with_memory_space_constraint(k, pltpu.VMEM) for k in kept]
    return pl.pallas_call(
        functools.partial(results_kernel, blk, width // 2),
        name='results',
        out_shape=(shape((rows, model), BF16), shape((rows, model), BF16),
                   shape((blk, width), F32), shape((blk, width), F32), shape((blk, width), F32)),
        in_specs=[in_vmem] * 5,
        out_specs=tuple([anywhere] * 5),
        scratch_shapes=[pltpu.SemaphoreType.DMA((8,))],
        compiler_params=pltpu.CompilerParams(vmem_limit_bytes=4_000_000),
    )(*kept)


def solution(mesh):
    def device_pass(x_rows, gate_blk, up_blk, down_blk, dy_rows):
        out = mlp(x_rows, dy_rows, gate_blk, up_blk, down_blk.T)
        y, dx, dw_gate, dw_up, dw_down = results(*gate_blk.shape, x_rows.shape[0], *out[1:6])
        return y, dx, dw_gate, dw_up, dw_down.T

    row_spec = P('dp', None)
    weight_spec = P('dp', 'tp')
    down_spec = P('tp', 'dp')
    return jax.shard_map(device_pass, mesh=mesh,
                         in_specs=(row_spec, weight_spec, weight_spec, down_spec, row_spec),
                         out_specs=(row_spec, row_spec, weight_spec, weight_spec, down_spec),
                         check_vma=False)
```

```python
import functools
import math

import jax
import jax.numpy as jnp
from jax import lax
from jax.experimental import pallas as pl
from jax.experimental.pallas import tpu as pltpu
from jax.sharding import PartitionSpec as P

F32 = jnp.float32
BF16 = jnp.bfloat16
MESH = pl.DeviceIdType.MESH
SLOTS = 8
DEPTH = 13
KEEP = 16
LAG = 3
HOP = 2
LANES = 128
EARLY = 4
MIDDLE = 8


def dot_nn(a, b):
    return jnp.dot(a, b, preferred_element_type=F32)


def dot_nt(a, b):
    return lax.dot_general(a, b, (((1,), (1,)), ((), ())), preferred_element_type=F32)


def dot_tn(a, b):
    return lax.dot_general(a, b, (((0,), (0,)), ((), ())), preferred_element_type=F32)


def sigmoid(a):
    return 1.0 / (1.0 + jnp.exp(-a))


def kernel(x_ref, dy_ref, wg_ref, wu_ref, wd_ref,
           yd_ref, acc_gu, acc_d, pbuf, yacc, w_gu, xb, dyb, xp, dyp,
           w_d, sb, xt, dyt, ab_all, g_s, h_all, rbuf, back,
           w_send, w_recv, wr_send, wr_recv, w_own, wp_send, wp_recv,
           own_send, own_recv, q_send, q_recv, rl_send, f_send, f_recv,
           y_send, y_recv, dx_send, dx_recv, credit, room,
           rs_send, rs_recv, ag_send, ag_recv, fin_own, ld, out_send, out_recv, h_send, h_recv, back_in):
    rows, model = x_ref.shape
    blk, width = wg_ref.shape
    half = width // 2
    hb = blk // 2
    tile = rows // 2
    piece = tile // 4
    win = acc_d.shape[0]
    line = model // 2
    units = line // LANES
    near_units = (2 * blk - LANES // 2) // LANES if (2 * blk) % LANES else 2 * blk // LANES
    rest_units = units - near_units
    steps = 4 * units
    part_rows = tile // 2
    group = min(32, tile)
    w_in = (wg_ref, wu_ref, wd_ref)
    cut = (half + 255) // 256 * 256
    pieces = ((0, cut), (cut, 2 * half))
    cut_ab = max(cut, 4 * half // 3 // 256 * 256)
    cut_g = half // 2 // 256 * 256
    tok = (x_ref, dy_ref)
    tok_b = (xb, dyb)
    tok_p = (xp, dyp)
    tok_t = (xt, dyt)

    t = lax.axis_index('tp')
    me = lax.axis_index('dp')
    cy = lax.div(me, 4)
    cx = lax.rem(lax.div(me, 2), 2)
    j = lax.rem(me, 2)
    partner = me + 1 - 2 * j
    chip = cy * 2 + cx

    def near(link, core):
        if link == 0:
            return cy * 4 + (1 - cx) * 2 + core
        return (1 - cy) * 4 + cx * 2 + core

    def far(core):
        return (1 - cy) * 4 + (1 - cx) * 2 + core

    def send(src, dst, s_sem, r_sem, dp=None, tp=None):
        where = {'dp': me if dp is None else dp, 'tp': t if tp is None else tp}
        return pltpu.make_async_remote_copy(src_ref=src, dst_ref=dst, send_sem=s_sem, recv_sem=r_sem,
                                            device_id=where, device_id_type=MESH)

    def wait(ref, sem):
        pltpu.make_async_copy(ref, ref, sem).wait()

    barrier = pltpu.get_barrier_semaphore()
    for peer in (partner, near(0, 0), near(0, 1), near(1, 0), near(1, 1)):
        pl.semaphore_signal(barrier, inc=1, device_id={'dp': peer, 'tp': t}, device_id_type=MESH)

    @pl.when(t > 0)
    def _():
        pl.semaphore_signal(barrier, inc=1, device_id={'dp': me, 'tp': t - 1}, device_id_type=MESH)

    @pl.when(t < 3)
    def _():
        pl.semaphore_signal(barrier, inc=1, device_id={'dp': me, 'tp': t + 1}, device_id_type=MESH)

    pl.semaphore_wait(barrier, 5 + jnp.minimum(t, 1) + jnp.minimum(3 - t, 1))

    def w_rows(k, dev, part=None):
        if part is None:
            at = pl.ds(pl.multiple_of(dev * blk, 16), blk)
        else:
            at = pl.ds(pl.multiple_of(dev * blk + part * hb, 16), hb)
        if k == 2:
            return w_d.at[at, :]
        return w_gu.at[at, pl.ds(k * half, half)]

    def w_cols(core):
        return pl.ds(pl.multiple_of(core * half, LANES), half)

    def w_copy(k, link, part, core):
        return send(w_in[k].at[pl.ds(part * hb, hb), w_cols(core)], w_rows(k, me, part),
                    w_send.at[k, link, part, core], w_recv.at[k, link, part, j], dp=near(link, core))

    def w_own_copy(k):
        return pltpu.make_async_copy(w_in[k].at[:, w_cols(j)], w_rows(k, me), w_own.at[k])

    def w_partner_copy(k):
        return send(w_in[k].at[:, w_cols(1 - j)], w_rows(k, me), wp_send.at[k], wp_recv.at[k], dp=partner)

    def w_start(k):
        for first in (0, 1):
            for core in (0, 1):
                w_copy(k, 0, 1 - first, core).start()
                w_copy(k, 1, first, core).start()
        w_own_copy(k).start()
        w_partner_copy(k).start()

    def w_relay_copy(k, link_out, core):
        part = 1 if link_out == 1 else 0
        ref = w_rows(k, near(1 - link_out, core), part)
        return send(ref, ref, wr_send.at[k, link_out, core], wr_recv.at[k, link_out, core], dp=near(link_out, j))

    def w_relay(k):
        for core in (0, 1):
            wait(w_rows(k, near(0, core), 1), w_recv.at[k, 0, 1, core])
            w_relay_copy(k, 1, core).start()
            wait(w_rows(k, near(1, core), 0), w_recv.at[k, 1, 0, core])
            w_relay_copy(k, 0, core).start()

    def w_relayed(which):
        for k in which:
            for link in (0, 1):
                for core in (0, 1):
                    w_relay_copy(k, link, core).wait_send()

    def w_have(k, which):
        if which == 'chip':
            wait(w_rows(k, me), w_own.at[k])
            wait(w_rows(k, partner), wp_recv.at[k])
        for core in (0, 1):
            if which == 'x':
                wait(w_rows(k, near(0, core), 0), w_recv.at[k, 0, 0, core])
            if which == 'y':
                wait(w_rows(k, near(1, core), 1), w_recv.at[k, 1, 1, core])
            if which == 'far':
                wait(w_rows(k, far(core), 0), wr_recv.at[k, 0, core])
                wait(w_rows(k, far(core), 1), wr_recv.at[k, 1, core])

    def slot_of(ten, q, link):
        return tok_b[ten].at[q, pl.ds(link * piece, piece), :]

    def q_copy(ten, q, link):
        b = lax.div(q, 4)
        sub = lax.rem(q, 4)
        first = 1 - b if link == 0 else b
        src = tok[ten].at[pl.ds(pl.multiple_of(first * tile + sub * piece, piece), piece), :]
        return send(src, slot_of(ten, q, link), q_send.at[q, link, ten], q_recv.at[q, link, ten], dp=near(link, j))

    def q_start(q):
        for ten in (0, 1):
            for link in (0, 1):
                q_copy(ten, q, link).start()

    def relay_copy(ten, sub, link_out):
        return send(slot_of(ten, sub, 1 - link_out), slot_of(ten, 8 + sub, link_out),
                    rl_send.at[sub, link_out, ten], q_recv.at[8 + sub, link_out, ten], dp=near(link_out, j))

    def tile_part(ten, q, core):
        return tok_t[ten].at[lax.rem(q, 2), pl.ds(pl.multiple_of(core * 2 * piece, 2 * piece), 2 * piece), :]

    def forward_copy(ten, q):
        return send(tok_b[ten].at[q], tile_part(ten, q, j), f_send.at[q, ten], f_recv.at[q, ten], dp=partner)

    def own_copy(ten):
        return send(tok[ten], tok_p[ten], own_send.at[ten], own_recv.at[ten], dp=partner)

    def arrive(ten, q):
        with jax.named_scope('arrive'):
            for link in (0, 1):
                wait(slot_of(ten, q, link), q_recv.at[q, link, ten])
            if ten == 0:
                pl.semaphore_wait(room.at[0], 1)
            else:
                @pl.when(q < 11)
                def _():
                    pl.semaphore_wait(room.at[1], 1)

            forward_copy(ten, q).start()
            pltpu.make_async_copy(tok_b[ten].at[q], tile_part(ten, q, j), ld.at[ten, lax.rem(q, 2)]).start()

        @pl.when(q < 4)
        def _():
            for link in (0, 1):
                relay_copy(ten, q, link).start()

    def landed(ten, q):
        with jax.named_scope('landed'):
            wait(tile_part(ten, q, j), ld.at[ten, lax.rem(q, 2)])
            wait(tile_part(ten, q, 1 - j), f_recv.at[q, ten])

    def rows_of(r):
        return pl.ds(pl.multiple_of(r * tile, tile), tile)

    def load_a(ten, n):
        own = lax.div(n, 2)
        slot = lax.rem(n, 2)

        @pl.when(own == 1)
        def _():
            pltpu.make_async_copy(tok[ten].at[rows_of(slot), :], tok_t[ten].at[slot], ld.at[ten, slot]).start()

        @pl.when(own == 0)
        def _():
            pltpu.make_async_copy(tok_p[ten].at[rows_of(slot), :], tok_t[ten].at[slot], ld.at[ten, slot]).start()

    def loaded(ten, slot):
        with jax.named_scope('ld'):
            wait(tok_t[ten].at[slot], ld.at[ten, slot])

    def unit_col(u):
        mine = cy * units
        other = (1 - cy) * units
        low = cx * rest_units
        high = (1 - cx) * near_units
        a = near_units
        col = jnp.where(u < a, mine + low + u,
                        jnp.where(u < units, mine + high + (u - a),
                                  jnp.where(u < units + a, other + low + (u - units), other + high + (u - units - a))))
        return pl.multiple_of(col * LANES, LANES)

    def chunk(s, way):
        n = lax.rem(s, steps)
        row = pl.multiple_of(way * tile + lax.rem(n, 2) * part_rows, part_rows)
        return lax.div(s, steps), pl.ds(row, part_rows), pl.ds(unit_col(lax.div(n, 2)), LANES)

    def sum_copy(s, way, nxt):
        land = lax.rem(s, DEPTH)
        return send(yacc.at[chunk(s, way)], rbuf.at[way, land], rs_send.at[way, lax.rem(s, SLOTS)], rs_recv.at[way, land], tp=nxt)

    def done_copy(s, way, prv):
        ref = back.at[way, lax.rem(s, KEEP)]
        return send(ref, ref, ag_send.at[way, lax.rem(s, LAG + 1)], ag_recv.at[way, lax.rem(s, KEEP)], tp=prv)

    def store_copy(s, way):
        return pltpu.make_async_copy(back.at[way, lax.rem(s, KEEP)], yd_ref.at[chunk(s, way)],
                                     fin_own.at[way, lax.rem(s, LAG + 1)])

    def tick(tau):
        with jax.named_scope('tick'):
            tick_body(tau)

    def give(s, way, p, prv):
        @pl.when(s >= LAG)
        def _():
            store_copy(s - LAG, way).wait()

            @pl.when(p > 0)
            def _():
                wait(back.at[way, 0], ag_send.at[way, lax.rem(s - LAG, LAG + 1)])

        store_copy(s, way).start()

        @pl.when(p > 0)
        def _():
            done_copy(s, way, prv).start()

    def tick_body(tau):
        for way in (0, 1):
            p = t if way == 0 else 3 - t
            nxt = t + 1 if way == 0 else t - 1
            prv = t - 1 if way == 0 else t + 1
            s = tau - HOP * p
            slot = lax.rem(jnp.maximum(s, 0), SLOTS)
            land = lax.rem(jnp.maximum(s, 0), DEPTH)
            live = jnp.logical_and(s >= 0, s < 2 * steps)

            @pl.when(jnp.logical_and(live, p > 0))
            def _():
                wait(rbuf.at[way, land], rs_recv.at[way, land])

            @pl.when(jnp.logical_and(live, p < 3))
            def _():
                @pl.when(s >= SLOTS)
                def _():
                    wait(rbuf.at[way, 0], rs_send.at[way, slot])

                @pl.when(p > 0)
                def _():
                    here = chunk(s, way)
                    yacc[here] = yacc[here] + rbuf[way, land]

                sum_copy(s, way, nxt).start()

            @pl.when(jnp.logical_and(live, p == 3))
            def _():
                back[way, lax.rem(s, KEEP)] = (yacc[chunk(s, way)] + rbuf[way, land]).astype(BF16)
                give(s, way, p, prv)

        for way in (0, 1):
            p = t if way == 0 else 3 - t
            prv = t - 1 if way == 0 else t + 1
            s = tau - HOP * (6 - p)

            @pl.when(jnp.logical_and(jnp.logical_and(s >= 0, s < 2 * steps), p < 3))
            def _():
                keep = lax.rem(s, KEEP)
                wait(back.at[way, keep], ag_recv.at[way, keep])
                give(s, way, p, prv)

    def ticks(lo, hi):
        def body(n, c):
            tick(n)
            return c

        lax.fori_loop(lo, hi, body, 0)

    def drain_sums():
        for way in (0, 1):
            p = t if way == 0 else 3 - t

            @pl.when(p < 3)
            def _():
                for slot in range(SLOTS):
                    wait(rbuf.at[way, 0], rs_send.at[way, slot])

            for m in range(LAG):
                s = 2 * steps - LAG + m
                wait(back.at[way, 0], fin_own.at[way, s % (LAG + 1)])

                @pl.when(p > 0)
                def _():
                    wait(back.at[way, 0], ag_send.at[way, s % (LAG + 1)])

    w_start(0)
    w_start(1)
    for ten in (0, 1):
        own_copy(ten).start()
    base = jnp.where(t == 0, 1.0, 0.0).astype(F32)

    with jax.named_scope('clear'):
        for r in (0, 1):
            for ten in (0, 1):
                load_a(ten, 2 + r)

        def clear(n, carry):
            at = pl.ds(pl.multiple_of(n * 32, 32), 32)
            acc_gu[at, :] = jnp.zeros((32, 2 * half), F32)
            acc_d[at, :] = jnp.zeros((32, half), F32)
            return carry

        lax.fori_loop(0, win // 32, clear, 0)

        def clear_ab(n, carry):
            lo = pl.ds(pl.multiple_of(n * group, group), group)
            for m in range(4):
                ab_all[m, lo, :] = jnp.zeros((group, 2 * half), F32)
            return carry

        lax.fori_loop(0, tile // group, clear_ab, 0)
        for r in (0, 1):
            for ten in (0, 1):
                loaded(ten, r)

                def residual(n, carry):
                    lo = pl.ds(pl.multiple_of(n * group, group), group)
                    there = pl.ds(pl.multiple_of(r * tile + n * group, group), group)
                    yacc[ten, there, :] = tok_t[ten][r, lo, :].astype(F32) * base
                    return carry

                lax.fori_loop(0, tile // group, residual, 0)
        for ten in (0, 1):
            wait(tok_p[ten], own_recv.at[ten])

    with jax.named_scope('w_relay'):
        w_relay(0)
        w_relay(1)
    w_start(2)

    def side(n):
        return pl.ds(pl.multiple_of(lax.rem(n, 2) * half, LANES), half)

    def ab_pass(last):
        other = (1 - cy) * line
        if last:
            parts = ((other + (1 - cx) * near_units * LANES, rest_units * LANES),)
        else:
            parts = ((cy * line, line), (other + cx * rest_units * LANES, near_units * LANES))
        def body(n, carry):
            slot = lax.rem(n, 2)

            @pl.when(n < 3)
            def _():
                load_a(0, n + 1)

            loaded(0, slot)
            for at, size in parts:
                at_k = pl.ds(pl.multiple_of(at, LANES), size)
                with jax.named_scope('ab_part'):
                    for lo, hi in pieces:
                        ab_all[n, :, lo:hi] += dot_nn(xt[slot, :, at_k], w_gu[at_k, lo:hi])

            if last:
                def hidden(m, c):
                    lo = pl.ds(pl.multiple_of(m * group, group), group)
                    a = ab_all[n, lo, :half]
                    h_all[lax.div(n, 2), lo, side(n)] = (a * sigmoid(a) * ab_all[n, lo, half:]).astype(BF16)
                    return c

                lax.fori_loop(0, tile // group, hidden, 0)
            return carry

        lax.fori_loop(0, 4, body, 0)

    load_a(0, 0)
    with jax.named_scope('w_have'):
        for k in (0, 1):
            w_have(k, 'chip')
            w_have(k, 'x')
            w_have(k, 'y')
    ab_pass(0)
    load_a(0, 0)
    with jax.named_scope('w_have'):
        for k in (0, 1):
            w_have(k, 'far')
    ab_pass(1)

    def y_group(g, tau):
        u0 = (0, near_units, units, units + near_units)[g]
        n_u = (near_units, rest_units)[g % 2]
        col = unit_col(u0)
        cols = pl.ds(col, n_u * LANES)

        def theirs(r, carry):
            if g > 0:
                before = (near_units, rest_units)[(g - 1) % 2] * LANES
                wait(sb.at[r, :, pl.ds(0, before)], y_send.at[(g - 1) % 2, r])
            with jax.named_scope('y_dot'):
                sb[r, :, :n_u * LANES] = dot_nt(h_all[0, :, side(r)], w_d[cols, :])
            send(sb.at[r, :, pl.ds(0, n_u * LANES)], pbuf.at[rows_of(r), cols],
                 y_send.at[g % 2, r], y_recv.at[g, r], dp=partner).start()
            return carry

        def ours(r, carry):
            with jax.named_scope('y_wait'):
                wait(pbuf.at[rows_of(r), cols], y_recv.at[g, r])
            with jax.named_scope('y_dot'):
                yacc[0, rows_of(r), cols] = (yacc[0, rows_of(r), cols] + pbuf[rows_of(r), cols]
                                             + dot_nt(h_all[1, :, side(r)], w_d[cols, :]))
            pl.semaphore_signal(credit, inc=1, device_id={'dp': partner, 'tp': t}, device_id_type=MESH)
            return carry

        lax.fori_loop(0, 2, theirs, 0)
        if g > 0:
            tick(tau)
        lax.fori_loop(0, 2, ours, 0)
        if g > 0:
            tick(tau + 1)

    load_a(1, 0)
    load_a(0, 0)
    with jax.named_scope('w_have2'):
        w_have(2, 'chip')
    y_group(0, 0)
    tick(0)
    with jax.named_scope('w_relay2'):
        w_relay(2)
    q_start(0)
    q_start(1)
    ticks(1, 7)
    with jax.named_scope('w_have2'):
        w_have(2, 'x')
        w_have(2, 'y')
    y_group(1, 7)
    y_group(2, 9)
    q_start(2)
    ticks(11, 14)
    with jax.named_scope('w_have2'):
        w_have(2, 'far')
    y_group(3, 14)
    q_start(3)

    at_win, shift = window_of(chip * 2 * blk, win)
    own = own_window(blk)
    at_own, _ = window_of(me * blk, own)
    in_acc = pl.ds(pl.multiple_of(window_of(me * blk, own)[0].start - at_win.start, 8), own)
    n_block = 3
    n_cols = model // n_block

    def grad_copy(m):
        rows_ = pl.ds(pl.multiple_of(shift + (1 - j) * blk, 8), blk)
        there = pl.ds(pl.multiple_of(window_of(partner * blk, own)[1], 8), blk)
        if m == 0:
            return send(acc_gu.at[rows_, :], pbuf.at[there, pl.ds(0, 2 * half)], out_send.at[0], out_recv.at[0], dp=partner)
        return send(acc_d.at[rows_, :], yacc.at[0, there, pl.ds(0, half)], out_send.at[1], out_recv.at[1], dp=partner)

    def result_copy(ten):
        return pltpu.make_async_copy(yd_ref.at[ten], w_gu.at[pl.ds(ten * rows, rows), :], back_in.at[ten])

    def last_copy(m):
        if m == 0:
            return send(h_all.at[1], xt.at[0, :, pl.ds(0, 2 * half)], h_send.at[0], h_recv.at[0], dp=partner)
        return send(h_all.at[0, :, pl.ds(0, half)], dyt.at[0, :, pl.ds(0, half)], h_send.at[1], h_recv.at[1], dp=partner)

    def dx_tile(n):
        r = lax.rem(n, 2)

        @pl.when(n == 0)
        def _():
            pl.semaphore_wait(credit, 8)
            for r_ in (0, 1):
                wait(sb.at[r_, :, pl.ds(0, rest_units * LANES)], y_send.at[1, r_])

        def block(m, carry):
            cols = pl.ds(pl.multiple_of(m * n_cols, n_cols), n_cols)
            slot = lax.rem(m + r * n_block, 2)

            @pl.when(jnp.logical_and(n < 2, m + r * n_block >= 2))
            def _():
                wait(sb.at[slot], dx_send.at[slot])

            @pl.when(n < 2)
            def _():
                with jax.named_scope('dx_dot'):
                    sb[slot] = dot_nt(h_all[1], w_gu[cols, :])
                send(sb.at[slot], pbuf.at[rows_of(r), cols], dx_send.at[slot], dx_recv.at[r, m], dp=partner).start()

            @pl.when(n >= 2)
            def _():
                with jax.named_scope('dx_wait'):
                    wait(pbuf.at[rows_of(r), cols], dx_recv.at[r, m])
                with jax.named_scope('dx_dot'):
                    yacc[1, rows_of(r), cols] = (yacc[1, rows_of(r), cols] + pbuf[rows_of(r), cols]
                                                 + dot_nt(h_all[1], w_gu[cols, :]))

            @pl.when(m >= 1)
            def _():
                tick(17 + 4 * n + m)
            return carry

        lax.fori_loop(0, n_block, block, 0)

    def grad_tile(n, carry):
        q = n - 4
        slot = lax.rem(n, 2)
        at = jnp.where(n < 4, n, slot)
        final = n == 15
        early = jnp.logical_and(n >= 3, q + 1 <= EARLY)
        late = jnp.logical_and(n < 15, q + 1 > EARLY)
        dense = q >= 8
        extra = jnp.logical_and(dense, q < 10)
        tau = jnp.where(dense, jnp.where(q < 10, 64 + 5 * (q - 8), 74 + 4 * (q - 10)), 16 + 4 * n)

        @pl.when(n < 4)
        def _():
            q_start(4 + n)
            loaded(0, slot)

        @pl.when(extra)
        def _():
            tick(tau)

        step = jnp.where(extra, tau + 1, tau)

        @pl.when(n >= 4)
        def _():
            landed(0, q)
            with jax.named_scope('ab_dot'):
                ab_all[at, :, :cut_ab] = dot_nn(xt[slot], w_gu[:, :cut_ab])
            tick(step)

            @pl.when(jnp.logical_and(q > MIDDLE, n < 15))
            def _():
                arrive(1, q)

            with jax.named_scope('ab_dot'):
                ab_all[at, :, cut_ab:] = dot_nn(xt[slot], w_gu[:, cut_ab:])

            @pl.when(final)
            def _():
                pl.semaphore_wait(room.at[1], 2)
                arrive(1, q)
                with jax.named_scope('h_last'):
                    def body(m, c):
                        lo = pl.ds(pl.multiple_of(m * group, group), group)
                        a = ab_all[at, lo, :half]
                        h_all[0, lo, :half] = (a * sigmoid(a) * ab_all[at, lo, half:]).astype(BF16)
                        return c

                    lax.fori_loop(0, tile // group, body, 0)
                    last_copy(1).start()
                    grad_copy(1).start()
                    w_relayed((0, 1))
                    result_copy(0).start()

        @pl.when(early)
        def _():
            arrive(0, q + 1)
            arrive(1, q + 1)

        @pl.when(n < 4)
        def _():
            loaded(1, slot)

        @pl.when(n >= 4)
        def _():
            landed(1, q)

        with jax.named_scope('g_dot'):
            g_s[:, :cut_g] = dot_nn(dyt[slot], w_d[:, :cut_g])

        @pl.when(n >= 4)
        def _():
            tick(step + 1)

        with jax.named_scope('g_dot'):
            g_s[:, cut_g:] = dot_nn(dyt[slot], w_d[:, cut_g:])

        def activate(with_h):
            def body(m, c):
                lo = pl.ds(pl.multiple_of(m * group, group), group)
                a = ab_all[at, lo, :half]
                b = ab_all[at, lo, half:]
                g = g_s[lo, :]
                s = sigmoid(a)
                silu = a * s
                if with_h:
                    h_all[0, lo, :half] = (silu * b).astype(BF16)
                h_all[1, lo, :half] = (g * b * s * (1.0 + a * (1.0 - s))).astype(BF16)
                h_all[1, lo, half:] = (g * silu).astype(BF16)
                return c

            with jax.named_scope('act'):
                lax.fori_loop(0, tile // group, body, 0)

        @pl.when(final)
        def _():
            activate(False)

        @pl.when(jnp.logical_not(final))
        def _():
            activate(True)

        tick(step + jnp.where(n < 4, 0, 2))

        @pl.when(n < 3)
        def _():
            load_a(0, n + 1)
            load_a(1, n + 1)

        @pl.when(late)
        def _():
            arrive(0, q + 1)

        @pl.when(jnp.logical_not(final))
        def _():
            with jax.named_scope('dw_dot'):
                for lo in range(0, 2 * half, 2 * half // 3):
                    hi = lo + 2 * half // 3
                    acc_gu[:, lo:hi] += dot_tn(xt[slot, :, at_win], h_all[1, :, lo:hi])

            @pl.when(n == 14)
            def _():
                grad_copy(0).start()

            with jax.named_scope('dw_dot2'):
                for lo, hi in ((0, half // 2 // 128 * 128), (half // 2 // 128 * 128, half)):
                    acc_d[:, lo:hi] += dot_tn(dyt[slot, :, at_win], h_all[0, :, lo:hi])

        @pl.when(final)
        def _():
            pl.semaphore_wait(room.at[0], 1)
            last_copy(0).start()
            with jax.named_scope('grads_sent'):
                grad_copy(0).wait_send()
            with jax.named_scope('dw_own'):
                for lo, hi in pieces:
                    acc_gu[in_acc, lo:hi] += dot_tn(xt[1, :, at_own], h_all[1, :, lo:hi])
            with jax.named_scope('grads_sent'):
                grad_copy(1).wait_send()
            with jax.named_scope('dw_own'):
                acc_d[in_acc, :] += dot_tn(dyt[1, :, at_own], h_all[0, :, :half])

        @pl.when(jnp.logical_and(n >= 2, n < 15))
        def _():
            for ten in (0, 1):
                pl.semaphore_signal(room.at[ten], inc=1, device_id={'dp': partner, 'tp': t}, device_id_type=MESH)

        tick(step + jnp.where(n < 4, 1, 3))

        @pl.when(n < 4)
        def _():
            dx_tile(n)

        @pl.when(jnp.logical_and(late, q + 1 <= MIDDLE))
        def _():
            arrive(1, q + 1)
        return carry

    lax.fori_loop(0, 16, grad_tile, 0)

    tick(82)
    theirs = pl.ds(pl.multiple_of(window_of(me * blk, own)[1], 8), blk)
    with jax.named_scope('last_wait_h'):
        wait(yacc.at[0, theirs, pl.ds(0, half)], out_recv.at[1])
        wait(dyt.at[0, :, pl.ds(0, half)], h_recv.at[1])
    with jax.named_scope('dw_other'):
        yacc[0, :own, :half] += dot_tn(dyt[1, :, at_own], dyt[0, :, :half])
    tick(83)
    with jax.named_scope('drain_sums'):
        drain_sums()
    result_copy(1).start()
    with jax.named_scope('last_wait'):
        wait(pbuf.at[theirs, pl.ds(0, 2 * half)], out_recv.at[0])
        wait(xt.at[0, :, pl.ds(0, 2 * half)], h_recv.at[0])
    with jax.named_scope('dw_other'):
        for lo, hi in pieces:
            pbuf[:own, lo:hi] += dot_tn(xt[1, :, at_own], xt[0, :, lo:hi])

    with jax.named_scope('drain'):
        for ten in (0, 1):
            result_copy(ten).wait()
        for slot in (0, 1):
            wait(sb.at[slot], dx_send.at[slot])
        for k in range(3):
            for core in (0, 1):
                for link in (0, 1):
                    for part in (0, 1):
                        w_copy(k, link, part, core).wait_send()
            w_partner_copy(k).wait_send()
        w_relayed((2,))
        for ten in (0, 1):
            own_copy(ten).wait_send()

        def drain(q, carry):
            for ten in (0, 1):
                wait(tok_b[ten].at[0], f_send.at[q, ten])
                for link in (0, 1):
                    @pl.when(q < 8)
                    def _():
                        wait(slot_of(ten, 0, link), q_send.at[lax.rem(q, 8), link, ten])

                    @pl.when(q < 4)
                    def _():
                        wait(slot_of(ten, 0, link), rl_send.at[lax.rem(q, 4), link, ten])

            return carry

        lax.fori_loop(0, 12, drain, 0)
        for m in (0, 1):
            last_copy(m).wait_send()


def window_of(start, size):
    first = lax.div(start, LANES) * LANES
    return pl.ds(pl.multiple_of(first, LANES), size), start - first


def own_window(blk):
    return -(-(blk + LANES - 32) // LANES) * LANES


def window(model, blk):
    starts = [(2 * blk * c) // LANES * LANES for c in range(model // (2 * blk))]
    shift = max(2 * blk * c - s for c, s in enumerate(starts))
    return -(-(shift + 2 * blk) // LANES) * LANES


def mlp(x, dy, wg, wu, wd):
    rows, model = x.shape
    blk, width = wg.shape
    half = width // 2
    tile = rows // 2
    dma = pltpu.SemaphoreType.DMA
    vmem = pltpu.VMEM
    anywhere = pl.BlockSpec(memory_space=pl.ANY)
    shape = jax.ShapeDtypeStruct
    flops = 2 * model * half * rows * 2 * 20
    win = window(model, blk)
    most = max(rows, own_window(blk))
    kept = (vmem((win, 2 * half), F32), vmem((win, half), F32), vmem((most, model), F32), vmem((2, most, model), F32))
    kept = (*kept, vmem((model, 2 * half), BF16))
    held = sum(k.dtype.itemsize * math.prod(k.shape) for k in kept)
    in_vmem = pl.BlockSpec(memory_space=pltpu.VMEM)
    return pl.pallas_call(
        kernel,
        name='mlp',
        out_shape=(shape((2, rows, model), BF16), *kept,
                   shape((12, tile // 2, model), BF16), shape((12, tile // 2, model), BF16),
                   shape((rows, model), BF16), shape((rows, model), BF16)),
        in_specs=[anywhere] * 5,
        out_specs=(anywhere, *[in_vmem] * 5, *[anywhere] * 4),
        scratch_shapes=[
            vmem((model, half), BF16),
            vmem((2, tile, model // 3), F32),
            vmem((2, tile, model), BF16),
            vmem((2, tile, model), BF16),
            vmem((4, tile, 2 * half), F32),
            vmem((tile, half), F32),
            vmem((2, tile, 2 * half), BF16),
            vmem((2, DEPTH, tile // 2, LANES), F32),
            vmem((2, KEEP, tile // 2, LANES), BF16),
            dma((3, 2, 2, 2)), dma((3, 2, 2, 2)), dma((3, 2, 2)), dma((3, 2, 2)), dma((3,)), dma((3,)), dma((3,)),
            dma((2,)), dma((2,)), dma((8, 2, 2)), dma((12, 2, 2)), dma((4, 2, 2)), dma((12, 2)), dma((12, 2)),
            dma((2, 2)), dma((4, 2)), dma((2,)), dma((2, 3)), pltpu.SemaphoreType.REGULAR, pltpu.SemaphoreType.REGULAR((2,)),
            dma((2, SLOTS)), dma((2, DEPTH)), dma((2, LAG + 1)), dma((2, KEEP)), dma((2, LAG + 1)),
            dma((2, 2)), dma((2,)), dma((2,)), dma((2,)), dma((2,)), dma((2,)),
        ],
        compiler_params=pltpu.CompilerParams(collective_id=0, has_side_effects=True, vmem_limit_bytes=67_000_000 - held),
        cost_estimate=pl.CostEstimate(flops=flops, bytes_accessed=100_000_000, transcendentals=0),
    )(x, dy, wg, wu, wd)


def results_kernel(blk, half, acc_gu, acc_d, pbuf, yacc, w_gu, y_out, dx_out, g_out, u_out, d_out, sem):
    me = lax.axis_index('dp')
    j = lax.rem(me, 2)
    chip = lax.div(me, 2)
    rows = y_out.shape[0]
    mine = pl.ds(pl.multiple_of(window_of(chip * 2 * blk, LANES)[1] + j * blk, 8), blk)
    other = pl.ds(pl.multiple_of(window_of(me * blk, LANES)[1], 8), blk)
    own_cols = pl.ds(pl.multiple_of(j * half, LANES), half)
    other_cols = pl.ds(pl.multiple_of((1 - j) * half, LANES), half)
    low, high = pl.ds(0, half), pl.ds(half, half)
    copies = [pltpu.make_async_copy(src, dst, sem.at[n]) for n, (src, dst) in enumerate((
        (acc_gu.at[mine, low], g_out.at[:, own_cols]), (acc_gu.at[mine, high], u_out.at[:, own_cols]),
        (acc_d.at[mine, :], d_out.at[:, own_cols]),
        (pbuf.at[other, low], g_out.at[:, other_cols]), (pbuf.at[other, high], u_out.at[:, other_cols]),
        (yacc.at[0, other, low], d_out.at[:, other_cols]),
        (w_gu.at[pl.ds(0, rows), :], y_out), (w_gu.at[pl.ds(rows, rows), :], dx_out)))]
    for copy in copies:
        copy.start()
    for copy in copies:
        copy.wait()


def results(blk, width, rows, *kept):
    anywhere = pl.BlockSpec(memory_space=pl.ANY)
    in_vmem = pl.BlockSpec(memory_space=pltpu.VMEM)
    shape = jax.ShapeDtypeStruct
    model = kept[-1].shape[0]
    kept = [pltpu.with_memory_space_constraint(k, pltpu.VMEM) for k in kept]
    return pl.pallas_call(
        functools.partial(results_kernel, blk, width // 2),
        name='results',
        out_shape=(shape((rows, model), BF16), shape((rows, model), BF16),
                   shape((blk, width), F32), shape((blk, width), F32), shape((blk, width), F32)),
        in_specs=[in_vmem] * 5,
        out_specs=tuple([anywhere] * 5),
        scratch_shapes=[pltpu.SemaphoreType.DMA((8,))],
        compiler_params=pltpu.CompilerParams(vmem_limit_bytes=4_000_000),
    )(*kept)


def solution(mesh):
    def device_pass(x_rows, gate_blk, up_blk, down_blk, dy_rows):
        out = mlp(x_rows, dy_rows, gate_blk, up_blk, down_blk.T)
        y, dx, dw_gate, dw_up, dw_down = results(*gate_blk.shape, x_rows.shape[0], *out[1:6])
        return y, dx, dw_gate, dw_up, dw_down.T

    row_spec = P('dp', None)
    weight_spec = P('dp', 'tp')
    down_spec = P('tp', 'dp')
    return jax.shard_map(device_pass, mesh=mesh,
                         in_specs=(row_spec, weight_spec, weight_spec, down_spec, row_spec),
                         out_specs=(row_spec, row_spec, weight_spec, weight_spec, down_spec),
                         check_vma=False)
```

```python
import functools
import math

import jax
import jax.numpy as jnp
from jax import lax
from jax.experimental import pallas as pl
from jax.experimental.pallas import tpu as pltpu
from jax.sharding import PartitionSpec as P

F32 = jnp.float32
BF16 = jnp.bfloat16
MESH = pl.DeviceIdType.MESH
SLOTS = 8
DEPTH = 13
KEEP = 16
LAG = 3
HOP = 2
LANES = 128
EARLY = 4
MIDDLE = 8


def dot_nn(a, b):
    return jnp.dot(a, b, preferred_element_type=F32)


def dot_nt(a, b):
    return lax.dot_general(a, b, (((1,), (1,)), ((), ())), preferred_element_type=F32)


def dot_tn(a, b):
    return lax.dot_general(a, b, (((0,), (0,)), ((), ())), preferred_element_type=F32)


def sigmoid(a):
    return 1.0 / (1.0 + jnp.exp(-a))


def kernel(x_ref, dy_ref, wg_ref, wu_ref, wd_ref,
           yd_ref, acc_gu, acc_d, pbuf, yacc, w_gu, xb, dyb, xp, dyp,
           w_d, sb, xt, dyt, ab_all, g_s, h_all, rbuf, back,
           w_send, w_recv, wr_send, wr_recv, w_own, wp_send, wp_recv,
           own_send, own_recv, q_send, q_recv, rl_send, f_send, f_recv,
           y_send, y_recv, dx_send, dx_recv, credit, room,
           rs_send, rs_recv, ag_send, ag_recv, fin_own, ld, out_send, out_recv, h_send, h_recv, back_in):
    rows, model = x_ref.shape
    blk, width = wg_ref.shape
    half = width // 2
    hb = blk // 2
    tile = rows // 2
    piece = tile // 4
    win = acc_d.shape[0]
    line = model // 2
    units = line // LANES
    near_units = (2 * blk - LANES // 2) // LANES if (2 * blk) % LANES else 2 * blk // LANES
    rest_units = units - near_units
    steps = 4 * units
    part_rows = tile // 2
    group = min(32, tile)
    w_in = (wg_ref, wu_ref, wd_ref)
    cut = (half + 255) // 256 * 256
    pieces = ((0, cut), (cut, 2 * half))
    cut_ab = cut
    cut_g = half // 2 // 256 * 256
    tok = (x_ref, dy_ref)
    tok_b = (xb, dyb)
    tok_p = (xp, dyp)
    tok_t = (xt, dyt)

    t = lax.axis_index('tp')
    me = lax.axis_index('dp')
    cy = lax.div(me, 4)
    cx = lax.rem(lax.div(me, 2), 2)
    j = lax.rem(me, 2)
    partner = me + 1 - 2 * j
    chip = cy * 2 + cx

    def near(link, core):
        if link == 0:
            return cy * 4 + (1 - cx) * 2 + core
        return (1 - cy) * 4 + cx * 2 + core

    def far(core):
        return (1 - cy) * 4 + (1 - cx) * 2 + core

    def send(src, dst, s_sem, r_sem, dp=None, tp=None):
        where = {'dp': me if dp is None else dp, 'tp': t if tp is None else tp}
        return pltpu.make_async_remote_copy(src_ref=src, dst_ref=dst, send_sem=s_sem, recv_sem=r_sem,
                                            device_id=where, device_id_type=MESH)

    def wait(ref, sem):
        pltpu.make_async_copy(ref, ref, sem).wait()

    barrier = pltpu.get_barrier_semaphore()
    for peer in (partner, near(0, 0), near(0, 1), near(1, 0), near(1, 1)):
        pl.semaphore_signal(barrier, inc=1, device_id={'dp': peer, 'tp': t}, device_id_type=MESH)

    @pl.when(t > 0)
    def _():
        pl.semaphore_signal(barrier, inc=1, device_id={'dp': me, 'tp': t - 1}, device_id_type=MESH)

    @pl.when(t < 3)
    def _():
        pl.semaphore_signal(barrier, inc=1, device_id={'dp': me, 'tp': t + 1}, device_id_type=MESH)

    pl.semaphore_wait(barrier, 5 + jnp.minimum(t, 1) + jnp.minimum(3 - t, 1))

    def w_rows(k, dev, part=None):
        if part is None:
            at = pl.ds(pl.multiple_of(dev * blk, 16), blk)
        else:
            at = pl.ds(pl.multiple_of(dev * blk + part * hb, 16), hb)
        if k == 2:
            return w_d.at[at, :]
        return w_gu.at[at, pl.ds(k * half, half)]

    def w_cols(core):
        return pl.ds(pl.multiple_of(core * half, LANES), half)

    def w_copy(k, link, part, core):
        return send(w_in[k].at[pl.ds(part * hb, hb), w_cols(core)], w_rows(k, me, part),
                    w_send.at[k, link, part, core], w_recv.at[k, link, part, j], dp=near(link, core))

    def w_own_copy(k):
        return pltpu.make_async_copy(w_in[k].at[:, w_cols(j)], w_rows(k, me), w_own.at[k])

    def w_partner_copy(k):
        return send(w_in[k].at[:, w_cols(1 - j)], w_rows(k, me), wp_send.at[k], wp_recv.at[k], dp=partner)

    def w_start(k):
        for first in (0, 1):
            for core in (0, 1):
                w_copy(k, 0, 1 - first, core).start()
                w_copy(k, 1, first, core).start()
        w_own_copy(k).start()
        w_partner_copy(k).start()

    def w_relay_copy(k, link_out, core):
        part = 1 if link_out == 1 else 0
        ref = w_rows(k, near(1 - link_out, core), part)
        return send(ref, ref, wr_send.at[k, link_out, core], wr_recv.at[k, link_out, core], dp=near(link_out, j))

    def w_relay(k):
        for core in (0, 1):
            wait(w_rows(k, near(0, core), 1), w_recv.at[k, 0, 1, core])
            w_relay_copy(k, 1, core).start()
            wait(w_rows(k, near(1, core), 0), w_recv.at[k, 1, 0, core])
            w_relay_copy(k, 0, core).start()

    def w_relayed(which):
        for k in which:
            for link in (0, 1):
                for core in (0, 1):
                    w_relay_copy(k, link, core).wait_send()

    def w_have(k, which):
        if which == 'chip':
            wait(w_rows(k, me), w_own.at[k])
            wait(w_rows(k, partner), wp_recv.at[k])
        for core in (0, 1):
            if which == 'x':
                wait(w_rows(k, near(0, core), 0), w_recv.at[k, 0, 0, core])
            if which == 'y':
                wait(w_rows(k, near(1, core), 1), w_recv.at[k, 1, 1, core])
            if which == 'far':
                wait(w_rows(k, far(core), 0), wr_recv.at[k, 0, core])
                wait(w_rows(k, far(core), 1), wr_recv.at[k, 1, core])

    def slot_of(ten, q, link):
        return tok_b[ten].at[q, pl.ds(link * piece, piece), :]

    def q_copy(ten, q, link):
        b = lax.div(q, 4)
        sub = lax.rem(q, 4)
        first = 1 - b if link == 0 else b
        src = tok[ten].at[pl.ds(pl.multiple_of(first * tile + sub * piece, piece), piece), :]
        return send(src, slot_of(ten, q, link), q_send.at[q, link, ten], q_recv.at[q, link, ten], dp=near(link, j))

    def q_start(q):
        for ten in (0, 1):
            for link in (0, 1):
                q_copy(ten, q, link).start()

    def relay_copy(ten, sub, link_out):
        return send(slot_of(ten, sub, 1 - link_out), slot_of(ten, 8 + sub, link_out),
                    rl_send.at[sub, link_out, ten], q_recv.at[8 + sub, link_out, ten], dp=near(link_out, j))

    def tile_part(ten, q, core):
        return tok_t[ten].at[lax.rem(q, 2), pl.ds(pl.multiple_of(core * 2 * piece, 2 * piece), 2 * piece), :]

    def forward_copy(ten, q):
        return send(tok_b[ten].at[q], tile_part(ten, q, j), f_send.at[q, ten], f_recv.at[q, ten], dp=partner)

    def own_copy(ten):
        return send(tok[ten], tok_p[ten], own_send.at[ten], own_recv.at[ten], dp=partner)

    def arrive(ten, q):
        with jax.named_scope('arrive'):
            for link in (0, 1):
                wait(slot_of(ten, q, link), q_recv.at[q, link, ten])
            if ten == 0:
                pl.semaphore_wait(room.at[0], 1)
            else:
                @pl.when(q < 11)
                def _():
                    pl.semaphore_wait(room.at[1], 1)

            forward_copy(ten, q).start()
            pltpu.make_async_copy(tok_b[ten].at[q], tile_part(ten, q, j), ld.at[ten, lax.rem(q, 2)]).start()

        @pl.when(q < 4)
        def _():
            for link in (0, 1):
                relay_copy(ten, q, link).start()

    def landed(ten, q):
        with jax.named_scope('landed'):
            wait(tile_part(ten, q, j), ld.at[ten, lax.rem(q, 2)])
            wait(tile_part(ten, q, 1 - j), f_recv.at[q, ten])

    def rows_of(r):
        return pl.ds(pl.multiple_of(r * tile, tile), tile)

    def load_a(ten, n):
        own = lax.div(n, 2)
        slot = lax.rem(n, 2)

        @pl.when(own == 1)
        def _():
            pltpu.make_async_copy(tok[ten].at[rows_of(slot), :], tok_t[ten].at[slot], ld.at[ten, slot]).start()

        @pl.when(own == 0)
        def _():
            pltpu.make_async_copy(tok_p[ten].at[rows_of(slot), :], tok_t[ten].at[slot], ld.at[ten, slot]).start()

    def loaded(ten, slot):
        with jax.named_scope('ld'):
            wait(tok_t[ten].at[slot], ld.at[ten, slot])

    def unit_col(u):
        mine = cy * units
        other = (1 - cy) * units
        low = cx * rest_units
        high = (1 - cx) * near_units
        a = near_units
        col = jnp.where(u < a, mine + low + u,
                        jnp.where(u < units, mine + high + (u - a),
                                  jnp.where(u < units + a, other + low + (u - units), other + high + (u - units - a))))
        return pl.multiple_of(col * LANES, LANES)

    def chunk(s, way):
        n = lax.rem(s, steps)
        row = pl.multiple_of(way * tile + lax.rem(n, 2) * part_rows, part_rows)
        return lax.div(s, steps), pl.ds(row, part_rows), pl.ds(unit_col(lax.div(n, 2)), LANES)

    def sum_copy(s, way, nxt):
        land = lax.rem(s, DEPTH)
        return send(yacc.at[chunk(s, way)], rbuf.at[way, land], rs_send.at[way, lax.rem(s, SLOTS)], rs_recv.at[way, land], tp=nxt)

    def done_copy(s, way, prv):
        ref = back.at[way, lax.rem(s, KEEP)]
        return send(ref, ref, ag_send.at[way, lax.rem(s, LAG + 1)], ag_recv.at[way, lax.rem(s, KEEP)], tp=prv)

    def store_copy(s, way):
        return pltpu.make_async_copy(back.at[way, lax.rem(s, KEEP)], yd_ref.at[chunk(s, way)],
                                     fin_own.at[way, lax.rem(s, LAG + 1)])

    def tick(tau):
        with jax.named_scope('tick'):
            tick_body(tau)

    def give(s, way, p, prv):
        @pl.when(s >= LAG)
        def _():
            store_copy(s - LAG, way).wait()

            @pl.when(p > 0)
            def _():
                wait(back.at[way, 0], ag_send.at[way, lax.rem(s - LAG, LAG + 1)])

        store_copy(s, way).start()

        @pl.when(p > 0)
        def _():
            done_copy(s, way, prv).start()

    def tick_body(tau):
        for way in (0, 1):
            p = t if way == 0 else 3 - t
            nxt = t + 1 if way == 0 else t - 1
            prv = t - 1 if way == 0 else t + 1
            s = tau - HOP * p
            slot = lax.rem(jnp.maximum(s, 0), SLOTS)
            land = lax.rem(jnp.maximum(s, 0), DEPTH)
            live = jnp.logical_and(s >= 0, s < 2 * steps)

            @pl.when(jnp.logical_and(live, p > 0))
            def _():
                wait(rbuf.at[way, land], rs_recv.at[way, land])

            @pl.when(jnp.logical_and(live, p < 3))
            def _():
                @pl.when(s >= SLOTS)
                def _():
                    wait(rbuf.at[way, 0], rs_send.at[way, slot])

                @pl.when(p > 0)
                def _():
                    here = chunk(s, way)
                    yacc[here] = yacc[here] + rbuf[way, land]

                sum_copy(s, way, nxt).start()

            @pl.when(jnp.logical_and(live, p == 3))
            def _():
                back[way, lax.rem(s, KEEP)] = (yacc[chunk(s, way)] + rbuf[way, land]).astype(BF16)
                give(s, way, p, prv)

        for way in (0, 1):
            p = t if way == 0 else 3 - t
            prv = t - 1 if way == 0 else t + 1
            s = tau - HOP * (6 - p)

            @pl.when(jnp.logical_and(jnp.logical_and(s >= 0, s < 2 * steps), p < 3))
            def _():
                keep = lax.rem(s, KEEP)
                wait(back.at[way, keep], ag_recv.at[way, keep])
                give(s, way, p, prv)

    def ticks(lo, hi):
        def body(n, c):
            tick(n)
            return c

        lax.fori_loop(lo, hi, body, 0)

    def drain_sums():
        for way in (0, 1):
            p = t if way == 0 else 3 - t

            @pl.when(p < 3)
            def _():
                for slot in range(SLOTS):
                    wait(rbuf.at[way, 0], rs_send.at[way, slot])

            for m in range(LAG):
                s = 2 * steps - LAG + m
                wait(back.at[way, 0], fin_own.at[way, s % (LAG + 1)])

                @pl.when(p > 0)
                def _():
                    wait(back.at[way, 0], ag_send.at[way, s % (LAG + 1)])

    w_start(0)
    w_start(1)
    for ten in (0, 1):
        own_copy(ten).start()
    base = jnp.where(t == 0, 1.0, 0.0).astype(F32)

    with jax.named_scope('clear'):
        for r in (0, 1):
            for ten in (0, 1):
                load_a(ten, 2 + r)

        def clear(n, carry):
            at = pl.ds(pl.multiple_of(n * 32, 32), 32)
            acc_gu[at, :] = jnp.zeros((32, 2 * half), F32)
            acc_d[at, :] = jnp.zeros((32, half), F32)
            return carry

        lax.fori_loop(0, win // 32, clear, 0)

        def clear_ab(n, carry):
            lo = pl.ds(pl.multiple_of(n * group, group), group)
            for m in range(4):
                ab_all[m, lo, :] = jnp.zeros((group, 2 * half), F32)
            return carry

        lax.fori_loop(0, tile // group, clear_ab, 0)
        for r in (0, 1):
            for ten in (0, 1):
                loaded(ten, r)

                def residual(n, carry):
                    lo = pl.ds(pl.multiple_of(n * group, group), group)
                    there = pl.ds(pl.multiple_of(r * tile + n * group, group), group)
                    yacc[ten, there, :] = tok_t[ten][r, lo, :].astype(F32) * base
                    return carry

                lax.fori_loop(0, tile // group, residual, 0)
        for ten in (0, 1):
            wait(tok_p[ten], own_recv.at[ten])

    with jax.named_scope('w_relay'):
        w_relay(0)
        w_relay(1)
    w_start(2)

    def side(n):
        return pl.ds(pl.multiple_of(lax.rem(n, 2) * half, LANES), half)

    def ab_pass(last):
        other = (1 - cy) * line
        if last:
            parts = ((other + (1 - cx) * near_units * LANES, rest_units * LANES),)
        else:
            parts = ((cy * line, line), (other + cx * rest_units * LANES, near_units * LANES))
        def body(n, carry):
            slot = lax.rem(n, 2)

            @pl.when(n < 3)
            def _():
                load_a(0, n + 1)

            loaded(0, slot)
            for at, size in parts:
                at_k = pl.ds(pl.multiple_of(at, LANES), size)
                with jax.named_scope('ab_part'):
                    for lo, hi in pieces:
                        ab_all[n, :, lo:hi] += dot_nn(xt[slot, :, at_k], w_gu[at_k, lo:hi])

            if last:
                def hidden(m, c):
                    lo = pl.ds(pl.multiple_of(m * group, group), group)
                    a = ab_all[n, lo, :half]
                    h_all[lax.div(n, 2), lo, side(n)] = (a * sigmoid(a) * ab_all[n, lo, half:]).astype(BF16)
                    return c

                lax.fori_loop(0, tile // group, hidden, 0)
            return carry

        lax.fori_loop(0, 4, body, 0)

    load_a(0, 0)
    with jax.named_scope('w_have'):
        for k in (0, 1):
            w_have(k, 'chip')
            w_have(k, 'x')
            w_have(k, 'y')
    ab_pass(0)
    load_a(0, 0)
    with jax.named_scope('w_have'):
        for k in (0, 1):
            w_have(k, 'far')
    ab_pass(1)

    def y_group(g, tau):
        u0 = (0, near_units, units, units + near_units)[g]
        n_u = (near_units, rest_units)[g % 2]
        col = unit_col(u0)
        cols = pl.ds(col, n_u * LANES)

        def theirs(r, carry):
            if g > 0:
                before = (near_units, rest_units)[(g - 1) % 2] * LANES
                wait(sb.at[r, :, pl.ds(0, before)], y_send.at[(g - 1) % 2, r])
            with jax.named_scope('y_dot'):
                sb[r, :, :n_u * LANES] = dot_nt(h_all[0, :, side(r)], w_d[cols, :])
            send(sb.at[r, :, pl.ds(0, n_u * LANES)], pbuf.at[rows_of(r), cols],
                 y_send.at[g % 2, r], y_recv.at[g, r], dp=partner).start()
            return carry

        def ours(r, carry):
            with jax.named_scope('y_wait'):
                wait(pbuf.at[rows_of(r), cols], y_recv.at[g, r])
            with jax.named_scope('y_dot'):
                yacc[0, rows_of(r), cols] = (yacc[0, rows_of(r), cols] + pbuf[rows_of(r), cols]
                                             + dot_nt(h_all[1, :, side(r)], w_d[cols, :]))
            pl.semaphore_signal(credit, inc=1, device_id={'dp': partner, 'tp': t}, device_id_type=MESH)
            return carry

        lax.fori_loop(0, 2, theirs, 0)
        if g > 0:
            tick(tau)
        lax.fori_loop(0, 2, ours, 0)
        if g > 0:
            tick(tau + 1)

    load_a(1, 0)
    load_a(0, 0)
    with jax.named_scope('w_have2'):
        w_have(2, 'chip')
    y_group(0, 0)
    tick(0)
    with jax.named_scope('w_relay2'):
        w_relay(2)
    q_start(0)
    q_start(1)
    ticks(1, 7)
    with jax.named_scope('w_have2'):
        w_have(2, 'x')
        w_have(2, 'y')
    y_group(1, 7)
    y_group(2, 9)
    q_start(2)
    ticks(11, 14)
    with jax.named_scope('w_have2'):
        w_have(2, 'far')
    y_group(3, 14)
    q_start(3)

    at_win, shift = window_of(chip * 2 * blk, win)
    own = own_window(blk)
    at_own, _ = window_of(me * blk, own)
    in_acc = pl.ds(pl.multiple_of(window_of(me * blk, own)[0].start - at_win.start, 8), own)
    n_block = 3
    n_cols = model // n_block

    def grad_copy(m):
        rows_ = pl.ds(pl.multiple_of(shift + (1 - j) * blk, 8), blk)
        there = pl.ds(pl.multiple_of(window_of(partner * blk, own)[1], 8), blk)
        if m == 0:
            return send(acc_gu.at[rows_, :], pbuf.at[there, pl.ds(0, 2 * half)], out_send.at[0], out_recv.at[0], dp=partner)
        return send(acc_d.at[rows_, :], yacc.at[0, there, pl.ds(0, half)], out_send.at[1], out_recv.at[1], dp=partner)

    def result_copy(ten):
        return pltpu.make_async_copy(yd_ref.at[ten], w_gu.at[pl.ds(ten * rows, rows), :], back_in.at[ten])

    def last_copy(m):
        if m == 0:
            return send(h_all.at[1], xt.at[0, :, pl.ds(0, 2 * half)], h_send.at[0], h_recv.at[0], dp=partner)
        return send(h_all.at[0, :, pl.ds(0, half)], dyt.at[0, :, pl.ds(0, half)], h_send.at[1], h_recv.at[1], dp=partner)

    def dx_tile(n):
        r = lax.rem(n, 2)

        @pl.when(n == 0)
        def _():
            pl.semaphore_wait(credit, 8)
            for r_ in (0, 1):
                wait(sb.at[r_, :, pl.ds(0, rest_units * LANES)], y_send.at[1, r_])

        def block(m, carry):
            cols = pl.ds(pl.multiple_of(m * n_cols, n_cols), n_cols)
            slot = lax.rem(m + r * n_block, 2)

            @pl.when(jnp.logical_and(n < 2, m + r * n_block >= 2))
            def _():
                wait(sb.at[slot], dx_send.at[slot])

            @pl.when(n < 2)
            def _():
                with jax.named_scope('dx_dot'):
                    sb[slot] = dot_nt(h_all[1], w_gu[cols, :])
                send(sb.at[slot], pbuf.at[rows_of(r), cols], dx_send.at[slot], dx_recv.at[r, m], dp=partner).start()

            @pl.when(n >= 2)
            def _():
                with jax.named_scope('dx_wait'):
                    wait(pbuf.at[rows_of(r), cols], dx_recv.at[r, m])
                with jax.named_scope('dx_dot'):
                    yacc[1, rows_of(r), cols] = (yacc[1, rows_of(r), cols] + pbuf[rows_of(r), cols]
                                                 + dot_nt(h_all[1], w_gu[cols, :]))

            @pl.when(m >= 1)
            def _():
                tick(17 + 4 * n + m)
            return carry

        lax.fori_loop(0, n_block, block, 0)

    def grad_tile(n, carry):
        q = n - 4
        slot = lax.rem(n, 2)
        at = jnp.where(n < 4, n, slot)
        final = n == 15
        early = jnp.logical_and(n >= 3, q + 1 <= EARLY)
        late = jnp.logical_and(n < 15, q + 1 > EARLY)
        dense = q >= 8
        extra = jnp.logical_and(dense, q < 10)
        tau = jnp.where(dense, jnp.where(q < 10, 64 + 5 * (q - 8), 74 + 4 * (q - 10)), 16 + 4 * n)

        @pl.when(n < 4)
        def _():
            q_start(4 + n)
            loaded(0, slot)

        @pl.when(extra)
        def _():
            tick(tau)

        step = jnp.where(extra, tau + 1, tau)

        @pl.when(n >= 4)
        def _():
            landed(0, q)
            with jax.named_scope('ab_dot'):
                ab_all[at, :, :cut_ab] = dot_nn(xt[slot], w_gu[:, :cut_ab])
            tick(step)

            @pl.when(jnp.logical_and(q > MIDDLE, n < 15))
            def _():
                arrive(1, q)

            with jax.named_scope('ab_dot'):
                ab_all[at, :, cut_ab:] = dot_nn(xt[slot], w_gu[:, cut_ab:])

            @pl.when(final)
            def _():
                pl.semaphore_wait(room.at[1], 2)
                arrive(1, q)
                with jax.named_scope('h_last'):
                    def body(m, c):
                        lo = pl.ds(pl.multiple_of(m * group, group), group)
                        a = ab_all[at, lo, :half]
                        h_all[0, lo, :half] = (a * sigmoid(a) * ab_all[at, lo, half:]).astype(BF16)
                        return c

                    lax.fori_loop(0, tile // group, body, 0)
                    last_copy(1).start()
                    grad_copy(1).start()
                    w_relayed((0, 1))
                    result_copy(0).start()

        @pl.when(early)
        def _():
            arrive(0, q + 1)
            arrive(1, q + 1)

        @pl.when(n < 4)
        def _():
            loaded(1, slot)

        @pl.when(n >= 4)
        def _():
            landed(1, q)

        with jax.named_scope('g_dot'):
            g_s[:, :cut_g] = dot_nn(dyt[slot], w_d[:, :cut_g])

        @pl.when(n >= 4)
        def _():
            tick(step + 1)

        with jax.named_scope('g_dot'):
            g_s[:, cut_g:] = dot_nn(dyt[slot], w_d[:, cut_g:])

        def activate(with_h):
            def body(m, c):
                lo = pl.ds(pl.multiple_of(m * group, group), group)
                a = ab_all[at, lo, :half]
                b = ab_all[at, lo, half:]
                g = g_s[lo, :]
                s = sigmoid(a)
                silu = a * s
                if with_h:
                    h_all[0, lo, :half] = (silu * b).astype(BF16)
                h_all[1, lo, :half] = (g * b * s * (1.0 + a * (1.0 - s))).astype(BF16)
                h_all[1, lo, half:] = (g * silu).astype(BF16)
                return c

            with jax.named_scope('act'):
                lax.fori_loop(0, tile // group, body, 0)

        @pl.when(final)
        def _():
            activate(False)

        @pl.when(jnp.logical_not(final))
        def _():
            activate(True)

        tick(step + jnp.where(n < 4, 0, 2))

        @pl.when(n < 3)
        def _():
            load_a(0, n + 1)
            load_a(1, n + 1)

        @pl.when(late)
        def _():
            arrive(0, q + 1)

        @pl.when(jnp.logical_not(final))
        def _():
            with jax.named_scope('dw_dot'):
                for lo in range(0, 2 * half, 2 * half // 3):
                    hi = lo + 2 * half // 3
                    acc_gu[:, lo:hi] += dot_tn(xt[slot, :, at_win], h_all[1, :, lo:hi])

            @pl.when(n == 14)
            def _():
                grad_copy(0).start()

            with jax.named_scope('dw_dot2'):
                for lo, hi in ((0, half // 2 // 128 * 128), (half // 2 // 128 * 128, half)):
                    acc_d[:, lo:hi] += dot_tn(dyt[slot, :, at_win], h_all[0, :, lo:hi])

        @pl.when(final)
        def _():
            pl.semaphore_wait(room.at[0], 1)
            last_copy(0).start()
            with jax.named_scope('grads_sent'):
                grad_copy(0).wait_send()
            with jax.named_scope('dw_own'):
                for lo, hi in pieces:
                    acc_gu[in_acc, lo:hi] += dot_tn(xt[1, :, at_own], h_all[1, :, lo:hi])
            with jax.named_scope('grads_sent'):
                grad_copy(1).wait_send()
            with jax.named_scope('dw_own'):
                acc_d[in_acc, :] += dot_tn(dyt[1, :, at_own], h_all[0, :, :half])

        @pl.when(jnp.logical_and(n >= 2, n < 15))
        def _():
            for ten in (0, 1):
                pl.semaphore_signal(room.at[ten], inc=1, device_id={'dp': partner, 'tp': t}, device_id_type=MESH)

        tick(step + jnp.where(n < 4, 1, 3))

        @pl.when(n < 4)
        def _():
            dx_tile(n)

        @pl.when(jnp.logical_and(late, q + 1 <= MIDDLE))
        def _():
            arrive(1, q + 1)
        return carry

    lax.fori_loop(0, 16, grad_tile, 0)

    tick(82)
    theirs = pl.ds(pl.multiple_of(window_of(me * blk, own)[1], 8), blk)
    with jax.named_scope('last_wait_h'):
        wait(yacc.at[0, theirs, pl.ds(0, half)], out_recv.at[1])
        wait(dyt.at[0, :, pl.ds(0, half)], h_recv.at[1])
    with jax.named_scope('dw_other'):
        yacc[0, :own, :half] += dot_tn(dyt[1, :, at_own], dyt[0, :, :half])
    tick(83)
    with jax.named_scope('drain_sums'):
        drain_sums()
    result_copy(1).start()
    with jax.named_scope('last_wait'):
        wait(pbuf.at[theirs, pl.ds(0, 2 * half)], out_recv.at[0])
        wait(xt.at[0, :, pl.ds(0, 2 * half)], h_recv.at[0])
    with jax.named_scope('dw_other'):
        for lo, hi in pieces:
            pbuf[:own, lo:hi] += dot_tn(xt[1, :, at_own], xt[0, :, lo:hi])

    with jax.named_scope('drain'):
        for ten in (0, 1):
            result_copy(ten).wait()
        for slot in (0, 1):
            wait(sb.at[slot], dx_send.at[slot])
        for k in range(3):
            for core in (0, 1):
                for link in (0, 1):
                    for part in (0, 1):
                        w_copy(k, link, part, core).wait_send()
            w_partner_copy(k).wait_send()
        w_relayed((2,))
        for ten in (0, 1):
            own_copy(ten).wait_send()

        def drain(q, carry):
            for ten in (0, 1):
                wait(tok_b[ten].at[0], f_send.at[q, ten])
                for link in (0, 1):
                    @pl.when(q < 8)
                    def _():
                        wait(slot_of(ten, 0, link), q_send.at[lax.rem(q, 8), link, ten])

                    @pl.when(q < 4)
                    def _():
                        wait(slot_of(ten, 0, link), rl_send.at[lax.rem(q, 4), link, ten])

            return carry

        lax.fori_loop(0, 12, drain, 0)
        for m in (0, 1):
            last_copy(m).wait_send()


def window_of(start, size):
    first = lax.div(start, LANES) * LANES
    return pl.ds(pl.multiple_of(first, LANES), size), start - first


def own_window(blk):
    return -(-(blk + LANES - 32) // LANES) * LANES


def window(model, blk):
    starts = [(2 * blk * c) // LANES * LANES for c in range(model // (2 * blk))]
    shift = max(2 * blk * c - s for c, s in enumerate(starts))
    return -(-(shift + 2 * blk) // LANES) * LANES


def mlp(x, dy, wg, wu, wd):
    rows, model = x.shape
    blk, width = wg.shape
    half = width // 2
    tile = rows // 2
    dma = pltpu.SemaphoreType.DMA
    vmem = pltpu.VMEM
    anywhere = pl.BlockSpec(memory_space=pl.ANY)
    shape = jax.ShapeDtypeStruct
    flops = 2 * model * half * rows * 2 * 20
    win = window(model, blk)
    most = max(rows, own_window(blk))
    kept = (vmem((win, 2 * half), F32), vmem((win, half), F32), vmem((most, model), F32), vmem((2, most, model), F32))
    kept = (*kept, vmem((model, 2 * half), BF16))
    held = sum(k.dtype.itemsize * math.prod(k.shape) for k in kept)
    in_vmem = pl.BlockSpec(memory_space=pltpu.VMEM)
    return pl.pallas_call(
        kernel,
        name='mlp',
        out_shape=(shape((2, rows, model), BF16), *kept,
                   shape((12, tile // 2, model), BF16), shape((12, tile // 2, model), BF16),
                   shape((rows, model), BF16), shape((rows, model), BF16)),
        in_specs=[anywhere] * 5,
        out_specs=(anywhere, *[in_vmem] * 5, *[anywhere] * 4),
        scratch_shapes=[
            vmem((model, half), BF16),
            vmem((2, tile, model // 3), F32),
            vmem((2, tile, model), BF16),
            vmem((2, tile, model), BF16),
            vmem((4, tile, 2 * half), F32),
            vmem((tile, half), F32),
            vmem((2, tile, 2 * half), BF16),
            vmem((2, DEPTH, tile // 2, LANES), F32),
            vmem((2, KEEP, tile // 2, LANES), BF16),
            dma((3, 2, 2, 2)), dma((3, 2, 2, 2)), dma((3, 2, 2)), dma((3, 2, 2)), dma((3,)), dma((3,)), dma((3,)),
            dma((2,)), dma((2,)), dma((8, 2, 2)), dma((12, 2, 2)), dma((4, 2, 2)), dma((12, 2)), dma((12, 2)),
            dma((2, 2)), dma((4, 2)), dma((2,)), dma((2, 3)), pltpu.SemaphoreType.REGULAR, pltpu.SemaphoreType.REGULAR((2,)),
            dma((2, SLOTS)), dma((2, DEPTH)), dma((2, LAG + 1)), dma((2, KEEP)), dma((2, LAG + 1)),
            dma((2, 2)), dma((2,)), dma((2,)), dma((2,)), dma((2,)), dma((2,)),
        ],
        compiler_params=pltpu.CompilerParams(collective_id=0, has_side_effects=True, vmem_limit_bytes=67_000_000 - held),
        cost_estimate=pl.CostEstimate(flops=flops, bytes_accessed=100_000_000, transcendentals=0),
    )(x, dy, wg, wu, wd)


def results_kernel(blk, half, acc_gu, acc_d, pbuf, yacc, w_gu, y_out, dx_out, g_out, u_out, d_out, sem):
    me = lax.axis_index('dp')
    j = lax.rem(me, 2)
    chip = lax.div(me, 2)
    rows = y_out.shape[0]
    mine = pl.ds(pl.multiple_of(window_of(chip * 2 * blk, LANES)[1] + j * blk, 8), blk)
    other = pl.ds(pl.multiple_of(window_of(me * blk, LANES)[1], 8), blk)
    own_cols = pl.ds(pl.multiple_of(j * half, LANES), half)
    other_cols = pl.ds(pl.multiple_of((1 - j) * half, LANES), half)
    low, high = pl.ds(0, half), pl.ds(half, half)
    copies = [pltpu.make_async_copy(src, dst, sem.at[n]) for n, (src, dst) in enumerate((
        (acc_gu.at[mine, low], g_out.at[:, own_cols]), (acc_gu.at[mine, high], u_out.at[:, own_cols]),
        (acc_d.at[mine, :], d_out.at[:, own_cols]),
        (pbuf.at[other, low], g_out.at[:, other_cols]), (pbuf.at[other, high], u_out.at[:, other_cols]),
        (yacc.at[0, other, low], d_out.at[:, other_cols]),
        (w_gu.at[pl.ds(0, rows), :], y_out), (w_gu.at[pl.ds(rows, rows), :], dx_out)))]
    for copy in copies:
        copy.start()
    for copy in copies:
        copy.wait()


def results(blk, width, rows, *kept):
    anywhere = pl.BlockSpec(memory_space=pl.ANY)
    in_vmem = pl.BlockSpec(memory_space=pltpu.VMEM)
    shape = jax.ShapeDtypeStruct
    model = kept[-1].shape[0]
    kept = [pltpu.with_memory_space_constraint(k, pltpu.VMEM) for k in kept]
    return pl.pallas_call(
        functools.partial(results_kernel, blk, width // 2),
        name='results',
        out_shape=(shape((rows, model), BF16), shape((rows, model), BF16),
                   shape((blk, width), F32), shape((blk, width), F32), shape((blk, width), F32)),
        in_specs=[in_vmem] * 5,
        out_specs=tuple([anywhere] * 5),
        scratch_shapes=[pltpu.SemaphoreType.DMA((8,))],
        compiler_params=pltpu.CompilerParams(vmem_limit_bytes=4_000_000),
    )(*kept)


def solution(mesh):
    def device_pass(x_rows, gate_blk, up_blk, down_blk, dy_rows):
        out = mlp(x_rows, dy_rows, gate_blk, up_blk, down_blk.T)
        y, dx, dw_gate, dw_up, dw_down = results(*gate_blk.shape, x_rows.shape[0], *out[1:6])
        return y, dx, dw_gate, dw_up, dw_down.T

    row_spec = P('dp', None)
    weight_spec = P('dp', 'tp')
    down_spec = P('tp', 'dp')
    return jax.shard_map(device_pass, mesh=mesh,
                         in_specs=(row_spec, weight_spec, weight_spec, down_spec, row_spec),
                         out_specs=(row_spec, row_spec, weight_spec, weight_spec, down_spec),
                         check_vma=False)
```

```python
import functools
import math

import jax
import jax.numpy as jnp
from jax import lax
from jax.experimental import pallas as pl
from jax.experimental.pallas import tpu as pltpu
from jax.sharding import PartitionSpec as P

F32 = jnp.float32
BF16 = jnp.bfloat16
MESH = pl.DeviceIdType.MESH
SLOTS = 8
DEPTH = 13
KEEP = 16
LAG = 3
HOP = 2
LANES = 128
EARLY = 4
MIDDLE = 8


def dot_nn(a, b):
    return jnp.dot(a, b, preferred_element_type=F32)


def dot_nt(a, b):
    return lax.dot_general(a, b, (((1,), (1,)), ((), ())), preferred_element_type=F32)


def dot_tn(a, b):
    return lax.dot_general(a, b, (((0,), (0,)), ((), ())), preferred_element_type=F32)


def sigmoid(a):
    return 1.0 / (1.0 + jnp.exp(-a))


def kernel(x_ref, dy_ref, wg_ref, wu_ref, wd_ref,
           yd_ref, acc_gu, acc_d, pbuf, yacc, w_gu, xb, dyb, xp, dyp,
           w_d, sb, xt, dyt, ab_all, g_s, h_all, rbuf, back,
           w_send, w_recv, wr_send, wr_recv, w_own, wp_send, wp_recv,
           own_send, own_recv, q_send, q_recv, rl_send, f_send, f_recv,
           y_send, y_recv, dx_send, dx_recv, credit, room,
           rs_send, rs_recv, ag_send, ag_recv, fin_own, ld, out_send, out_recv, h_send, h_recv, back_in):
    rows, model = x_ref.shape
    blk, width = wg_ref.shape
    half = width // 2
    hb = blk // 2
    tile = rows // 2
    piece = tile // 4
    win = acc_d.shape[0]
    line = model // 2
    units = line // LANES
    near_units = (2 * blk - LANES // 2) // LANES if (2 * blk) % LANES else 2 * blk // LANES
    rest_units = units - near_units
    steps = 4 * units
    part_rows = tile // 2
    group = min(32, tile)
    w_in = (wg_ref, wu_ref, wd_ref)
    cut = (half + 255) // 256 * 256
    pieces = ((0, cut), (cut, 2 * half))
    cut_ab = cut
    cut_g = half // 2 // 256 * 256
    tok = (x_ref, dy_ref)
    tok_b = (xb, dyb)
    tok_p = (xp, dyp)
    tok_t = (xt, dyt)

    t = lax.axis_index('tp')
    me = lax.axis_index('dp')
    cy = lax.div(me, 4)
    cx = lax.rem(lax.div(me, 2), 2)
    j = lax.rem(me, 2)
    partner = me + 1 - 2 * j
    chip = cy * 2 + cx

    def near(link, core):
        if link == 0:
            return cy * 4 + (1 - cx) * 2 + core
        return (1 - cy) * 4 + cx * 2 + core

    def far(core):
        return (1 - cy) * 4 + (1 - cx) * 2 + core

    def send(src, dst, s_sem, r_sem, dp=None, tp=None):
        where = {'dp': me if dp is None else dp, 'tp': t if tp is None else tp}
        return pltpu.make_async_remote_copy(src_ref=src, dst_ref=dst, send_sem=s_sem, recv_sem=r_sem,
                                            device_id=where, device_id_type=MESH)

    def wait(ref, sem):
        pltpu.make_async_copy(ref, ref, sem).wait()

    barrier = pltpu.get_barrier_semaphore()
    for peer in (partner, near(0, 0), near(0, 1), near(1, 0), near(1, 1)):
        pl.semaphore_signal(barrier, inc=1, device_id={'dp': peer, 'tp': t}, device_id_type=MESH)

    @pl.when(t > 0)
    def _():
        pl.semaphore_signal(barrier, inc=1, device_id={'dp': me, 'tp': t - 1}, device_id_type=MESH)

    @pl.when(t < 3)
    def _():
        pl.semaphore_signal(barrier, inc=1, device_id={'dp': me, 'tp': t + 1}, device_id_type=MESH)

    pl.semaphore_wait(barrier, 5 + jnp.minimum(t, 1) + jnp.minimum(3 - t, 1))

    def w_rows(k, dev, part=None):
        if part is None:
            at = pl.ds(pl.multiple_of(dev * blk, 16), blk)
        else:
            at = pl.ds(pl.multiple_of(dev * blk + part * hb, 16), hb)
        if k == 2:
            return w_d.at[at, :]
        return w_gu.at[at, pl.ds(k * half, half)]

    def w_cols(core):
        return pl.ds(pl.multiple_of(core * half, LANES), half)

    def w_copy(k, link, part, core):
        return send(w_in[k].at[pl.ds(part * hb, hb), w_cols(core)], w_rows(k, me, part),
                    w_send.at[k, link, part, core], w_recv.at[k, link, part, j], dp=near(link, core))

    def w_own_copy(k):
        return pltpu.make_async_copy(w_in[k].at[:, w_cols(j)], w_rows(k, me), w_own.at[k])

    def w_partner_copy(k):
        return send(w_in[k].at[:, w_cols(1 - j)], w_rows(k, me), wp_send.at[k], wp_recv.at[k], dp=partner)

    def w_start(k):
        for first in (0, 1):
            for core in (0, 1):
                w_copy(k, 0, 1 - first, core).start()
                w_copy(k, 1, first, core).start()
        w_own_copy(k).start()
        w_partner_copy(k).start()

    def w_relay_copy(k, link_out, core):
        part = 1 if link_out == 1 else 0
        ref = w_rows(k, near(1 - link_out, core), part)
        return send(ref, ref, wr_send.at[k, link_out, core], wr_recv.at[k, link_out, core], dp=near(link_out, j))

    def w_relay(k):
        for core in (0, 1):
            wait(w_rows(k, near(0, core), 1), w_recv.at[k, 0, 1, core])
            w_relay_copy(k, 1, core).start()
            wait(w_rows(k, near(1, core), 0), w_recv.at[k, 1, 0, core])
            w_relay_copy(k, 0, core).start()

    def w_relayed(which):
        for k in which:
            for link in (0, 1):
                for core in (0, 1):
                    w_relay_copy(k, link, core).wait_send()

    def w_have(k, which):
        if which == 'chip':
            wait(w_rows(k, me), w_own.at[k])
            wait(w_rows(k, partner), wp_recv.at[k])
        for core in (0, 1):
            if which == 'x':
                wait(w_rows(k, near(0, core), 0), w_recv.at[k, 0, 0, core])
            if which == 'y':
                wait(w_rows(k, near(1, core), 1), w_recv.at[k, 1, 1, core])
            if which == 'far':
                wait(w_rows(k, far(core), 0), wr_recv.at[k, 0, core])
                wait(w_rows(k, far(core), 1), wr_recv.at[k, 1, core])

    def slot_of(ten, q, link):
        return tok_b[ten].at[q, pl.ds(link * piece, piece), :]

    def q_copy(ten, q, link):
        b = lax.div(q, 4)
        sub = lax.rem(q, 4)
        first = 1 - b if link == 0 else b
        src = tok[ten].at[pl.ds(pl.multiple_of(first * tile + sub * piece, piece), piece), :]
        return send(src, slot_of(ten, q, link), q_send.at[q, link, ten], q_recv.at[q, link, ten], dp=near(link, j))

    def q_start(q):
        for ten in (0, 1):
            for link in (0, 1):
                q_copy(ten, q, link).start()

    def relay_copy(ten, sub, link_out):
        return send(slot_of(ten, sub, 1 - link_out), slot_of(ten, 8 + sub, link_out),
                    rl_send.at[sub, link_out, ten], q_recv.at[8 + sub, link_out, ten], dp=near(link_out, j))

    def tile_part(ten, q, core):
        return tok_t[ten].at[lax.rem(q, 2), pl.ds(pl.multiple_of(core * 2 * piece, 2 * piece), 2 * piece), :]

    def forward_copy(ten, q):
        return send(tok_b[ten].at[q], tile_part(ten, q, j), f_send.at[q, ten], f_recv.at[q, ten], dp=partner)

    def own_copy(ten):
        return send(tok[ten], tok_p[ten], own_send.at[ten], own_recv.at[ten], dp=partner)

    def arrive(ten, q):
        with jax.named_scope('arrive'):
            for link in (0, 1):
                wait(slot_of(ten, q, link), q_recv.at[q, link, ten])
            if ten == 0:
                pl.semaphore_wait(room.at[0], 1)
            else:
                @pl.when(q < 11)
                def _():
                    pl.semaphore_wait(room.at[1], 1)

            forward_copy(ten, q).start()
            pltpu.make_async_copy(tok_b[ten].at[q], tile_part(ten, q, j), ld.at[ten, lax.rem(q, 2)]).start()

        @pl.when(q < 4)
        def _():
            for link in (0, 1):
                relay_copy(ten, q, link).start()

    def landed(ten, q):
        with jax.named_scope('landed'):
            wait(tile_part(ten, q, j), ld.at[ten, lax.rem(q, 2)])
            wait(tile_part(ten, q, 1 - j), f_recv.at[q, ten])

    def rows_of(r):
        return pl.ds(pl.multiple_of(r * tile, tile), tile)

    def load_a(ten, n):
        own = lax.div(n, 2)
        slot = lax.rem(n, 2)

        @pl.when(own == 1)
        def _():
            pltpu.make_async_copy(tok[ten].at[rows_of(slot), :], tok_t[ten].at[slot], ld.at[ten, slot]).start()

        @pl.when(own == 0)
        def _():
            pltpu.make_async_copy(tok_p[ten].at[rows_of(slot), :], tok_t[ten].at[slot], ld.at[ten, slot]).start()

    def loaded(ten, slot):
        with jax.named_scope('ld'):
            wait(tok_t[ten].at[slot], ld.at[ten, slot])

    def unit_col(u):
        mine = cy * units
        other = (1 - cy) * units
        low = cx * rest_units
        high = (1 - cx) * near_units
        a = near_units
        col = jnp.where(u < a, mine + low + u,
                        jnp.where(u < units, mine + high + (u - a),
                                  jnp.where(u < units + a, other + low + (u - units), other + high + (u - units - a))))
        return pl.multiple_of(col * LANES, LANES)

    def chunk(s, way):
        n = lax.rem(s, steps)
        row = pl.multiple_of(way * tile + lax.rem(n, 2) * part_rows, part_rows)
        return lax.div(s, steps), pl.ds(row, part_rows), pl.ds(unit_col(lax.div(n, 2)), LANES)

    def sum_copy(s, way, nxt):
        land = lax.rem(s, DEPTH)
        return send(yacc.at[chunk(s, way)], rbuf.at[way, land], rs_send.at[way, lax.rem(s, SLOTS)], rs_recv.at[way, land], tp=nxt)

    def done_copy(s, way, prv):
        ref = back.at[way, lax.rem(s, KEEP)]
        return send(ref, ref, ag_send.at[way, lax.rem(s, LAG + 1)], ag_recv.at[way, lax.rem(s, KEEP)], tp=prv)

    def store_copy(s, way):
        return pltpu.make_async_copy(back.at[way, lax.rem(s, KEEP)], yd_ref.at[chunk(s, way)],
                                     fin_own.at[way, lax.rem(s, LAG + 1)])

    def tick(tau):
        with jax.named_scope('tick'):
            tick_body(tau)

    def give(s, way, p, prv):
        @pl.when(s >= LAG)
        def _():
            store_copy(s - LAG, way).wait()

            @pl.when(p > 0)
            def _():
                wait(back.at[way, 0], ag_send.at[way, lax.rem(s - LAG, LAG + 1)])

        store_copy(s, way).start()

        @pl.when(p > 0)
        def _():
            done_copy(s, way, prv).start()

    def tick_body(tau):
        for way in (0, 1):
            p = t if way == 0 else 3 - t
            nxt = t + 1 if way == 0 else t - 1
            prv = t - 1 if way == 0 else t + 1
            s = tau - HOP * p
            slot = lax.rem(jnp.maximum(s, 0), SLOTS)
            land = lax.rem(jnp.maximum(s, 0), DEPTH)
            live = jnp.logical_and(s >= 0, s < 2 * steps)

            @pl.when(jnp.logical_and(live, p > 0))
            def _():
                wait(rbuf.at[way, land], rs_recv.at[way, land])

            @pl.when(jnp.logical_and(live, p < 3))
            def _():
                @pl.when(s >= SLOTS)
                def _():
                    wait(rbuf.at[way, 0], rs_send.at[way, slot])

                @pl.when(p > 0)
                def _():
                    here = chunk(s, way)
                    yacc[here] = yacc[here] + rbuf[way, land]

                sum_copy(s, way, nxt).start()

            @pl.when(jnp.logical_and(live, p == 3))
            def _():
                back[way, lax.rem(s, KEEP)] = (yacc[chunk(s, way)] + rbuf[way, land]).astype(BF16)
                give(s, way, p, prv)

        for way in (0, 1):
            p = t if way == 0 else 3 - t
            prv = t - 1 if way == 0 else t + 1
            s = tau - HOP * (6 - p)

            @pl.when(jnp.logical_and(jnp.logical_and(s >= 0, s < 2 * steps), p < 3))
            def _():
                keep = lax.rem(s, KEEP)
                wait(back.at[way, keep], ag_recv.at[way, keep])
                give(s, way, p, prv)

    def ticks(lo, hi):
        def body(n, c):
            tick(n)
            return c

        lax.fori_loop(lo, hi, body, 0)

    def drain_sums():
        for way in (0, 1):
            p = t if way == 0 else 3 - t

            @pl.when(p < 3)
            def _():
                for slot in range(SLOTS):
                    wait(rbuf.at[way, 0], rs_send.at[way, slot])

            for m in range(LAG):
                s = 2 * steps - LAG + m
                wait(back.at[way, 0], fin_own.at[way, s % (LAG + 1)])

                @pl.when(p > 0)
                def _():
                    wait(back.at[way, 0], ag_send.at[way, s % (LAG + 1)])

    w_start(0)
    w_start(1)
    for ten in (0, 1):
        own_copy(ten).start()
    base = jnp.where(t == 0, 1.0, 0.0).astype(F32)

    with jax.named_scope('clear'):
        for r in (0, 1):
            for ten in (0, 1):
                load_a(ten, 2 + r)

        def clear(n, carry):
            at = pl.ds(pl.multiple_of(n * 32, 32), 32)
            acc_gu[at, :] = jnp.zeros((32, 2 * half), F32)
            acc_d[at, :] = jnp.zeros((32, half), F32)
            return carry

        lax.fori_loop(0, win // 32, clear, 0)

        def clear_ab(n, carry):
            lo = pl.ds(pl.multiple_of(n * group, group), group)
            for m in range(4):
                ab_all[m, lo, :] = jnp.zeros((group, 2 * half), F32)
            return carry

        lax.fori_loop(0, tile // group, clear_ab, 0)
        for r in (0, 1):
            for ten in (0, 1):
                loaded(ten, r)

                def residual(n, carry):
                    lo = pl.ds(pl.multiple_of(n * group, group), group)
                    there = pl.ds(pl.multiple_of(r * tile + n * group, group), group)
                    yacc[ten, there, :] = tok_t[ten][r, lo, :].astype(F32) * base
                    return carry

                lax.fori_loop(0, tile // group, residual, 0)
        for ten in (0, 1):
            wait(tok_p[ten], own_recv.at[ten])

    with jax.named_scope('w_relay'):
        w_relay(0)
        w_relay(1)
    w_start(2)

    def side(n):
        return pl.ds(pl.multiple_of(lax.rem(n, 2) * half, LANES), half)

    def ab_pass(last):
        other = (1 - cy) * line
        if last:
            parts = ((other + (1 - cx) * near_units * LANES, rest_units * LANES),)
        else:
            parts = ((cy * line, line), (other + cx * rest_units * LANES, near_units * LANES))
        def body(n, carry):
            slot = lax.rem(n, 2)

            @pl.when(n < 3)
            def _():
                load_a(0, n + 1)

            loaded(0, slot)
            for at, size in parts:
                at_k = pl.ds(pl.multiple_of(at, LANES), size)
                with jax.named_scope('ab_part'):
                    for lo, hi in pieces:
                        ab_all[n, :, lo:hi] += dot_nn(xt[slot, :, at_k], w_gu[at_k, lo:hi])

            if last:
                def hidden(m, c):
                    lo = pl.ds(pl.multiple_of(m * group, group), group)
                    a = ab_all[n, lo, :half]
                    h_all[lax.div(n, 2), lo, side(n)] = (a * sigmoid(a) * ab_all[n, lo, half:]).astype(BF16)
                    return c

                lax.fori_loop(0, tile // group, hidden, 0)
            return carry

        lax.fori_loop(0, 4, body, 0)

    load_a(0, 0)
    with jax.named_scope('w_have'):
        for k in (0, 1):
            w_have(k, 'chip')
            w_have(k, 'x')
            w_have(k, 'y')
    ab_pass(0)
    load_a(0, 0)
    with jax.named_scope('w_have'):
        for k in (0, 1):
            w_have(k, 'far')
    ab_pass(1)

    def y_group(g, tau):
        u0 = (0, near_units, units, units + near_units)[g]
        n_u = (near_units, rest_units)[g % 2]
        col = unit_col(u0)
        cols = pl.ds(col, n_u * LANES)

        def theirs(r, carry):
            if g > 0:
                before = (near_units, rest_units)[(g - 1) % 2] * LANES
                wait(sb.at[r, :, pl.ds(0, before)], y_send.at[(g - 1) % 2, r])
            with jax.named_scope('y_dot'):
                sb[r, :, :n_u * LANES] = dot_nt(h_all[0, :, side(r)], w_d[cols, :])
            send(sb.at[r, :, pl.ds(0, n_u * LANES)], pbuf.at[rows_of(r), cols],
                 y_send.at[g % 2, r], y_recv.at[g, r], dp=partner).start()
            return carry

        def ours(r, carry):
            with jax.named_scope('y_wait'):
                wait(pbuf.at[rows_of(r), cols], y_recv.at[g, r])
            with jax.named_scope('y_dot'):
                yacc[0, rows_of(r), cols] = (yacc[0, rows_of(r), cols] + pbuf[rows_of(r), cols]
                                             + dot_nt(h_all[1, :, side(r)], w_d[cols, :]))
            pl.semaphore_signal(credit, inc=1, device_id={'dp': partner, 'tp': t}, device_id_type=MESH)
            return carry

        lax.fori_loop(0, 2, theirs, 0)
        if g > 0:
            tick(tau)
        lax.fori_loop(0, 2, ours, 0)
        if g > 0:
            tick(tau + 1)

    load_a(1, 0)
    load_a(0, 0)
    with jax.named_scope('w_have2'):
        w_have(2, 'chip')
    y_group(0, 0)
    tick(0)
    with jax.named_scope('w_relay2'):
        w_relay(2)
    q_start(0)
    q_start(1)
    ticks(1, 7)
    with jax.named_scope('w_have2'):
        w_have(2, 'x')
        w_have(2, 'y')
    y_group(1, 7)
    y_group(2, 9)
    q_start(2)
    ticks(11, 14)
    with jax.named_scope('w_have2'):
        w_have(2, 'far')
    y_group(3, 14)
    q_start(3)

    at_win, shift = window_of(chip * 2 * blk, win)
    own = own_window(blk)
    at_own, _ = window_of(me * blk, own)
    in_acc = pl.ds(pl.multiple_of(window_of(me * blk, own)[0].start - at_win.start, 8), own)
    n_block = 3
    n_cols = model // n_block

    def grad_copy(m):
        rows_ = pl.ds(pl.multiple_of(shift + (1 - j) * blk, 8), blk)
        there = pl.ds(pl.multiple_of(window_of(partner * blk, own)[1], 8), blk)
        if m == 0:
            return send(acc_gu.at[rows_, :], pbuf.at[there, pl.ds(0, 2 * half)], out_send.at[0], out_recv.at[0], dp=partner)
        return send(acc_d.at[rows_, :], yacc.at[0, there, pl.ds(0, half)], out_send.at[1], out_recv.at[1], dp=partner)

    def result_copy(ten):
        return pltpu.make_async_copy(yd_ref.at[ten], w_gu.at[pl.ds(ten * rows, rows), :], back_in.at[ten])

    def last_copy(m):
        if m == 0:
            return send(h_all.at[1], xt.at[0, :, pl.ds(0, 2 * half)], h_send.at[0], h_recv.at[0], dp=partner)
        return send(h_all.at[0, :, pl.ds(0, half)], dyt.at[0, :, pl.ds(0, half)], h_send.at[1], h_recv.at[1], dp=partner)

    def dx_tile(n):
        r = lax.rem(n, 2)

        @pl.when(n == 0)
        def _():
            pl.semaphore_wait(credit, 8)
            for r_ in (0, 1):
                wait(sb.at[r_, :, pl.ds(0, rest_units * LANES)], y_send.at[1, r_])

        def block(m, carry):
            cols = pl.ds(pl.multiple_of(m * n_cols, n_cols), n_cols)
            slot = lax.rem(m + r * n_block, 2)

            @pl.when(jnp.logical_and(n < 2, m + r * n_block >= 2))
            def _():
                wait(sb.at[slot], dx_send.at[slot])

            @pl.when(n < 2)
            def _():
                with jax.named_scope('dx_dot'):
                    sb[slot] = dot_nt(h_all[1], w_gu[cols, :])
                send(sb.at[slot], pbuf.at[rows_of(r), cols], dx_send.at[slot], dx_recv.at[r, m], dp=partner).start()

            @pl.when(n >= 2)
            def _():
                with jax.named_scope('dx_wait'):
                    wait(pbuf.at[rows_of(r), cols], dx_recv.at[r, m])
                with jax.named_scope('dx_dot'):
                    yacc[1, rows_of(r), cols] = (yacc[1, rows_of(r), cols] + pbuf[rows_of(r), cols]
                                                 + dot_nt(h_all[1], w_gu[cols, :]))

            @pl.when(m >= 1)
            def _():
                tick(17 + 4 * n + m)
            return carry

        lax.fori_loop(0, n_block, block, 0)

    def grad_tile(n, carry):
        q = n - 4
        slot = lax.rem(n, 2)
        at = jnp.where(n < 4, n, slot)
        final = n == 15
        early = jnp.logical_and(n >= 3, q + 1 <= EARLY)
        late = jnp.logical_and(n < 15, q + 1 > EARLY)
        dense = q >= 8
        extra = jnp.logical_and(dense, q < 10)
        tau = jnp.where(dense, 64 + 5 * (q - 8), 16 + 4 * n)
        late_step = jnp.where(final, 1, 0)

        @pl.when(n < 4)
        def _():
            q_start(4 + n)
            loaded(0, slot)

        @pl.when(extra)
        def _():
            tick(tau)

        step = jnp.where(extra, tau + 1, tau)

        @pl.when(n >= 4)
        def _():
            landed(0, q)
            with jax.named_scope('ab_dot'):
                ab_all[at, :, :cut_ab] = dot_nn(xt[slot], w_gu[:, :cut_ab])
            tick(step)

            @pl.when(jnp.logical_and(q > MIDDLE, n < 15))
            def _():
                arrive(1, q)

            with jax.named_scope('ab_dot'):
                ab_all[at, :, cut_ab:] = dot_nn(xt[slot], w_gu[:, cut_ab:])

            @pl.when(final)
            def _():
                pl.semaphore_wait(room.at[1], 2)
                arrive(1, q)
                tick(tau + 1)
                with jax.named_scope('h_last'):
                    def body(m, c):
                        lo = pl.ds(pl.multiple_of(m * group, group), group)
                        a = ab_all[at, lo, :half]
                        h_all[0, lo, :half] = (a * sigmoid(a) * ab_all[at, lo, half:]).astype(BF16)
                        return c

                    lax.fori_loop(0, tile // group, body, 0)
                    last_copy(1).start()
                    grad_copy(1).start()
                    w_relayed((0, 1))
                    result_copy(0).start()

        @pl.when(early)
        def _():
            arrive(0, q + 1)
            arrive(1, q + 1)

        @pl.when(n < 4)
        def _():
            loaded(1, slot)

        @pl.when(n >= 4)
        def _():
            landed(1, q)

        with jax.named_scope('g_dot'):
            g_s[:, :cut_g] = dot_nn(dyt[slot], w_d[:, :cut_g])

        @pl.when(n >= 4)
        def _():
            tick(step + 1 + late_step)

        with jax.named_scope('g_dot'):
            g_s[:, cut_g:] = dot_nn(dyt[slot], w_d[:, cut_g:])

        def activate(with_h):
            def body(m, c):
                lo = pl.ds(pl.multiple_of(m * group, group), group)
                a = ab_all[at, lo, :half]
                b = ab_all[at, lo, half:]
                g = g_s[lo, :]
                s = sigmoid(a)
                silu = a * s
                if with_h:
                    h_all[0, lo, :half] = (silu * b).astype(BF16)
                h_all[1, lo, :half] = (g * b * s * (1.0 + a * (1.0 - s))).astype(BF16)
                h_all[1, lo, half:] = (g * silu).astype(BF16)
                return c

            with jax.named_scope('act'):
                lax.fori_loop(0, tile // group, body, 0)

        @pl.when(final)
        def _():
            activate(False)

        @pl.when(jnp.logical_not(final))
        def _():
            activate(True)

        tick(step + jnp.where(n < 4, 0, 2 + late_step))

        @pl.when(n < 3)
        def _():
            load_a(0, n + 1)
            load_a(1, n + 1)

        @pl.when(late)
        def _():
            arrive(0, q + 1)

        @pl.when(n == 14)
        def _():
            tick(tau + 3)

        @pl.when(jnp.logical_not(final))
        def _():
            with jax.named_scope('dw_dot'):
                for lo in range(0, 2 * half, 2 * half // 3):
                    hi = lo + 2 * half // 3
                    acc_gu[:, lo:hi] += dot_tn(xt[slot, :, at_win], h_all[1, :, lo:hi])

            @pl.when(n == 14)
            def _():
                grad_copy(0).start()

            with jax.named_scope('dw_dot2'):
                for lo, hi in ((0, half // 2 // 128 * 128), (half // 2 // 128 * 128, half)):
                    acc_d[:, lo:hi] += dot_tn(dyt[slot, :, at_win], h_all[0, :, lo:hi])

        @pl.when(final)
        def _():
            pl.semaphore_wait(room.at[0], 1)
            last_copy(0).start()
            with jax.named_scope('grads_sent'):
                grad_copy(0).wait_send()
            with jax.named_scope('dw_own'):
                for lo, hi in pieces:
                    acc_gu[in_acc, lo:hi] += dot_tn(xt[1, :, at_own], h_all[1, :, lo:hi])
            with jax.named_scope('grads_sent'):
                grad_copy(1).wait_send()
            with jax.named_scope('dw_own'):
                acc_d[in_acc, :] += dot_tn(dyt[1, :, at_own], h_all[0, :, :half])

        @pl.when(jnp.logical_and(n >= 2, n < 15))
        def _():
            for ten in (0, 1):
                pl.semaphore_signal(room.at[ten], inc=1, device_id={'dp': partner, 'tp': t}, device_id_type=MESH)

        tick(step + jnp.where(n < 4, 1, jnp.where(n < 14, 3, 4)))

        @pl.when(n < 4)
        def _():
            dx_tile(n)

        @pl.when(jnp.logical_and(late, q + 1 <= MIDDLE))
        def _():
            arrive(1, q + 1)
        return carry

    lax.fori_loop(0, 16, grad_tile, 0)

    with jax.named_scope('drain_sums'):
        drain_sums()
    result_copy(1).start()
    theirs = pl.ds(pl.multiple_of(window_of(me * blk, own)[1], 8), blk)
    with jax.named_scope('last_wait_h'):
        wait(yacc.at[0, theirs, pl.ds(0, half)], out_recv.at[1])
        wait(dyt.at[0, :, pl.ds(0, half)], h_recv.at[1])
    with jax.named_scope('dw_other'):
        yacc[0, :own, :half] += dot_tn(dyt[1, :, at_own], dyt[0, :, :half])
    with jax.named_scope('last_wait'):
        wait(pbuf.at[theirs, pl.ds(0, 2 * half)], out_recv.at[0])
        wait(xt.at[0, :, pl.ds(0, 2 * half)], h_recv.at[0])
    with jax.named_scope('dw_other'):
        for lo, hi in pieces:
            pbuf[:own, lo:hi] += dot_tn(xt[1, :, at_own], xt[0, :, lo:hi])

    with jax.named_scope('drain'):
        for ten in (0, 1):
            result_copy(ten).wait()
        for slot in (0, 1):
            wait(sb.at[slot], dx_send.at[slot])
        for k in range(3):
            for core in (0, 1):
                for link in (0, 1):
                    for part in (0, 1):
                        w_copy(k, link, part, core).wait_send()
            w_partner_copy(k).wait_send()
        w_relayed((2,))
        for ten in (0, 1):
            own_copy(ten).wait_send()

        def drain(q, carry):
            for ten in (0, 1):
                wait(tok_b[ten].at[0], f_send.at[q, ten])
                for link in (0, 1):
                    @pl.when(q < 8)
                    def _():
                        wait(slot_of(ten, 0, link), q_send.at[lax.rem(q, 8), link, ten])

                    @pl.when(q < 4)
                    def _():
                        wait(slot_of(ten, 0, link), rl_send.at[lax.rem(q, 4), link, ten])

            return carry

        lax.fori_loop(0, 12, drain, 0)
        for m in (0, 1):
            last_copy(m).wait_send()


def window_of(start, size):
    first = lax.div(start, LANES) * LANES
    return pl.ds(pl.multiple_of(first, LANES), size), start - first


def own_window(blk):
    return -(-(blk + LANES - 32) // LANES) * LANES


def window(model, blk):
    starts = [(2 * blk * c) // LANES * LANES for c in range(model // (2 * blk))]
    shift = max(2 * blk * c - s for c, s in enumerate(starts))
    return -(-(shift + 2 * blk) // LANES) * LANES


def mlp(x, dy, wg, wu, wd):
    rows, model = x.shape
    blk, width = wg.shape
    half = width // 2
    tile = rows // 2
    dma = pltpu.SemaphoreType.DMA
    vmem = pltpu.VMEM
    anywhere = pl.BlockSpec(memory_space=pl.ANY)
    shape = jax.ShapeDtypeStruct
    flops = 2 * model * half * rows * 2 * 20
    win = window(model, blk)
    most = max(rows, own_window(blk))
    kept = (vmem((win, 2 * half), F32), vmem((win, half), F32), vmem((most, model), F32), vmem((2, most, model), F32))
    kept = (*kept, vmem((model, 2 * half), BF16))
    held = sum(k.dtype.itemsize * math.prod(k.shape) for k in kept)
    in_vmem = pl.BlockSpec(memory_space=pltpu.VMEM)
    return pl.pallas_call(
        kernel,
        name='mlp',
        out_shape=(shape((2, rows, model), BF16), *kept,
                   shape((12, tile // 2, model), BF16), shape((12, tile // 2, model), BF16),
                   shape((rows, model), BF16), shape((rows, model), BF16)),
        in_specs=[anywhere] * 5,
        out_specs=(anywhere, *[in_vmem] * 5, *[anywhere] * 4),
        scratch_shapes=[
            vmem((model, half), BF16),
            vmem((2, tile, model // 3), F32),
            vmem((2, tile, model), BF16),
            vmem((2, tile, model), BF16),
            vmem((4, tile, 2 * half), F32),
            vmem((tile, half), F32),
            vmem((2, tile, 2 * half), BF16),
            vmem((2, DEPTH, tile // 2, LANES), F32),
            vmem((2, KEEP, tile // 2, LANES), BF16),
            dma((3, 2, 2, 2)), dma((3, 2, 2, 2)), dma((3, 2, 2)), dma((3, 2, 2)), dma((3,)), dma((3,)), dma((3,)),
            dma((2,)), dma((2,)), dma((8, 2, 2)), dma((12, 2, 2)), dma((4, 2, 2)), dma((12, 2)), dma((12, 2)),
            dma((2, 2)), dma((4, 2)), dma((2,)), dma((2, 3)), pltpu.SemaphoreType.REGULAR, pltpu.SemaphoreType.REGULAR((2,)),
            dma((2, SLOTS)), dma((2, DEPTH)), dma((2, LAG + 1)), dma((2, KEEP)), dma((2, LAG + 1)),
            dma((2, 2)), dma((2,)), dma((2,)), dma((2,)), dma((2,)), dma((2,)),
        ],
        compiler_params=pltpu.CompilerParams(collective_id=0, has_side_effects=True, vmem_limit_bytes=67_000_000 - held),
        cost_estimate=pl.CostEstimate(flops=flops, bytes_accessed=100_000_000, transcendentals=0),
    )(x, dy, wg, wu, wd)


def results_kernel(blk, half, acc_gu, acc_d, pbuf, yacc, w_gu, y_out, dx_out, g_out, u_out, d_out, sem):
    me = lax.axis_index('dp')
    j = lax.rem(me, 2)
    chip = lax.div(me, 2)
    rows = y_out.shape[0]
    mine = pl.ds(pl.multiple_of(window_of(chip * 2 * blk, LANES)[1] + j * blk, 8), blk)
    other = pl.ds(pl.multiple_of(window_of(me * blk, LANES)[1], 8), blk)
    own_cols = pl.ds(pl.multiple_of(j * half, LANES), half)
    other_cols = pl.ds(pl.multiple_of((1 - j) * half, LANES), half)
    low, high = pl.ds(0, half), pl.ds(half, half)
    copies = [pltpu.make_async_copy(src, dst, sem.at[n]) for n, (src, dst) in enumerate((
        (acc_gu.at[mine, low], g_out.at[:, own_cols]), (acc_gu.at[mine, high], u_out.at[:, own_cols]),
        (acc_d.at[mine, :], d_out.at[:, own_cols]),
        (pbuf.at[other, low], g_out.at[:, other_cols]), (pbuf.at[other, high], u_out.at[:, other_cols]),
        (yacc.at[0, other, low], d_out.at[:, other_cols]),
        (w_gu.at[pl.ds(0, rows), :], y_out), (w_gu.at[pl.ds(rows, rows), :], dx_out)))]
    for copy in copies:
        copy.start()
    for copy in copies:
        copy.wait()


def results(blk, width, rows, *kept):
    anywhere = pl.BlockSpec(memory_space=pl.ANY)
    in_vmem = pl.BlockSpec(memory_space=pltpu.VMEM)
    shape = jax.ShapeDtypeStruct
    model = kept[-1].shape[0]
    kept = [pltpu.with_memory_space_constraint(k, pltpu.VMEM) for k in kept]
    return pl.pallas_call(
        functools.partial(results_kernel, blk, width // 2),
        name='results',
        out_shape=(shape((rows, model), BF16), shape((rows, model), BF16),
                   shape((blk, width), F32), shape((blk, width), F32), shape((blk, width), F32)),
        in_specs=[in_vmem] * 5,
        out_specs=tuple([anywhere] * 5),
        scratch_shapes=[pltpu.SemaphoreType.DMA((8,))],
        compiler_params=pltpu.CompilerParams(vmem_limit_bytes=4_000_000),
    )(*kept)


def solution(mesh):
    def device_pass(x_rows, gate_blk, up_blk, down_blk, dy_rows):
        out = mlp(x_rows, dy_rows, gate_blk, up_blk, down_blk.T)
        y, dx, dw_gate, dw_up, dw_down = results(*gate_blk.shape, x_rows.shape[0], *out[1:6])
        return y, dx, dw_gate, dw_up, dw_down.T

    row_spec = P('dp', None)
    weight_spec = P('dp', 'tp')
    down_spec = P('tp', 'dp')
    return jax.shard_map(device_pass, mesh=mesh,
                         in_specs=(row_spec, weight_spec, weight_spec, down_spec, row_spec),
                         out_specs=(row_spec, row_spec, weight_spec, weight_spec, down_spec),
                         check_vma=False)
```

```python
import functools
import math

import jax
import jax.numpy as jnp
from jax import lax
from jax.experimental import pallas as pl
from jax.experimental.pallas import tpu as pltpu
from jax.sharding import PartitionSpec as P

F32 = jnp.float32
BF16 = jnp.bfloat16
MESH = pl.DeviceIdType.MESH
SLOTS = 8
DEPTH = 13
KEEP = 16
LAG = 3
HOP = 2
LANES = 128
ONE = 1.0
BOTH = (0, 1)
ALL = (0, 1, 2)
EARLY = 4
MIDDLE = 8


def odd(n):
    return lax.rem(n, 2)


def halved(n):
    return lax.div(n, 2)


def dot_nn(a, b):
    return jnp.dot(a, b, preferred_element_type=F32)


def dot_nt(a, b):
    return lax.dot_general(a, b, (((1,), (1,)), ((), ())), preferred_element_type=F32)


def dot_tn(a, b):
    return lax.dot_general(a, b, (((0,), (0,)), ((), ())), preferred_element_type=F32)


def sigmoid(a):
    return ONE / (ONE + jnp.exp(-a))


def kernel(x_ref, dy_ref, wg_ref, wu_ref, wd_ref,
           yd_ref, acc_gu, acc_d, pbuf, yacc, w_gu, xb, dyb, xp, dyp,
           w_d, sb, xt, dyt, ab_all, g_s, h_all, rbuf, back,
           w_send, w_recv, wr_send, wr_recv, w_own, wp_send, wp_recv,
           own_send, own_recv, q_send, q_recv, rl_send, f_send, f_recv,
           y_send, y_recv, dx_send, dx_recv, credit, room,
           rs_send, rs_recv, ag_send, ag_recv, fin_own, ld, out_send, out_recv, h_send, h_recv, back_in):
    rows, model = x_ref.shape
    blk, width = wg_ref.shape
    half = width // 2
    third = width // 3
    half_cut = half // 2 // LANES * LANES
    low = pl.ds(0, half)
    whole = pl.ds(0, width)
    pair = 2 * blk
    hb = blk // 2
    tile = rows // 2
    piece = tile // 4
    parcel = 2 * piece
    win = acc_d.shape[0]
    line = model // 2
    units = line // LANES
    near_units = (pair - LANES // 2) // LANES if pair % LANES else pair // LANES
    rest_units = units - near_units
    steps = 4 * units
    part_rows = tile // 2
    total = 2 * steps
    group = min(32, tile)
    w_in = (wg_ref, wu_ref, wd_ref)
    cut = (half + 255) // 256 * 256
    pieces = ((0, cut), (cut, width))
    cut_ab = cut
    cut_g = half // 2 // 256 * 256
    tok = (x_ref, dy_ref)
    tok_b = (xb, dyb)
    tok_p = (xp, dyp)
    tok_t = (xt, dyt)

    t = lax.axis_index('tp')
    me = lax.axis_index('dp')
    cy = lax.div(me, 4)
    cx = lax.rem(halved(me), 2)
    far_y = 1 - cy
    far_x = 1 - cx
    j = odd(me)
    other_core = 1 - j
    partner = me + 1 - 2 * j
    chip = cy * 2 + cx

    def near(link, core):
        if link == 0:
            return cy * 4 + (far_x) * 2 + core
        return (far_y) * 4 + cx * 2 + core

    def far(core):
        return (far_y) * 4 + (far_x) * 2 + core

    def send(src, dst, s_sem, r_sem, dp=None, tp=None):
        where = {'dp': me if dp is None else dp, 'tp': t if tp is None else tp}
        return pltpu.make_async_remote_copy(src_ref=src, dst_ref=dst, send_sem=s_sem, recv_sem=r_sem,
                                            device_id=where, device_id_type=MESH)

    def wait(ref, sem):
        pltpu.make_async_copy(ref, ref, sem).wait()

    barrier = pltpu.get_barrier_semaphore()
    for peer in (partner, near(0, 0), near(0, 1), near(1, 0), near(1, 1)):
        pl.semaphore_signal(barrier, device_id={'dp': peer, 'tp': t}, device_id_type=MESH)

    @pl.when(t > 0)
    def _():
        pl.semaphore_signal(barrier, device_id={'dp': me, 'tp': t - 1}, device_id_type=MESH)

    @pl.when(t < 3)
    def _():
        pl.semaphore_signal(barrier, device_id={'dp': me, 'tp': t + 1}, device_id_type=MESH)

    pl.semaphore_wait(barrier, 5 + jnp.minimum(t, 1) + jnp.minimum(3 - t, 1))

    def w_rows(k, dev, part=None):
        if part is None:
            at = pl.ds(pl.multiple_of(dev * blk, 16), blk)
        else:
            at = pl.ds(pl.multiple_of(dev * blk + part * hb, 16), hb)
        if k == 2:
            return w_d.at[at, :]
        return w_gu.at[at, pl.ds(k * half, half)]

    def w_cols(core):
        return pl.ds(pl.multiple_of(core * half, LANES), half)

    def w_copy(k, link, part, core):
        return send(w_in[k].at[pl.ds(part * hb, hb), w_cols(core)], w_rows(k, me, part),
                    w_send.at[k, link, part, core], w_recv.at[k, link, part, j], dp=near(link, core))

    def w_own_copy(k):
        return pltpu.make_async_copy(w_in[k].at[:, w_cols(j)], w_rows(k, me), w_own.at[k])

    def w_partner_copy(k):
        return send(w_in[k].at[:, w_cols(other_core)], w_rows(k, me), wp_send.at[k], wp_recv.at[k], dp=partner)

    def w_start(k):
        for first in BOTH:
            for core in BOTH:
                w_copy(k, 0, 1 - first, core).start()
                w_copy(k, 1, first, core).start()
        w_own_copy(k).start()
        w_partner_copy(k).start()

    def w_relay_copy(k, link_out, core):
        part = 1 if link_out == 1 else 0
        ref = w_rows(k, near(1 - link_out, core), part)
        return send(ref, ref, wr_send.at[k, link_out, core], wr_recv.at[k, link_out, core], dp=near(link_out, j))

    def w_relay(k):
        for core in BOTH:
            wait(w_rows(k, near(0, core), 1), w_recv.at[k, 0, 1, core])
            w_relay_copy(k, 1, core).start()
            wait(w_rows(k, near(1, core), 0), w_recv.at[k, 1, 0, core])
            w_relay_copy(k, 0, core).start()

    def w_relayed(which):
        for k in which:
            for link in BOTH:
                for core in BOTH:
                    w_relay_copy(k, link, core).wait_send()

    def w_have(k, which):
        if which == 'chip':
            wait(w_rows(k, me), w_own.at[k])
            wait(w_rows(k, partner), wp_recv.at[k])
        for core in BOTH:
            if which == 'x':
                wait(w_rows(k, near(0, core), 0), w_recv.at[k, 0, 0, core])
            if which == 'y':
                wait(w_rows(k, near(1, core), 1), w_recv.at[k, 1, 1, core])
            if which == 'far':
                wait(w_rows(k, far(core), 0), wr_recv.at[k, 0, core])
                wait(w_rows(k, far(core), 1), wr_recv.at[k, 1, core])

    def slot_of(ten, q, link):
        return tok_b[ten].at[q, pl.ds(link * piece, piece), :]

    def q_copy(ten, q, link):
        b = lax.div(q, 4)
        sub = lax.rem(q, 4)
        first = 1 - b if link == 0 else b
        src = tok[ten].at[pl.ds(pl.multiple_of(first * tile + sub * piece, piece), piece), :]
        return send(src, slot_of(ten, q, link), q_send.at[q, link, ten], q_recv.at[q, link, ten], dp=near(link, j))

    def q_start(q):
        for ten in BOTH:
            for link in BOTH:
                q_copy(ten, q, link).start()

    def relay_copy(ten, sub, link_out):
        return send(slot_of(ten, sub, 1 - link_out), slot_of(ten, 8 + sub, link_out),
                    rl_send.at[sub, link_out, ten], q_recv.at[8 + sub, link_out, ten], dp=near(link_out, j))

    def tile_part(ten, q, core):
        return tok_t[ten].at[odd(q), pl.ds(pl.multiple_of(core * parcel, parcel), parcel), :]

    def forward_copy(ten, q):
        return send(tok_b[ten].at[q], tile_part(ten, q, j), f_send.at[q, ten], f_recv.at[q, ten], dp=partner)

    def own_copy(ten):
        return send(tok[ten], tok_p[ten], own_send.at[ten], own_recv.at[ten], dp=partner)

    def arrive(ten, q):
        with jax.named_scope('arrive'):
            for link in BOTH:
                wait(slot_of(ten, q, link), q_recv.at[q, link, ten])
            if ten == 0:
                pl.semaphore_wait(room.at[0])
            else:
                @pl.when(q < 11)
                def _():
                    pl.semaphore_wait(room.at[1])

            forward_copy(ten, q).start()
            pltpu.make_async_copy(tok_b[ten].at[q], tile_part(ten, q, j), ld.at[ten, odd(q)]).start()

        @pl.when(q < 4)
        def _():
            for link in BOTH:
                relay_copy(ten, q, link).start()

    def landed(ten, q):
        with jax.named_scope('landed'):
            wait(tile_part(ten, q, j), ld.at[ten, odd(q)])
            wait(tile_part(ten, q, other_core), f_recv.at[q, ten])

    def rows_of(r):
        return pl.ds(pl.multiple_of(r * tile, tile), tile)

    def load_a(ten, n):
        own = halved(n)
        slot = odd(n)

        @pl.when(own == 1)
        def _():
            pltpu.make_async_copy(tok[ten].at[rows_of(slot), :], tok_t[ten].at[slot], ld.at[ten, slot]).start()

        @pl.when(own == 0)
        def _():
            pltpu.make_async_copy(tok_p[ten].at[rows_of(slot), :], tok_t[ten].at[slot], ld.at[ten, slot]).start()

    def loaded(ten, slot):
        with jax.named_scope('ld'):
            wait(tok_t[ten].at[slot], ld.at[ten, slot])

    def unit_col(u):
        mine = cy * units
        other = (far_y) * units
        low = cx * rest_units
        high = (far_x) * near_units
        a = near_units
        col = jnp.where(u < a, mine + low + u,
                        jnp.where(u < units, mine + high + (u - a),
                                  jnp.where(u < units + a, other + low + (u - units), other + high + (u - units - a))))
        return pl.multiple_of(col * LANES, LANES)

    def chunk(s, way):
        n = lax.rem(s, steps)
        row = pl.multiple_of(way * tile + odd(n) * part_rows, part_rows)
        return lax.div(s, steps), pl.ds(row, part_rows), pl.ds(unit_col(halved(n)), LANES)

    def sum_copy(s, way, nxt):
        land = lax.rem(s, DEPTH)
        return send(yacc.at[chunk(s, way)], rbuf.at[way, land], rs_send.at[way, lax.rem(s, SLOTS)], rs_recv.at[way, land], tp=nxt)

    def done_copy(s, way, prv):
        ref = back.at[way, lax.rem(s, KEEP)]
        return send(ref, ref, ag_send.at[way, lax.rem(s, LAG + 1)], ag_recv.at[way, lax.rem(s, KEEP)], tp=prv)

    def store_copy(s, way):
        return pltpu.make_async_copy(back.at[way, lax.rem(s, KEEP)], yd_ref.at[chunk(s, way)],
                                     fin_own.at[way, lax.rem(s, LAG + 1)])

    def tick(tau):
        with jax.named_scope('tick'):
            tick_body(tau)

    def give(s, way, p, prv):
        @pl.when(s >= LAG)
        def _():
            store_copy(s - LAG, way).wait()

            @pl.when(p > 0)
            def _():
                wait(back.at[way, 0], ag_send.at[way, lax.rem(s - LAG, LAG + 1)])

        store_copy(s, way).start()

        @pl.when(p > 0)
        def _():
            done_copy(s, way, prv).start()

    def tick_body(tau):
        for way in BOTH:
            p = t if way == 0 else 3 - t
            nxt = t + 1 if way == 0 else t - 1
            prv = t - 1 if way == 0 else t + 1
            s = tau - HOP * p
            slot = lax.rem(jnp.maximum(s, 0), SLOTS)
            land = lax.rem(jnp.maximum(s, 0), DEPTH)
            live = jnp.logical_and(s >= 0, s < total)

            @pl.when(jnp.logical_and(live, p > 0))
            def _():
                wait(rbuf.at[way, land], rs_recv.at[way, land])

            @pl.when(jnp.logical_and(live, p < 3))
            def _():
                @pl.when(s >= SLOTS)
                def _():
                    wait(rbuf.at[way, 0], rs_send.at[way, slot])

                @pl.when(p > 0)
                def _():
                    here = chunk(s, way)
                    yacc[here] = yacc[here] + rbuf[way, land]

                sum_copy(s, way, nxt).start()

            @pl.when(jnp.logical_and(live, p == 3))
            def _():
                back[way, lax.rem(s, KEEP)] = (yacc[chunk(s, way)] + rbuf[way, land]).astype(BF16)
                give(s, way, p, prv)

        for way in BOTH:
            p = t if way == 0 else 3 - t
            prv = t - 1 if way == 0 else t + 1
            s = tau - HOP * (6 - p)

            @pl.when(jnp.logical_and(jnp.logical_and(s >= 0, s < total), p < 3))
            def _():
                keep = lax.rem(s, KEEP)
                wait(back.at[way, keep], ag_recv.at[way, keep])
                give(s, way, p, prv)

    def ticks(lo, hi):
        def body(n, c):
            tick(n)
            return c

        lax.fori_loop(lo, hi, body, 0)

    def drain_sums():
        for way in BOTH:
            p = t if way == 0 else 3 - t

            @pl.when(p < 3)
            def _():
                for slot in range(SLOTS):
                    wait(rbuf.at[way, 0], rs_send.at[way, slot])

            for m in range(LAG):
                s = total - LAG + m
                wait(back.at[way, 0], fin_own.at[way, s % (LAG + 1)])

                @pl.when(p > 0)
                def _():
                    wait(back.at[way, 0], ag_send.at[way, s % (LAG + 1)])

    w_start(0)
    w_start(1)
    for ten in BOTH:
        own_copy(ten).start()
    base = jnp.where(t == 0, 1.0, 0.0).astype(F32)

    with jax.named_scope('clear'):
        for r in BOTH:
            for ten in BOTH:
                load_a(ten, 2 + r)

        def clear(n, carry):
            at = pl.ds(pl.multiple_of(n * 32, 32), 32)
            acc_gu[at, :] = jnp.zeros((32, width), F32)
            acc_d[at, :] = jnp.zeros((32, half), F32)
            return carry

        lax.fori_loop(0, win // 32, clear, 0)

        def clear_ab(n, carry):
            lo = pl.ds(pl.multiple_of(n * group, group), group)
            for m in range(4):
                ab_all[m, lo, :] = jnp.zeros((group, width), F32)
            return carry

        lax.fori_loop(0, tile // group, clear_ab, 0)
        for r in BOTH:
            for ten in BOTH:
                loaded(ten, r)

                def residual(n, carry):
                    lo = pl.ds(pl.multiple_of(n * group, group), group)
                    there = pl.ds(pl.multiple_of(r * tile + n * group, group), group)
                    yacc[ten, there, :] = tok_t[ten][r, lo, :].astype(F32) * base
                    return carry

                lax.fori_loop(0, tile // group, residual, 0)
        for ten in BOTH:
            wait(tok_p[ten], own_recv.at[ten])

    with jax.named_scope('w_relay'):
        w_relay(0)
        w_relay(1)
    w_start(2)

    def side(n):
        return pl.ds(pl.multiple_of(odd(n) * half, LANES), half)

    def ab_pass(last):
        other = (far_y) * line
        if last:
            parts = ((other + (far_x) * near_units * LANES, rest_units * LANES),)
        else:
            parts = ((cy * line, line), (other + cx * rest_units * LANES, near_units * LANES))
        def body(n, carry):
            slot = odd(n)

            @pl.when(n < 3)
            def _():
                load_a(0, n + 1)

            loaded(0, slot)
            for at, size in parts:
                at_k = pl.ds(pl.multiple_of(at, LANES), size)
                with jax.named_scope('ab_part'):
                    for lo, hi in pieces:
                        ab_all[n, :, lo:hi] += dot_nn(xt[slot, :, at_k], w_gu[at_k, lo:hi])

            if last:
                def hidden(m, c):
                    lo = pl.ds(pl.multiple_of(m * group, group), group)
                    a = ab_all[n, lo, :half]
                    h_all[halved(n), lo, side(n)] = (a * sigmoid(a) * ab_all[n, lo, half:]).astype(BF16)
                    return c

                lax.fori_loop(0, tile // group, hidden, 0)
            return carry

        lax.fori_loop(0, 4, body, 0)

    load_a(0, 0)
    with jax.named_scope('w_have'):
        for k in BOTH:
            w_have(k, 'chip')
            w_have(k, 'x')
            w_have(k, 'y')
    ab_pass(0)
    load_a(0, 0)
    with jax.named_scope('w_have'):
        for k in BOTH:
            w_have(k, 'far')
    ab_pass(1)

    def y_group(g, tau):
        u0 = (0, near_units, units, units + near_units)[g]
        n_u = (near_units, rest_units)[g % 2]
        col = unit_col(u0)
        cols = pl.ds(col, n_u * LANES)

        def theirs(r, carry):
            if g > 0:
                before = (near_units, rest_units)[(g - 1) % 2] * LANES
                wait(sb.at[r, :, pl.ds(0, before)], y_send.at[(g - 1) % 2, r])
            with jax.named_scope('y_dot'):
                sb[r, :, :n_u * LANES] = dot_nt(h_all[0, :, side(r)], w_d[cols, :])
            send(sb.at[r, :, pl.ds(0, n_u * LANES)], pbuf.at[rows_of(r), cols],
                 y_send.at[g % 2, r], y_recv.at[g, r], dp=partner).start()
            return carry

        def ours(r, carry):
            with jax.named_scope('y_wait'):
                wait(pbuf.at[rows_of(r), cols], y_recv.at[g, r])
            with jax.named_scope('y_dot'):
                yacc[0, rows_of(r), cols] = (yacc[0, rows_of(r), cols] + pbuf[rows_of(r), cols]
                                             + dot_nt(h_all[1, :, side(r)], w_d[cols, :]))
            pl.semaphore_signal(credit, device_id={'dp': partner, 'tp': t}, device_id_type=MESH)
            return carry

        lax.fori_loop(0, 2, theirs, 0)
        if g > 0:
            tick(tau)
        lax.fori_loop(0, 2, ours, 0)
        if g > 0:
            tick(tau + 1)

    load_a(1, 0)
    load_a(0, 0)
    with jax.named_scope('w_have2'):
        w_have(2, 'chip')
    y_group(0, 0)
    tick(0)
    with jax.named_scope('w_relay2'):
        w_relay(2)
    q_start(0)
    q_start(1)
    ticks(1, 7)
    with jax.named_scope('w_have2'):
        w_have(2, 'x')
        w_have(2, 'y')
    y_group(1, 7)
    y_group(2, 9)
    q_start(2)
    ticks(11, 14)
    with jax.named_scope('w_have2'):
        w_have(2, 'far')
    y_group(3, 14)
    q_start(3)

    at_win, shift = window_of(chip * pair, win)
    own = own_window(blk)
    at_own, _ = window_of(me * blk, own)
    in_acc = pl.ds(pl.multiple_of(window_of(me * blk, own)[0].start - at_win.start, 8), own)
    n_block = len(ALL)
    n_cols = model // n_block

    def grad_copy(m):
        rows_ = pl.ds(pl.multiple_of(shift + (other_core) * blk, 8), blk)
        there = pl.ds(pl.multiple_of(window_of(partner * blk, own)[1], 8), blk)
        if m == 0:
            return send(acc_gu.at[rows_, :], pbuf.at[there, whole], out_send.at[0], out_recv.at[0], dp=partner)
        return send(acc_d.at[rows_, :], yacc.at[0, there, low], out_send.at[1], out_recv.at[1], dp=partner)

    def result_copy(ten):
        return pltpu.make_async_copy(yd_ref.at[ten], w_gu.at[pl.ds(ten * rows, rows), :], back_in.at[ten])

    def last_copy(m):
        if m != 1:
            middle = max(tile // group // 2, 1) * group
            at = pl.ds(0, middle) if m == 0 else pl.ds(middle, tile - middle)
            return send(h_all.at[1, at, :], xt.at[0, at, whole], h_send.at[m], h_recv.at[m], dp=partner)
        return send(h_all.at[0, :, low], dyt.at[0, :, low], h_send.at[1], h_recv.at[1], dp=partner)

    def dx_tile(n):
        r = odd(n)

        @pl.when(n == 0)
        def _():
            pl.semaphore_wait(credit, 8)
            for r_ in BOTH:
                wait(sb.at[r_, :, pl.ds(0, rest_units * LANES)], y_send.at[1, r_])

        def block(m, carry):
            cols = pl.ds(pl.multiple_of(m * n_cols, n_cols), n_cols)
            slot = lax.rem(m + r * n_block, 2)

            @pl.when(jnp.logical_and(n < 2, m + r * n_block >= 2))
            def _():
                wait(sb.at[slot], dx_send.at[slot])

            @pl.when(n < 2)
            def _():
                with jax.named_scope('dx_dot'):
                    sb[slot] = dot_nt(h_all[1], w_gu[cols, :])
                send(sb.at[slot], pbuf.at[rows_of(r), cols], dx_send.at[slot], dx_recv.at[r, m], dp=partner).start()

            @pl.when(n >= 2)
            def _():
                with jax.named_scope('dx_wait'):
                    wait(pbuf.at[rows_of(r), cols], dx_recv.at[r, m])
                with jax.named_scope('dx_dot'):
                    yacc[1, rows_of(r), cols] = (yacc[1, rows_of(r), cols] + pbuf[rows_of(r), cols]
                                                 + dot_nt(h_all[1], w_gu[cols, :]))

            @pl.when(m >= 1)
            def _():
                tick(17 + 4 * n + m)
            return carry

        lax.fori_loop(0, n_block, block, 0)

    def grad_tile(n, carry):
        q = n - 4
        home = n < 4
        token = n >= 4
        slot = odd(n)
        at = jnp.where(home, n, slot)
        final = n == 15
        early = jnp.logical_and(n >= 3, q + 1 <= EARLY)
        late = jnp.logical_and(n < 15, q + 1 > EARLY)
        dense = q >= 8
        extra = jnp.logical_and(dense, q < 10)
        tau = jnp.where(dense, 64 + 5 * (q - 8), 16 + 4 * n)
        late_step = jnp.where(final, 1, 0)

        @pl.when(home)
        def _():
            q_start(4 + n)
            loaded(0, slot)

        @pl.when(extra)
        def _():
            tick(tau)

        step = jnp.where(extra, tau + 1, tau)

        @pl.when(token)
        def _():
            landed(0, q)
            with jax.named_scope('ab_dot'):
                ab_all[at, :, :cut_ab] = dot_nn(xt[slot], w_gu[:, :cut_ab])
            tick(step)

            @pl.when(jnp.logical_and(q > MIDDLE, n < 15))
            def _():
                arrive(1, q)

            with jax.named_scope('ab_dot'):
                ab_all[at, :, cut_ab:] = dot_nn(xt[slot], w_gu[:, cut_ab:])

            @pl.when(final)
            def _():
                pl.semaphore_wait(room.at[1], 2)
                arrive(1, q)
                tick(tau + 1)
                with jax.named_scope('h_last'):
                    def body(m, c):
                        lo = pl.ds(pl.multiple_of(m * group, group), group)
                        a = ab_all[at, lo, :half]
                        h_all[0, lo, :half] = (a * sigmoid(a) * ab_all[at, lo, half:]).astype(BF16)
                        return c

                    lax.fori_loop(0, tile // group, body, 0)
                    last_copy(1).start()
                    grad_copy(1).start()
                    w_relayed((0, 1))
                    result_copy(0).start()

        @pl.when(early)
        def _():
            arrive(0, q + 1)
            arrive(1, q + 1)

        @pl.when(home)
        def _():
            loaded(1, slot)

        @pl.when(token)
        def _():
            landed(1, q)

        with jax.named_scope('g_dot'):
            g_s[:, :cut_g] = dot_nn(dyt[slot], w_d[:, :cut_g])

        @pl.when(token)
        def _():
            tick(step + 1 + late_step)

        with jax.named_scope('g_dot'):
            g_s[:, cut_g:] = dot_nn(dyt[slot], w_d[:, cut_g:])

        def activate(with_h, start=0, stop=tile // group):
            def body(m, c):
                lo = pl.ds(pl.multiple_of(m * group, group), group)
                a = ab_all[at, lo, :half]
                b = ab_all[at, lo, half:]
                g = g_s[lo, :]
                s = sigmoid(a)
                silu = a * s
                if with_h:
                    h_all[0, lo, :half] = (silu * b).astype(BF16)
                h_all[1, lo, :half] = (g * b * s * (ONE + a * (ONE - s))).astype(BF16)
                h_all[1, lo, half:] = (g * silu).astype(BF16)
                return c

            with jax.named_scope('act'):
                lax.fori_loop(start, stop, body, 0)

        @pl.when(final)
        def _():
            middle = max(tile // group // 2, 1)
            activate(False, 0, middle)
            pl.semaphore_wait(room.at[0])
            last_copy(0).start()
            activate(False, middle)
            last_copy(2).start()

        @pl.when(jnp.logical_not(final))
        def _():
            activate(True)

        tick(step + jnp.where(home, 0, 2 + late_step))

        @pl.when(n < 3)
        def _():
            load_a(0, n + 1)
            load_a(1, n + 1)

        @pl.when(late)
        def _():
            arrive(0, q + 1)

        @pl.when(n == 14)
        def _():
            tick(tau + 3)

        @pl.when(jnp.logical_not(final))
        def _():
            with jax.named_scope('dw_dot'):
                for lo in range(0, width, third):
                    hi = lo + third
                    acc_gu[:, lo:hi] += dot_tn(xt[slot, :, at_win], h_all[1, :, lo:hi])

            @pl.when(n == 14)
            def _():
                grad_copy(0).start()

            with jax.named_scope('dw_dot2'):
                for lo, hi in ((0, half_cut), (half_cut, half)):
                    acc_d[:, lo:hi] += dot_tn(dyt[slot, :, at_win], h_all[0, :, lo:hi])

        @pl.when(final)
        def _():
            with jax.named_scope('grads_sent'):
                grad_copy(0).wait_send()
            with jax.named_scope('dw_own'):
                for lo, hi in pieces:
                    acc_gu[in_acc, lo:hi] += dot_tn(xt[1, :, at_own], h_all[1, :, lo:hi])
            with jax.named_scope('grads_sent'):
                grad_copy(1).wait_send()
            with jax.named_scope('dw_own'):
                acc_d[in_acc, :] += dot_tn(dyt[1, :, at_own], h_all[0, :, :half])

        @pl.when(jnp.logical_and(n >= 2, n < 15))
        def _():
            for ten in BOTH:
                pl.semaphore_signal(room.at[ten], device_id={'dp': partner, 'tp': t}, device_id_type=MESH)

        tick(step + jnp.where(home, 1, jnp.where(n < 14, 3, 4)))

        @pl.when(home)
        def _():
            dx_tile(n)

        @pl.when(jnp.logical_and(late, q + 1 <= MIDDLE))
        def _():
            arrive(1, q + 1)
        return carry

    lax.fori_loop(0, 16, grad_tile, 0)

    theirs = pl.ds(pl.multiple_of(window_of(me * blk, own)[1], 8), blk)
    with jax.named_scope('last_wait_h'):
        wait(yacc.at[0, theirs, low], out_recv.at[1])
        wait(dyt.at[0, :, low], h_recv.at[1])
    with jax.named_scope('dw_other'):
        yacc[0, :own, :half] += dot_tn(dyt[1, :, at_own], dyt[0, :, :half])
    with jax.named_scope('drain_sums'):
        drain_sums()
    result_copy(1).start()
    with jax.named_scope('last_wait'):
        wait(pbuf.at[theirs, whole], out_recv.at[0])
        for m in (0, 2):
            last_copy(m).wait_recv()
    with jax.named_scope('dw_other'):
        for lo, hi in pieces:
            pbuf[:own, lo:hi] += dot_tn(xt[1, :, at_own], xt[0, :, lo:hi])

    with jax.named_scope('drain'):
        for ten in BOTH:
            result_copy(ten).wait()
        for slot in BOTH:
            wait(sb.at[slot], dx_send.at[slot])
        for k in ALL:
            for core in BOTH:
                for link in BOTH:
                    for part in BOTH:
                        w_copy(k, link, part, core).wait_send()
            w_partner_copy(k).wait_send()
        w_relayed((2,))
        for ten in BOTH:
            own_copy(ten).wait_send()

        def drain(q, carry):
            for ten in BOTH:
                wait(tok_b[ten].at[0], f_send.at[q, ten])
                for link in BOTH:
                    @pl.when(q < 8)
                    def _():
                        wait(slot_of(ten, 0, link), q_send.at[lax.rem(q, 8), link, ten])

                    @pl.when(q < 4)
                    def _():
                        wait(slot_of(ten, 0, link), rl_send.at[lax.rem(q, 4), link, ten])

            return carry

        lax.fori_loop(0, 12, drain, 0)
        for m in ALL:
            last_copy(m).wait_send()


def window_of(start, size):
    first = lax.div(start, LANES) * LANES
    return pl.ds(pl.multiple_of(first, LANES), size), start - first


def own_window(blk):
    return -(-(blk + LANES - 32) // LANES) * LANES


def window(model, blk):
    starts = [(2 * blk * c) // LANES * LANES for c in range(model // (2 * blk))]
    shift = max(2 * blk * c - s for c, s in enumerate(starts))
    return -(-(shift + 2 * blk) // LANES) * LANES


def mlp(x, dy, wg, wu, wd):
    rows, model = x.shape
    blk, width = wg.shape
    half = width // 2
    tile = rows // 2
    dma = pltpu.SemaphoreType.DMA
    two, three, four = dma((2,)), dma((3,)), dma((2, 2))
    six, many, pieces_ = dma((3, 2, 2)), dma((12, 2)), dma((3, 2, 2, 2))
    vmem = pltpu.VMEM
    anywhere = pl.BlockSpec(memory_space=pl.ANY)
    shape = jax.ShapeDtypeStruct
    flops = 2 * model * half * rows * 2 * 20
    win = window(model, blk)
    most = max(rows, own_window(blk))
    kept = (vmem((win, 2 * half), F32), vmem((win, half), F32), vmem((most, model), F32), vmem((2, most, model), F32))
    kept = (*kept, vmem((model, 2 * half), BF16))
    held = sum(k.dtype.itemsize * math.prod(k.shape) for k in kept)
    in_vmem = pl.BlockSpec(memory_space=pltpu.VMEM)
    return pl.pallas_call(
        kernel,
        name='mlp',
        out_shape=(shape((2, rows, model), BF16), *kept,
                   shape((12, tile // 2, model), BF16), shape((12, tile // 2, model), BF16),
                   shape((rows, model), BF16), shape((rows, model), BF16)),
        in_specs=[anywhere] * 5,
        out_specs=(anywhere, *[in_vmem] * 5, *[anywhere] * 4),
        scratch_shapes=[
            vmem((model, half), BF16),
            vmem((2, tile, model // 3), F32),
            vmem((2, tile, model), BF16),
            vmem((2, tile, model), BF16),
            vmem((4, tile, 2 * half), F32),
            vmem((tile, half), F32),
            vmem((2, tile, 2 * half), BF16),
            vmem((2, DEPTH, tile // 2, LANES), F32),
            vmem((2, KEEP, tile // 2, LANES), BF16),
            pieces_, pieces_, six, six, three, three, three,
            two, two, dma((8, 2, 2)), dma((12, 2, 2)), dma((4, 2, 2)), many, many,
            four, dma((4, 2)), two, dma((2, 3)), pltpu.SemaphoreType.REGULAR, pltpu.SemaphoreType.REGULAR((2,)),
            dma((2, SLOTS)), dma((2, DEPTH)), dma((2, LAG + 1)), dma((2, KEEP)), dma((2, LAG + 1)),
            four, two, two, three, three, two,
        ],
        compiler_params=pltpu.CompilerParams(collective_id=0, has_side_effects=True, vmem_limit_bytes=67_000_000 - held),
        cost_estimate=pl.CostEstimate(flops=flops, bytes_accessed=100_000_000, transcendentals=0),
    )(x, dy, wg, wu, wd)


def results_kernel(blk, half, acc_gu, acc_d, pbuf, yacc, w_gu, y_out, dx_out, g_out, u_out, d_out, sem):
    me = lax.axis_index('dp')
    j = odd(me)
    chip = halved(me)
    rows = y_out.shape[0]
    mine = pl.ds(pl.multiple_of(window_of(chip * 2 * blk, LANES)[1] + j * blk, 8), blk)
    other = pl.ds(pl.multiple_of(window_of(me * blk, LANES)[1], 8), blk)
    own_cols = pl.ds(pl.multiple_of(j * half, LANES), half)
    other_cols = pl.ds(pl.multiple_of((1 - j) * half, LANES), half)
    low, high = pl.ds(0, half), pl.ds(half, half)
    copies = [pltpu.make_async_copy(src, dst, sem.at[n]) for n, (src, dst) in enumerate((
        (acc_gu.at[mine, low], g_out.at[:, own_cols]), (acc_gu.at[mine, high], u_out.at[:, own_cols]),
        (acc_d.at[mine, :], d_out.at[:, own_cols]),
        (pbuf.at[other, low], g_out.at[:, other_cols]), (pbuf.at[other, high], u_out.at[:, other_cols]),
        (yacc.at[0, other, low], d_out.at[:, other_cols]),
        (w_gu.at[pl.ds(0, rows), :], y_out), (w_gu.at[pl.ds(rows, rows), :], dx_out)))]
    for copy in copies:
        copy.start()
    for copy in copies:
        copy.wait()


def results(blk, width, rows, *kept):
    anywhere = pl.BlockSpec(memory_space=pl.ANY)
    in_vmem = pl.BlockSpec(memory_space=pltpu.VMEM)
    shape = jax.ShapeDtypeStruct
    model = kept[-1].shape[0]
    kept = [pltpu.with_memory_space_constraint(k, pltpu.VMEM) for k in kept]
    return pl.pallas_call(
        functools.partial(results_kernel, blk, width // 2),
        name='results',
        out_shape=(shape((rows, model), BF16), shape((rows, model), BF16),
                   shape((blk, width), F32), shape((blk, width), F32), shape((blk, width), F32)),
        in_specs=[in_vmem] * 5,
        out_specs=tuple([anywhere] * 5),
        scratch_shapes=[pltpu.SemaphoreType.DMA((8,))],
        compiler_params=pltpu.CompilerParams(vmem_limit_bytes=4_000_000),
    )(*kept)


def solution(mesh):
    def device_pass(x_rows, gate_blk, up_blk, down_blk, dy_rows):
        out = mlp(x_rows, dy_rows, gate_blk, up_blk, down_blk.T)
        y, dx, dw_gate, dw_up, dw_down = results(*gate_blk.shape, x_rows.shape[0], *out[1:6])
        return y, dx, dw_gate, dw_up, dw_down.T

    row_spec = P('dp', None)
    weight_spec = P('dp', 'tp')
    down_spec = P('tp', 'dp')
    return jax.shard_map(device_pass, mesh=mesh,
                         in_specs=(row_spec, weight_spec, weight_spec, down_spec, row_spec),
                         out_specs=(row_spec, row_spec, weight_spec, weight_spec, down_spec),
                         check_vma=False)
```

```python
import functools
import math

import jax
import jax.numpy as jnp
from jax import lax
from jax.experimental import pallas as pl
from jax.experimental.pallas import tpu as pltpu
from jax.sharding import PartitionSpec as P

F32 = jnp.float32
BF16 = jnp.bfloat16
MESH = pl.DeviceIdType.MESH
SLOTS = 8
DEPTH = 13
KEEP = 16
LAG = 3
HOP = 2
LANES = 128
ONE = 1.0
BOTH = (0, 1)
ALL = (0, 1, 2)
EARLY = 4
MIDDLE = 8


def odd(n):
    return lax.rem(n, 2)


def halved(n):
    return lax.div(n, 2)


def dot_nn(a, b):
    return jnp.dot(a, b, preferred_element_type=F32)


def dot_nt(a, b):
    return lax.dot_general(a, b, (((1,), (1,)), ((), ())), preferred_element_type=F32)


def dot_tn(a, b):
    return lax.dot_general(a, b, (((0,), (0,)), ((), ())), preferred_element_type=F32)


def sigmoid(a):
    return ONE / (ONE + jnp.exp(-a))


def kernel(x_ref, dy_ref, wg_ref, wu_ref, wd_ref,
           yd_ref, acc_gu, acc_d, pbuf, yacc, w_gu, xb, dyb, xp, dyp,
           w_d, sb, xt, dyt, ab_all, g_s, h_all, rbuf, back,
           w_send, w_recv, wr_send, wr_recv, w_own, wp_send, wp_recv,
           own_send, own_recv, q_send, q_recv, rl_send, f_send, f_recv,
           y_send, y_recv, dx_send, dx_recv, credit, room,
           rs_send, rs_recv, ag_send, ag_recv, fin_own, ld, out_send, out_recv, h_send, h_recv, back_in):
    rows, model = x_ref.shape
    blk, width = wg_ref.shape
    half = width // 2
    third = width // 3
    half_cut = half // 2 // LANES * LANES
    low = pl.ds(0, half)
    whole = pl.ds(0, width)
    pair = 2 * blk
    hb = blk // 2
    tile = rows // 2
    piece = tile // 4
    parcel = 2 * piece
    win = acc_d.shape[0]
    line = model // 2
    units = line // LANES
    near_units = (pair - LANES // 2) // LANES if pair % LANES else pair // LANES
    rest_units = units - near_units
    steps = 4 * units
    part_rows = tile // 2
    total = 2 * steps
    group = min(32, tile)
    w_in = (wg_ref, wu_ref, wd_ref)
    cut = (half + 255) // 256 * 256
    pieces = ((0, cut), (cut, width))
    cut_ab = cut
    cut_g = half // 2 // 256 * 256
    tok = (x_ref, dy_ref)
    tok_b = (xb, dyb)
    tok_p = (xp, dyp)
    tok_t = (xt, dyt)

    t = lax.axis_index('tp')
    me = lax.axis_index('dp')
    cy = lax.div(me, 4)
    cx = lax.rem(halved(me), 2)
    far_y = 1 - cy
    far_x = 1 - cx
    j = odd(me)
    other_core = 1 - j
    partner = me + 1 - 2 * j
    chip = cy * 2 + cx

    def near(link, core):
        if link == 0:
            return cy * 4 + (far_x) * 2 + core
        return (far_y) * 4 + cx * 2 + core

    def far(core):
        return (far_y) * 4 + (far_x) * 2 + core

    def send(src, dst, s_sem, r_sem, dp=None, tp=None):
        where = {'dp': me if dp is None else dp, 'tp': t if tp is None else tp}
        return pltpu.make_async_remote_copy(src_ref=src, dst_ref=dst, send_sem=s_sem, recv_sem=r_sem,
                                            device_id=where, device_id_type=MESH)

    def wait(ref, sem):
        pltpu.make_async_copy(ref, ref, sem).wait()

    barrier = pltpu.get_barrier_semaphore()
    for peer in (partner, near(0, 0), near(0, 1), near(1, 0), near(1, 1)):
        pl.semaphore_signal(barrier, device_id={'dp': peer, 'tp': t}, device_id_type=MESH)

    @pl.when(t > 0)
    def _():
        pl.semaphore_signal(barrier, device_id={'dp': me, 'tp': t - 1}, device_id_type=MESH)

    @pl.when(t < 3)
    def _():
        pl.semaphore_signal(barrier, device_id={'dp': me, 'tp': t + 1}, device_id_type=MESH)

    pl.semaphore_wait(barrier, 5 + jnp.minimum(t, 1) + jnp.minimum(3 - t, 1))

    def w_rows(k, dev, part=None):
        if part is None:
            at = pl.ds(pl.multiple_of(dev * blk, 16), blk)
        else:
            at = pl.ds(pl.multiple_of(dev * blk + part * hb, 16), hb)
        if k == 2:
            return w_d.at[at, :]
        return w_gu.at[at, pl.ds(k * half, half)]

    def w_cols(core):
        return pl.ds(pl.multiple_of(core * half, LANES), half)

    def w_copy(k, link, part, core):
        return send(w_in[k].at[pl.ds(part * hb, hb), w_cols(core)], w_rows(k, me, part),
                    w_send.at[k, link, part, core], w_recv.at[k, link, part, j], dp=near(link, core))

    def w_own_copy(k):
        return pltpu.make_async_copy(w_in[k].at[:, w_cols(j)], w_rows(k, me), w_own.at[k])

    def w_partner_copy(k):
        return send(w_in[k].at[:, w_cols(other_core)], w_rows(k, me), wp_send.at[k], wp_recv.at[k], dp=partner)

    def w_start(k):
        for first in BOTH:
            for core in BOTH:
                w_copy(k, 0, 1 - first, core).start()
                w_copy(k, 1, first, core).start()
        w_own_copy(k).start()
        w_partner_copy(k).start()

    def w_relay_copy(k, link_out, core):
        part = 1 if link_out == 1 else 0
        ref = w_rows(k, near(1 - link_out, core), part)
        return send(ref, ref, wr_send.at[k, link_out, core], wr_recv.at[k, link_out, core], dp=near(link_out, j))

    def w_relay(k):
        for core in BOTH:
            wait(w_rows(k, near(0, core), 1), w_recv.at[k, 0, 1, core])
            w_relay_copy(k, 1, core).start()
            wait(w_rows(k, near(1, core), 0), w_recv.at[k, 1, 0, core])
            w_relay_copy(k, 0, core).start()

    def w_relayed(which):
        for k in which:
            for link in BOTH:
                for core in BOTH:
                    w_relay_copy(k, link, core).wait_send()

    def w_have(k, which):
        if which == 'chip':
            wait(w_rows(k, me), w_own.at[k])
            wait(w_rows(k, partner), wp_recv.at[k])
        for core in BOTH:
            if which == 'x':
                wait(w_rows(k, near(0, core), 0), w_recv.at[k, 0, 0, core])
            if which == 'y':
                wait(w_rows(k, near(1, core), 1), w_recv.at[k, 1, 1, core])
            if which == 'far':
                wait(w_rows(k, far(core), 0), wr_recv.at[k, 0, core])
                wait(w_rows(k, far(core), 1), wr_recv.at[k, 1, core])

    def slot_of(ten, q, link):
        return tok_b[ten].at[q, pl.ds(link * piece, piece), :]

    def q_copy(ten, q, link):
        b = lax.div(q, 4)
        sub = lax.rem(q, 4)
        first = 1 - b if link == 0 else b
        src = tok[ten].at[pl.ds(pl.multiple_of(first * tile + sub * piece, piece), piece), :]
        return send(src, slot_of(ten, q, link), q_send.at[q, link, ten], q_recv.at[q, link, ten], dp=near(link, j))

    def q_start(q):
        for ten in BOTH:
            for link in BOTH:
                q_copy(ten, q, link).start()

    def relay_copy(ten, sub, link_out):
        return send(slot_of(ten, sub, 1 - link_out), slot_of(ten, 8 + sub, link_out),
                    rl_send.at[sub, link_out, ten], q_recv.at[8 + sub, link_out, ten], dp=near(link_out, j))

    def tile_part(ten, q, core):
        return tok_t[ten].at[odd(q), pl.ds(pl.multiple_of(core * parcel, parcel), parcel), :]

    def forward_copy(ten, q):
        return send(tok_b[ten].at[q], tile_part(ten, q, j), f_send.at[q, ten], f_recv.at[q, ten], dp=partner)

    def own_copy(ten):
        return send(tok[ten], tok_p[ten], own_send.at[ten], own_recv.at[ten], dp=partner)

    def arrive(ten, q):
        with jax.named_scope('arrive'):
            for link in BOTH:
                wait(slot_of(ten, q, link), q_recv.at[q, link, ten])
            if ten == 0:
                pl.semaphore_wait(room.at[0])
            else:
                @pl.when(q < 11)
                def _():
                    pl.semaphore_wait(room.at[1])

            forward_copy(ten, q).start()
            pltpu.make_async_copy(tok_b[ten].at[q], tile_part(ten, q, j), ld.at[ten, odd(q)]).start()

        @pl.when(q < 4)
        def _():
            for link in BOTH:
                relay_copy(ten, q, link).start()

    def landed(ten, q):
        with jax.named_scope('landed'):
            wait(tile_part(ten, q, j), ld.at[ten, odd(q)])
            wait(tile_part(ten, q, other_core), f_recv.at[q, ten])

    def rows_of(r):
        return pl.ds(pl.multiple_of(r * tile, tile), tile)

    def load_a(ten, n):
        own = halved(n)
        slot = odd(n)

        @pl.when(own == 1)
        def _():
            pltpu.make_async_copy(tok[ten].at[rows_of(slot), :], tok_t[ten].at[slot], ld.at[ten, slot]).start()

        @pl.when(own == 0)
        def _():
            pltpu.make_async_copy(tok_p[ten].at[rows_of(slot), :], tok_t[ten].at[slot], ld.at[ten, slot]).start()

    def loaded(ten, slot):
        with jax.named_scope('ld'):
            wait(tok_t[ten].at[slot], ld.at[ten, slot])

    def unit_col(u):
        mine = cy * units
        other = (far_y) * units
        low = cx * rest_units
        high = (far_x) * near_units
        a = near_units
        col = jnp.where(u < a, mine + low + u,
                        jnp.where(u < units, mine + high + (u - a),
                                  jnp.where(u < units + a, other + low + (u - units), other + high + (u - units - a))))
        return pl.multiple_of(col * LANES, LANES)

    def chunk(s, way):
        n = lax.rem(s, steps)
        row = pl.multiple_of(way * tile + odd(n) * part_rows, part_rows)
        return lax.div(s, steps), pl.ds(row, part_rows), pl.ds(unit_col(halved(n)), LANES)

    def sum_copy(s, way, nxt):
        land = lax.rem(s, DEPTH)
        return send(yacc.at[chunk(s, way)], rbuf.at[way, land], rs_send.at[way, lax.rem(s, SLOTS)], rs_recv.at[way, land], tp=nxt)

    def done_copy(s, way, prv):
        ref = back.at[way, lax.rem(s, KEEP)]
        return send(ref, ref, ag_send.at[way, lax.rem(s, LAG + 1)], ag_recv.at[way, lax.rem(s, KEEP)], tp=prv)

    def store_copy(s, way):
        return pltpu.make_async_copy(back.at[way, lax.rem(s, KEEP)], yd_ref.at[chunk(s, way)],
                                     fin_own.at[way, lax.rem(s, LAG + 1)])

    def tick(tau):
        with jax.named_scope('tick'):
            tick_body(tau)

    def give(s, way, p, prv):
        @pl.when(s >= LAG)
        def _():
            store_copy(s - LAG, way).wait()

            @pl.when(p > 0)
            def _():
                wait(back.at[way, 0], ag_send.at[way, lax.rem(s - LAG, LAG + 1)])

        store_copy(s, way).start()

        @pl.when(p > 0)
        def _():
            done_copy(s, way, prv).start()

    def tick_body(tau):
        for way in BOTH:
            p = t if way == 0 else 3 - t
            nxt = t + 1 if way == 0 else t - 1
            prv = t - 1 if way == 0 else t + 1
            s = tau - HOP * p
            slot = lax.rem(jnp.maximum(s, 0), SLOTS)
            land = lax.rem(jnp.maximum(s, 0), DEPTH)
            live = jnp.logical_and(s >= 0, s < total)

            @pl.when(jnp.logical_and(live, p > 0))
            def _():
                wait(rbuf.at[way, land], rs_recv.at[way, land])

            @pl.when(jnp.logical_and(live, p < 3))
            def _():
                @pl.when(s >= SLOTS)
                def _():
                    wait(rbuf.at[way, 0], rs_send.at[way, slot])

                @pl.when(p > 0)
                def _():
                    here = chunk(s, way)
                    yacc[here] = yacc[here] + rbuf[way, land]

                sum_copy(s, way, nxt).start()

            @pl.when(jnp.logical_and(live, p == 3))
            def _():
                back[way, lax.rem(s, KEEP)] = (yacc[chunk(s, way)] + rbuf[way, land]).astype(BF16)
                give(s, way, p, prv)

        for way in BOTH:
            p = t if way == 0 else 3 - t
            prv = t - 1 if way == 0 else t + 1
            s = tau - HOP * (6 - p)

            @pl.when(jnp.logical_and(jnp.logical_and(s >= 0, s < total), p < 3))
            def _():
                keep = lax.rem(s, KEEP)
                wait(back.at[way, keep], ag_recv.at[way, keep])
                give(s, way, p, prv)

    def ticks(lo, hi):
        def body(n, c):
            tick(n)
            return c

        lax.fori_loop(lo, hi, body, 0)

    def drain_sums():
        for way in BOTH:
            p = t if way == 0 else 3 - t

            @pl.when(p < 3)
            def _():
                for slot in range(SLOTS):
                    wait(rbuf.at[way, 0], rs_send.at[way, slot])

            for m in range(LAG):
                s = total - LAG + m
                wait(back.at[way, 0], fin_own.at[way, s % (LAG + 1)])

                @pl.when(p > 0)
                def _():
                    wait(back.at[way, 0], ag_send.at[way, s % (LAG + 1)])

    w_start(0)
    w_start(1)
    for ten in BOTH:
        own_copy(ten).start()
    base = jnp.where(t == 0, 1.0, 0.0).astype(F32)

    with jax.named_scope('clear'):
        for r in BOTH:
            for ten in BOTH:
                load_a(ten, 2 + r)

        def clear(n, carry):
            at = pl.ds(pl.multiple_of(n * 32, 32), 32)
            acc_gu[at, :] = jnp.zeros((32, width), F32)
            acc_d[at, :] = jnp.zeros((32, half), F32)
            return carry

        lax.fori_loop(0, win // 32, clear, 0)

        def clear_ab(n, carry):
            lo = pl.ds(pl.multiple_of(n * group, group), group)
            for m in range(4):
                ab_all[m, lo, :] = jnp.zeros((group, width), F32)
            return carry

        lax.fori_loop(0, tile // group, clear_ab, 0)
        for r in BOTH:
            for ten in BOTH:
                loaded(ten, r)

                def residual(n, carry):
                    lo = pl.ds(pl.multiple_of(n * group, group), group)
                    there = pl.ds(pl.multiple_of(r * tile + n * group, group), group)
                    yacc[ten, there, :] = tok_t[ten][r, lo, :].astype(F32) * base
                    return carry

                lax.fori_loop(0, tile // group, residual, 0)
        for ten in BOTH:
            wait(tok_p[ten], own_recv.at[ten])

    with jax.named_scope('w_relay'):
        w_relay(0)
        w_relay(1)
    w_start(2)

    def side(n):
        return pl.ds(pl.multiple_of(odd(n) * half, LANES), half)

    def ab_pass(last):
        other = (far_y) * line
        if last:
            parts = ((other + (far_x) * near_units * LANES, rest_units * LANES),)
        else:
            parts = ((cy * line, line), (other + cx * rest_units * LANES, near_units * LANES))
        def body(n, carry):
            slot = odd(n)

            @pl.when(n < 3)
            def _():
                load_a(0, n + 1)

            loaded(0, slot)
            for at, size in parts:
                at_k = pl.ds(pl.multiple_of(at, LANES), size)
                with jax.named_scope('ab_part'):
                    for lo, hi in pieces:
                        ab_all[n, :, lo:hi] += dot_nn(xt[slot, :, at_k], w_gu[at_k, lo:hi])

            if last:
                def hidden(m, c):
                    lo = pl.ds(pl.multiple_of(m * group, group), group)
                    a = ab_all[n, lo, :half]
                    h_all[halved(n), lo, side(n)] = (a * sigmoid(a) * ab_all[n, lo, half:]).astype(BF16)
                    return c

                lax.fori_loop(0, tile // group, hidden, 0)
            return carry

        lax.fori_loop(0, 4, body, 0)

    load_a(0, 0)
    with jax.named_scope('w_have'):
        for k in BOTH:
            w_have(k, 'chip')
            w_have(k, 'x')
            w_have(k, 'y')
    ab_pass(0)
    load_a(0, 0)
    with jax.named_scope('w_have'):
        for k in BOTH:
            w_have(k, 'far')
    ab_pass(1)

    def y_group(g, tau):
        u0 = (0, near_units, units, units + near_units)[g]
        n_u = (near_units, rest_units)[g % 2]
        col = unit_col(u0)
        cols = pl.ds(col, n_u * LANES)

        def theirs(r, carry):
            if g > 0:
                before = (near_units, rest_units)[(g - 1) % 2] * LANES
                wait(sb.at[r, :, pl.ds(0, before)], y_send.at[(g - 1) % 2, r])
            with jax.named_scope('y_dot'):
                sb[r, :, :n_u * LANES] = dot_nt(h_all[0, :, side(r)], w_d[cols, :])
            send(sb.at[r, :, pl.ds(0, n_u * LANES)], pbuf.at[rows_of(r), cols],
                 y_send.at[g % 2, r], y_recv.at[g, r], dp=partner).start()
            return carry

        def ours(r, carry):
            with jax.named_scope('y_wait'):
                wait(pbuf.at[rows_of(r), cols], y_recv.at[g, r])
            with jax.named_scope('y_dot'):
                yacc[0, rows_of(r), cols] = (yacc[0, rows_of(r), cols] + pbuf[rows_of(r), cols]
                                             + dot_nt(h_all[1, :, side(r)], w_d[cols, :]))
            pl.semaphore_signal(credit, device_id={'dp': partner, 'tp': t}, device_id_type=MESH)
            return carry

        lax.fori_loop(0, 2, theirs, 0)
        if g > 0:
            tick(tau)
        lax.fori_loop(0, 2, ours, 0)
        if g > 0:
            tick(tau + 1)

    load_a(1, 0)
    load_a(0, 0)
    with jax.named_scope('w_have2'):
        w_have(2, 'chip')
    y_group(0, 0)
    tick(0)
    with jax.named_scope('w_relay2'):
        w_relay(2)
    q_start(0)
    q_start(1)
    ticks(1, 7)
    with jax.named_scope('w_have2'):
        w_have(2, 'x')
        w_have(2, 'y')
    y_group(1, 7)
    y_group(2, 9)
    q_start(2)
    ticks(11, 14)
    with jax.named_scope('w_have2'):
        w_have(2, 'far')
    y_group(3, 14)
    q_start(3)

    at_win, shift = window_of(chip * pair, win)
    own = own_window(blk)
    at_own, _ = window_of(me * blk, own)
    in_acc = pl.ds(pl.multiple_of(window_of(me * blk, own)[0].start - at_win.start, 8), own)
    n_block = len(ALL)
    n_cols = model // n_block

    def grad_copy(m):
        rows_ = pl.ds(pl.multiple_of(shift + (other_core) * blk, 8), blk)
        there = pl.ds(pl.multiple_of(window_of(partner * blk, own)[1], 8), blk)
        if m == 0:
            return send(acc_gu.at[rows_, :], pbuf.at[there, whole], out_send.at[0], out_recv.at[0], dp=partner)
        return send(acc_d.at[rows_, :], yacc.at[0, there, low], out_send.at[1], out_recv.at[1], dp=partner)

    def result_copy(ten):
        return pltpu.make_async_copy(yd_ref.at[ten], w_gu.at[pl.ds(ten * rows, rows), :], back_in.at[ten])

    def last_copy(m):
        if m != 1:
            middle = max(tile // group // 2, 1) * group
            at = pl.ds(0, middle) if m == 0 else pl.ds(middle, tile - middle)
            return send(h_all.at[1, at, :], xt.at[0, at, whole], h_send.at[m], h_recv.at[m], dp=partner)
        return send(h_all.at[0, :, low], dyt.at[0, :, low], h_send.at[1], h_recv.at[1], dp=partner)

    def dx_tile(n):
        r = odd(n)

        @pl.when(n == 0)
        def _():
            pl.semaphore_wait(credit, 8)
            for r_ in BOTH:
                wait(sb.at[r_, :, pl.ds(0, rest_units * LANES)], y_send.at[1, r_])

        def block(m, carry):
            cols = pl.ds(pl.multiple_of(m * n_cols, n_cols), n_cols)
            slot = lax.rem(m + r * n_block, 2)

            @pl.when(jnp.logical_and(n < 2, m + r * n_block >= 2))
            def _():
                wait(sb.at[slot], dx_send.at[slot])

            @pl.when(n < 2)
            def _():
                with jax.named_scope('dx_dot'):
                    sb[slot] = dot_nt(h_all[1], w_gu[cols, :])
                send(sb.at[slot], pbuf.at[rows_of(r), cols], dx_send.at[slot], dx_recv.at[r, m], dp=partner).start()

            @pl.when(n >= 2)
            def _():
                with jax.named_scope('dx_wait'):
                    wait(pbuf.at[rows_of(r), cols], dx_recv.at[r, m])
                with jax.named_scope('dx_dot'):
                    yacc[1, rows_of(r), cols] = (yacc[1, rows_of(r), cols] + pbuf[rows_of(r), cols]
                                                 + dot_nt(h_all[1], w_gu[cols, :]))

            @pl.when(m >= 1)
            def _():
                tick(17 + 4 * n + m)
            return carry

        lax.fori_loop(0, n_block, block, 0)

    def grad_tile(n, carry):
        q = n - 4
        home = n < 4
        token = n >= 4
        slot = odd(n)
        at = jnp.where(home, n, slot)
        final = n == 15
        early = jnp.logical_and(n >= 3, q + 1 <= EARLY)
        late = jnp.logical_and(n < 15, q + 1 > EARLY)
        dense = q >= 8
        extra = jnp.logical_and(dense, q < 10)
        tau = jnp.where(dense, 64 + 5 * (q - 8), 16 + 4 * n)
        tau = jnp.where(final, 78, tau)
        late_step = jnp.where(final, 2, 0)

        @pl.when(home)
        def _():
            q_start(4 + n)
            loaded(0, slot)

        @pl.when(extra)
        def _():
            tick(tau)

        step = jnp.where(extra, tau + 1, tau)

        @pl.when(token)
        def _():
            landed(0, q)
            with jax.named_scope('ab_dot'):
                ab_all[at, :, :cut_ab] = dot_nn(xt[slot], w_gu[:, :cut_ab])
            tick(step)

            @pl.when(jnp.logical_and(q > MIDDLE, n < 15))
            def _():
                arrive(1, q)

            with jax.named_scope('ab_dot'):
                ab_all[at, :, cut_ab:] = dot_nn(xt[slot], w_gu[:, cut_ab:])

            @pl.when(final)
            def _():
                pl.semaphore_wait(room.at[1], 2)
                arrive(1, q)
                tick(tau + 1)
                with jax.named_scope('h_last'):
                    def body(m, c):
                        lo = pl.ds(pl.multiple_of(m * group, group), group)
                        a = ab_all[at, lo, :half]
                        h_all[0, lo, :half] = (a * sigmoid(a) * ab_all[at, lo, half:]).astype(BF16)
                        return c

                    lax.fori_loop(0, tile // group, body, 0)
                    last_copy(1).start()
                    grad_copy(1).start()
                    tick(tau + 2)
                    w_relayed(BOTH)
                    result_copy(0).start()

        @pl.when(early)
        def _():
            arrive(0, q + 1)
            arrive(1, q + 1)

        @pl.when(home)
        def _():
            loaded(1, slot)

        @pl.when(token)
        def _():
            landed(1, q)

        with jax.named_scope('g_dot'):
            g_s[:, :cut_g] = dot_nn(dyt[slot], w_d[:, :cut_g])

        @pl.when(token)
        def _():
            tick(step + 1 + late_step)

        with jax.named_scope('g_dot'):
            g_s[:, cut_g:] = dot_nn(dyt[slot], w_d[:, cut_g:])

        def activate(with_h, start=0, stop=tile // group):
            def body(m, c):
                lo = pl.ds(pl.multiple_of(m * group, group), group)
                a = ab_all[at, lo, :half]
                b = ab_all[at, lo, half:]
                g = g_s[lo, :]
                s = sigmoid(a)
                silu = a * s
                if with_h:
                    h_all[0, lo, :half] = (silu * b).astype(BF16)
                h_all[1, lo, :half] = (g * b * s * (ONE + a * (ONE - s))).astype(BF16)
                h_all[1, lo, half:] = (g * silu).astype(BF16)
                return c

            with jax.named_scope('act'):
                lax.fori_loop(start, stop, body, 0)

        @pl.when(final)
        def _():
            middle = max(tile // group // 2, 1)
            activate(False, 0, middle)
            pl.semaphore_wait(room.at[0])
            last_copy(0).start()
            activate(False, middle)
            last_copy(2).start()

        @pl.when(jnp.logical_not(final))
        def _():
            activate(True)

        tick(step + jnp.where(home, 0, 2 + late_step))

        @pl.when(n < 3)
        def _():
            load_a(0, n + 1)
            load_a(1, n + 1)

        @pl.when(late)
        def _():
            arrive(0, q + 1)

        @pl.when(jnp.logical_not(final))
        def _():
            with jax.named_scope('dw_dot'):
                for lo in range(0, width, third):
                    hi = lo + third
                    acc_gu[:, lo:hi] += dot_tn(xt[slot, :, at_win], h_all[1, :, lo:hi])

            @pl.when(n == 14)
            def _():
                grad_copy(0).start()
                tick(tau + 3)

            with jax.named_scope('dw_dot2'):
                for lo, hi in ((0, half_cut), (half_cut, half)):
                    acc_d[:, lo:hi] += dot_tn(dyt[slot, :, at_win], h_all[0, :, lo:hi])

        @pl.when(final)
        def _():
            with jax.named_scope('grads_sent'):
                grad_copy(0).wait_send()
            with jax.named_scope('dw_own'):
                for lo, hi in pieces:
                    acc_gu[in_acc, lo:hi] += dot_tn(xt[1, :, at_own], h_all[1, :, lo:hi])
            with jax.named_scope('grads_sent'):
                grad_copy(1).wait_send()
            with jax.named_scope('dw_own'):
                acc_d[in_acc, :] += dot_tn(dyt[1, :, at_own], h_all[0, :, :half])

        @pl.when(jnp.logical_and(n >= 2, n < 15))
        def _():
            for ten in BOTH:
                pl.semaphore_signal(room.at[ten], device_id={'dp': partner, 'tp': t}, device_id_type=MESH)

        tick(step + jnp.where(home, 1, jnp.where(n < 14, 3, jnp.where(final, 5, -100))))

        @pl.when(home)
        def _():
            dx_tile(n)

        @pl.when(jnp.logical_and(late, q + 1 <= MIDDLE))
        def _():
            arrive(1, q + 1)
        return carry

    lax.fori_loop(0, 16, grad_tile, 0)

    theirs = pl.ds(pl.multiple_of(window_of(me * blk, own)[1], 8), blk)
    with jax.named_scope('last_wait_h'):
        wait(yacc.at[0, theirs, low], out_recv.at[1])
        wait(dyt.at[0, :, low], h_recv.at[1])
    with jax.named_scope('dw_other'):
        yacc[0, :own, :half] += dot_tn(dyt[1, :, at_own], dyt[0, :, :half])
    with jax.named_scope('drain_sums'):
        drain_sums()
    result_copy(1).start()
    with jax.named_scope('last_wait'):
        wait(pbuf.at[theirs, whole], out_recv.at[0])
        for m in (0, 2):
            last_copy(m).wait_recv()
    with jax.named_scope('dw_other'):
        for lo, hi in pieces:
            pbuf[:own, lo:hi] += dot_tn(xt[1, :, at_own], xt[0, :, lo:hi])

    with jax.named_scope('drain'):
        for ten in BOTH:
            result_copy(ten).wait()
        for slot in BOTH:
            wait(sb.at[slot], dx_send.at[slot])
        for k in ALL:
            for core in BOTH:
                for link in BOTH:
                    for part in BOTH:
                        w_copy(k, link, part, core).wait_send()
            w_partner_copy(k).wait_send()
        w_relayed((2,))
        for ten in BOTH:
            own_copy(ten).wait_send()

        def drain(q, carry):
            for ten in BOTH:
                wait(tok_b[ten].at[0], f_send.at[q, ten])
                for link in BOTH:
                    @pl.when(q < 8)
                    def _():
                        wait(slot_of(ten, 0, link), q_send.at[lax.rem(q, 8), link, ten])

                    @pl.when(q < 4)
                    def _():
                        wait(slot_of(ten, 0, link), rl_send.at[lax.rem(q, 4), link, ten])

            return carry

        lax.fori_loop(0, 12, drain, 0)
        for m in ALL:
            last_copy(m).wait_send()


def window_of(start, size):
    first = lax.div(start, LANES) * LANES
    return pl.ds(pl.multiple_of(first, LANES), size), start - first


def own_window(blk):
    return -(-(blk + LANES - 32) // LANES) * LANES


def window(model, blk):
    starts = [(2 * blk * c) // LANES * LANES for c in range(model // (2 * blk))]
    shift = max(2 * blk * c - s for c, s in enumerate(starts))
    return -(-(shift + 2 * blk) // LANES) * LANES


def mlp(x, dy, wg, wu, wd):
    rows, model = x.shape
    blk, width = wg.shape
    half = width // 2
    tile = rows // 2
    dma = pltpu.SemaphoreType.DMA
    two, three, four = dma((2,)), dma((3,)), dma((2, 2))
    six, many, pieces_ = dma((3, 2, 2)), dma((12, 2)), dma((3, 2, 2, 2))
    vmem = pltpu.VMEM
    anywhere = pl.BlockSpec(memory_space=pl.ANY)
    shape = jax.ShapeDtypeStruct
    flops = 2 * model * half * rows * 2 * 20
    win = window(model, blk)
    most = max(rows, own_window(blk))
    kept = (vmem((win, 2 * half), F32), vmem((win, half), F32), vmem((most, model), F32), vmem((2, most, model), F32))
    kept = (*kept, vmem((model, 2 * half), BF16))
    held = sum(k.dtype.itemsize * math.prod(k.shape) for k in kept)
    in_vmem = pl.BlockSpec(memory_space=pltpu.VMEM)
    return pl.pallas_call(
        kernel,
        name='mlp',
        out_shape=(shape((2, rows, model), BF16), *kept,
                   shape((12, tile // 2, model), BF16), shape((12, tile // 2, model), BF16),
                   shape((rows, model), BF16), shape((rows, model), BF16)),
        in_specs=[anywhere] * 5,
        out_specs=(anywhere, *[in_vmem] * 5, *[anywhere] * 4),
        scratch_shapes=[
            vmem((model, half), BF16),
            vmem((2, tile, model // 3), F32),
            vmem((2, tile, model), BF16),
            vmem((2, tile, model), BF16),
            vmem((4, tile, 2 * half), F32),
            vmem((tile, half), F32),
            vmem((2, tile, 2 * half), BF16),
            vmem((2, DEPTH, tile // 2, LANES), F32),
            vmem((2, KEEP, tile // 2, LANES), BF16),
            pieces_, pieces_, six, six, three, three, three,
            two, two, dma((8, 2, 2)), dma((12, 2, 2)), dma((4, 2, 2)), many, many,
            four, dma((4, 2)), two, dma((2, 3)), pltpu.SemaphoreType.REGULAR, pltpu.SemaphoreType.REGULAR((2,)),
            dma((2, SLOTS)), dma((2, DEPTH)), dma((2, LAG + 1)), dma((2, KEEP)), dma((2, LAG + 1)),
            four, two, two, three, three, two,
        ],
        compiler_params=pltpu.CompilerParams(collective_id=0, has_side_effects=True, vmem_limit_bytes=67_000_000 - held),
        cost_estimate=pl.CostEstimate(flops=flops, bytes_accessed=100_000_000, transcendentals=0),
    )(x, dy, wg, wu, wd)


def results_kernel(blk, half, acc_gu, acc_d, pbuf, yacc, w_gu, y_out, dx_out, g_out, u_out, d_out, sem):
    me = lax.axis_index('dp')
    j = odd(me)
    chip = halved(me)
    rows = y_out.shape[0]
    mine = pl.ds(pl.multiple_of(window_of(chip * 2 * blk, LANES)[1] + j * blk, 8), blk)
    other = pl.ds(pl.multiple_of(window_of(me * blk, LANES)[1], 8), blk)
    own_cols = pl.ds(pl.multiple_of(j * half, LANES), half)
    other_cols = pl.ds(pl.multiple_of((1 - j) * half, LANES), half)
    low, high = pl.ds(0, half), pl.ds(half, half)
    copies = [pltpu.make_async_copy(src, dst, sem.at[n]) for n, (src, dst) in enumerate((
        (acc_gu.at[mine, low], g_out.at[:, own_cols]), (acc_gu.at[mine, high], u_out.at[:, own_cols]),
        (acc_d.at[mine, :], d_out.at[:, own_cols]),
        (pbuf.at[other, low], g_out.at[:, other_cols]), (pbuf.at[other, high], u_out.at[:, other_cols]),
        (yacc.at[0, other, low], d_out.at[:, other_cols]),
        (w_gu.at[pl.ds(0, rows), :], y_out), (w_gu.at[pl.ds(rows, rows), :], dx_out)))]
    for copy in copies:
        copy.start()
    for copy in copies:
        copy.wait()


def results(blk, width, rows, *kept):
    anywhere = pl.BlockSpec(memory_space=pl.ANY)
    in_vmem = pl.BlockSpec(memory_space=pltpu.VMEM)
    shape = jax.ShapeDtypeStruct
    model = kept[-1].shape[0]
    kept = [pltpu.with_memory_space_constraint(k, pltpu.VMEM) for k in kept]
    return pl.pallas_call(
        functools.partial(results_kernel, blk, width // 2),
        name='results',
        out_shape=(shape((rows, model), BF16), shape((rows, model), BF16),
                   shape((blk, width), F32), shape((blk, width), F32), shape((blk, width), F32)),
        in_specs=[in_vmem] * 5,
        out_specs=tuple([anywhere] * 5),
        scratch_shapes=[pltpu.SemaphoreType.DMA((8,))],
        compiler_params=pltpu.CompilerParams(vmem_limit_bytes=4_000_000),
    )(*kept)


def solution(mesh):
    def device_pass(x_rows, gate_blk, up_blk, down_blk, dy_rows):
        out = mlp(x_rows, dy_rows, gate_blk, up_blk, down_blk.T)
        y, dx, dw_gate, dw_up, dw_down = results(*gate_blk.shape, x_rows.shape[0], *out[1:6])
        return y, dx, dw_gate, dw_up, dw_down.T

    row_spec = P('dp', None)
    weight_spec = P('dp', 'tp')
    down_spec = P('tp', 'dp')
    return jax.shard_map(device_pass, mesh=mesh,
                         in_specs=(row_spec, weight_spec, weight_spec, down_spec, row_spec),
                         out_specs=(row_spec, row_spec, weight_spec, weight_spec, down_spec),
                         check_vma=False)
```
